32 devices in a mesh: dp: 8 (over z, y), mp: 4 (over x, core).
Axes of the slice: x: 2, y: 2, z: 4, core: 2. Of those that a mesh axis runs over, the one named last changes fastest.
Arguments:
- hidden_in: bfloat16 [8, 1024, 1280], P('dp', 'mp'), may hold values from -6 to 6
- segment_ids: int32 [8, 1024], P('dp'), may hold values from 0 to 15, never falling along the last dimension, each value on 1 to 512 neighbouring positions
- attn_gain: float32 [1280], replicated, may hold values from 0.1 to 1.9
- query_weight: bfloat16 [1280, 1280], P(None, 'mp'), may hold values from -0.15625 to 0.15625
- key_weight: bfloat16 [1280, 1280], P(None, 'mp'), may hold values from -0.15625 to 0.15625
- value_weight: bfloat16 [1280, 1280], P(None, 'mp'), may hold values from -0.15625 to 0.15625
- out_weight: bfloat16 [1280, 1280], P('mp'), may hold values from -0.625 to 0.625
- mlp_gain: float32 [1280], replicated, may hold values from 0.1 to 1.9
- up_weight: bfloat16 [1280, 5120], P(None, 'mp'), may hold values from -0.15625 to 0.15625
- down_weight: bfloat16 [5120, 1280], P('mp'), may hold values from -0.078125 to 0.078125
- out_cotangent: bfloat16 [8, 1024, 1280], P('dp', 'mp'), may hold values from -6 to 6
Outputs:
- result: bfloat16 [8, 1024, 1280], P('dp', 'mp')
- input_grad: float32 [8, 1024, 1280], P('dp', 'mp')
- attn_gain_grad: float32 [1280], replicated
- query_grad: float32 [1280, 1280], P(None, 'mp')
- key_grad: float32 [1280, 1280], P(None, 'mp')
- value_grad: float32 [1280, 1280], P(None, 'mp')
- out_grad: float32 [1280, 1280], P('mp')
- mlp_gain_grad: float32 [1280], replicated
- up_grad: float32 [1280, 5120], P(None, 'mp')
- down_grad: float32 [5120, 1280], P('mp')
The draws below stay inside these ranges and needn't reach their ends.
Inputs may be any that keep to these rules, and one draw needn't show every extreme that they name: `segment_ids`: within each row the ids never fall; each segment is a run of 1 to 512 tokens, and one segment has exactly 512.
All inputs are finite; a program needn't handle non-finite values.
Results may differ from the reference program's by a relative error of at most 0.012.
The reference program's roundings to bfloat16 on the way count: a program that leaves them out, or rounds other values in their place, can miss the bound.
Values may be sent and summed in bfloat16 or wider, within the bound.
A program may use at most 128 MiB of HBM per device.

```python
import math
import jax
import jax.numpy as jnp
import numpy as np
from jax import lax

D = 1280
HEADS = 16
HEAD = 80
FF = 5120
SEQ = 1024
ROWS = 8


def level_of(rng, shape, cuts, least, top_value):
    loudness = 1.0
    for dim, shards_of in cuts:
        draws = jax.random.uniform(jax.random.fold_in(jax.random.fold_in(rng, 6), dim), (shards_of,), jnp.float32, least / len(cuts), top_value / len(cuts))
        loudness = loudness * jnp.repeat(jnp.exp(draws), shape[dim] // shards_of).reshape((-1,) + (1,) * (len(shape) - 1 - dim))
    return loudness


def length_profile(amount, total, most, lean):
    portions = [(1 << 20) // math.isqrt(grade ** lean) + 1 for grade in range(2, amount + 1)]
    spare, holding = total - most - (amount - 1), [1] * (amount - 1)
    while spare > 0:
        movable = [i for i in range(amount - 1) if holding[i] < most]
        whole, remaining = sum([portions[i] for i in movable]), spare
        for i in movable:
            addition = min(most - holding[i], max(1, remaining * portions[i] // whole), spare)
            holding[i] = holding[i] + addition
            spare = spare - addition
    return np.array([most] + holding)


def ragged(key, count, total, reach, skew):
    if count == 2:
        one = jax.random.randint(key, (), max(1, total - reach), min(reach, total - 1) + 1)
        return jnp.stack([one, total - one])
    sizes = jnp.asarray(length_profile(count, total, reach, skew), jnp.int32)
    twos = (count - 1) // 2
    giver, taker = sizes[1:1 + 2 * twos:2], sizes[2:2 + 2 * twos:2]
    margin = jnp.minimum(giver - 1, reach - taker)
    passed = jax.random.randint(jax.random.fold_in(key, 1), (twos,), 0, 1 << 20) % (margin + 1)
    sizes = sizes.at[1:1 + 2 * twos:2].set(giver - passed).at[2:2 + 2 * twos:2].set(taker + passed)
    return sizes[jax.random.permutation(jax.random.fold_in(key, 2), count)]


def scatter_about(rng, dims, width, reach, split=(), kind=jnp.bfloat16):
    level = level_of(rng, dims, split, -0.22, 0.18) if split else 1.0
    drawn = jax.random.normal(rng, dims, jnp.float32) * width * level
    return jnp.minimum(jnp.maximum(drawn, -reach), reach).astype(kind)


def setup_inputs(seed: int = 0) -> dict:
    splits = jax.random.split(jax.random.key(seed), 12)
    hidden_in = scatter_about(splits[0], (ROWS, SEQ, D), 1.0, 6.0, ((0, 8), (1, 4)))
    segment_ids = jax.vmap(lambda own: jnp.searchsorted(jnp.cumsum(ragged(own, max(4, SEQ // 64), SEQ, SEQ // 2, 1)), jnp.arange(SEQ), side="right"))(jax.random.split(splits[1], ROWS)).reshape((ROWS, SEQ)).astype(jnp.int32)
    attn_gain = jnp.clip(1.0 + 0.18 * jax.random.normal(splits[2], (D,), jnp.float32), 0.1, 1.9)
    query_weight = scatter_about(splits[3], (D, D), D ** -0.5, 0.15625, ((1, 4),))
    key_weight = scatter_about(splits[4], (D, D), D ** -0.5, 0.15625, ((1, 4),))
    value_weight = scatter_about(splits[5], (D, D), D ** -0.5, 0.15625, ((1, 4),))
    out_weight = scatter_about(splits[6], (D, D), (D // 16) ** -0.5, 0.625, ((0, 4),))
    mlp_gain = jnp.clip(1.0 + 0.18 * jax.random.normal(splits[7], (D,), jnp.float32), 0.1, 1.9)
    up_weight = scatter_about(splits[8], (D, FF), D ** -0.5, 0.15625, ((1, 4),))
    down_weight = scatter_about(splits[9], (FF, D), FF ** -0.5, 0.078125, ((0, 4),))
    out_cotangent = scatter_about(splits[10], (ROWS, SEQ, D), 1.0, 6.0, ((0, 8), (1, 4)))
    return dict(hidden_in=hidden_in, segment_ids=segment_ids, attn_gain=attn_gain, query_weight=query_weight, key_weight=key_weight, value_weight=value_weight, out_weight=out_weight, mlp_gain=mlp_gain, up_weight=up_weight, down_weight=down_weight, out_cotangent=out_cotangent)


@jax.custom_vjp
def low(v):
    return lax.optimization_barrier(v.astype(jnp.bfloat16)).astype(jnp.float32)

@jax.custom_vjp
def low_back(v):
    return v

def low_keep(v):
    return (low(v), None)

def low_pass(kept, grad):
    return (grad,)

def back_keep(v):
    return (v, None)

def back_low(kept, grad):
    return (low(grad),)
low.defvjp(low_keep, low_pass)
low_back.defvjp(back_keep, back_low)
HIGH = lax.Precision.HIGHEST

def normalize(values, gain):
    return values * lax.rsqrt(lax.optimization_barrier(jnp.mean(values * values, -1, keepdims=True)) + 1e-06) * gain

def project(left, weight):
    return jnp.einsum('rsd,de->rse', left, weight, precision=HIGH)

def rotary_tables(segments_row):
    seq_len = segments_row.shape[0]
    places = jnp.arange(seq_len, dtype=jnp.int32)
    starts_here = jnp.concatenate([jnp.ones((1,), bool), segments_row[1:] != segments_row[:-1]])
    first = lax.cummax(jnp.where(starts_here, places, jnp.zeros_like(places)), axis=0)
    position = (places - first).astype(jnp.float32)
    half = HEAD // 2
    freqs = jnp.exp(jnp.arange(half, dtype=jnp.float32) * (-2.0 * math.log(10000.0) / HEAD))
    angles = position[:, None] * freqs[None, :]
    return (jnp.cos(angles)[:, None, :], jnp.sin(angles)[:, None, :])

def rotate(values, cosine, sine):
    half = values.shape[-1] // 2
    first, second = (values[..., :half], values[..., half:])
    return jnp.concatenate([first * cosine - second * sine, second * cosine + first * sine], -1)

def attend_row(inputs):
    query_proj, key_proj, value_proj, segments_row = inputs
    seq_len = query_proj.shape[0]
    cosine, sine = rotary_tables(segments_row)
    queries = low(rotate(query_proj.reshape(seq_len, HEADS, HEAD), cosine, sine))
    keys = low(rotate(key_proj.reshape(seq_len, HEADS, HEAD), cosine, sine))
    values = low(value_proj.reshape(seq_len, HEADS, HEAD))
    scores = low_back(jnp.einsum('qhd,khd->hqk', queries, keys, precision=HIGH) * (1.0 / math.sqrt(HEAD)))
    places = jnp.arange(seq_len, dtype=jnp.int32)
    allowed = (places[:, None] >= places[None, :]) & (segments_row[:, None] == segments_row[None, :])
    scores = jnp.where(allowed[None], scores, jnp.float32(-1e+30))
    top = lax.optimization_barrier(jnp.max(scores, -1, keepdims=True))
    expo = jnp.exp(scores - top)
    probs = low(expo / lax.optimization_barrier(jnp.sum(expo, -1, keepdims=True)))
    mixed = jnp.einsum('hqk,khd->qhd', probs, values, precision=HIGH)
    return mixed.reshape(seq_len, HEADS * HEAD)

def reference(hidden_in, segment_ids, attn_gain, query_weight, key_weight, value_weight, out_weight, mlp_gain, up_weight, down_weight, out_cotangent):

    def forward(x_float, gain_one, w_query, w_key, w_value, w_out, gain_two, w_up, w_down):
        normed_one = low(normalize(x_float, gain_one))
        query_proj = low_back(project(normed_one, w_query))
        key_proj = low_back(project(normed_one, w_key))
        value_proj = low_back(project(normed_one, w_value))
        mixed = lax.map(jax.checkpoint(attend_row), (query_proj, key_proj, value_proj, segment_ids))
        mixed = low(low_back(mixed))
        resid = x_float + low_back(project(mixed, w_out))
        normed_two = low(normalize(resid, gain_two))
        up_pre = low_back(project(normed_two, w_up))
        hidden = low(jax.nn.gelu(up_pre, approximate=True))
        return resid + low_back(project(hidden, w_down))
    primals = (hidden_in.astype(jnp.float32), attn_gain.astype(jnp.float32), query_weight.astype(jnp.float32), key_weight.astype(jnp.float32), value_weight.astype(jnp.float32), out_weight.astype(jnp.float32), mlp_gain.astype(jnp.float32), up_weight.astype(jnp.float32), down_weight.astype(jnp.float32))
    output, pull = jax.vjp(forward, *primals)
    grads = pull(out_cotangent.astype(jnp.float32))
    return (output.astype(jnp.bfloat16), grads[0], grads[1], grads[2], grads[3], grads[4], grads[5], grads[6], grads[7], grads[8])
```

```python
import math

import jax
import jax.numpy as jnp
from jax import lax
from jax.experimental import pallas as pl
from jax.experimental.pallas import tpu as pltpu
from jax.sharding import PartitionSpec as P

HEAD = 80


EPS = 1e-06
MASKED = -1e30
GELU_C = math.sqrt(2.0 / math.pi)
GELU_K = 0.044715


def normalize(values, gain):
    inverse = lax.rsqrt(jnp.mean(values * values, -1, keepdims=True) + EPS)
    normed = values * inverse
    return (normed * gain, normed, inverse)


def norm_back(upstream, normed, inverse, gain):
    scaled = upstream * gain
    inner = jnp.mean(scaled * normed, -1, keepdims=True)
    return (inverse * (scaled - normed * inner), jnp.sum(upstream * normed, axis=(0, 1)))


def gelu_slope(values):
    tangent = jnp.tanh(GELU_C * (values + GELU_K * values * values * values))
    return 0.5 * (1.0 + tangent) + 0.5 * values * (1.0 - tangent * tangent) * GELU_C * (
        1.0 + 3.0 * GELU_K * values * values
    )


def project(left, weight):
    return jnp.einsum("rsd,de->rse", left, weight, preferred_element_type=jnp.float32)


def project_back(left, weight):
    return jnp.einsum("rse,de->rsd", left, weight, preferred_element_type=jnp.float32)


def weight_grad(left, right):
    return jnp.einsum("rsd,rse->de", left, right, preferred_element_type=jnp.float32)


def rotary_tables(segments, head_size):
    seq_len = segments.shape[1]
    places = jnp.arange(seq_len, dtype=jnp.int32)
    starts_here = jnp.concatenate(
        [jnp.ones((segments.shape[0], 1), bool), segments[:, 1:] != segments[:, :-1]], axis=1
    )
    first = lax.cummax(jnp.where(starts_here, places[None, :], 0), axis=1)
    position = (places[None, :] - first).astype(jnp.float32)
    half = head_size // 2
    freqs = jnp.exp(jnp.arange(half, dtype=jnp.float32) * (-2.0 * math.log(10000.0) / head_size))
    angles = position[:, :, None] * freqs[None, None, :]
    return (jnp.cos(angles)[:, :, None, :], jnp.sin(angles)[:, :, None, :])


def rotate(values, cosine, sine):
    half = values.shape[-1] // 2
    first, second = (values[..., :half], values[..., half:])
    return jnp.concatenate([first * cosine - second * sine, second * cosine + first * sine], -1)


def rotate_back(grads, cosine, sine):
    half = grads.shape[-1] // 2
    first, second = (grads[..., :half], grads[..., half:])
    return jnp.concatenate([first * cosine + second * sine, second * cosine - first * sine], -1)


def allowed_block(segments_row, start, size):
    seq_len = segments_row.shape[0]
    query_pos = start + jnp.arange(size, dtype=jnp.int32)
    key_pos = jnp.arange(seq_len, dtype=jnp.int32)
    query_seg = segments_row[start : start + size]
    return (query_pos[:, None] >= key_pos[None, :]) & (query_seg[:, None] == segments_row[None, :])


def block_scores(query_block, keys, allowed, scale):
    scores = (
        jnp.einsum("qhd,khd->hqk", query_block, keys, preferred_element_type=jnp.float32) * scale
    )
    return jnp.where(allowed[None], scores, MASKED)


def attend_forward(queries, keys, values, segments_row, scale, block):
    outputs = []
    sums = []
    for start in range(0, queries.shape[0], block):
        allowed = allowed_block(segments_row, start, block)
        scores = block_scores(queries[start : start + block], keys, allowed, scale)
        top = jnp.max(scores, -1, keepdims=True)
        expo = jnp.exp(scores - top)
        total = jnp.sum(expo, -1, keepdims=True)
        probs = (expo / total).astype(jnp.bfloat16)
        outputs.append(
            jnp.einsum("hqk,khd->qhd", probs, values, preferred_element_type=jnp.float32)
        )
        sums.append(top + jnp.log(total))
    return (jnp.concatenate(outputs, 0), jnp.concatenate(sums, 1))


def attend_back(queries, keys, values, grad_mixed, log_sums, segments_row, scale, block):
    key_total = jnp.zeros(keys.shape, jnp.float32)
    value_total = jnp.zeros(values.shape, jnp.float32)
    query_parts = []
    for start in range(0, queries.shape[0], block):
        allowed = allowed_block(segments_row, start, block)
        query_block = queries[start : start + block]
        scores = block_scores(query_block, keys, allowed, scale)
        probs = jnp.exp(scores - log_sums[:, start : start + block])
        grad_block = grad_mixed[start : start + block]
        grad_probs = jnp.einsum(
            "qhd,khd->hqk", grad_block, values, preferred_element_type=jnp.float32
        )
        inner = jnp.sum(probs * grad_probs, -1, keepdims=True)
        grad_scores = (probs * (grad_probs - inner)).astype(jnp.bfloat16)
        query_parts.append(
            jnp.einsum("hqk,khd->qhd", grad_scores, keys, preferred_element_type=jnp.float32)
            * scale
        )
        key_total = (
            key_total
            + jnp.einsum(
                "hqk,qhd->khd", grad_scores, query_block, preferred_element_type=jnp.float32
            )
            * scale
        )
        value_total = value_total + jnp.einsum(
            "hqk,qhd->khd",
            probs.astype(jnp.bfloat16),
            grad_block,
            preferred_element_type=jnp.float32,
        )
    return (jnp.concatenate(query_parts, 0), key_total, value_total)


MESH = pl.DeviceIdType.MESH
CHUNK = 64
SLOTS = 8
STAGES = 6
(R1Z, R2Z, R3Z, FZM, FZA, FZB, R1Y, R2Y, R3Y, FYI, FYY) = range(11)
(S0Z, S0Y, S1Z, S1Y, S2Z, S2Y, S3ZM, S3ZE, S3YE, S3YY, S4Z, S4Y) = range(12)


def add_rows(total_ref, row, count, *others):
    value = total_ref[pl.ds(row, count), :].astype(jnp.float32)
    for other in others:
        value = value + other[...].astype(jnp.float32)
    total_ref[pl.ds(row, count), :] = value.astype(jnp.bfloat16)


class Reducer:
    def __init__(self, rows, bufs, send_sem, recv_sem, pairs):
        self.rows, self.bufs, self.send_sem, self.recv_sem, self.pairs = rows, bufs, send_sem, recv_sem, pairs
        dp = lax.axis_index("dp")
        self.place, self.side = lax.div(dp, 2), lax.rem(dp, 2)
        self.inner = (self.place == 1) | (self.place == 2)
        self.end = jnp.logical_not(self.inner)
        self.mate = 2 * (self.place + 1 - 2 * lax.rem(self.place, 2)) + self.side
        self.across = 2 * (3 - self.place) + self.side
        self.twin = 2 * self.place + 1 - self.side
        self.half_z = lax.div(self.place, 2)
        self.half_y = self.side

    def copy(self, source, target, send, recv, slot, device):
        return pltpu.make_async_remote_copy(
            src_ref=source,
            dst_ref=target,
            send_sem=self.send_sem.at[send, slot],
            recv_sem=self.recv_sem.at[recv, slot],
            device_id={"dp": device},
            device_id_type=MESH,
        )

    def whole_z(self, pair):
        return pl.multiple_of(pair * (2 * CHUNK), CHUNK)

    def at_z(self, pair, half):
        return pl.multiple_of(pair * (2 * CHUNK) + half * (CHUNK // 2), CHUNK // 2)

    def at_y(self, pair, half):
        return pl.multiple_of(pair * (2 * CHUNK) + CHUNK + half * (CHUNK // 2), CHUNK // 2)

    def moves(self, pair):
        slot = lax.rem(pair, SLOTS)
        rows, (one_z, two_z, three_z, one_y, two_y, three_y) = self.rows, self.bufs
        half = CHUNK // 2
        mine_z, mine_y = self.half_z, self.half_y
        own_z = rows.at[pl.ds(self.at_z(pair, mine_z), half), :]
        rest_z = rows.at[pl.ds(self.at_z(pair, 1 - mine_z), half), :]
        own_y = rows.at[pl.ds(self.at_y(pair, mine_y), half), :]
        rest_y = rows.at[pl.ds(self.at_y(pair, 1 - mine_y), half), :]
        all_z = rows.at[pl.ds(self.whole_z(pair), CHUNK), :]
        return dict(
            s0z=lambda: self.copy(all_z, one_z.at[slot], S0Z, R1Z, slot, self.mate),
            s0y=lambda: self.copy(rest_y, one_y.at[slot], S0Y, R1Y, slot, self.twin),
            s1z=lambda: self.copy(rest_z, two_z.at[slot], S1Z, R2Z, slot, self.across),
            s1y=lambda: self.copy(two_y.at[slot], two_y.at[slot], S1Y, R2Y, slot, self.mate),
            s2z=lambda: self.copy(own_z, three_z.at[slot], S2Z, R3Z, slot, self.twin),
            s2y=lambda: self.copy(own_y, three_y.at[slot], S2Y, R3Y, slot, self.across),
            s3zm=lambda: self.copy(own_z, own_z, S3ZM, FZM, slot, self.across),
            s3ze=lambda: self.copy(own_z, own_z, S3ZE, FZA, slot, self.mate),
            s3ye=lambda: self.copy(own_y, own_y, S3YE, FYI, slot, self.mate),
            s3yy=lambda: self.copy(own_y, own_y, S3YY, FYY, slot, self.twin),
            s4z=lambda: self.copy(rest_z, rest_z, S4Z, FZB, slot, self.mate),
            s4y=lambda: self.copy(own_y, own_y, S4Y, FYY, slot, self.twin),
        )

    def when(self, slot_index, stage, role, body):
        pair = slot_index - stage
        live = (pair >= 0) & (pair < self.pairs)
        if role is not None:
            live = live & role

        @pl.when(live)
        def _():
            body(pair)

    def slot(self, index):
        half = CHUNK // 2
        one_z, two_z, three_z, one_y, two_y, three_y = self.bufs

        def last(pair):
            m = self.moves(pair)
            @pl.when(self.end)
            def _():
                m["s3ze"]().wait_recv()
                m["s4z"]().wait_recv()
                m["s1y"]().wait_send()
                m["s4y"]().wait_send()
                m["s4y"]().wait_recv()

            @pl.when(self.inner)
            def _():
                m["s3zm"]().wait_send()
                m["s3ze"]().wait_send()
                m["s3ye"]().wait_send()
                m["s3yy"]().wait_send()
                m["s4z"]().wait_send()
                m["s3yy"]().wait_recv()

        def fourth_inner(pair):
            m = self.moves(pair)
            m["s3zm"]().wait_recv()
            m["s4z"]().start()

        def fourth_end(pair):
            m = self.moves(pair)
            m["s3ye"]().wait_recv()
            m["s4y"]().start()

        def third(pair):
            m = self.moves(pair)
            slot = lax.rem(pair, SLOTS)
            m["s2z"]().wait()
            m["s2y"]().wait()
            add_rows(self.rows, self.at_z(pair, self.half_z), half, three_z.at[slot])
            add_rows(self.rows, self.at_y(pair, self.half_y), half, three_y.at[slot])
            m["s3ze"]().start()
            m["s3zm"]().start()
            m["s3ye"]().start()
            m["s3yy"]().start()

        def second(pair):
            m = self.moves(pair)
            slot = lax.rem(pair, SLOTS)
            m["s1z"]().wait()
            m["s1y"]().wait_recv()
            m["s0y"]().wait_send()
            add_rows(
                self.rows, self.at_z(pair, self.half_z), half,
                one_z.at[slot, pl.ds(pl.multiple_of(self.half_z * half, half), half), :], two_z.at[slot],
            )
            add_rows(self.rows, self.at_y(pair, self.half_y), half, one_y.at[slot], two_y.at[slot])
            m["s2z"]().start()
            m["s2y"]().start()

        def first_inner(pair):
            m = self.moves(pair)
            slot = lax.rem(pair, SLOTS)
            m["s0z"]().wait_recv()
            m["s0y"]().wait_recv()
            other = 1 - self.half_z
            add_rows(
                self.rows, self.at_z(pair, other), half,
                one_z.at[slot, pl.ds(pl.multiple_of(other * half, half), half), :],
            )
            m["s1z"]().start()

        def first_end(pair):
            m = self.moves(pair)
            slot = lax.rem(pair, SLOTS)
            m["s0y"]().wait()
            m["s0z"]().wait_send()
            mine = self.rows[pl.ds(self.at_y(pair, self.half_y), half), :].astype(jnp.float32)
            two_y[slot] = (mine + one_y[slot].astype(jnp.float32)).astype(jnp.bfloat16)
            m["s1y"]().start()

        def start(pair):
            m = self.moves(pair)
            m["s0y"]().start()

            @pl.when(self.end)
            def _():
                m["s0z"]().start()

        self.when(index, 0, None, start)
        self.when(index, 1, self.end, first_end)
        self.when(index, 1, self.inner, first_inner)
        self.when(index, 2, self.inner, second)
        self.when(index, 3, self.inner, third)
        self.when(index, 4, self.inner, fourth_inner)
        self.when(index, 4, self.end, fourth_end)
        self.when(index, 5, None, last)

    def greet(self, barrier):
        for device in (self.mate, self.across, self.twin):
            pl.semaphore_signal(barrier, inc=1, device_id={"dp": device}, device_id_type=MESH)
        return 3


def reducer_scratch(width):
    half = CHUNK // 2
    return [
        pltpu.VMEM((SLOTS, CHUNK, width), jnp.bfloat16),
        pltpu.VMEM((SLOTS, half, width), jnp.bfloat16),
        pltpu.VMEM((SLOTS, half, width), jnp.bfloat16),
        pltpu.VMEM((SLOTS, half, width), jnp.bfloat16),
        pltpu.VMEM((SLOTS, half, width), jnp.bfloat16),
        pltpu.VMEM((SLOTS, half, width), jnp.bfloat16),
        pltpu.SemaphoreType.DMA((12, SLOTS)),
        pltpu.SemaphoreType.DMA((11, SLOTS)),
    ]


def reduce_kernel(
    down, up, outg, qg, kg, vg, down_o, up_o, out_o, q_o, k_o, v_o,
    rows, b0, b1, b2, b3, b4, b5, send_sem, recv_sem, stage, stage_sem, load_sem, tstage, tsem,
):
    width = rows.shape[1]
    local = outg.shape[0]
    hidden = down.shape[0]
    pairs = rows.shape[0] // (2 * CHUNK)
    red = Reducer(rows, (b0, b1, b2, b3, b4, b5), send_sem, recv_sem, pairs)
    barrier = pltpu.get_barrier_semaphore()
    count = red.greet(barrier)
    loads, at = [], 0
    for i, source in enumerate((down, up, outg, qg, kg, vg)):
        loads.append(pltpu.make_async_copy(source, rows.at[pl.ds(at, source.shape[0]), :], load_sem.at[i]))
        at += source.shape[0]
    for load in loads:
        load.start()
    pl.semaphore_wait(barrier, count)
    for load in loads:
        load.wait()

    def put(pair, target, base, count=2 * CHUNK):
        slot = lax.rem(pair, 2)
        return pltpu.make_async_copy(
            stage.at[slot, pl.ds(0, count), :], target.at[pl.ds(pl.multiple_of(base, CHUNK), count), :], stage_sem.at[slot]
        )

    down_pairs = hidden // (2 * CHUNK)

    def out_pair(pair, first):
        slot = lax.rem(pair, 2)

        @pl.when(pair >= 2)
        def _():
            put(pair, down_o, 0).wait()

        stage[slot] = rows[pl.ds(pl.multiple_of(pair * 2 * CHUNK, 2 * CHUNK), 2 * CHUNK), :].astype(jnp.float32)

        @pl.when(pair < down_pairs)
        def _():
            put(pair, down_o, pair * 2 * CHUNK).start()

        @pl.when((pair >= down_pairs) & (pair < 2 * down_pairs))
        def _():
            put(pair, up_o, (pair - down_pairs) * 2 * CHUNK).start()

        @pl.when(pair >= 2 * down_pairs)
        def _():
            put(pair, out_o, (pair - 2 * down_pairs) * 2 * CHUNK).start()

    whole_out = local // (2 * CHUNK)
    plain = 2 * down_pairs + whole_out

    def step(index, carry):
        red.slot(index)
        pair = index - 5

        @pl.when((pair >= 0) & (pair < plain))
        def _():
            out_pair(pair, 0)

        return carry

    lax.fori_loop(0, pairs + STAGES - 1, step, 0)
    left = local - whole_out * 2 * CHUNK
    base = 2 * hidden
    for pair in (plain, plain + 1):
        put(pair, down_o, 0).wait()
    if left:
        stage[0, pl.ds(0, left), :] = rows[pl.ds(base + whole_out * 2 * CHUNK, left), :].astype(jnp.float32)
        put(0, out_o, whole_out * 2 * CHUNK, left).start()
        put(0, out_o, whole_out * 2 * CHUNK, left).wait()
    block = 256
    eye = (lax.broadcasted_iota(jnp.int32, (block, block), 0) == lax.broadcasted_iota(jnp.int32, (block, block), 1)).astype(jnp.bfloat16)
    copies = []
    n = 0
    for i, target in enumerate((q_o, k_o, v_o)):
        row = base + local * (i + 1)
        for b in range(width // block):
            slot = n % 2
            if n >= 2:
                copies[n - 2].wait()
            tstage[slot] = lax.dot_general(
                eye, rows[pl.ds(row, local), pl.ds(b * block, block)], (((1,), (1,)), ((), ())), preferred_element_type=jnp.float32
            )
            c = pltpu.make_async_copy(tstage.at[slot], target.at[pl.ds(b * block, block), :], tsem.at[slot])
            c.start()
            copies.append(c)
            n += 1
    copies[-2].wait()
    copies[-1].wait()


def reduce_grads(down, up, outg, qg, kg, vg):
    local, width = outg.shape
    hidden = down.shape[0]
    total = 2 * hidden + 4 * local
    f32 = jnp.float32
    shapes = [(hidden, width), (hidden, width), (local, width)] + [(width, local)] * 3
    return pl.pallas_call(
        reduce_kernel,
        out_shape=[jax.ShapeDtypeStruct(s, f32) for s in shapes],
        in_specs=[pl.BlockSpec(memory_space=pl.ANY)] * 6,
        out_specs=[pl.BlockSpec(memory_space=pl.ANY)] * 6,
        scratch_shapes=[pltpu.VMEM((total, width), jnp.bfloat16)]
        + reducer_scratch(width)
        + [
            pltpu.VMEM((2, 2 * CHUNK, width), f32),
            pltpu.SemaphoreType.DMA((2,)),
            pltpu.SemaphoreType.DMA((6,)),
            pltpu.VMEM((2, 256, local), f32),
            pltpu.SemaphoreType.DMA((2,)),
        ],
        compiler_params=pltpu.CompilerParams(collective_id=0, has_side_effects=True, vmem_limit_bytes=40 * 2**20),
    )(down, up, outg, qg, kg, vg)


def reduce_all(parts):
    if lax.axis_size("dp") == 8:
        return reduce_grads(*parts)
    sums = [part.astype(jnp.float32) for part in lax.psum(parts, "dp")]
    return sums[:3] + [part.T for part in sums[3:]]


def on_device(
    hidden_in,
    segment_ids,
    attn_gain,
    query_weight,
    key_weight,
    value_weight,
    out_weight,
    mlp_gain,
    up_weight,
    down_weight,
    out_cotangent,
):
    row_count = segment_ids.shape[0]
    seq_len = segment_ids.shape[1]
    local_width = query_weight.shape[1]
    head_count = local_width // HEAD
    scale = 1.0 / math.sqrt(HEAD)
    block = min(512, seq_len)
    head_shape = (row_count, seq_len, head_count, HEAD)
    x_float = hidden_in.astype(jnp.float32)
    scaled_one, normed_one, inverse_one = normalize(x_float, attn_gain)
    rows_one = lax.all_gather(scaled_one.astype(jnp.bfloat16), "mp", axis=1, tiled=True)
    cosine, sine = rotary_tables(segment_ids, HEAD)
    queries = rotate(project(rows_one, query_weight).reshape(head_shape), cosine, sine).astype(
        jnp.bfloat16
    )
    keys = rotate(project(rows_one, key_weight).reshape(head_shape), cosine, sine).astype(
        jnp.bfloat16
    )
    values = project(rows_one, value_weight).reshape(head_shape).astype(jnp.bfloat16)
    row_index = 0
    mixed_one, log_one = attend_forward(
        queries[row_index], keys[row_index], values[row_index], segment_ids[row_index], scale, block
    )
    mixed_rows = [mixed_one]
    log_rows = [log_one]
    mixed = jnp.stack(mixed_rows, 0).reshape(row_count, seq_len, local_width).astype(jnp.bfloat16)
    attn_share = lax.psum_scatter(project(mixed, out_weight), "mp", scatter_dimension=1, tiled=True)
    resid = x_float + attn_share
    scaled_two, normed_two, inverse_two = normalize(resid, mlp_gain)
    rows_two = lax.all_gather(scaled_two.astype(jnp.bfloat16), "mp", axis=1, tiled=True)
    up_pre = project(rows_two, up_weight)
    hidden = jax.nn.gelu(up_pre, approximate=True).astype(jnp.bfloat16)
    mlp_share = lax.psum_scatter(
        project(hidden, down_weight).astype(jnp.bfloat16), "mp", scatter_dimension=1, tiled=True
    ).astype(jnp.float32)
    result = (resid + mlp_share).astype(jnp.bfloat16)
    grad_top = out_cotangent.astype(jnp.float32)
    grad_rows = lax.all_gather(out_cotangent, "mp", axis=1, tiled=True)
    down_total = weight_grad(hidden, grad_rows).astype(jnp.bfloat16)
    grad_hidden = project_back(grad_rows, down_weight)
    grad_up_pre = (grad_hidden * gelu_slope(up_pre)).astype(jnp.bfloat16)
    up_total = weight_grad(rows_two, grad_up_pre).astype(jnp.bfloat16)
    grad_two = lax.psum_scatter(
        project_back(grad_up_pre, up_weight), "mp", scatter_dimension=1, tiled=True
    )
    resid_part, mlp_gain_part = norm_back(grad_two, normed_two, inverse_two, mlp_gain)
    grad_resid = grad_top + resid_part
    branch_rows = lax.all_gather(grad_resid.astype(jnp.bfloat16), "mp", axis=1, tiled=True)
    out_total = weight_grad(mixed, branch_rows).astype(jnp.bfloat16)
    grad_mixed = project_back(branch_rows, out_weight).astype(jnp.bfloat16).reshape(head_shape)
    row_index = 0
    grad_q, grad_k, grad_v = attend_back(
        queries[row_index],
        keys[row_index],
        values[row_index],
        grad_mixed[row_index],
        log_rows[row_index],
        segment_ids[row_index],
        scale,
        block,
    )
    query_rows = [grad_q]
    key_rows = [grad_k]
    value_rows = [grad_v]
    grad_query = (
        rotate_back(jnp.stack(query_rows, 0), cosine, sine)
        .astype(jnp.bfloat16)
        .reshape(row_count, seq_len, local_width)
    )
    grad_key = (
        rotate_back(jnp.stack(key_rows, 0), cosine, sine)
        .astype(jnp.bfloat16)
        .reshape(row_count, seq_len, local_width)
    )
    grad_value = (
        jnp.stack(value_rows, 0).astype(jnp.bfloat16).reshape(row_count, seq_len, local_width)
    )
    bf = jnp.bfloat16
    query_total = weight_grad(grad_query, rows_one).astype(bf)
    key_total = weight_grad(grad_key, rows_one).astype(bf)
    value_total = weight_grad(grad_value, rows_one).astype(bf)
    grad_terms = (
        project_back(grad_query, query_weight)
        + project_back(grad_key, key_weight)
        + project_back(grad_value, value_weight)
    )
    grad_one = lax.psum_scatter(grad_terms, "mp", scatter_dimension=1, tiled=True)
    input_part, attn_gain_part = norm_back(grad_one, normed_one, inverse_one, attn_gain)
    input_grad = grad_resid + input_part
    attn_gain_part, mlp_gain_part = lax.psum((attn_gain_part, mlp_gain_part), ("dp", "mp"))
    down_total, up_total, out_total, query_total, key_total, value_total = reduce_all(
        (down_total, up_total, out_total, query_total, key_total, value_total)
    )
    return (
        result,
        input_grad,
        attn_gain_part,
        query_total,
        key_total,
        value_total,
        out_total,
        mlp_gain_part,
        up_total,
        down_total,
    )


def solution(mesh):
    return jax.shard_map(
        on_device,
        mesh=mesh,
        in_specs=(
            P("dp", "mp", None),
            P("dp", None),
            P(),
            P(None, "mp"),
            P(None, "mp"),
            P(None, "mp"),
            P("mp", None),
            P(),
            P(None, "mp"),
            P("mp", None),
            P("dp", "mp", None),
        ),
        out_specs=(
            P("dp", "mp", None),
            P("dp", "mp", None),
            P(),
            P(None, "mp"),
            P(None, "mp"),
            P(None, "mp"),
            P("mp", None),
            P(),
            P(None, "mp"),
            P("mp", None),
        ),
        check_vma=False,
    )
```

```python
import math

import jax
import jax.numpy as jnp
from jax import lax
from jax.experimental import pallas as pl
from jax.experimental.pallas import tpu as pltpu
from jax.sharding import PartitionSpec as P

HEAD = 80


EPS = 1e-06
MASKED = -1e30
GELU_C = math.sqrt(2.0 / math.pi)
GELU_K = 0.044715


def normalize(values, gain):
    inverse = lax.rsqrt(jnp.mean(values * values, -1, keepdims=True) + EPS)
    normed = values * inverse
    return (normed * gain, normed, inverse)


def norm_back(upstream, normed, inverse, gain):
    scaled = upstream * gain
    inner = jnp.mean(scaled * normed, -1, keepdims=True)
    return (inverse * (scaled - normed * inner), jnp.sum(upstream * normed, axis=(0, 1)))


def gelu_slope(values):
    tangent = jnp.tanh(GELU_C * (values + GELU_K * values * values * values))
    return 0.5 * (1.0 + tangent) + 0.5 * values * (1.0 - tangent * tangent) * GELU_C * (
        1.0 + 3.0 * GELU_K * values * values
    )


def project(left, weight):
    return jnp.einsum("rsd,de->rse", left, weight, preferred_element_type=jnp.float32)


def project_back(left, weight):
    return jnp.einsum("rse,de->rsd", left, weight, preferred_element_type=jnp.float32)


def weight_grad(left, right):
    return jnp.einsum("rsd,rse->de", left, right, preferred_element_type=jnp.float32)


def rotary_tables(segments, head_size):
    seq_len = segments.shape[1]
    places = jnp.arange(seq_len, dtype=jnp.int32)
    starts_here = jnp.concatenate(
        [jnp.ones((segments.shape[0], 1), bool), segments[:, 1:] != segments[:, :-1]], axis=1
    )
    first = lax.cummax(jnp.where(starts_here, places[None, :], 0), axis=1)
    position = (places[None, :] - first).astype(jnp.float32)
    half = head_size // 2
    freqs = jnp.exp(jnp.arange(half, dtype=jnp.float32) * (-2.0 * math.log(10000.0) / head_size))
    angles = position[:, :, None] * freqs[None, None, :]
    return (jnp.cos(angles)[:, :, None, :], jnp.sin(angles)[:, :, None, :])


def rotate(values, cosine, sine):
    half = values.shape[-1] // 2
    first, second = (values[..., :half], values[..., half:])
    return jnp.concatenate([first * cosine - second * sine, second * cosine + first * sine], -1)


def rotate_back(grads, cosine, sine):
    half = grads.shape[-1] // 2
    first, second = (grads[..., :half], grads[..., half:])
    return jnp.concatenate([first * cosine + second * sine, second * cosine - first * sine], -1)


def allowed_block(segments_row, start, size):
    seq_len = segments_row.shape[0]
    query_pos = start + jnp.arange(size, dtype=jnp.int32)
    key_pos = jnp.arange(seq_len, dtype=jnp.int32)
    query_seg = segments_row[start : start + size]
    return (query_pos[:, None] >= key_pos[None, :]) & (query_seg[:, None] == segments_row[None, :])


def block_scores(query_block, keys, allowed, scale):
    scores = (
        jnp.einsum("qhd,khd->hqk", query_block, keys, preferred_element_type=jnp.float32) * scale
    )
    return jnp.where(allowed[None], scores, MASKED)


def attend_forward(queries, keys, values, segments_row, scale, block):
    outputs = []
    sums = []
    for start in range(0, queries.shape[0], block):
        allowed = allowed_block(segments_row, start, block)
        scores = block_scores(queries[start : start + block], keys, allowed, scale)
        top = jnp.max(scores, -1, keepdims=True)
        expo = jnp.exp(scores - top)
        total = jnp.sum(expo, -1, keepdims=True)
        probs = (expo / total).astype(jnp.bfloat16)
        outputs.append(
            jnp.einsum("hqk,khd->qhd", probs, values, preferred_element_type=jnp.float32)
        )
        sums.append(top + jnp.log(total))
    return (jnp.concatenate(outputs, 0), jnp.concatenate(sums, 1))


def attend_back(queries, keys, values, grad_mixed, log_sums, segments_row, scale, block):
    key_total = jnp.zeros(keys.shape, jnp.float32)
    value_total = jnp.zeros(values.shape, jnp.float32)
    query_parts = []
    for start in range(0, queries.shape[0], block):
        allowed = allowed_block(segments_row, start, block)
        query_block = queries[start : start + block]
        scores = block_scores(query_block, keys, allowed, scale)
        probs = jnp.exp(scores - log_sums[:, start : start + block])
        grad_block = grad_mixed[start : start + block]
        grad_probs = jnp.einsum(
            "qhd,khd->hqk", grad_block, values, preferred_element_type=jnp.float32
        )
        inner = jnp.sum(probs * grad_probs, -1, keepdims=True)
        grad_scores = (probs * (grad_probs - inner)).astype(jnp.bfloat16)
        query_parts.append(
            jnp.einsum("hqk,khd->qhd", grad_scores, keys, preferred_element_type=jnp.float32)
            * scale
        )
        key_total = (
            key_total
            + jnp.einsum(
                "hqk,qhd->khd", grad_scores, query_block, preferred_element_type=jnp.float32
            )
            * scale
        )
        value_total = value_total + jnp.einsum(
            "hqk,qhd->khd",
            probs.astype(jnp.bfloat16),
            grad_block,
            preferred_element_type=jnp.float32,
        )
    return (jnp.concatenate(query_parts, 0), key_total, value_total)


MESH = pl.DeviceIdType.MESH
CHUNK = 64
SLOTS = 6
STAGES = 6
(R1Z, R2Z, R3Z, FZM, FZA, FZB, R1Y, R2Y, R3Y, FYI, FYY) = range(11)
(S0Z, S0Y, S1Z, S1Y, S2Z, S2Y, S3ZM, S3ZE, S3YE, S3YY, S4Z, S4Y) = range(12)


def add_rows(total_ref, row, count, *others):
    value = total_ref[pl.ds(row, count), :].astype(jnp.float32)
    for other in others:
        value = value + other[...].astype(jnp.float32)
    total_ref[pl.ds(row, count), :] = value.astype(jnp.bfloat16)


class Reducer:
    def __init__(self, rows, bufs, send_sem, recv_sem, pairs):
        self.rows, self.bufs, self.send_sem, self.recv_sem, self.pairs = rows, bufs, send_sem, recv_sem, pairs
        dp = lax.axis_index("dp")
        self.place, self.side = lax.div(dp, 2), lax.rem(dp, 2)
        self.inner = (self.place == 1) | (self.place == 2)
        self.end = jnp.logical_not(self.inner)
        self.mate = 2 * (self.place + 1 - 2 * lax.rem(self.place, 2)) + self.side
        self.across = 2 * (3 - self.place) + self.side
        self.twin = 2 * self.place + 1 - self.side
        self.half_z = lax.div(self.place, 2)
        self.half_y = self.side

    def copy(self, source, target, send, recv, slot, device):
        return pltpu.make_async_remote_copy(
            src_ref=source,
            dst_ref=target,
            send_sem=self.send_sem.at[send, slot],
            recv_sem=self.recv_sem.at[recv, slot],
            device_id={"dp": device},
            device_id_type=MESH,
        )

    def whole_z(self, pair):
        return pl.multiple_of(pair * (2 * CHUNK), CHUNK)

    def at_z(self, pair, half):
        return pl.multiple_of(pair * (2 * CHUNK) + half * (CHUNK // 2), CHUNK // 2)

    def at_y(self, pair, half):
        return pl.multiple_of(pair * (2 * CHUNK) + CHUNK + half * (CHUNK // 2), CHUNK // 2)

    def moves(self, pair):
        slot = lax.rem(pair, SLOTS)
        rows, (one_z, two_z, three_z, one_y, two_y, three_y) = self.rows, self.bufs
        half = CHUNK // 2
        mine_z, mine_y = self.half_z, self.half_y
        own_z = rows.at[pl.ds(self.at_z(pair, mine_z), half), :]
        rest_z = rows.at[pl.ds(self.at_z(pair, 1 - mine_z), half), :]
        own_y = rows.at[pl.ds(self.at_y(pair, mine_y), half), :]
        rest_y = rows.at[pl.ds(self.at_y(pair, 1 - mine_y), half), :]
        all_z = rows.at[pl.ds(self.whole_z(pair), CHUNK), :]
        return dict(
            s0z=lambda: self.copy(all_z, one_z.at[slot], S0Z, R1Z, slot, self.mate),
            s0y=lambda: self.copy(rest_y, one_y.at[slot], S0Y, R1Y, slot, self.twin),
            s1z=lambda: self.copy(rest_z, two_z.at[slot], S1Z, R2Z, slot, self.across),
            s1y=lambda: self.copy(two_y.at[slot], two_y.at[slot], S1Y, R2Y, slot, self.mate),
            s2z=lambda: self.copy(own_z, three_z.at[slot], S2Z, R3Z, slot, self.twin),
            s2y=lambda: self.copy(own_y, three_y.at[slot], S2Y, R3Y, slot, self.across),
            s3zm=lambda: self.copy(own_z, own_z, S3ZM, FZM, slot, self.across),
            s3ze=lambda: self.copy(own_z, own_z, S3ZE, FZA, slot, self.mate),
            s3ye=lambda: self.copy(own_y, own_y, S3YE, FYI, slot, self.mate),
            s3yy=lambda: self.copy(own_y, own_y, S3YY, FYY, slot, self.twin),
            s4z=lambda: self.copy(rest_z, rest_z, S4Z, FZB, slot, self.mate),
            s4y=lambda: self.copy(own_y, own_y, S4Y, FYY, slot, self.twin),
        )

    def when(self, slot_index, stage, role, body):
        pair = slot_index - stage
        live = (pair >= 0) & (pair < self.pairs)
        if role is not None:
            live = live & role

        @pl.when(live)
        def _():
            body(pair)

    def slot(self, index):
        half = CHUNK // 2
        one_z, two_z, three_z, one_y, two_y, three_y = self.bufs

        def last(pair):
            m = self.moves(pair)
            @pl.when(self.end)
            def _():
                m["s3ze"]().wait_recv()
                m["s4z"]().wait_recv()
                m["s1y"]().wait_send()
                m["s4y"]().wait_send()
                m["s4y"]().wait_recv()

            @pl.when(self.inner)
            def _():
                m["s3zm"]().wait_send()
                m["s3ze"]().wait_send()
                m["s3ye"]().wait_send()
                m["s3yy"]().wait_send()
                m["s4z"]().wait_send()
                m["s3yy"]().wait_recv()

        def fourth_inner(pair):
            m = self.moves(pair)
            m["s3zm"]().wait_recv()
            m["s4z"]().start()

        def fourth_end(pair):
            m = self.moves(pair)
            m["s3ye"]().wait_recv()
            m["s4y"]().start()

        def third(pair):
            m = self.moves(pair)
            slot = lax.rem(pair, SLOTS)
            m["s2z"]().wait()
            m["s2y"]().wait()
            add_rows(self.rows, self.at_z(pair, self.half_z), half, three_z.at[slot])
            add_rows(self.rows, self.at_y(pair, self.half_y), half, three_y.at[slot])
            m["s3ze"]().start()
            m["s3zm"]().start()
            m["s3ye"]().start()
            m["s3yy"]().start()

        def second(pair):
            m = self.moves(pair)
            slot = lax.rem(pair, SLOTS)
            m["s1z"]().wait()
            m["s1y"]().wait_recv()
            m["s0y"]().wait_send()
            add_rows(
                self.rows, self.at_z(pair, self.half_z), half,
                one_z.at[slot, pl.ds(pl.multiple_of(self.half_z * half, half), half), :], two_z.at[slot],
            )
            add_rows(self.rows, self.at_y(pair, self.half_y), half, one_y.at[slot], two_y.at[slot])
            m["s2z"]().start()
            m["s2y"]().start()

        def first_inner(pair):
            m = self.moves(pair)
            slot = lax.rem(pair, SLOTS)
            m["s0z"]().wait_recv()
            m["s0y"]().wait_recv()
            other = 1 - self.half_z
            add_rows(
                self.rows, self.at_z(pair, other), half,
                one_z.at[slot, pl.ds(pl.multiple_of(other * half, half), half), :],
            )
            m["s1z"]().start()

        def first_end(pair):
            m = self.moves(pair)
            slot = lax.rem(pair, SLOTS)
            m["s0y"]().wait()
            m["s0z"]().wait_send()
            mine = self.rows[pl.ds(self.at_y(pair, self.half_y), half), :].astype(jnp.float32)
            two_y[slot] = (mine + one_y[slot].astype(jnp.float32)).astype(jnp.bfloat16)
            m["s1y"]().start()

        def start(pair):
            m = self.moves(pair)
            m["s0y"]().start()

            @pl.when(self.end)
            def _():
                m["s0z"]().start()

        self.when(index, 0, None, start)
        self.when(index, 1, self.end, first_end)
        self.when(index, 1, self.inner, first_inner)
        self.when(index, 2, self.inner, second)
        self.when(index, 3, self.inner, third)
        self.when(index, 4, self.inner, fourth_inner)
        self.when(index, 4, self.end, fourth_end)
        self.when(index, 5, None, last)

    def greet(self, barrier):
        for device in (self.mate, self.across, self.twin):
            pl.semaphore_signal(barrier, inc=1, device_id={"dp": device}, device_id_type=MESH)
        return 3


def reducer_scratch(width):
    half = CHUNK // 2
    return [
        pltpu.VMEM((SLOTS, CHUNK, width), jnp.bfloat16),
        pltpu.VMEM((SLOTS, half, width), jnp.bfloat16),
        pltpu.VMEM((SLOTS, half, width), jnp.bfloat16),
        pltpu.VMEM((SLOTS, half, width), jnp.bfloat16),
        pltpu.VMEM((SLOTS, half, width), jnp.bfloat16),
        pltpu.VMEM((SLOTS, half, width), jnp.bfloat16),
        pltpu.SemaphoreType.DMA((12, SLOTS)),
        pltpu.SemaphoreType.DMA((11, SLOTS)),
    ]


HEAD_PAD = 128
BLOCK_SEQ = 256
SPAN = 512


def pad_matrix(local, padded, transposed):
    shape, feature_dim = ((padded, local), 1) if transposed else ((local, padded), 0)
    feature = lax.broadcasted_iota(jnp.int32, shape, feature_dim)
    lane = lax.broadcasted_iota(jnp.int32, shape, 1 - feature_dim)
    head = jnp.zeros(shape, jnp.int32)
    for h in range(1, local // HEAD):
        head = head + (feature >= h * HEAD).astype(jnp.int32)
    within = feature - head * HEAD
    target = head * HEAD_PAD + within + jnp.where(within >= HEAD // 2, HEAD_PAD // 2 - HEAD // 2, 0)
    return jnp.where(lane == target, 1.0, 0.0).astype(jnp.bfloat16)


def dot(a, b):
    return jnp.dot(a, b, preferred_element_type=jnp.float32)


def dot_nt(a, b):
    return lax.dot_general(a, b, (((1,), (1,)), ((), ())), preferred_element_type=jnp.float32)


def dot_tn(a, b):
    return lax.dot_general(a, b, (((0,), (0,)), ((), ())), preferred_element_type=jnp.float32)


def segment_columns(seg):
    lines = jnp.broadcast_to(seg.astype(jnp.float32), (16, seg.shape[1])).astype(jnp.bfloat16)
    pick = (lax.broadcasted_iota(jnp.int32, (16, 128), 0) == 0).astype(jnp.float32).astype(jnp.bfloat16)
    return dot_tn(lines, pick)


def rotary_into(seg, cos_ref, sin_ref):
    seq = seg.shape[1]
    ids = segment_columns(seg)
    first = jnp.zeros((seq, 128), jnp.float32)
    row = seg.astype(jnp.float32)
    for s in range(1, 16):
        before = jnp.sum(jnp.where(row < s, 1.0, 0.0), axis=1, keepdims=True)
        first = jnp.where(ids == s, before, first)
    position = lax.broadcasted_iota(jnp.int32, (seq, 128), 0).astype(jnp.float32) - first
    lane = lax.broadcasted_iota(jnp.int32, (1, 128), 1)
    upper = lane >= HEAD_PAD // 2
    index = jnp.where(upper, lane - HEAD_PAD // 2, lane)
    freqs = jnp.exp(index.astype(jnp.float32) * (-2.0 * math.log(10000.0) / HEAD))
    freqs = jnp.where(index < HEAD // 2, freqs, 0.0)
    angles = position * freqs
    cos_ref[...] = jnp.cos(angles)
    sin_ref[...] = jnp.where(upper, jnp.sin(angles), -jnp.sin(angles))


class Ring4:
    def __init__(self):
        mp = lax.axis_index("mp")
        chip, core = lax.div(mp, 2), lax.rem(mp, 2)
        self.me = mp
        self.core = 2 * chip + 1 - core
        self.chip = 2 * (1 - chip) + core
        self.far = 2 * (1 - chip) + 1 - core


def block_rows(index):
    return pl.ds(pl.multiple_of(index * BLOCK_SEQ, BLOCK_SEQ), BLOCK_SEQ)


class Gather:
    def __init__(self, ring, rows, sems):
        def copy(block, device, which):
            return pltpu.make_async_remote_copy(
                src_ref=rows.at[block_rows(block), :],
                dst_ref=rows.at[block_rows(block), :],
                send_sem=sems.at[0, which],
                recv_sem=sems.at[1, which],
                device_id={"mp": device},
                device_id_type=MESH,
            )

        self.near = lambda: copy(ring.me, ring.core, 0)
        self.across = lambda: copy(ring.me, ring.chip, 1)
        self.onward = lambda: copy(ring.chip, ring.core, 2)

    def forward(self):
        self.across().wait_recv()
        self.onward().start()

    def finish(self):
        self.onward().wait()


class Scatter:
    def __init__(self, ring, send_core, recv_core, send_chip, recv_chip, sems):
        self.bufs = (send_core, recv_core, send_chip, recv_chip)

        def copy(source, target, device, which):
            return pltpu.make_async_remote_copy(
                src_ref=source,
                dst_ref=target,
                send_sem=sems.at[0, which],
                recv_sem=sems.at[1, which],
                device_id={"mp": device},
                device_id_type=MESH,
            )

        self.far = lambda: copy(send_core.at[0], recv_core.at[0], ring.core, 0)
        self.core = lambda: copy(send_core.at[1], recv_core.at[1], ring.core, 1)
        self.chip = lambda: copy(send_chip, recv_chip, ring.chip, 2)


def greet_mp(ring, barrier):
    for device in (ring.core, ring.chip):
        pl.semaphore_signal(barrier, inc=1, device_id={"mp": device}, device_id_type=MESH)
    return 2


def norm_rows(values):
    inverse = lax.rsqrt(jnp.mean(values * values, -1, keepdims=True) + EPS)
    return values * inverse, inverse


def qkv_block(rows, weights, cos_ref, sin_ref, out, block):
    at = block_rows(block)
    turned = 2 * (weights.shape[1] // 3) // 256
    tiles = weights.shape[1] // 256

    def one(n, turn):
        cols = pl.ds(pl.multiple_of(n * 256, 256), 256)
        value = dot(rows[at, :], weights[:, cols])
        if turn:
            cosine, sine = cos_ref[at, :], sin_ref[at, :]
            halves = [value[:, j * 128 : j * 128 + 128] for j in range(2)]
            value = jnp.concatenate([h * cosine + pltpu.roll(h, 64, 1) * sine for h in halves], axis=1)
        out[at, cols] = value.astype(jnp.bfloat16)

    @pl.loop(0, turned)
    def _(n):
        one(n, True)

    @pl.loop(turned, tiles)
    def _(n):
        one(n, False)


def masks_into(seg, ids_ref, bias_ref):
    seq = seg.shape[1]
    for i in range(seq // BLOCK_SEQ):
        low = max(0, i * BLOCK_SEQ - SPAN)
        high = (i + 1) * BLOCK_SEQ
        shape = (BLOCK_SEQ, high - low)
        query = i * BLOCK_SEQ + lax.broadcasted_iota(jnp.int32, shape, 0)
        key = low + lax.broadcasted_iota(jnp.int32, shape, 1)
        ids = ids_ref[pl.ds(i * BLOCK_SEQ, BLOCK_SEQ), :][:, :1]
        same = ids == seg[:, low:high].astype(jnp.float32)
        bias_ref[pl.ds(i * BLOCK_SEQ, BLOCK_SEQ), pl.ds(0, high - low)] = jnp.where((query >= key) & same, 0.0, MASKED).astype(bias_ref.dtype)


def attend_all(qkv, out, bias_ref, heads, scale):
    seq = qkv.shape[0]
    width = heads * HEAD_PAD

    @pl.loop(0, heads)
    def _(h):
        lanes = [pl.ds(pl.multiple_of(part * width + h * HEAD_PAD, HEAD_PAD), HEAD_PAD) for part in range(3)]
        for i in range(seq // BLOCK_SEQ):
            low, high = max(0, i * BLOCK_SEQ - SPAN), (i + 1) * BLOCK_SEQ
            rows, keys = pl.ds(i * BLOCK_SEQ, BLOCK_SEQ), pl.ds(low, high - low)
            scores = dot_nt(qkv[rows, lanes[0]], qkv[keys, lanes[1]]) + bias_ref[rows, pl.ds(0, high - low)]
            top = jnp.max(scores, -1, keepdims=True)
            expo = jnp.exp((scores - top) * scale)
            probs = expo * (1.0 / jnp.sum(expo, -1, keepdims=True))
            out[rows, lanes[0]] = dot(probs.astype(jnp.bfloat16), qkv[keys, lanes[2]]).astype(jnp.bfloat16)


def front_kernel(
    x, g, seg, gain, wq, wk, wv, wo,
    resid_o, h1_o, grow_o, qkv_o, mix_o, wqkv_o, wout_o, cos_o, sin_o,
    rows_one, rows_g, qkv, mixed, raw, raw_out, wqkv, wout, cos_ref, sin_ref, ids_ref, bias_ref,
    send_core, recv_core, send_chip, recv_chip, load_sem, save_sem, one_sem, g_sem, rs_sem,
):
    ring = Ring4()
    local, width = wo.shape
    padded = wout.shape[0]
    heads = local // HEAD
    barrier = pltpu.get_barrier_semaphore()
    count = greet_mp(ring, barrier)
    loads = [pltpu.make_async_copy(w, raw.at[i], load_sem.at[i]) for i, w in enumerate((wq, wk, wv))]
    loads.append(pltpu.make_async_copy(wo, raw_out, load_sem.at[3]))
    own_g = pltpu.make_async_copy(g, rows_g.at[block_rows(ring.me), :], load_sem.at[4])
    for load in loads:
        load.start()
    own_g.start()
    values, _ = norm_rows(x[...].astype(jnp.float32))
    rows_one[block_rows(ring.me), :] = (values * gain[...]).astype(jnp.bfloat16)
    pl.semaphore_wait(barrier, count)
    one, all_g = Gather(ring, rows_one, one_sem), Gather(ring, rows_g, g_sem)
    scatter = Scatter(ring, send_core, recv_core, send_chip, recv_chip, rs_sem)
    one.across().start()
    one.near().start()
    spread = pad_matrix(local, padded, False)
    for i, load in enumerate(loads[:3]):
        load.wait()
        wqkv[:, pl.ds(i * padded, padded)] = dot(raw[i], spread).astype(jnp.bfloat16)
    loads[3].wait()
    wout[...] = dot(pad_matrix(local, padded, True), raw_out[...]).astype(jnp.bfloat16)
    own_g.wait()
    ids_ref[...] = segment_columns(seg[...])
    rotary_into(seg[...], cos_ref, sin_ref)
    qkv_block(rows_one, wqkv, cos_ref, sin_ref, qkv, ring.me)
    one.near().wait_recv()
    qkv_block(rows_one, wqkv, cos_ref, sin_ref, qkv, ring.core)
    masks_into(seg[...], ids_ref, bias_ref)
    one.forward()
    one.across().wait_send()
    all_g.across().start()
    all_g.near().start()
    qkv_block(rows_one, wqkv, cos_ref, sin_ref, qkv, ring.chip)
    one.onward().wait_recv()
    qkv_block(rows_one, wqkv, cos_ref, sin_ref, qkv, ring.far)
    attend_all(qkv, mixed, bias_ref, heads, 1.0 / math.sqrt(HEAD))
    saves = [
        pltpu.make_async_copy(source, target, save_sem.at[i])
        for i, (source, target) in enumerate(
            ((rows_one, h1_o), (qkv, qkv_o), (mixed, mix_o), (wqkv, wqkv_o), (wout, wout_o), (cos_ref, cos_o), (sin_ref, sin_o), (rows_g, grow_o))
        )
    ]
    for save in saves[:7]:
        save.start()

    def term(block):
        return dot(mixed[block_rows(block), :], wout[...])

    send_core[0] = term(ring.far).astype(jnp.bfloat16)
    scatter.far().start()
    send_core[1] = term(ring.core).astype(jnp.bfloat16)
    scatter.core().start()
    chip_term = term(ring.chip)
    scatter.far().wait_recv()
    send_chip[...] = (chip_term + recv_core[0].astype(jnp.float32)).astype(jnp.bfloat16)
    scatter.chip().start()
    all_g.forward()
    own = x[...].astype(jnp.float32) + term(ring.me)
    scatter.core().wait_recv()
    own = own + recv_core[1].astype(jnp.float32)
    all_g.near().wait_recv()
    all_g.onward().wait_recv()
    saves[7].start()
    scatter.chip().wait_recv()
    resid_o[...] = own + recv_chip[...].astype(jnp.float32)
    for gather in (one, all_g):
        gather.near().wait_send()
        gather.onward().wait_send()
    all_g.across().wait_send()
    one_done = (scatter.far(), scatter.core(), scatter.chip())
    for copy in one_done:
        copy.wait_send()
    for save in saves:
        save.wait()


def front(x, g, seg, gain, wq, wk, wv, wo):
    bf, f32 = jnp.bfloat16, jnp.float32
    local, width = wo.shape
    padded = local // HEAD * HEAD_PAD
    seq, rows = seg.shape[1], x.shape[0]
    shapes = [((rows, width), f32), ((seq, width), bf), ((seq, width), bf), ((seq, 3 * padded), bf), ((seq, padded), bf), ((width, 3 * padded), bf), ((padded, width), bf), ((seq, 128), f32), ((seq, 128), f32)]
    vm, hbm = pl.BlockSpec(memory_space=pltpu.VMEM), pl.BlockSpec(memory_space=pl.ANY)
    sem = pltpu.SemaphoreType.DMA
    return pl.pallas_call(
        front_kernel,
        out_shape=[jax.ShapeDtypeStruct(s, d) for s, d in shapes],
        in_specs=[vm, vm, vm, vm, hbm, hbm, hbm, hbm],
        out_specs=[vm] + [hbm] * 8,
        scratch_shapes=[
            pltpu.VMEM((seq, width), bf), pltpu.VMEM((seq, width), bf), pltpu.VMEM((seq, 3 * padded), bf), pltpu.VMEM((seq, padded), bf),
            pltpu.VMEM((3, width, local), bf), pltpu.VMEM((local, width), bf), pltpu.VMEM((width, 3 * padded), bf), pltpu.VMEM((padded, width), bf),
            pltpu.VMEM((seq, 128), f32), pltpu.VMEM((seq, 128), f32), pltpu.VMEM((seq, 128), f32), pltpu.VMEM((seq, SPAN + BLOCK_SEQ), f32),
            pltpu.VMEM((2, rows, width), bf), pltpu.VMEM((2, rows, width), bf), pltpu.VMEM((rows, width), bf), pltpu.VMEM((rows, width), bf),
            sem((5,)), sem((8,)), sem((2, 3)), sem((2, 3)), sem((2, 3)),
        ],
        compiler_params=pltpu.CompilerParams(collective_id=1, has_side_effects=True, vmem_limit_bytes=60 * 2**20),
    )(x, g, seg, gain.reshape(1, -1), wq, wk, wv, wo)


def gelu_parts(u):
    tangent = jnp.tanh(GELU_C * (u + GELU_K * u * u * u))
    return tangent


def tail_kernel(
    x, resid, seg, gain_one, gain_two, wup, wdown, h1, grow, qkv_in, mix_in, wqkv_in, wout_in, cos_in, sin_in,
    result_o, input_o, gains_o, down_o, up_o, out_o, q_o, k_o, v_o,
    rows, b0, b1, b2, b3, b4, b5, send_sem, recv_sem, stage, stage_sem, tstage, tsem,
    w_up, w_down, w_qkv, w_out, rows_one, rows_g, rows_two, hidden, grad_up, branch, qkv, mixed, grad_mixed,
    cos_ref, sin_ref, bias_ref, term_ref, key_sum, value_sum,
    send_core, recv_core, send_chip, recv_chip, gain_acc, gain_recv,
    load_sem, two_sem, branch_sem, rs_sem, rs2_sem, rs3_sem, gain_sem, free_sem,
):
    bf, f32 = jnp.bfloat16, jnp.float32
    ring = Ring4()
    seq, width = rows_two.shape
    units = w_up.shape[1]
    padded = w_out.shape[0]
    heads = padded // HEAD_PAD
    local = heads * HEAD
    pairs = rows.shape[0] // (2 * CHUNK)
    scale = 1.0 / math.sqrt(HEAD)
    red = Reducer(rows, (b0, b1, b2, b3, b4, b5), send_sem, recv_sem, pairs)
    barrier = pltpu.get_barrier_semaphore()
    count = greet_mp(ring, barrier) + red.greet(barrier)
    places = ((wup, w_up), (grow, rows_g), (wdown, w_down), (mix_in, mixed), (wout_in, w_out), (cos_in, cos_ref), (sin_in, sin_ref), (qkv_in, qkv), (wqkv_in, w_qkv), (h1, rows_one))
    loads = [pltpu.make_async_copy(source, target, load_sem.at[i]) for i, (source, target) in enumerate(places)]
    loads[0].start()
    loads[1].start()
    normed, _ = norm_rows(resid[...])
    rows_two[block_rows(ring.me), :] = (normed * gain_two[...]).astype(bf)
    pl.semaphore_wait(barrier, count)
    two, all_branch = Gather(ring, rows_two, two_sem), Gather(ring, branch, branch_sem)
    first = Scatter(ring, send_core, recv_core, send_chip, recv_chip, rs_sem)
    second = Scatter(ring, send_core, recv_core, send_chip, recv_chip, rs2_sem)
    third = Scatter(ring, send_core, recv_core, send_chip, recv_chip, rs3_sem)
    two.across().start()
    two.near().start()
    for load in loads[2:]:
        load.start()

    base = 2 * units
    down_pairs = units // (2 * CHUNK)
    whole_out = local // (2 * CHUNK)
    plain = 2 * down_pairs + whole_out

    def put(pair, target, row, many=2 * CHUNK):
        slot = lax.rem(pair, 2)
        return pltpu.make_async_copy(
            stage.at[slot, pl.ds(0, many), :], target.at[pl.ds(pl.multiple_of(row, CHUNK), many), :], stage_sem.at[slot]
        )

    def out_pair(pair):
        @pl.when(pair >= 2)
        def _():
            put(pair, down_o, 0).wait()

        stage[lax.rem(pair, 2)] = rows[pl.ds(pl.multiple_of(pair * 2 * CHUNK, 2 * CHUNK), 2 * CHUNK), :].astype(f32)

        @pl.when(pair < down_pairs)
        def _():
            put(pair, down_o, pair * 2 * CHUNK).start()

        @pl.when((pair >= down_pairs) & (pair < 2 * down_pairs))
        def _():
            put(pair, up_o, (pair - down_pairs) * 2 * CHUNK).start()

        @pl.when(pair >= 2 * down_pairs)
        def _():
            put(pair, out_o, (pair - 2 * down_pairs) * 2 * CHUNK).start()

    def slot(index):
        red.slot(index)
        pair = index - (STAGES - 1)

        @pl.when((pair >= 0) & (pair < plain))
        def _():
            out_pair(pair)

    def tile(n):
        return pl.ds(pl.multiple_of(n * 256, 256), 256)

    def up_block(block):
        @pl.loop(0, units // 256)
        def _(n):
            u = dot(rows_two[block_rows(block), :], w_up[:, tile(n)])
            tangent = jnp.tanh(GELU_C * (u + GELU_K * u * u * u))
            hidden[block_rows(block), tile(n)] = (0.5 * u * (1.0 + tangent)).astype(bf)

    loads[0].wait()
    up_block(ring.me)
    two.near().wait_recv()
    up_block(ring.core)
    key_sum[...] = segment_columns(seg[...])
    masks_into(seg[...], key_sum, bias_ref)
    two.forward()
    up_block(ring.chip)
    two.onward().wait_recv()
    up_block(ring.far)
    loads[1].wait()

    @pl.loop(0, units // 256)
    def _(i):
        rows[tile(i), :] = dot_tn(hidden[:, tile(i)], rows_g[...]).astype(bf)
        slot(i)

    loads[2].wait()

    def order(k):
        there = k < 2
        chip = lax.div(ring.me, 2)
        core = lax.rem(ring.me, 2)
        flip = 1 - lax.rem(k, 2)
        to_chip = jnp.where(there, 1 - chip, chip)
        to_core = jnp.where(flip == 1, 1 - core, core)
        return 2 * to_chip + to_core

    def hand_on(k, scatter, start):
        @pl.when(k == 0)
        def _():
            send_core[0] = term_ref[...].astype(bf)
            scatter.far().start()

        @pl.when(k == 1)
        def _():
            scatter.far().wait_recv()
            send_chip[...] = (term_ref[...] + recv_core[0].astype(f32)).astype(bf)
            scatter.chip().start()

        @pl.when(k == 2)
        def _():
            send_core[1] = term_ref[...].astype(bf)
            scatter.core().start()

        @pl.when(k == 3)
        def _():
            scatter.core().wait_recv()
            term_ref[...] = term_ref[...] + recv_core[1].astype(f32)

    def settle(scatter):
        for copy in (scatter.far(), scatter.core()):
            copy.wait_send()
        scatter.chip().wait()
        return term_ref[...] + recv_chip[...].astype(f32)

    @pl.loop(0, 4)
    def _(k):
        at = block_rows(order(k))

        @pl.loop(0, units // 256)
        def _(n):
            u = dot(rows_two[at, :], w_up[:, tile(n)])
            upstream = dot_nt(rows_g[at, :], w_down[tile(n), :])
            tangent = jnp.tanh(GELU_C * (u + GELU_K * u * u * u))
            slope = 0.5 * (1.0 + tangent) + 0.5 * u * (1.0 - tangent * tangent) * GELU_C * (1.0 + 3.0 * GELU_K * u * u)
            grad_up[at, tile(n)] = (upstream * slope).astype(bf)

        @pl.loop(0, width // 256)
        def _(n):
            term_ref[:, tile(n)] = dot_nt(grad_up[at, :], w_up[tile(n), :])

        hand_on(k, first, None)
        slot(5 + k)

    def up_rows(i):
        rows[pl.ds(pl.multiple_of(units + i * 256, 256), 256), :] = dot_tn(rows_two[:, tile(i)], grad_up[...]).astype(bf)

    @pl.loop(0, 2)
    def _(i):
        up_rows(i)
        slot(9 + i)

    grad_two = settle(first)
    normed, inverse = norm_rows(resid[...])
    scaled = grad_two * gain_two[...]
    part = inverse * (scaled - normed * jnp.mean(scaled * normed, -1, keepdims=True))
    mlp_part = jnp.sum(grad_two * normed, axis=0, keepdims=True)
    gain_acc[0] = jnp.zeros(gain_acc.shape[1:], f32)
    gain_acc[0, 1:2, :] = mlp_part
    mine = rows_g[block_rows(ring.me), :].astype(f32) + part
    input_o[...] = mine
    branch[block_rows(ring.me), :] = mine.astype(bf)
    all_branch.across().start()
    all_branch.near().start()

    @pl.loop(2, units // 256)
    def _(i):
        up_rows(i)
        slot(9 + i)

    for load in loads[3:]:
        load.wait()
    all_branch.near().wait_recv()
    all_branch.forward()
    all_branch.onward().wait_recv()

    def head_rows(left, lane, right, row):
        value = dot_tn(left[:, lane], right[...])
        halves = [value[at : at + HEAD // 2, :] for at in (0, 64, 128, 192)]
        rows[pl.ds(pl.multiple_of(row, 16), 2 * HEAD), :] = jnp.concatenate(halves, axis=0).astype(bf)

    @pl.loop(0, heads // 2)
    def _(j):
        head_rows(mixed, tile(j), branch, base + j * 2 * HEAD)

    @pl.loop(0, 4)
    def _(b):
        grad_mixed[block_rows(b), :] = dot_nt(branch[block_rows(b), :], w_out[...]).astype(bf)

    @pl.loop(0, heads)
    def _(h):
        lanes = [pl.ds(pl.multiple_of(n * padded + h * HEAD_PAD, HEAD_PAD), HEAD_PAD) for n in range(3)]
        key_sum[...] = jnp.zeros_like(key_sum)
        value_sum[...] = jnp.zeros_like(value_sum)
        for i in range(seq // BLOCK_SEQ):
            low, high = max(0, i * BLOCK_SEQ - SPAN), (i + 1) * BLOCK_SEQ
            at, keys = pl.ds(i * BLOCK_SEQ, BLOCK_SEQ), pl.ds(low, high - low)
            query, upstream = qkv[at, lanes[0]], grad_mixed[at, lanes[0]]
            scores = dot_nt(query, qkv[keys, lanes[1]]) + bias_ref[at, pl.ds(0, high - low)]
            top = jnp.max(scores, -1, keepdims=True)
            expo = jnp.exp((scores - top) * scale)
            probs = expo * (1.0 / jnp.sum(expo, -1, keepdims=True))
            grad_probs = dot_nt(upstream, qkv[keys, lanes[2]])
            inner = jnp.sum(probs * grad_probs, -1, keepdims=True)
            grad_scores = (probs * (grad_probs - inner)).astype(bf)
            value_sum[keys, :] += dot_tn(probs.astype(bf), upstream)
            key_sum[keys, :] += dot_tn(grad_scores, query)
            turned = dot(grad_scores, qkv[keys, lanes[1]]) * scale
            qkv[at, lanes[0]] = (turned * cos_ref[at, :] - pltpu.roll(turned, 64, 1) * sin_ref[at, :]).astype(bf)
            if i == 1:
                slot(14 + 2 * h)
        turned = key_sum[...] * scale
        qkv[:, lanes[1]] = (turned * cos_ref[...] - pltpu.roll(turned, 64, 1) * sin_ref[...]).astype(bf)
        qkv[:, lanes[2]] = value_sum[...].astype(bf)
        at = block_rows(order(h))

        @pl.loop(0, width // 256)
        def _(n):
            term_ref[:, tile(n)] = dot(hidden[at, :], w_down[:, tile(n)])

        hand_on(h, second, None)
        slot(15 + 2 * h)

    @pl.loop(0, 3)
    def _(part):
        for j in range(heads // 2):
            lane = pl.ds(pl.multiple_of(part * padded + j * 256, 256), 256)
            head_rows(qkv, lane, rows_one, base + (part + 1) * local + j * 2 * HEAD)
        slot(22 + part)

    result_o[...] = (resid[...] + settle(second)).astype(bf)
    for device in (ring.core, ring.chip):
        pl.semaphore_signal(free_sem, inc=1, device_id={"mp": device}, device_id_type=MESH)
    pl.semaphore_wait(free_sem, 2)

    @pl.loop(0, 4)
    def _(k):
        at = block_rows(order(k))

        @pl.loop(0, width // 256)
        def _(n):
            term_ref[:, tile(n)] = dot_nt(qkv[at, :], w_qkv[tile(n), :])

        hand_on(k, third, None)
        slot(25 + k)

    eye = jnp.where(
        lax.broadcasted_iota(jnp.int32, (256, 256), 0) == lax.broadcasted_iota(jnp.int32, (256, 256), 1), 1.0, 0.0
    ).astype(bf)

    def tput(n, target):
        return pltpu.make_async_copy(tstage.at[lax.rem(n, 2)], target.at[tile(n), :], tsem.at[lax.rem(n, 2)])

    def turn_out(part, target):
        row = base + local * (part + 1)

        @pl.loop(0, width // 256)
        def _(n):
            @pl.when(n >= 2)
            def _():
                tput(n, target).wait()

            tstage[lax.rem(n, 2)] = dot_nt(eye, rows[pl.ds(row, local), tile(n)])
            tput(n, target).start()

        for n in (width // 256 - 2, width // 256 - 1):
            tput(n, target).wait()

    slot(29)
    grad_one = settle(third)
    normed, inverse = norm_rows(x[...].astype(f32))
    scaled = grad_one * gain_one[...]
    input_o[...] = input_o[...] + inverse * (scaled - normed * jnp.mean(scaled * normed, -1, keepdims=True))
    gain_acc[0, 0:1, :] = jnp.sum(grad_one * normed, axis=0, keepdims=True)

    def exchange(step):
        names = ({"mp": ring.core}, {"mp": ring.chip}, {"dp": red.twin}, {"dp": red.mate}, {"dp": red.across})
        return pltpu.make_async_remote_copy(
            src_ref=gain_acc.at[step], dst_ref=gain_recv.at[step], send_sem=gain_sem.at[0, step], recv_sem=gain_sem.at[1, step],
            device_id=names[step], device_id_type=MESH,
        )

    last = pairs + STAGES - 1

    @pl.loop(30, last)
    def _(index):
        for step in range(5):

            @pl.when(index == 30 + step)
            def _():
                if step:
                    exchange(step - 1).wait_recv()
                    gain_acc[step] = gain_acc[step - 1] + gain_recv[step - 1]
                exchange(step).start()

        slot(index)

        @pl.when(index == 30)
        def _():
            turn_out(0, q_o)

        @pl.when(index == 33)
        def _():
            turn_out(1, k_o)

    exchange(4).wait_recv()
    gains_o[...] = gain_acc[4] + gain_recv[4]
    turn_out(2, v_o)
    for pair in (plain, plain + 1):
        put(pair, down_o, 0).wait()
    left = local - whole_out * 2 * CHUNK
    if left:
        stage[0, pl.ds(0, left), :] = rows[pl.ds(base + whole_out * 2 * CHUNK, left), :].astype(f32)
        put(0, out_o, whole_out * 2 * CHUNK, left).start()
        put(0, out_o, whole_out * 2 * CHUNK, left).wait()
    for step in range(5):
        exchange(step).wait_send()
    for gather in (two, all_branch):
        gather.near().wait_send()
        gather.across().wait_send()
        gather.onward().wait_send()


def tail(x, resid, seg, gain_one, gain_two, wup, wdown, h1, grow, qkv, mixed, wqkv, wout, cos, sin):
    bf, f32 = jnp.bfloat16, jnp.float32
    own, width = x.shape
    units = wup.shape[1]
    seq = seg.shape[1]
    padded = wout.shape[0]
    local = padded // HEAD_PAD * HEAD
    total = 2 * units + 4 * local
    vm, hbm = pl.BlockSpec(memory_space=pltpu.VMEM), pl.BlockSpec(memory_space=pl.ANY)
    sem = pltpu.SemaphoreType.DMA
    shapes = [((own, width), bf), ((own, width), f32), ((8, width), f32), ((units, width), f32), ((width, units), f32), ((local, width), f32)] + [((width, local), f32)] * 3
    tall = pltpu.VMEM((seq, width), bf)
    return pl.pallas_call(
        tail_kernel,
        out_shape=[jax.ShapeDtypeStruct(s, d) for s, d in shapes],
        in_specs=[vm] * 5 + [hbm] * 10,
        out_specs=[vm] * 3 + [hbm] * 6,
        scratch_shapes=[pltpu.VMEM((total, width), bf)]
        + reducer_scratch(width)
        + [
            pltpu.VMEM((2, 2 * CHUNK, width), f32), sem((2,)), pltpu.VMEM((2, 256, local), f32), sem((2,)),
            pltpu.VMEM((width, units), bf), pltpu.VMEM((units, width), bf), pltpu.VMEM((width, 3 * padded), bf), pltpu.VMEM((padded, width), bf),
            tall, tall, tall, pltpu.VMEM((seq, units), bf), pltpu.VMEM((seq, units), bf), tall,
            pltpu.VMEM((seq, 3 * padded), bf), pltpu.VMEM((seq, padded), bf), pltpu.VMEM((seq, padded), bf),
            pltpu.VMEM((seq, 128), f32), pltpu.VMEM((seq, 128), f32), pltpu.VMEM((seq, SPAN + BLOCK_SEQ), bf),
            pltpu.VMEM((own, width), f32), pltpu.VMEM((seq, HEAD_PAD), f32), pltpu.VMEM((seq, HEAD_PAD), f32),
            pltpu.VMEM((2, own, width), bf), pltpu.VMEM((2, own, width), bf), pltpu.VMEM((own, width), bf), pltpu.VMEM((own, width), bf),
            pltpu.VMEM((5, 8, width), f32), pltpu.VMEM((5, 8, width), f32),
            sem((10,)), sem((2, 3)), sem((2, 3)), sem((2, 3)), sem((2, 3)), sem((2, 3)), sem((2, 5)), pltpu.SemaphoreType.REGULAR,
        ],
        compiler_params=pltpu.CompilerParams(collective_id=2, has_side_effects=True, vmem_limit_bytes=67043328),
    )(x, resid, seg, gain_one.reshape(1, -1), gain_two.reshape(1, -1), wup, wdown, h1, grow, qkv, mixed, wqkv, wout, cos, sin)


def on_device(
    hidden_in,
    segment_ids,
    attn_gain,
    query_weight,
    key_weight,
    value_weight,
    out_weight,
    mlp_gain,
    up_weight,
    down_weight,
    out_cotangent,
):
    row_count = segment_ids.shape[0]
    seq_len = segment_ids.shape[1]
    local_width = query_weight.shape[1]
    head_count = local_width // HEAD
    scale = 1.0 / math.sqrt(HEAD)
    block = min(512, seq_len)
    head_shape = (row_count, seq_len, head_count, HEAD)
    x_float = hidden_in.astype(jnp.float32)
    scaled_one, normed_one, inverse_one = normalize(x_float, attn_gain)
    rows_one = lax.all_gather(scaled_one.astype(jnp.bfloat16), "mp", axis=1, tiled=True)
    cosine, sine = rotary_tables(segment_ids, HEAD)
    queries = rotate(project(rows_one, query_weight).reshape(head_shape), cosine, sine).astype(
        jnp.bfloat16
    )
    keys = rotate(project(rows_one, key_weight).reshape(head_shape), cosine, sine).astype(
        jnp.bfloat16
    )
    values = project(rows_one, value_weight).reshape(head_shape).astype(jnp.bfloat16)
    row_index = 0
    mixed_one, log_one = attend_forward(
        queries[row_index], keys[row_index], values[row_index], segment_ids[row_index], scale, block
    )
    mixed_rows = [mixed_one]
    log_rows = [log_one]
    mixed = jnp.stack(mixed_rows, 0).reshape(row_count, seq_len, local_width).astype(jnp.bfloat16)
    attn_share = lax.psum_scatter(project(mixed, out_weight), "mp", scatter_dimension=1, tiled=True)
    resid = x_float + attn_share
    scaled_two, normed_two, inverse_two = normalize(resid, mlp_gain)
    rows_two = lax.all_gather(scaled_two.astype(jnp.bfloat16), "mp", axis=1, tiled=True)
    up_pre = project(rows_two, up_weight)
    hidden = jax.nn.gelu(up_pre, approximate=True).astype(jnp.bfloat16)
    mlp_share = lax.psum_scatter(
        project(hidden, down_weight).astype(jnp.bfloat16), "mp", scatter_dimension=1, tiled=True
    ).astype(jnp.float32)
    result = (resid + mlp_share).astype(jnp.bfloat16)
    grad_top = out_cotangent.astype(jnp.float32)
    grad_rows = lax.all_gather(out_cotangent, "mp", axis=1, tiled=True)
    down_total = weight_grad(hidden, grad_rows)
    grad_hidden = project_back(grad_rows, down_weight)
    grad_up_pre = (grad_hidden * gelu_slope(up_pre)).astype(jnp.bfloat16)
    up_total = weight_grad(rows_two, grad_up_pre)
    grad_two = lax.psum_scatter(
        project_back(grad_up_pre, up_weight), "mp", scatter_dimension=1, tiled=True
    )
    resid_part, mlp_gain_part = norm_back(grad_two, normed_two, inverse_two, mlp_gain)
    grad_resid = grad_top + resid_part
    branch_rows = lax.all_gather(grad_resid.astype(jnp.bfloat16), "mp", axis=1, tiled=True)
    out_total = weight_grad(mixed, branch_rows)
    grad_mixed = project_back(branch_rows, out_weight).astype(jnp.bfloat16).reshape(head_shape)
    row_index = 0
    grad_q, grad_k, grad_v = attend_back(
        queries[row_index],
        keys[row_index],
        values[row_index],
        grad_mixed[row_index],
        log_rows[row_index],
        segment_ids[row_index],
        scale,
        block,
    )
    query_rows = [grad_q]
    key_rows = [grad_k]
    value_rows = [grad_v]
    grad_query = (
        rotate_back(jnp.stack(query_rows, 0), cosine, sine)
        .astype(jnp.bfloat16)
        .reshape(row_count, seq_len, local_width)
    )
    grad_key = (
        rotate_back(jnp.stack(key_rows, 0), cosine, sine)
        .astype(jnp.bfloat16)
        .reshape(row_count, seq_len, local_width)
    )
    grad_value = (
        jnp.stack(value_rows, 0).astype(jnp.bfloat16).reshape(row_count, seq_len, local_width)
    )
    query_total = weight_grad(rows_one, grad_query)
    key_total = weight_grad(rows_one, grad_key)
    value_total = weight_grad(rows_one, grad_value)
    grad_terms = (
        project_back(grad_query, query_weight)
        + project_back(grad_key, key_weight)
        + project_back(grad_value, value_weight)
    )
    grad_one = lax.psum_scatter(grad_terms, "mp", scatter_dimension=1, tiled=True)
    input_part, attn_gain_part = norm_back(grad_one, normed_one, inverse_one, attn_gain)
    input_grad = grad_resid + input_part
    attn_gain_part, mlp_gain_part = lax.psum((attn_gain_part, mlp_gain_part), "mp")
    (
        query_total,
        key_total,
        value_total,
        out_total,
        attn_gain_part,
        mlp_gain_part,
        up_total,
        down_total,
    ) = lax.psum(
        (
            query_total,
            key_total,
            value_total,
            out_total,
            attn_gain_part,
            mlp_gain_part,
            up_total,
            down_total,
        ),
        "dp",
    )
    return (
        result,
        input_grad,
        attn_gain_part,
        query_total,
        key_total,
        value_total,
        out_total,
        mlp_gain_part,
        up_total,
        down_total,
    )


def on_device_kernels(
    hidden_in, segment_ids, attn_gain, query_weight, key_weight, value_weight, out_weight, mlp_gain, up_weight, down_weight, out_cotangent
):
    resid, h1, grow, qkv, mixed, wqkv, wout, cos, sin = front(
        hidden_in[0], out_cotangent[0], segment_ids, attn_gain, query_weight, key_weight, value_weight, out_weight
    )
    result, input_grad, gains, down, up, out, query, key, value = tail(
        hidden_in[0], resid, segment_ids, attn_gain, mlp_gain, up_weight, down_weight, h1, grow, qkv, mixed, wqkv, wout, cos, sin
    )
    return (result[None], input_grad[None], gains[0], query, key, value, out, gains[1], up, down)


def solution(mesh):
    return jax.shard_map(
        on_device_kernels if mesh.shape["dp"] == 8 else on_device,
        mesh=mesh,
        in_specs=(
            P("dp", "mp", None),
            P("dp", None),
            P(),
            P(None, "mp"),
            P(None, "mp"),
            P(None, "mp"),
            P("mp", None),
            P(),
            P(None, "mp"),
            P("mp", None),
            P("dp", "mp", None),
        ),
        out_specs=(
            P("dp", "mp", None),
            P("dp", "mp", None),
            P(),
            P(None, "mp"),
            P(None, "mp"),
            P(None, "mp"),
            P("mp", None),
            P(),
            P(None, "mp"),
            P("mp", None),
        ),
        check_vma=False,
    )
```

```python
import math

import jax
import jax.numpy as jnp
from jax import lax
from jax.experimental import pallas as pl
from jax.experimental.pallas import tpu as pltpu
from jax.sharding import PartitionSpec as P

HEAD = 80


EPS = 1e-06
MASKED = -1e30
GELU_C = math.sqrt(2.0 / math.pi)
GELU_K = 0.044715


def normalize(values, gain):
    inverse = lax.rsqrt(jnp.mean(values * values, -1, keepdims=True) + EPS)
    normed = values * inverse
    return (normed * gain, normed, inverse)


def norm_back(upstream, normed, inverse, gain):
    scaled = upstream * gain
    inner = jnp.mean(scaled * normed, -1, keepdims=True)
    return (inverse * (scaled - normed * inner), jnp.sum(upstream * normed, axis=(0, 1)))


def gelu_slope(values):
    tangent = jnp.tanh(GELU_C * (values + GELU_K * values * values * values))
    return 0.5 * (1.0 + tangent) + 0.5 * values * (1.0 - tangent * tangent) * GELU_C * (
        1.0 + 3.0 * GELU_K * values * values
    )


def project(left, weight):
    return jnp.einsum("rsd,de->rse", left, weight, preferred_element_type=jnp.float32)


def project_back(left, weight):
    return jnp.einsum("rse,de->rsd", left, weight, preferred_element_type=jnp.float32)


def weight_grad(left, right):
    return jnp.einsum("rsd,rse->de", left, right, preferred_element_type=jnp.float32)


def rotary_tables(segments, head_size):
    seq_len = segments.shape[1]
    places = jnp.arange(seq_len, dtype=jnp.int32)
    starts_here = jnp.concatenate(
        [jnp.ones((segments.shape[0], 1), bool), segments[:, 1:] != segments[:, :-1]], axis=1
    )
    first = lax.cummax(jnp.where(starts_here, places[None, :], 0), axis=1)
    position = (places[None, :] - first).astype(jnp.float32)
    half = head_size // 2
    freqs = jnp.exp(jnp.arange(half, dtype=jnp.float32) * (-2.0 * math.log(10000.0) / head_size))
    angles = position[:, :, None] * freqs[None, None, :]
    return (jnp.cos(angles)[:, :, None, :], jnp.sin(angles)[:, :, None, :])


def rotate(values, cosine, sine):
    half = values.shape[-1] // 2
    first, second = (values[..., :half], values[..., half:])
    return jnp.concatenate([first * cosine - second * sine, second * cosine + first * sine], -1)


def rotate_back(grads, cosine, sine):
    half = grads.shape[-1] // 2
    first, second = (grads[..., :half], grads[..., half:])
    return jnp.concatenate([first * cosine + second * sine, second * cosine - first * sine], -1)


def allowed_block(segments_row, start, size):
    seq_len = segments_row.shape[0]
    query_pos = start + jnp.arange(size, dtype=jnp.int32)
    key_pos = jnp.arange(seq_len, dtype=jnp.int32)
    query_seg = segments_row[start : start + size]
    return (query_pos[:, None] >= key_pos[None, :]) & (query_seg[:, None] == segments_row[None, :])


def block_scores(query_block, keys, allowed, scale):
    scores = (
        jnp.einsum("qhd,khd->hqk", query_block, keys, preferred_element_type=jnp.float32) * scale
    )
    return jnp.where(allowed[None], scores, MASKED)


def attend_forward(queries, keys, values, segments_row, scale, block):
    outputs = []
    sums = []
    for start in range(0, queries.shape[0], block):
        allowed = allowed_block(segments_row, start, block)
        scores = block_scores(queries[start : start + block], keys, allowed, scale)
        top = jnp.max(scores, -1, keepdims=True)
        expo = jnp.exp(scores - top)
        total = jnp.sum(expo, -1, keepdims=True)
        probs = (expo / total).astype(jnp.bfloat16)
        outputs.append(
            jnp.einsum("hqk,khd->qhd", probs, values, preferred_element_type=jnp.float32)
        )
        sums.append(top + jnp.log(total))
    return (jnp.concatenate(outputs, 0), jnp.concatenate(sums, 1))


def attend_back(queries, keys, values, grad_mixed, log_sums, segments_row, scale, block):
    key_total = jnp.zeros(keys.shape, jnp.float32)
    value_total = jnp.zeros(values.shape, jnp.float32)
    query_parts = []
    for start in range(0, queries.shape[0], block):
        allowed = allowed_block(segments_row, start, block)
        query_block = queries[start : start + block]
        scores = block_scores(query_block, keys, allowed, scale)
        probs = jnp.exp(scores - log_sums[:, start : start + block])
        grad_block = grad_mixed[start : start + block]
        grad_probs = jnp.einsum(
            "qhd,khd->hqk", grad_block, values, preferred_element_type=jnp.float32
        )
        inner = jnp.sum(probs * grad_probs, -1, keepdims=True)
        grad_scores = (probs * (grad_probs - inner)).astype(jnp.bfloat16)
        query_parts.append(
            jnp.einsum("hqk,khd->qhd", grad_scores, keys, preferred_element_type=jnp.float32)
            * scale
        )
        key_total = (
            key_total
            + jnp.einsum(
                "hqk,qhd->khd", grad_scores, query_block, preferred_element_type=jnp.float32
            )
            * scale
        )
        value_total = value_total + jnp.einsum(
            "hqk,qhd->khd",
            probs.astype(jnp.bfloat16),
            grad_block,
            preferred_element_type=jnp.float32,
        )
    return (jnp.concatenate(query_parts, 0), key_total, value_total)


MESH = pl.DeviceIdType.MESH
CHUNK = 64
SLOTS = 6
STAGES = 6
(R1Z, R2Z, R3Z, FZM, FZA, FZB, R1Y, R2Y, R3Y, FYI, FYY) = range(11)
(S0Z, S0Y, S1Z, S1Y, S2Z, S2Y, S3ZM, S3ZE, S3YE, S3YY, S4Z, S4Y) = range(12)


def add_rows(total_ref, row, count, *others):
    value = total_ref[pl.ds(row, count), :].astype(jnp.float32)
    for other in others:
        value = value + other[...].astype(jnp.float32)
    total_ref[pl.ds(row, count), :] = value.astype(jnp.bfloat16)


class Reducer:
    def __init__(self, rows, bufs, send_sem, recv_sem, pairs):
        self.rows, self.bufs, self.send_sem, self.recv_sem, self.pairs = rows, bufs, send_sem, recv_sem, pairs
        dp = lax.axis_index("dp")
        self.place, self.side = lax.div(dp, 2), lax.rem(dp, 2)
        self.inner = (self.place == 1) | (self.place == 2)
        self.end = jnp.logical_not(self.inner)
        self.mate = 2 * (self.place + 1 - 2 * lax.rem(self.place, 2)) + self.side
        self.across = 2 * (3 - self.place) + self.side
        self.twin = 2 * self.place + 1 - self.side
        self.half_z = lax.div(self.place, 2)
        self.half_y = self.side

    def copy(self, source, target, send, recv, slot, device):
        return pltpu.make_async_remote_copy(
            src_ref=source,
            dst_ref=target,
            send_sem=self.send_sem.at[send, slot],
            recv_sem=self.recv_sem.at[recv, slot],
            device_id={"dp": device},
            device_id_type=MESH,
        )

    def whole_z(self, pair):
        return pl.multiple_of(pair * (2 * CHUNK), CHUNK)

    def at_z(self, pair, half):
        return pl.multiple_of(pair * (2 * CHUNK) + half * (CHUNK // 2), CHUNK // 2)

    def at_y(self, pair, half):
        return pl.multiple_of(pair * (2 * CHUNK) + CHUNK + half * (CHUNK // 2), CHUNK // 2)

    def moves(self, pair):
        slot = lax.rem(pair, SLOTS)
        rows, (one_z, two_z, three_z, one_y, two_y, three_y) = self.rows, self.bufs
        half = CHUNK // 2
        mine_z, mine_y = self.half_z, self.half_y
        own_z = rows.at[pl.ds(self.at_z(pair, mine_z), half), :]
        rest_z = rows.at[pl.ds(self.at_z(pair, 1 - mine_z), half), :]
        own_y = rows.at[pl.ds(self.at_y(pair, mine_y), half), :]
        rest_y = rows.at[pl.ds(self.at_y(pair, 1 - mine_y), half), :]
        all_z = rows.at[pl.ds(self.whole_z(pair), CHUNK), :]
        return dict(
            s0z=lambda: self.copy(all_z, one_z.at[slot], S0Z, R1Z, slot, self.mate),
            s0y=lambda: self.copy(rest_y, one_y.at[slot], S0Y, R1Y, slot, self.twin),
            s1z=lambda: self.copy(rest_z, two_z.at[slot], S1Z, R2Z, slot, self.across),
            s1y=lambda: self.copy(two_y.at[slot], two_y.at[slot], S1Y, R2Y, slot, self.mate),
            s2z=lambda: self.copy(own_z, three_z.at[slot], S2Z, R3Z, slot, self.twin),
            s2y=lambda: self.copy(own_y, three_y.at[slot], S2Y, R3Y, slot, self.across),
            s3zm=lambda: self.copy(own_z, own_z, S3ZM, FZM, slot, self.across),
            s3ze=lambda: self.copy(own_z, own_z, S3ZE, FZA, slot, self.mate),
            s3ye=lambda: self.copy(own_y, own_y, S3YE, FYI, slot, self.mate),
            s3yy=lambda: self.copy(own_y, own_y, S3YY, FYY, slot, self.twin),
            s4z=lambda: self.copy(rest_z, rest_z, S4Z, FZB, slot, self.mate),
            s4y=lambda: self.copy(own_y, own_y, S4Y, FYY, slot, self.twin),
        )

    def when(self, slot_index, stage, role, body):
        pair = slot_index - stage
        live = (pair >= 0) & (pair < self.pairs)
        if role is not None:
            live = live & role

        @pl.when(live)
        def _():
            body(pair)

    def slot(self, index):
        half = CHUNK // 2
        one_z, two_z, three_z, one_y, two_y, three_y = self.bufs

        def last(pair):
            m = self.moves(pair)
            @pl.when(self.end)
            def _():
                m["s3ze"]().wait_recv()
                m["s4z"]().wait_recv()
                m["s1y"]().wait_send()
                m["s4y"]().wait_send()
                m["s4y"]().wait_recv()

            @pl.when(self.inner)
            def _():
                m["s3zm"]().wait_send()
                m["s3ze"]().wait_send()
                m["s3ye"]().wait_send()
                m["s3yy"]().wait_send()
                m["s4z"]().wait_send()
                m["s3yy"]().wait_recv()

        def fourth_inner(pair):
            m = self.moves(pair)
            m["s3zm"]().wait_recv()
            m["s4z"]().start()

        def fourth_end(pair):
            m = self.moves(pair)
            m["s3ye"]().wait_recv()
            m["s4y"]().start()

        def third(pair):
            m = self.moves(pair)
            slot = lax.rem(pair, SLOTS)
            m["s2z"]().wait()
            m["s2y"]().wait()
            add_rows(self.rows, self.at_z(pair, self.half_z), half, three_z.at[slot])
            add_rows(self.rows, self.at_y(pair, self.half_y), half, three_y.at[slot])
            m["s3ze"]().start()
            m["s3zm"]().start()
            m["s3ye"]().start()
            m["s3yy"]().start()

        def second(pair):
            m = self.moves(pair)
            slot = lax.rem(pair, SLOTS)
            m["s1z"]().wait()
            m["s1y"]().wait_recv()
            m["s0y"]().wait_send()
            add_rows(
                self.rows, self.at_z(pair, self.half_z), half,
                one_z.at[slot, pl.ds(pl.multiple_of(self.half_z * half, half), half), :], two_z.at[slot],
            )
            add_rows(self.rows, self.at_y(pair, self.half_y), half, one_y.at[slot], two_y.at[slot])
            m["s2z"]().start()
            m["s2y"]().start()

        def first_inner(pair):
            m = self.moves(pair)
            slot = lax.rem(pair, SLOTS)
            m["s0z"]().wait_recv()
            m["s0y"]().wait_recv()
            other = 1 - self.half_z
            add_rows(
                self.rows, self.at_z(pair, other), half,
                one_z.at[slot, pl.ds(pl.multiple_of(other * half, half), half), :],
            )
            m["s1z"]().start()

        def first_end(pair):
            m = self.moves(pair)
            slot = lax.rem(pair, SLOTS)
            m["s0y"]().wait()
            m["s0z"]().wait_send()
            mine = self.rows[pl.ds(self.at_y(pair, self.half_y), half), :].astype(jnp.float32)
            two_y[slot] = (mine + one_y[slot].astype(jnp.float32)).astype(jnp.bfloat16)
            m["s1y"]().start()

        def start(pair):
            m = self.moves(pair)
            m["s0y"]().start()

            @pl.when(self.end)
            def _():
                m["s0z"]().start()

        self.when(index, 0, None, start)
        self.when(index, 1, self.end, first_end)
        self.when(index, 1, self.inner, first_inner)
        self.when(index, 2, self.inner, second)
        self.when(index, 3, self.inner, third)
        self.when(index, 4, self.inner, fourth_inner)
        self.when(index, 4, self.end, fourth_end)
        self.when(index, 5, None, last)

    def greet(self, barrier):
        for device in (self.mate, self.across, self.twin):
            pl.semaphore_signal(barrier, inc=1, device_id={"dp": device}, device_id_type=MESH)
        return 3


def reducer_scratch(width):
    half = CHUNK // 2
    return [
        pltpu.VMEM((SLOTS, CHUNK, width), jnp.bfloat16),
        pltpu.VMEM((SLOTS, half, width), jnp.bfloat16),
        pltpu.VMEM((SLOTS, half, width), jnp.bfloat16),
        pltpu.VMEM((SLOTS, half, width), jnp.bfloat16),
        pltpu.VMEM((SLOTS, half, width), jnp.bfloat16),
        pltpu.VMEM((SLOTS, half, width), jnp.bfloat16),
        pltpu.SemaphoreType.DMA((12, SLOTS)),
        pltpu.SemaphoreType.DMA((11, SLOTS)),
    ]


HEAD_PAD = 128
BLOCK_SEQ = 256
SPAN = 512


def pad_matrix(local, padded):
    shape = (padded, local)
    feature = lax.broadcasted_iota(jnp.int32, shape, 1)
    lane = lax.broadcasted_iota(jnp.int32, shape, 0)
    head = jnp.zeros(shape, jnp.int32)
    for h in range(1, local // HEAD):
        head = head + (feature >= h * HEAD).astype(jnp.int32)
    within = feature - head * HEAD
    target = head * HEAD_PAD + within + jnp.where(within >= HEAD // 2, HEAD_PAD // 2 - HEAD // 2, 0)
    return jnp.where(lane == target, 1.0, 0.0).astype(jnp.bfloat16)


def dot(a, b):
    return jnp.dot(a, b, preferred_element_type=jnp.float32)


def dot_nt(a, b):
    return lax.dot_general(a, b, (((1,), (1,)), ((), ())), preferred_element_type=jnp.float32)


def dot_tn(a, b):
    return lax.dot_general(a, b, (((0,), (0,)), ((), ())), preferred_element_type=jnp.float32)


def segment_columns(seg):
    lines = jnp.broadcast_to(seg.astype(jnp.float32), (16, seg.shape[1])).astype(jnp.bfloat16)
    pick = (lax.broadcasted_iota(jnp.int32, (16, 128), 0) == 0).astype(jnp.float32).astype(jnp.bfloat16)
    return dot_tn(lines, pick)


def rotary_into(seg, cos_ref, sin_ref):
    seq = seg.shape[1]
    ids = segment_columns(seg)
    first = jnp.zeros((seq, 128), jnp.float32)
    row = seg.astype(jnp.float32)
    for s in range(1, 16):
        before = jnp.sum(jnp.where(row < s, 1.0, 0.0), axis=1, keepdims=True)
        first = jnp.where(ids == s, before, first)
    position = lax.broadcasted_iota(jnp.int32, (seq, 128), 0).astype(jnp.float32) - first
    lane = lax.broadcasted_iota(jnp.int32, (1, 128), 1)
    upper = lane >= HEAD_PAD // 2
    index = jnp.where(upper, lane - HEAD_PAD // 2, lane)
    freqs = jnp.exp(index.astype(jnp.float32) * (-2.0 * math.log(10000.0) / HEAD))
    freqs = jnp.where(index < HEAD // 2, freqs, 0.0)
    angles = position * freqs
    cos_ref[...] = jnp.cos(angles)
    sin_ref[...] = jnp.where(upper, jnp.sin(angles), -jnp.sin(angles))


class Ring4:
    def __init__(self):
        mp = lax.axis_index("mp")
        chip, core = lax.div(mp, 2), lax.rem(mp, 2)
        self.me = mp
        self.core = 2 * chip + 1 - core
        self.chip = 2 * (1 - chip) + core
        self.far = 2 * (1 - chip) + 1 - core


def block_rows(index):
    return pl.ds(pl.multiple_of(index * BLOCK_SEQ, BLOCK_SEQ), BLOCK_SEQ)


class Gather:
    def __init__(self, ring, rows, sems, parts=1):
        self.parts = parts
        size = BLOCK_SEQ // parts

        def copy(block, device, which, part):
            at = pl.ds(pl.multiple_of(block * BLOCK_SEQ + part * size, size), size)
            return pltpu.make_async_remote_copy(
                src_ref=rows.at[at, :],
                dst_ref=rows.at[at, :],
                send_sem=sems.at[0, which * parts + part],
                recv_sem=sems.at[1, which * parts + part],
                device_id={"mp": device},
                device_id_type=MESH,
            )

        self.near = lambda part=0: copy(ring.me, ring.core, 0, part)
        self.across = lambda part=0: copy(ring.me, ring.chip, 1, part)
        self.onward = lambda part=0: copy(ring.chip, ring.core, 2, part)

    def start(self, part=0):
        self.across(part).start()
        self.near(part).start()

    def forward(self):
        for part in range(self.parts):
            self.across(part).wait_recv()
            self.onward(part).start()

    def near_in(self):
        for part in range(self.parts):
            self.near(part).wait_recv()

    def onward_in(self):
        for part in range(self.parts):
            self.onward(part).wait_recv()

    def sent(self):
        for part in range(self.parts):
            self.near(part).wait_send()
            self.across(part).wait_send()
            self.onward(part).wait_send()


class Scatter:
    def __init__(self, ring, send_core, recv_core, send_chip, recv_chip, sems, parts=1):
        self.parts = parts
        size = BLOCK_SEQ // parts

        def copy(source, target, device, which, part):
            at = pl.ds(part * size, size)
            return pltpu.make_async_remote_copy(
                src_ref=source.at[at, :],
                dst_ref=target.at[at, :],
                send_sem=sems.at[0, which * parts + part],
                recv_sem=sems.at[1, which * parts + part],
                device_id={"mp": device},
                device_id_type=MESH,
            )

        self.far = lambda part=0: copy(send_core.at[0], recv_core.at[0], ring.core, 0, part)
        self.core = lambda part=0: copy(send_core.at[1], recv_core.at[1], ring.core, 1, part)
        self.chip = lambda part=0: copy(send_chip, recv_chip, ring.chip, 2, part)


def greet_mp(ring, barrier):
    for device in (ring.core, ring.chip):
        pl.semaphore_signal(barrier, inc=1, device_id={"mp": device}, device_id_type=MESH)
    return 2


def norm_rows(values):
    inverse = lax.rsqrt(jnp.mean(values * values, -1, keepdims=True) + EPS)
    return values * inverse, inverse


def qkv_block(rows, weights, cos_ref, sin_ref, out, block):
    at = block_rows(block)
    turned = 2 * (weights.shape[0] // 3) // 256
    tiles = weights.shape[0] // 256

    def one(n, turn):
        cols = pl.ds(pl.multiple_of(n * 256, 256), 256)
        value = dot_nt(rows[at, :], weights[cols, :])
        if turn:
            cosine, sine = cos_ref[at, :], sin_ref[at, :]
            halves = [value[:, j * 128 : j * 128 + 128] for j in range(2)]
            value = jnp.concatenate([h * cosine + pltpu.roll(h, 64, 1) * sine for h in halves], axis=1)
        out[at, cols] = value.astype(jnp.bfloat16)

    @pl.loop(0, turned)
    def _(n):
        one(n, True)

    @pl.loop(turned, tiles)
    def _(n):
        one(n, False)


def masks_into(seg, ids_ref, bias_ref):
    seq = seg.shape[1]
    for i in range(seq // BLOCK_SEQ):
        low = max(0, i * BLOCK_SEQ - SPAN)
        high = (i + 1) * BLOCK_SEQ
        shape = (BLOCK_SEQ, high - low)
        query = i * BLOCK_SEQ + lax.broadcasted_iota(jnp.int32, shape, 0)
        key = low + lax.broadcasted_iota(jnp.int32, shape, 1)
        ids = ids_ref[pl.ds(i * BLOCK_SEQ, BLOCK_SEQ), :][:, :1]
        same = ids == seg[:, low:high].astype(jnp.float32)
        bias_ref[pl.ds(i * BLOCK_SEQ, BLOCK_SEQ), pl.ds(0, high - low)] = jnp.where((query >= key) & same, 0.0, MASKED).astype(bias_ref.dtype)


def attend(qkv, out, bias_ref, heads, scale, blocks):
    width = heads * HEAD_PAD

    @pl.loop(0, heads)
    def _(h):
        lanes = [pl.ds(pl.multiple_of(part * width + h * HEAD_PAD, HEAD_PAD), HEAD_PAD) for part in range(3)]
        for i in blocks:
            low, high = max(0, i * BLOCK_SEQ - SPAN), (i + 1) * BLOCK_SEQ
            rows, keys = pl.ds(i * BLOCK_SEQ, BLOCK_SEQ), pl.ds(low, high - low)
            scores = dot_nt(qkv[rows, lanes[0]], qkv[keys, lanes[1]]) + bias_ref[rows, pl.ds(0, high - low)]
            top = jnp.max(scores, -1, keepdims=True)
            expo = jnp.exp((scores - top) * scale)
            probs = expo * (1.0 / jnp.sum(expo, -1, keepdims=True))
            out[rows, lanes[0]] = dot(probs.astype(jnp.bfloat16), qkv[keys, lanes[2]]).astype(jnp.bfloat16)


def layer_kernel(
    x, g, seg, gain_one, gain_two, wq, wk, wv, wo, wup, wdown,
    result_o, input_o, gains_o, sums_o,
    rows, b0, b1, b2, b3, b4, b5, send_sem, recv_sem, save_sem,
    w_up, w_down, w_qkv, w_out, rows_one, rows_g, rows_two, hidden, grad_up, branch, qkv, mixed, grad_mixed,
    cos_ref, sin_ref, bias_ref, resid, term_ref, key_sum, value_sum,
    send_core, recv_core, send_chip, recv_chip, gain_acc, gain_recv,
    load_sem, one_sem, g_sem, two_sem, branch_sem, rs0_sem, rs_sem, rs2_sem, rs3_sem, gain_sem, free_sem,
):
    bf, f32 = jnp.bfloat16, jnp.float32
    ring = Ring4()
    seq, width = rows_two.shape
    units = w_up.shape[1]
    padded = w_out.shape[0]
    heads = padded // HEAD_PAD
    local = heads * HEAD
    pairs = rows.shape[0] // (2 * CHUNK)
    scale = 1.0 / math.sqrt(HEAD)
    half = BLOCK_SEQ // 2
    chip = lax.div(ring.me, 2)
    red = Reducer(rows, (b0, b1, b2, b3, b4, b5), send_sem, recv_sem, pairs)
    barrier = pltpu.get_barrier_semaphore()
    count = greet_mp(ring, barrier) + red.greet(barrier)
    places = [(w, rows.at[pl.ds(i * local, local), :]) for i, w in enumerate((wq, wk, wv, wo))]
    places += [(g, rows_g.at[block_rows(ring.me), :]), (wup, w_up), (wdown, w_down)]
    loads = [pltpu.make_async_copy(source, target, load_sem.at[i]) for i, (source, target) in enumerate(places)]
    for load in loads[:5]:
        load.start()
    normed, _ = norm_rows(x[...].astype(f32))
    rows_one[block_rows(ring.me), :] = (normed * gain_one[...]).astype(bf)
    one, all_g = Gather(ring, rows_one, one_sem, 2), Gather(ring, rows_g, g_sem)
    two, all_branch = Gather(ring, rows_two, two_sem, 2), Gather(ring, branch, branch_sem)
    ahead = Scatter(ring, send_core, recv_core, send_chip, recv_chip, rs0_sem, 2)
    first = Scatter(ring, send_core, recv_core, send_chip, recv_chip, rs_sem)
    second = Scatter(ring, send_core, recv_core, send_chip, recv_chip, rs2_sem)
    third = Scatter(ring, send_core, recv_core, send_chip, recv_chip, rs3_sem)
    pl.semaphore_wait(barrier, count)
    one.start(0)
    one.start(1)
    for load in loads[5:]:
        load.start()

    spread = pad_matrix(local, padded)
    for i in range(3):
        loads[i].wait()
        w_qkv[pl.ds(i * padded, padded), :] = dot(spread, rows[pl.ds(i * local, local), :]).astype(bf)
    loads[3].wait()
    w_out[...] = dot(spread, rows[pl.ds(3 * local, local), :]).astype(bf)
    rotary_into(seg[...], cos_ref, sin_ref)
    qkv_block(rows_one, w_qkv, cos_ref, sin_ref, qkv, ring.me)
    one.near_in()
    qkv_block(rows_one, w_qkv, cos_ref, sin_ref, qkv, ring.core)
    key_sum[...] = segment_columns(seg[...])
    masks_into(seg[...], key_sum, bias_ref)
    loads[4].wait()
    one.forward()
    one.across(0).wait_send()
    one.across(1).wait_send()
    all_g.start()
    qkv_block(rows_one, w_qkv, cos_ref, sin_ref, qkv, ring.chip)
    one.onward_in()
    qkv_block(rows_one, w_qkv, cos_ref, sin_ref, qkv, ring.far)

    early, late = (0, 1), (2, 3)

    @pl.when(chip == 0)
    def _():
        attend(qkv, mixed, bias_ref, heads, scale, late)

    @pl.when(chip == 1)
    def _():
        attend(qkv, mixed, bias_ref, heads, scale, early)

    def term(block, part):
        at = pl.ds(pl.multiple_of(block * BLOCK_SEQ + part * half, half), half)
        return dot(mixed[at, :], w_out[...])

    parts = [pl.ds(p * half, half) for p in range(2)]
    for p in range(2):
        send_core[0, parts[p], :] = term(ring.far, p).astype(bf)
        ahead.far(p).start()
    for p in range(2):
        value = term(ring.chip, p)
        ahead.far(p).wait_recv()
        send_chip[parts[p], :] = (value + recv_core[0, parts[p], :].astype(f32)).astype(bf)
        ahead.chip(p).start()

    @pl.when(chip == 0)
    def _():
        attend(qkv, mixed, bias_ref, heads, scale, early)

    @pl.when(chip == 1)
    def _():
        attend(qkv, mixed, bias_ref, heads, scale, late)

    for p in range(2):
        send_core[1, parts[p], :] = term(ring.core, p).astype(bf)
        ahead.core(p).start()
    all_g.forward()
    for p in range(2):
        resid[parts[p], :] = x[parts[p], :].astype(f32) + term(ring.me, p)
    for p in range(2):
        ahead.core(p).wait_recv()
        ahead.chip(p).wait_recv()
        value = resid[parts[p], :] + recv_core[1, parts[p], :].astype(f32) + recv_chip[parts[p], :].astype(f32)
        resid[parts[p], :] = value
        normed, _ = norm_rows(value)
        at = pl.ds(pl.multiple_of(ring.me * BLOCK_SEQ + p * half, half), half)
        rows_two[at, :] = (normed * gain_two[...]).astype(bf)
        two.start(p)
    for p in range(2):
        ahead.far(p).wait_send()
        ahead.core(p).wait_send()
        ahead.chip(p).wait_send()

    base = 2 * units

    def put(pair):
        at = pl.ds(pl.multiple_of(pair * 2 * CHUNK, 2 * CHUNK), 2 * CHUNK)
        return pltpu.make_async_copy(rows.at[at, :], sums_o.at[at, :], save_sem.at[lax.rem(pair, 4)])

    def slot(index):
        red.slot(index)
        pair = index - (STAGES - 1)

        @pl.when(pair >= 4)
        def _():
            put(pair - 4).wait()

        @pl.when(pair >= 0)
        def _():
            put(pair).start()

    def tile(n):
        return pl.ds(pl.multiple_of(n * 256, 256), 256)

    def up_tile(block, n):
        u = dot(rows_two[block_rows(block), :], w_up[:, tile(n)])
        tangent = jnp.tanh(GELU_C * (u + GELU_K * u * u * u))
        hidden[block_rows(block), tile(n)] = (0.5 * u * (1.0 + tangent)).astype(bf)

    def up_block(block):
        @pl.loop(0, units // 256)
        def _(n):
            up_tile(block, n)

    loads[5].wait()
    up_block(ring.me)
    two.near_in()
    up_block(ring.core)
    all_g.near_in()
    all_g.onward_in()
    two.forward()
    two.onward_in()

    @pl.loop(0, units // 256)
    def _(n):
        for block in (ring.chip, ring.far):
            up_tile(block, n)
        rows[tile(n), :] = dot_tn(hidden[:, tile(n)], rows_g[...]).astype(bf)
        slot(n)

    loads[6].wait()

    def order(k):
        there = k < 2
        core = lax.rem(ring.me, 2)
        flip = 1 - lax.rem(k, 2)
        to_chip = jnp.where(there, 1 - chip, chip)
        to_core = jnp.where(flip == 1, 1 - core, core)
        return 2 * to_chip + to_core

    def hand_on(k, scatter, start):
        @pl.when(k == 0)
        def _():
            send_core[0] = term_ref[...].astype(bf)
            scatter.far().start()

        @pl.when(k == 1)
        def _():
            scatter.far().wait_recv()
            send_chip[...] = (term_ref[...] + recv_core[0].astype(f32)).astype(bf)
            scatter.chip().start()

        @pl.when(k == 2)
        def _():
            send_core[1] = term_ref[...].astype(bf)
            scatter.core().start()

        @pl.when(k == 3)
        def _():
            scatter.core().wait_recv()
            term_ref[...] = term_ref[...] + recv_core[1].astype(f32)

    def settle(scatter):
        for copy in (scatter.far(), scatter.core()):
            copy.wait_send()
        scatter.chip().wait()
        return term_ref[...] + recv_chip[...].astype(f32)

    @pl.loop(0, 4)
    def _(k):
        at = block_rows(order(k))

        @pl.loop(0, units // 256)
        def _(n):
            u = dot(rows_two[at, :], w_up[:, tile(n)])
            upstream = dot_nt(rows_g[at, :], w_down[tile(n), :])
            tangent = jnp.tanh(GELU_C * (u + GELU_K * u * u * u))
            slope = 0.5 * (1.0 + tangent) + 0.5 * u * (1.0 - tangent * tangent) * GELU_C * (1.0 + 3.0 * GELU_K * u * u)
            grad_up[at, tile(n)] = (upstream * slope).astype(bf)

        @pl.loop(0, width // 256)
        def _(n):
            term_ref[:, tile(n)] = dot_nt(grad_up[at, :], w_up[tile(n), :])

        hand_on(k, first, None)
        slot(5 + k)

    def up_rows(i):
        rows[pl.ds(pl.multiple_of(units + i * 256, 256), 256), :] = dot_tn(rows_two[:, tile(i)], grad_up[...]).astype(bf)

    @pl.loop(0, 2)
    def _(i):
        up_rows(i)
        slot(9 + i)

    grad_two = settle(first)
    normed, inverse = norm_rows(resid[...])
    scaled = grad_two * gain_two[...]
    part = inverse * (scaled - normed * jnp.mean(scaled * normed, -1, keepdims=True))
    mlp_part = jnp.sum(grad_two * normed, axis=0, keepdims=True)
    gain_acc[0] = jnp.zeros(gain_acc.shape[1:], f32)
    gain_acc[0, 1:2, :] = mlp_part
    mine = rows_g[block_rows(ring.me), :].astype(f32) + part
    input_o[...] = mine
    branch[block_rows(ring.me), :] = mine.astype(bf)
    all_branch.across().start()
    all_branch.near().start()

    @pl.loop(2, units // 256)
    def _(i):
        up_rows(i)
        slot(9 + i)

    all_branch.near().wait_recv()
    all_branch.forward()
    all_branch.onward().wait_recv()

    def head_rows(left, lane, right, row):
        value = dot_tn(left[:, lane], right[...])
        halves = [value[at : at + HEAD // 2, :] for at in (0, 64, 128, 192)]
        rows[pl.ds(pl.multiple_of(row, 16), 2 * HEAD), :] = jnp.concatenate(halves, axis=0).astype(bf)

    @pl.loop(0, heads // 2)
    def _(j):
        head_rows(mixed, tile(j), branch, base + j * 2 * HEAD)

    @pl.loop(0, 4)
    def _(b):
        grad_mixed[block_rows(b), :] = dot_nt(branch[block_rows(b), :], w_out[...]).astype(bf)

    @pl.loop(0, heads)
    def _(h):
        lanes = [pl.ds(pl.multiple_of(n * padded + h * HEAD_PAD, HEAD_PAD), HEAD_PAD) for n in range(3)]
        key_sum[...] = jnp.zeros_like(key_sum)
        value_sum[...] = jnp.zeros_like(value_sum)
        for i in range(seq // BLOCK_SEQ):
            low, high = max(0, i * BLOCK_SEQ - SPAN), (i + 1) * BLOCK_SEQ
            at, keys = pl.ds(i * BLOCK_SEQ, BLOCK_SEQ), pl.ds(low, high - low)
            query, upstream = qkv[at, lanes[0]], grad_mixed[at, lanes[0]]
            scores = dot_nt(query, qkv[keys, lanes[1]]) + bias_ref[at, pl.ds(0, high - low)]
            top = jnp.max(scores, -1, keepdims=True)
            expo = jnp.exp((scores - top) * scale)
            probs = expo * (1.0 / jnp.sum(expo, -1, keepdims=True))
            grad_probs = dot_nt(upstream, qkv[keys, lanes[2]])
            inner = jnp.sum(probs * grad_probs, -1, keepdims=True)
            grad_scores = (probs * (grad_probs - inner)).astype(bf)
            value_sum[keys, :] += dot_tn(probs.astype(bf), upstream)
            key_sum[keys, :] += dot_tn(grad_scores, query)
            turned = dot(grad_scores, qkv[keys, lanes[1]]) * scale
            qkv[at, lanes[0]] = (turned * cos_ref[at, :] - pltpu.roll(turned, 64, 1) * sin_ref[at, :]).astype(bf)
            if i == 1:
                slot(14 + 2 * h)
        turned = key_sum[...] * scale
        qkv[:, lanes[1]] = (turned * cos_ref[...] - pltpu.roll(turned, 64, 1) * sin_ref[...]).astype(bf)
        qkv[:, lanes[2]] = value_sum[...].astype(bf)
        at = block_rows(order(h))

        @pl.loop(0, width // 256)
        def _(n):
            term_ref[:, tile(n)] = dot(hidden[at, :], w_down[:, tile(n)])

        hand_on(h, second, None)
        slot(15 + 2 * h)

    @pl.loop(0, 3)
    def _(part):
        for j in range(heads // 2):
            lane = pl.ds(pl.multiple_of(part * padded + j * 256, 256), 256)
            head_rows(qkv, lane, rows_one, base + (part + 1) * local + j * 2 * HEAD)
        slot(22 + part)

    result_o[...] = (resid[...] + settle(second)).astype(bf)
    for device in (ring.core, ring.chip):
        pl.semaphore_signal(free_sem, inc=1, device_id={"mp": device}, device_id_type=MESH)
    pl.semaphore_wait(free_sem, 2)

    @pl.loop(0, 4)
    def _(k):
        at = block_rows(order(k))

        @pl.loop(0, width // 256)
        def _(n):
            term_ref[:, tile(n)] = dot(qkv[at, :], w_qkv[:, tile(n)])

        hand_on(k, third, None)
        slot(25 + k)

    slot(29)
    grad_one = settle(third)
    normed, inverse = norm_rows(x[...].astype(f32))
    scaled = grad_one * gain_one[...]
    input_o[...] = input_o[...] + inverse * (scaled - normed * jnp.mean(scaled * normed, -1, keepdims=True))
    gain_acc[0, 0:1, :] = jnp.sum(grad_one * normed, axis=0, keepdims=True)

    def exchange(step):
        names = ({"mp": ring.core}, {"mp": ring.chip}, {"dp": red.twin}, {"dp": red.mate}, {"dp": red.across})
        return pltpu.make_async_remote_copy(
            src_ref=gain_acc.at[step], dst_ref=gain_recv.at[step], send_sem=gain_sem.at[0, step], recv_sem=gain_sem.at[1, step],
            device_id=names[step], device_id_type=MESH,
        )

    last = pairs + STAGES - 1

    @pl.loop(30, last)
    def _(index):
        for step in range(5):

            @pl.when(index == 30 + step)
            def _():
                if step:
                    exchange(step - 1).wait_recv()
                    gain_acc[step] = gain_acc[step - 1] + gain_recv[step - 1]
                exchange(step).start()

        slot(index)

    exchange(4).wait_recv()
    gains_o[...] = gain_acc[4] + gain_recv[4]
    for pair in range(pairs - 4, pairs):
        put(pair).wait()
    for step in range(5):
        exchange(step).wait_send()
    for part in range(2):
        one.near(part).wait_send()
        one.onward(part).wait_send()
    for gather in (all_g, two, all_branch):
        gather.sent()


def layer(x, g, seg, gain_one, gain_two, wq, wk, wv, wo, wup, wdown):
    bf, f32 = jnp.bfloat16, jnp.float32
    own, width = x.shape
    units = wup.shape[1]
    seq = seg.shape[1]
    local = wo.shape[0]
    padded = local // HEAD * HEAD_PAD
    total = 2 * units + 4 * local
    vm, hbm = pl.BlockSpec(memory_space=pltpu.VMEM), pl.BlockSpec(memory_space=pl.ANY)
    sem = pltpu.SemaphoreType.DMA
    shapes = [((own, width), bf), ((own, width), f32), ((8, width), f32), ((total, width), bf)]
    tall = pltpu.VMEM((seq, width), bf)
    return pl.pallas_call(
        layer_kernel,
        out_shape=[jax.ShapeDtypeStruct(s, d) for s, d in shapes],
        in_specs=[vm, hbm, vm, vm, vm] + [hbm] * 6,
        out_specs=[vm] * 3 + [hbm],
        scratch_shapes=[pltpu.VMEM((total, width), bf)]
        + reducer_scratch(width)
        + [
            sem((4,)),
            pltpu.VMEM((width, units), bf), pltpu.VMEM((units, width), bf), pltpu.VMEM((3 * padded, width), bf), pltpu.VMEM((padded, width), bf),
            tall, tall, tall, pltpu.VMEM((seq, units), bf), pltpu.VMEM((seq, units), bf), tall,
            pltpu.VMEM((seq, 3 * padded), bf), pltpu.VMEM((seq, padded), bf), pltpu.VMEM((seq, padded), bf),
            pltpu.VMEM((seq, 128), f32), pltpu.VMEM((seq, 128), f32), pltpu.VMEM((seq, SPAN + BLOCK_SEQ), bf),
            pltpu.VMEM((own, width), f32), pltpu.VMEM((own, width), f32), pltpu.VMEM((seq, HEAD_PAD), f32), pltpu.VMEM((seq, HEAD_PAD), f32),
            pltpu.VMEM((2, own, width), bf), pltpu.VMEM((2, own, width), bf), pltpu.VMEM((own, width), bf), pltpu.VMEM((own, width), bf),
            pltpu.VMEM((5, 8, width), f32), pltpu.VMEM((5, 8, width), f32),
            sem((7,)), sem((2, 6)), sem((2, 3)), sem((2, 6)), sem((2, 3)), sem((2, 6)), sem((2, 3)), sem((2, 3)), sem((2, 3)), sem((2, 5)),
            pltpu.SemaphoreType.REGULAR,
        ],
        compiler_params=pltpu.CompilerParams(collective_id=0, has_side_effects=True, vmem_limit_bytes=67043328),
    )(x, g, seg, gain_one, gain_two, wq, wk, wv, wo, wup, wdown)


def finish_kernel(result, input_grad, gains, sums, result_o, input_o, one_o, two_o, down_o, up_o, out_o, q_o, k_o, v_o, inbox, outbox, side_one, side_two, in_sem, out_sem, side_sem):
    step = out_o.shape[0]
    targets = [(down_o, i * step) for i in range(down_o.shape[0] // step)] + [(up_o, i * step) for i in range(up_o.shape[0] // step)]
    targets += [(t, 0) for t in (out_o, q_o, k_o, v_o)]
    count, depth = len(targets), inbox.shape[0]
    bring = [pltpu.make_async_copy(result, side_one, side_sem.at[0]), pltpu.make_async_copy(input_grad, side_two, side_sem.at[1])]
    take = [pltpu.make_async_copy(side_one, result_o, side_sem.at[2]), pltpu.make_async_copy(side_two, input_o, side_sem.at[3])]

    def read(i):
        return pltpu.make_async_copy(sums.at[pl.ds(i * step, step), :], inbox.at[i % depth], in_sem.at[i % depth])

    def write(i):
        target, at = targets[i]
        return pltpu.make_async_copy(outbox.at[i % depth], target.at[pl.ds(at, step), :], out_sem.at[i % depth])

    for i in range(depth):
        read(i).start()
    for side in bring:
        side.start()
    one_o[...] = gains[0, :]
    two_o[...] = gains[1, :]
    for i in range(count):
        read(i).wait()
        if i >= depth:
            write(i - depth).wait()
        outbox[i % depth] = inbox[i % depth].astype(jnp.float32)
        write(i).start()
        if i + depth < count:
            read(i + depth).start()
        if i == depth:
            for come, go in zip(bring, take):
                come.wait()
                go.start()
    for i in range(count - depth, count):
        write(i).wait()
    for side in take:
        side.wait()


def finish(result, input_grad, gains, sums, units, local):
    bf, f32 = jnp.bfloat16, jnp.float32
    own, width = result.shape
    vm, hbm = pl.BlockSpec(memory_space=pltpu.VMEM), pl.BlockSpec(memory_space=pl.ANY)
    sem = pltpu.SemaphoreType.DMA
    shapes = [((own, width), bf), ((own, width), f32), ((width,), f32), ((width,), f32), ((units, width), f32), ((width, units), f32)] + [((local, width), f32)] * 4
    return pl.pallas_call(
        finish_kernel,
        out_shape=[jax.ShapeDtypeStruct(s, d) for s, d in shapes],
        in_specs=[hbm, hbm, vm, hbm],
        out_specs=[hbm, hbm, vm, vm] + [hbm] * 6,
        scratch_shapes=[pltpu.VMEM((3, local, width), bf), pltpu.VMEM((3, local, width), f32), pltpu.VMEM((own, width), bf), pltpu.VMEM((own, width), f32), sem((3,)), sem((3,)), sem((4,))],
        compiler_params=pltpu.CompilerParams(vmem_limit_bytes=67043328),
    )(result, input_grad, gains, sums)


def on_device(
    hidden_in,
    segment_ids,
    attn_gain,
    query_weight,
    key_weight,
    value_weight,
    out_weight,
    mlp_gain,
    up_weight,
    down_weight,
    out_cotangent,
):
    row_count = segment_ids.shape[0]
    seq_len = segment_ids.shape[1]
    local_width = query_weight.shape[1]
    head_count = local_width // HEAD
    scale = 1.0 / math.sqrt(HEAD)
    block = min(512, seq_len)
    head_shape = (row_count, seq_len, head_count, HEAD)
    x_float = hidden_in.astype(jnp.float32)
    scaled_one, normed_one, inverse_one = normalize(x_float, attn_gain)
    rows_one = lax.all_gather(scaled_one.astype(jnp.bfloat16), "mp", axis=1, tiled=True)
    cosine, sine = rotary_tables(segment_ids, HEAD)
    queries = rotate(project(rows_one, query_weight).reshape(head_shape), cosine, sine).astype(
        jnp.bfloat16
    )
    keys = rotate(project(rows_one, key_weight).reshape(head_shape), cosine, sine).astype(
        jnp.bfloat16
    )
    values = project(rows_one, value_weight).reshape(head_shape).astype(jnp.bfloat16)
    row_index = 0
    mixed_one, log_one = attend_forward(
        queries[row_index], keys[row_index], values[row_index], segment_ids[row_index], scale, block
    )
    mixed_rows = [mixed_one]
    log_rows = [log_one]
    mixed = jnp.stack(mixed_rows, 0).reshape(row_count, seq_len, local_width).astype(jnp.bfloat16)
    attn_share = lax.psum_scatter(project(mixed, out_weight), "mp", scatter_dimension=1, tiled=True)
    resid = x_float + attn_share
    scaled_two, normed_two, inverse_two = normalize(resid, mlp_gain)
    rows_two = lax.all_gather(scaled_two.astype(jnp.bfloat16), "mp", axis=1, tiled=True)
    up_pre = project(rows_two, up_weight)
    hidden = jax.nn.gelu(up_pre, approximate=True).astype(jnp.bfloat16)
    mlp_share = lax.psum_scatter(
        project(hidden, down_weight).astype(jnp.bfloat16), "mp", scatter_dimension=1, tiled=True
    ).astype(jnp.float32)
    result = (resid + mlp_share).astype(jnp.bfloat16)
    grad_top = out_cotangent.astype(jnp.float32)
    grad_rows = lax.all_gather(out_cotangent, "mp", axis=1, tiled=True)
    down_total = weight_grad(hidden, grad_rows)
    grad_hidden = project_back(grad_rows, down_weight)
    grad_up_pre = (grad_hidden * gelu_slope(up_pre)).astype(jnp.bfloat16)
    up_total = weight_grad(rows_two, grad_up_pre)
    grad_two = lax.psum_scatter(
        project_back(grad_up_pre, up_weight), "mp", scatter_dimension=1, tiled=True
    )
    resid_part, mlp_gain_part = norm_back(grad_two, normed_two, inverse_two, mlp_gain)
    grad_resid = grad_top + resid_part
    branch_rows = lax.all_gather(grad_resid.astype(jnp.bfloat16), "mp", axis=1, tiled=True)
    out_total = weight_grad(mixed, branch_rows)
    grad_mixed = project_back(branch_rows, out_weight).astype(jnp.bfloat16).reshape(head_shape)
    row_index = 0
    grad_q, grad_k, grad_v = attend_back(
        queries[row_index],
        keys[row_index],
        values[row_index],
        grad_mixed[row_index],
        log_rows[row_index],
        segment_ids[row_index],
        scale,
        block,
    )
    query_rows = [grad_q]
    key_rows = [grad_k]
    value_rows = [grad_v]
    grad_query = (
        rotate_back(jnp.stack(query_rows, 0), cosine, sine)
        .astype(jnp.bfloat16)
        .reshape(row_count, seq_len, local_width)
    )
    grad_key = (
        rotate_back(jnp.stack(key_rows, 0), cosine, sine)
        .astype(jnp.bfloat16)
        .reshape(row_count, seq_len, local_width)
    )
    grad_value = (
        jnp.stack(value_rows, 0).astype(jnp.bfloat16).reshape(row_count, seq_len, local_width)
    )
    query_total = weight_grad(rows_one, grad_query)
    key_total = weight_grad(rows_one, grad_key)
    value_total = weight_grad(rows_one, grad_value)
    grad_terms = (
        project_back(grad_query, query_weight)
        + project_back(grad_key, key_weight)
        + project_back(grad_value, value_weight)
    )
    grad_one = lax.psum_scatter(grad_terms, "mp", scatter_dimension=1, tiled=True)
    input_part, attn_gain_part = norm_back(grad_one, normed_one, inverse_one, attn_gain)
    input_grad = grad_resid + input_part
    attn_gain_part, mlp_gain_part = lax.psum((attn_gain_part, mlp_gain_part), "mp")
    (
        query_total,
        key_total,
        value_total,
        out_total,
        attn_gain_part,
        mlp_gain_part,
        up_total,
        down_total,
    ) = lax.psum(
        (
            query_total,
            key_total,
            value_total,
            out_total,
            attn_gain_part,
            mlp_gain_part,
            up_total,
            down_total,
        ),
        "dp",
    )
    return (
        result,
        input_grad,
        attn_gain_part,
        query_total,
        key_total,
        value_total,
        out_total,
        mlp_gain_part,
        up_total,
        down_total,
    )


def on_device_kernels(
    hidden_in, segment_ids, attn_gain, query_weight, key_weight, value_weight, out_weight, mlp_gain, up_weight, down_weight, out_cotangent
):
    sums = layer(
        hidden_in[0], out_cotangent[0], segment_ids, attn_gain, mlp_gain,
        query_weight.T, key_weight.T, value_weight.T, out_weight, up_weight, down_weight,
    )
    result, input_grad, one, two, down, up, out, query, key, value = finish(*sums, up_weight.shape[1], out_weight.shape[0])
    return (result[None], input_grad[None], one, query.T, key.T, value.T, out, two, up, down)


def solution(mesh):
    return jax.shard_map(
        on_device_kernels if mesh.shape["dp"] == 8 else on_device,
        mesh=mesh,
        in_specs=(
            P("dp", "mp", None),
            P("dp", None),
            P(),
            P(None, "mp"),
            P(None, "mp"),
            P(None, "mp"),
            P("mp", None),
            P(),
            P(None, "mp"),
            P("mp", None),
            P("dp", "mp", None),
        ),
        out_specs=(
            P("dp", "mp", None),
            P("dp", "mp", None),
            P(),
            P(None, "mp"),
            P(None, "mp"),
            P(None, "mp"),
            P("mp", None),
            P(),
            P(None, "mp"),
            P("mp", None),
        ),
        check_vma=False,
    )
```

```python
import math

import jax
import jax.numpy as jnp
from jax import lax
from jax.experimental import pallas as pl
from jax.experimental.pallas import tpu as pltpu
from jax.sharding import PartitionSpec as P

HEAD = 80


EPS = 1e-06
MASKED = -1e30
GELU_C = math.sqrt(2.0 / math.pi)
GELU_K = 0.044715


def normalize(values, gain):
    inverse = lax.rsqrt(jnp.mean(values * values, -1, keepdims=True) + EPS)
    normed = values * inverse
    return (normed * gain, normed, inverse)


def norm_back(upstream, normed, inverse, gain):
    scaled = upstream * gain
    inner = jnp.mean(scaled * normed, -1, keepdims=True)
    return (inverse * (scaled - normed * inner), jnp.sum(upstream * normed, axis=(0, 1)))


def gelu_slope(values):
    tangent = jnp.tanh(GELU_C * (values + GELU_K * values * values * values))
    return 0.5 * (1.0 + tangent) + 0.5 * values * (1.0 - tangent * tangent) * GELU_C * (
        1.0 + 3.0 * GELU_K * values * values
    )


def project(left, weight):
    return jnp.einsum("rsd,de->rse", left, weight, preferred_element_type=jnp.float32)


def project_back(left, weight):
    return jnp.einsum("rse,de->rsd", left, weight, preferred_element_type=jnp.float32)


def weight_grad(left, right):
    return jnp.einsum("rsd,rse->de", left, right, preferred_element_type=jnp.float32)


def rotary_tables(segments, head_size):
    seq_len = segments.shape[1]
    places = jnp.arange(seq_len, dtype=jnp.int32)
    starts_here = jnp.concatenate(
        [jnp.ones((segments.shape[0], 1), bool), segments[:, 1:] != segments[:, :-1]], axis=1
    )
    first = lax.cummax(jnp.where(starts_here, places[None, :], 0), axis=1)
    position = (places[None, :] - first).astype(jnp.float32)
    half = head_size // 2
    freqs = jnp.exp(jnp.arange(half, dtype=jnp.float32) * (-2.0 * math.log(10000.0) / head_size))
    angles = position[:, :, None] * freqs[None, None, :]
    return (jnp.cos(angles)[:, :, None, :], jnp.sin(angles)[:, :, None, :])


def rotate(values, cosine, sine):
    half = values.shape[-1] // 2
    first, second = (values[..., :half], values[..., half:])
    return jnp.concatenate([first * cosine - second * sine, second * cosine + first * sine], -1)


def rotate_back(grads, cosine, sine):
    half = grads.shape[-1] // 2
    first, second = (grads[..., :half], grads[..., half:])
    return jnp.concatenate([first * cosine + second * sine, second * cosine - first * sine], -1)


def allowed_block(segments_row, start, size):
    seq_len = segments_row.shape[0]
    query_pos = start + jnp.arange(size, dtype=jnp.int32)
    key_pos = jnp.arange(seq_len, dtype=jnp.int32)
    query_seg = segments_row[start : start + size]
    return (query_pos[:, None] >= key_pos[None, :]) & (query_seg[:, None] == segments_row[None, :])


def block_scores(query_block, keys, allowed, scale):
    scores = (
        jnp.einsum("qhd,khd->hqk", query_block, keys, preferred_element_type=jnp.float32) * scale
    )
    return jnp.where(allowed[None], scores, MASKED)


def attend_forward(queries, keys, values, segments_row, scale, block):
    outputs = []
    sums = []
    for start in range(0, queries.shape[0], block):
        allowed = allowed_block(segments_row, start, block)
        scores = block_scores(queries[start : start + block], keys, allowed, scale)
        top = jnp.max(scores, -1, keepdims=True)
        expo = jnp.exp(scores - top)
        total = jnp.sum(expo, -1, keepdims=True)
        probs = (expo / total).astype(jnp.bfloat16)
        outputs.append(
            jnp.einsum("hqk,khd->qhd", probs, values, preferred_element_type=jnp.float32)
        )
        sums.append(top + jnp.log(total))
    return (jnp.concatenate(outputs, 0), jnp.concatenate(sums, 1))


def attend_back(queries, keys, values, grad_mixed, log_sums, segments_row, scale, block):
    key_total = jnp.zeros(keys.shape, jnp.float32)
    value_total = jnp.zeros(values.shape, jnp.float32)
    query_parts = []
    for start in range(0, queries.shape[0], block):
        allowed = allowed_block(segments_row, start, block)
        query_block = queries[start : start + block]
        scores = block_scores(query_block, keys, allowed, scale)
        probs = jnp.exp(scores - log_sums[:, start : start + block])
        grad_block = grad_mixed[start : start + block]
        grad_probs = jnp.einsum(
            "qhd,khd->hqk", grad_block, values, preferred_element_type=jnp.float32
        )
        inner = jnp.sum(probs * grad_probs, -1, keepdims=True)
        grad_scores = (probs * (grad_probs - inner)).astype(jnp.bfloat16)
        query_parts.append(
            jnp.einsum("hqk,khd->qhd", grad_scores, keys, preferred_element_type=jnp.float32)
            * scale
        )
        key_total = (
            key_total
            + jnp.einsum(
                "hqk,qhd->khd", grad_scores, query_block, preferred_element_type=jnp.float32
            )
            * scale
        )
        value_total = value_total + jnp.einsum(
            "hqk,qhd->khd",
            probs.astype(jnp.bfloat16),
            grad_block,
            preferred_element_type=jnp.float32,
        )
    return (jnp.concatenate(query_parts, 0), key_total, value_total)


MESH = pl.DeviceIdType.MESH
CHUNK = 64
SLOTS = 6
STAGES = 6
(R1Z, R2Z, R3Z, FZM, FZA, FZB, R1Y, R2Y, R3Y, FYI, FYY) = range(11)
(S0Z, S0Y, S1Z, S1Y, S2Z, S2Y, S3ZM, S3ZE, S3YE, S3YY, S4Z, S4Y) = range(12)


def add_rows(total_ref, row, count, *others):
    value = total_ref[pl.ds(row, count), :].astype(jnp.float32)
    for other in others:
        value = value + other[...].astype(jnp.float32)
    total_ref[pl.ds(row, count), :] = value.astype(jnp.bfloat16)


class Reducer:
    def __init__(self, rows, bufs, send_sem, recv_sem, pairs):
        self.rows, self.bufs, self.send_sem, self.recv_sem, self.pairs = rows, bufs, send_sem, recv_sem, pairs
        dp = lax.axis_index("dp")
        self.place, self.side = lax.div(dp, 2), lax.rem(dp, 2)
        self.inner = (self.place == 1) | (self.place == 2)
        self.end = jnp.logical_not(self.inner)
        self.mate = 2 * (self.place + 1 - 2 * lax.rem(self.place, 2)) + self.side
        self.across = 2 * (3 - self.place) + self.side
        self.twin = 2 * self.place + 1 - self.side
        self.half_z = lax.div(self.place, 2)
        self.half_y = self.side

    def copy(self, source, target, send, recv, slot, device):
        return pltpu.make_async_remote_copy(
            src_ref=source,
            dst_ref=target,
            send_sem=self.send_sem.at[send, slot],
            recv_sem=self.recv_sem.at[recv, slot],
            device_id={"dp": device},
            device_id_type=MESH,
        )

    def whole_z(self, pair):
        return pl.multiple_of(pair * (2 * CHUNK), CHUNK)

    def at_z(self, pair, half):
        return pl.multiple_of(pair * (2 * CHUNK) + half * (CHUNK // 2), CHUNK // 2)

    def at_y(self, pair, half):
        return pl.multiple_of(pair * (2 * CHUNK) + CHUNK + half * (CHUNK // 2), CHUNK // 2)

    def moves(self, pair):
        slot = lax.rem(pair, SLOTS)
        rows, (one_z, two_z, three_z, one_y, two_y, three_y) = self.rows, self.bufs
        half = CHUNK // 2
        mine_z, mine_y = self.half_z, self.half_y
        own_z = rows.at[pl.ds(self.at_z(pair, mine_z), half), :]
        rest_z = rows.at[pl.ds(self.at_z(pair, 1 - mine_z), half), :]
        own_y = rows.at[pl.ds(self.at_y(pair, mine_y), half), :]
        rest_y = rows.at[pl.ds(self.at_y(pair, 1 - mine_y), half), :]
        all_z = rows.at[pl.ds(self.whole_z(pair), CHUNK), :]
        return dict(
            s0z=lambda: self.copy(all_z, one_z.at[slot], S0Z, R1Z, slot, self.mate),
            s0y=lambda: self.copy(rest_y, one_y.at[slot], S0Y, R1Y, slot, self.twin),
            s1z=lambda: self.copy(rest_z, two_z.at[slot], S1Z, R2Z, slot, self.across),
            s1y=lambda: self.copy(two_y.at[slot], two_y.at[slot], S1Y, R2Y, slot, self.mate),
            s2z=lambda: self.copy(own_z, three_z.at[slot], S2Z, R3Z, slot, self.twin),
            s2y=lambda: self.copy(own_y, three_y.at[slot], S2Y, R3Y, slot, self.across),
            s3zm=lambda: self.copy(own_z, own_z, S3ZM, FZM, slot, self.across),
            s3ze=lambda: self.copy(own_z, own_z, S3ZE, FZA, slot, self.mate),
            s3ye=lambda: self.copy(own_y, own_y, S3YE, FYI, slot, self.mate),
            s3yy=lambda: self.copy(own_y, own_y, S3YY, FYY, slot, self.twin),
            s4z=lambda: self.copy(rest_z, rest_z, S4Z, FZB, slot, self.mate),
            s4y=lambda: self.copy(own_y, own_y, S4Y, FYY, slot, self.twin),
        )

    def when(self, slot_index, stage, role, body):
        pair = slot_index - stage
        live = (pair >= 0) & (pair < self.pairs)
        if role is not None:
            live = live & role

        @pl.when(live)
        def _():
            body(pair)

    def slot(self, index):
        half = CHUNK // 2
        one_z, two_z, three_z, one_y, two_y, three_y = self.bufs

        def last(pair):
            m = self.moves(pair)
            @pl.when(self.end)
            def _():
                m["s3ze"]().wait_recv()
                m["s4z"]().wait_recv()
                m["s1y"]().wait_send()
                m["s4y"]().wait_send()
                m["s4y"]().wait_recv()

            @pl.when(self.inner)
            def _():
                m["s3zm"]().wait_send()
                m["s3ze"]().wait_send()
                m["s3ye"]().wait_send()
                m["s3yy"]().wait_send()
                m["s4z"]().wait_send()
                m["s3yy"]().wait_recv()

        def fourth_inner(pair):
            m = self.moves(pair)
            m["s3zm"]().wait_recv()
            m["s4z"]().start()

        def fourth_end(pair):
            m = self.moves(pair)
            m["s3ye"]().wait_recv()
            m["s4y"]().start()

        def third(pair):
            m = self.moves(pair)
            slot = lax.rem(pair, SLOTS)
            m["s2z"]().wait()
            m["s2y"]().wait()
            add_rows(self.rows, self.at_z(pair, self.half_z), half, three_z.at[slot])
            add_rows(self.rows, self.at_y(pair, self.half_y), half, three_y.at[slot])
            m["s3ze"]().start()
            m["s3zm"]().start()
            m["s3ye"]().start()
            m["s3yy"]().start()

        def second(pair):
            m = self.moves(pair)
            slot = lax.rem(pair, SLOTS)
            m["s1z"]().wait()
            m["s1y"]().wait_recv()
            m["s0y"]().wait_send()
            add_rows(
                self.rows, self.at_z(pair, self.half_z), half,
                one_z.at[slot, pl.ds(pl.multiple_of(self.half_z * half, half), half), :], two_z.at[slot],
            )
            add_rows(self.rows, self.at_y(pair, self.half_y), half, one_y.at[slot], two_y.at[slot])
            m["s2z"]().start()
            m["s2y"]().start()

        def first_inner(pair):
            m = self.moves(pair)
            slot = lax.rem(pair, SLOTS)
            m["s0z"]().wait_recv()
            m["s0y"]().wait_recv()
            other = 1 - self.half_z
            add_rows(
                self.rows, self.at_z(pair, other), half,
                one_z.at[slot, pl.ds(pl.multiple_of(other * half, half), half), :],
            )
            m["s1z"]().start()

        def first_end(pair):
            m = self.moves(pair)
            slot = lax.rem(pair, SLOTS)
            m["s0y"]().wait()
            m["s0z"]().wait_send()
            mine = self.rows[pl.ds(self.at_y(pair, self.half_y), half), :].astype(jnp.float32)
            two_y[slot] = (mine + one_y[slot].astype(jnp.float32)).astype(jnp.bfloat16)
            m["s1y"]().start()

        def start(pair):
            m = self.moves(pair)
            m["s0y"]().start()

            @pl.when(self.end)
            def _():
                m["s0z"]().start()

        self.when(index, 0, None, start)
        self.when(index, 1, self.end, first_end)
        self.when(index, 1, self.inner, first_inner)
        self.when(index, 2, self.inner, second)
        self.when(index, 3, self.inner, third)
        self.when(index, 4, self.inner, fourth_inner)
        self.when(index, 4, self.end, fourth_end)
        self.when(index, 5, None, last)

    def greet(self, barrier):
        for device in (self.mate, self.across, self.twin):
            pl.semaphore_signal(barrier, inc=1, device_id={"dp": device}, device_id_type=MESH)
        return 3


def reducer_scratch(width):
    half = CHUNK // 2
    return [
        pltpu.VMEM((SLOTS, CHUNK, width), jnp.bfloat16),
        pltpu.VMEM((SLOTS, half, width), jnp.bfloat16),
        pltpu.VMEM((SLOTS, half, width), jnp.bfloat16),
        pltpu.VMEM((SLOTS, half, width), jnp.bfloat16),
        pltpu.VMEM((SLOTS, half, width), jnp.bfloat16),
        pltpu.VMEM((SLOTS, half, width), jnp.bfloat16),
        pltpu.SemaphoreType.DMA((12, SLOTS)),
        pltpu.SemaphoreType.DMA((11, SLOTS)),
    ]


HEAD_PAD = 128
BLOCK_SEQ = 256
SPAN = 512


def pad_matrix(local, padded):
    shape = (padded, local)
    feature = lax.broadcasted_iota(jnp.int32, shape, 1)
    lane = lax.broadcasted_iota(jnp.int32, shape, 0)
    head = jnp.zeros(shape, jnp.int32)
    for h in range(1, local // HEAD):
        head = head + (feature >= h * HEAD).astype(jnp.int32)
    within = feature - head * HEAD
    target = head * HEAD_PAD + within + jnp.where(within >= HEAD // 2, HEAD_PAD // 2 - HEAD // 2, 0)
    return jnp.where(lane == target, 1.0, 0.0).astype(jnp.bfloat16)


def dot(a, b):
    return jnp.dot(a, b, preferred_element_type=jnp.float32)


def dot_nt(a, b):
    return lax.dot_general(a, b, (((1,), (1,)), ((), ())), preferred_element_type=jnp.float32)


def dot_tn(a, b):
    return lax.dot_general(a, b, (((0,), (0,)), ((), ())), preferred_element_type=jnp.float32)


def segment_columns(seg):
    lines = jnp.broadcast_to(seg.astype(jnp.float32), (16, seg.shape[1])).astype(jnp.bfloat16)
    pick = (lax.broadcasted_iota(jnp.int32, (16, 128), 0) == 0).astype(jnp.float32).astype(jnp.bfloat16)
    return dot_tn(lines, pick)


def rotary_into(seg, cos_ref, sin_ref):
    seq = seg.shape[1]
    ids = segment_columns(seg)
    first = jnp.zeros((seq, 128), jnp.float32)
    row = seg.astype(jnp.float32)
    for s in range(1, 16):
        before = jnp.sum(jnp.where(row < s, 1.0, 0.0), axis=1, keepdims=True)
        first = jnp.where(ids == s, before, first)
    position = lax.broadcasted_iota(jnp.int32, (seq, 128), 0).astype(jnp.float32) - first
    lane = lax.broadcasted_iota(jnp.int32, (1, 128), 1)
    upper = lane >= HEAD_PAD // 2
    index = jnp.where(upper, lane - HEAD_PAD // 2, lane)
    freqs = jnp.exp(index.astype(jnp.float32) * (-2.0 * math.log(10000.0) / HEAD))
    freqs = jnp.where(index < HEAD // 2, freqs, 0.0)
    angles = position * freqs
    cos_ref[...] = jnp.cos(angles)
    sin_ref[...] = jnp.where(upper, jnp.sin(angles), -jnp.sin(angles))


class Ring4:
    def __init__(self):
        mp = lax.axis_index("mp")
        chip, core = lax.div(mp, 2), lax.rem(mp, 2)
        self.me = mp
        self.core = 2 * chip + 1 - core
        self.chip = 2 * (1 - chip) + core
        self.far = 2 * (1 - chip) + 1 - core


def block_rows(index):
    return pl.ds(pl.multiple_of(index * BLOCK_SEQ, BLOCK_SEQ), BLOCK_SEQ)


class Gather:
    def __init__(self, ring, rows, sems, parts=1):
        self.parts = parts
        size = BLOCK_SEQ // parts

        def copy(block, device, which, part):
            at = pl.ds(pl.multiple_of(block * BLOCK_SEQ + part * size, size), size)
            return pltpu.make_async_remote_copy(
                src_ref=rows.at[at, :],
                dst_ref=rows.at[at, :],
                send_sem=sems.at[0, which * parts + part],
                recv_sem=sems.at[1, which * parts + part],
                device_id={"mp": device},
                device_id_type=MESH,
            )

        self.near = lambda part=0: copy(ring.me, ring.core, 0, part)
        self.across = lambda part=0: copy(ring.me, ring.chip, 1, part)
        self.onward = lambda part=0: copy(ring.chip, ring.core, 2, part)

    def start(self, part=0):
        self.across(part).start()
        self.near(part).start()

    def forward(self):
        for part in range(self.parts):
            self.across(part).wait_recv()
            self.onward(part).start()

    def near_in(self):
        for part in range(self.parts):
            self.near(part).wait_recv()

    def onward_in(self):
        for part in range(self.parts):
            self.onward(part).wait_recv()

    def sent(self):
        for part in range(self.parts):
            self.near(part).wait_send()
            self.across(part).wait_send()
            self.onward(part).wait_send()


class Scatter:
    def __init__(self, ring, send_core, recv_core, send_chip, recv_chip, sems, parts=1):
        self.parts = parts
        size = BLOCK_SEQ // parts

        def copy(source, target, device, which, part):
            at = pl.ds(part * size, size)
            return pltpu.make_async_remote_copy(
                src_ref=source.at[at, :],
                dst_ref=target.at[at, :],
                send_sem=sems.at[0, which * parts + part],
                recv_sem=sems.at[1, which * parts + part],
                device_id={"mp": device},
                device_id_type=MESH,
            )

        self.far = lambda part=0: copy(send_core.at[0], recv_core.at[0], ring.core, 0, part)
        self.core = lambda part=0: copy(send_core.at[1], recv_core.at[1], ring.core, 1, part)
        self.chip = lambda part=0: copy(send_chip, recv_chip, ring.chip, 2, part)


def greet_mp(ring, barrier):
    for device in (ring.core, ring.chip):
        pl.semaphore_signal(barrier, inc=1, device_id={"mp": device}, device_id_type=MESH)
    return 2


def norm_rows(values):
    inverse = lax.rsqrt(jnp.mean(values * values, -1, keepdims=True) + EPS)
    return values * inverse, inverse


def qkv_block(rows, weights, cos_ref, sin_ref, out, block):
    at = block_rows(block)
    turned = 2 * (weights.shape[0] // 3) // 256
    tiles = weights.shape[0] // 256

    def one(n, turn):
        cols = pl.ds(pl.multiple_of(n * 256, 256), 256)
        value = dot_nt(rows[at, :], weights[cols, :])
        if turn:
            cosine, sine = cos_ref[at, :], sin_ref[at, :]
            halves = [value[:, j * 128 : j * 128 + 128] for j in range(2)]
            value = jnp.concatenate([h * cosine + pltpu.roll(h, 64, 1) * sine for h in halves], axis=1)
        out[at, cols] = value.astype(jnp.bfloat16)

    @pl.loop(0, turned)
    def _(n):
        one(n, True)

    @pl.loop(turned, tiles)
    def _(n):
        one(n, False)


def masks_into(seg, ids_ref, bias_ref):
    seq = seg.shape[1]
    for i in range(seq // BLOCK_SEQ):
        low = max(0, i * BLOCK_SEQ - SPAN)
        high = (i + 1) * BLOCK_SEQ
        shape = (BLOCK_SEQ, high - low)
        query = i * BLOCK_SEQ + lax.broadcasted_iota(jnp.int32, shape, 0)
        key = low + lax.broadcasted_iota(jnp.int32, shape, 1)
        ids = ids_ref[pl.ds(i * BLOCK_SEQ, BLOCK_SEQ), :][:, :1]
        same = ids == seg[:, low:high].astype(jnp.float32)
        bias_ref[pl.ds(i * BLOCK_SEQ, BLOCK_SEQ), pl.ds(0, high - low)] = jnp.where((query >= key) & same, 0.0, MASKED).astype(bias_ref.dtype)


def attend(qkv, out, bias_ref, heads, scale, blocks):
    width = heads * HEAD_PAD

    @pl.loop(0, heads)
    def _(h):
        lanes = [pl.ds(pl.multiple_of(part * width + h * HEAD_PAD, HEAD_PAD), HEAD_PAD) for part in range(3)]
        for i in blocks:
            low, high = max(0, i * BLOCK_SEQ - SPAN), (i + 1) * BLOCK_SEQ
            rows, keys = pl.ds(i * BLOCK_SEQ, BLOCK_SEQ), pl.ds(low, high - low)
            scores = dot_nt(qkv[rows, lanes[0]], qkv[keys, lanes[1]]) + bias_ref[rows, pl.ds(0, high - low)]
            top = jnp.max(scores, -1, keepdims=True)
            expo = jnp.exp((scores - top) * scale)
            probs = expo * (1.0 / jnp.sum(expo, -1, keepdims=True))
            out[rows, lanes[0]] = dot(probs.astype(jnp.bfloat16), qkv[keys, lanes[2]]).astype(jnp.bfloat16)


def layer_kernel(
    x, g, seg, gain_one, gain_two, wq, wk, wv, wo, wup, wdown,
    result_o, input_o, gains_o, sums_o,
    rows, b0, b1, b2, b3, b4, b5, send_sem, recv_sem, save_sem,
    w_up, w_down, w_qkv, w_out, rows_one, rows_g, rows_two, hidden, grad_up, branch, qkv, mixed, grad_mixed,
    cos_ref, sin_ref, bias_ref, resid, term_ref, key_sum, value_sum,
    send_core, recv_core, send_chip, recv_chip, gain_acc, gain_recv,
    load_sem, one_sem, g_sem, two_sem, branch_sem, rs0_sem, rs_sem, rs2_sem, rs3_sem, gain_sem, free_sem, ready_sem,
):
    bf, f32 = jnp.bfloat16, jnp.float32
    ring = Ring4()
    seq, width = rows_two.shape
    units = w_up.shape[1]
    padded = w_out.shape[0]
    heads = padded // HEAD_PAD
    local = heads * HEAD
    pairs = rows.shape[0] // (2 * CHUNK)
    scale = 1.0 / math.sqrt(HEAD)
    half = BLOCK_SEQ // 2
    chip = lax.div(ring.me, 2)
    red = Reducer(rows, (b0, b1, b2, b3, b4, b5), send_sem, recv_sem, pairs)
    barrier = pltpu.get_barrier_semaphore()
    count = greet_mp(ring, barrier) + red.greet(barrier)
    places = [(w, rows.at[pl.ds(i * local, local), :]) for i, w in enumerate((wq, wk, wv, wo))]
    places += [(g, rows_g.at[block_rows(ring.me), :]), (wup, w_up), (wdown, w_down)]
    loads = [pltpu.make_async_copy(source, target, load_sem.at[i]) for i, (source, target) in enumerate(places)]
    for load in loads[:5]:
        load.start()
    normed, _ = norm_rows(x[...].astype(f32))
    rows_one[block_rows(ring.me), :] = (normed * gain_one[...]).astype(bf)
    one, all_g = Gather(ring, rows_one, one_sem, 2), Gather(ring, rows_g, g_sem)
    two, all_branch = Gather(ring, rows_two, two_sem, 2), Gather(ring, branch, branch_sem)
    ahead = Scatter(ring, send_core, recv_core, send_chip, recv_chip, rs0_sem, 2)
    first = Scatter(ring, send_core, recv_core, send_chip, recv_chip, rs_sem)
    second = Scatter(ring, send_core, recv_core, send_chip, recv_chip, rs2_sem)
    third = Scatter(ring, send_core, recv_core, send_chip, recv_chip, rs3_sem)
    pl.semaphore_wait(barrier, count)
    one.start(0)
    one.start(1)
    for load in loads[5:]:
        load.start()

    spread = pad_matrix(local, padded)
    for i in range(3):
        loads[i].wait()
        w_qkv[pl.ds(i * padded, padded), :] = dot(spread, rows[pl.ds(i * local, local), :]).astype(bf)
    loads[3].wait()
    w_out[...] = dot(spread, rows[pl.ds(3 * local, local), :]).astype(bf)
    rotary_into(seg[...], cos_ref, sin_ref)
    qkv_block(rows_one, w_qkv, cos_ref, sin_ref, qkv, ring.me)
    one.near_in()
    qkv_block(rows_one, w_qkv, cos_ref, sin_ref, qkv, ring.core)
    key_sum[...] = segment_columns(seg[...])
    masks_into(seg[...], key_sum, bias_ref)
    loads[4].wait()
    one.forward()
    one.across(0).wait_send()
    one.across(1).wait_send()
    all_g.start()
    qkv_block(rows_one, w_qkv, cos_ref, sin_ref, qkv, ring.chip)
    one.onward_in()
    qkv_block(rows_one, w_qkv, cos_ref, sin_ref, qkv, ring.far)

    early, late = (0, 1), (2, 3)

    @pl.when(chip == 0)
    def _():
        attend(qkv, mixed, bias_ref, heads, scale, late)

    @pl.when(chip == 1)
    def _():
        attend(qkv, mixed, bias_ref, heads, scale, early)

    def term(block, part):
        at = pl.ds(pl.multiple_of(block * BLOCK_SEQ + part * half, half), half)
        return dot(mixed[at, :], w_out[...])

    parts = [pl.ds(p * half, half) for p in range(2)]
    for p in range(2):
        send_core[0, parts[p], :] = term(ring.far, p).astype(bf)
        ahead.far(p).start()
    for p in range(2):
        value = term(ring.chip, p)
        ahead.far(p).wait_recv()
        send_chip[parts[p], :] = (value + recv_core[0, parts[p], :].astype(f32)).astype(bf)
        ahead.chip(p).start()

    @pl.when(chip == 0)
    def _():
        attend(qkv, mixed, bias_ref, heads, scale, early)

    @pl.when(chip == 1)
    def _():
        attend(qkv, mixed, bias_ref, heads, scale, late)

    for p in range(2):
        send_core[1, parts[p], :] = term(ring.core, p).astype(bf)
        ahead.core(p).start()
    all_g.forward()
    for p in range(2):
        resid[parts[p], :] = x[parts[p], :].astype(f32) + term(ring.me, p)
    for p in range(2):
        ahead.core(p).wait_recv()
        ahead.chip(p).wait_recv()
        value = resid[parts[p], :] + recv_core[1, parts[p], :].astype(f32) + recv_chip[parts[p], :].astype(f32)
        resid[parts[p], :] = value
        normed, _ = norm_rows(value)
        at = pl.ds(pl.multiple_of(ring.me * BLOCK_SEQ + p * half, half), half)
        rows_two[at, :] = (normed * gain_two[...]).astype(bf)
        two.start(p)
    for p in range(2):
        ahead.far(p).wait_send()
        ahead.core(p).wait_send()
        ahead.chip(p).wait_send()

    base = 2 * units

    def put(pair):
        at = pl.ds(pl.multiple_of(pair * 2 * CHUNK, 2 * CHUNK), 2 * CHUNK)
        return pltpu.make_async_copy(rows.at[at, :], sums_o.at[at, :], save_sem.at[lax.rem(pair, 4)])

    def slot(index):
        red.slot(index)
        pair = index - (STAGES - 1)

        @pl.when(pair >= 4)
        def _():
            put(pair - 4).wait()

        @pl.when(pair >= 0)
        def _():
            put(pair).start()

    def tile(n):
        return pl.ds(pl.multiple_of(n * 256, 256), 256)

    def up_tile(block, n):
        u = dot(rows_two[block_rows(block), :], w_up[:, tile(n)])
        tangent = jnp.tanh(GELU_C * (u + GELU_K * u * u * u))
        hidden[block_rows(block), tile(n)] = (0.5 * u * (1.0 + tangent)).astype(bf)

    def up_block(block):
        @pl.loop(0, units // 256)
        def _(n):
            up_tile(block, n)

    loads[5].wait()
    up_block(ring.me)
    two.near_in()
    up_block(ring.core)
    all_g.near_in()
    all_g.onward_in()
    two.forward()
    two.onward_in()

    loads[6].wait()

    def order(k):
        there = k < 2
        core = lax.rem(ring.me, 2)
        flip = 1 - lax.rem(k, 2)
        to_chip = jnp.where(there, 1 - chip, chip)
        to_core = jnp.where(flip == 1, 1 - core, core)
        return 2 * to_chip + to_core

    def hand_on(k, scatter, start):
        @pl.when(k == 0)
        def _():
            send_core[0] = term_ref[...].astype(bf)
            scatter.far().start()

        @pl.when(k == 1)
        def _():
            scatter.far().wait_recv()
            send_chip[...] = (term_ref[...] + recv_core[0].astype(f32)).astype(bf)
            scatter.chip().start()

        @pl.when(k == 2)
        def _():
            send_core[1] = term_ref[...].astype(bf)
            scatter.core().start()

        @pl.when(k == 3)
        def _():
            scatter.core().wait_recv()
            term_ref[...] = term_ref[...] + recv_core[1].astype(f32)

    def settle(scatter):
        for copy in (scatter.far(), scatter.core()):
            copy.wait_send()
        scatter.chip().wait()
        return term_ref[...] + recv_chip[...].astype(f32)

    def grad_tile(at, n):
        u = dot(rows_two[at, :], w_up[:, tile(n)])
        upstream = dot_nt(rows_g[at, :], w_down[tile(n), :])
        tangent = jnp.tanh(GELU_C * (u + GELU_K * u * u * u))
        slope = 0.5 * (1.0 + tangent) + 0.5 * u * (1.0 - tangent * tangent) * GELU_C * (1.0 + 3.0 * GELU_K * u * u)
        grad_up[at, tile(n)] = (upstream * slope).astype(bf)

    @pl.loop(0, units // 256)
    def _(n):
        for block in (ring.chip, ring.far):
            up_tile(block, n)
        rows[tile(n), :] = dot_tn(hidden[:, tile(n)], rows_g[...]).astype(bf)
        slot(n)

        @pl.loop(0, 3)
        def _(k):
            grad_tile(block_rows(order(k)), n)

    @pl.loop(0, 4)
    def _(k):
        @pl.loop(0, 2)
        def _(j):
            @pl.when(2 * k + j < units // 256)
            def _():
                grad_tile(block_rows(order(3)), 2 * k + j)

        at = block_rows(order(k))

        @pl.loop(0, width // 256)
        def _(n):
            term_ref[:, tile(n)] = dot_nt(grad_up[at, :], w_up[tile(n), :])

        hand_on(k, first, None)
        slot(5 + k)

    def up_rows(i):
        rows[pl.ds(pl.multiple_of(units + i * 256, 256), 256), :] = dot_tn(rows_two[:, tile(i)], grad_up[...]).astype(bf)

    up_rows(0)
    slot(9)
    grad_two = settle(first)
    normed, inverse = norm_rows(resid[...])
    scaled = grad_two * gain_two[...]
    part = inverse * (scaled - normed * jnp.mean(scaled * normed, -1, keepdims=True))
    mlp_part = jnp.sum(grad_two * normed, axis=0, keepdims=True)
    gain_acc[0] = jnp.zeros(gain_acc.shape[1:], f32)
    gain_acc[0, 1:2, :] = mlp_part
    mine = rows_g[block_rows(ring.me), :].astype(f32) + part
    input_o[...] = mine
    branch[block_rows(ring.me), :] = mine.astype(bf)
    all_branch.across().start()
    all_branch.near().start()
    for device in (ring.core, ring.chip):
        pl.semaphore_signal(ready_sem, inc=1, device_id={"mp": device}, device_id_type=MESH)

    def head_rows(left, lane, right, row):
        value = dot_tn(left[:, lane], right[...])
        halves = [value[at : at + HEAD // 2, :] for at in (0, 64, 128, 192)]
        rows[pl.ds(pl.multiple_of(row, 16), 2 * HEAD), :] = jnp.concatenate(halves, axis=0).astype(bf)

    @pl.loop(1, units // 256)
    def _(i):
        up_rows(i)

        @pl.when(i == 1)
        def _():
            pl.semaphore_wait(ready_sem, 2)

        at = block_rows(order(i - 1))

        @pl.loop(0, width // 256)
        def _(n):
            term_ref[:, tile(n)] = dot(hidden[at, :], w_down[:, tile(n)])

        hand_on(i - 1, second, None)

        @pl.when(i == 4)
        def _():
            all_branch.near().wait_recv()
            all_branch.forward()
            all_branch.onward().wait_recv()

            @pl.loop(0, heads // 2)
            def _(j):
                head_rows(mixed, tile(j), branch, base + j * 2 * HEAD)

        slot(9 + i)

    @pl.loop(0, 4)
    def _(b):
        grad_mixed[block_rows(b), :] = dot_nt(branch[block_rows(b), :], w_out[...]).astype(bf)

    @pl.loop(0, heads)
    def _(h):
        lanes = [pl.ds(pl.multiple_of(n * padded + h * HEAD_PAD, HEAD_PAD), HEAD_PAD) for n in range(3)]
        key_sum[...] = jnp.zeros_like(key_sum)
        value_sum[...] = jnp.zeros_like(value_sum)
        for i in range(seq // BLOCK_SEQ):
            low, high = max(0, i * BLOCK_SEQ - SPAN), (i + 1) * BLOCK_SEQ
            at, keys = pl.ds(i * BLOCK_SEQ, BLOCK_SEQ), pl.ds(low, high - low)
            query, upstream = qkv[at, lanes[0]], grad_mixed[at, lanes[0]]
            scores = dot_nt(query, qkv[keys, lanes[1]]) + bias_ref[at, pl.ds(0, high - low)]
            top = jnp.max(scores, -1, keepdims=True)
            expo = jnp.exp((scores - top) * scale)
            probs = expo * (1.0 / jnp.sum(expo, -1, keepdims=True))
            grad_probs = dot_nt(upstream, qkv[keys, lanes[2]])
            inner = jnp.sum(probs * grad_probs, -1, keepdims=True)
            grad_scores = (probs * (grad_probs - inner)).astype(bf)
            value_sum[keys, :] += dot_tn(probs.astype(bf), upstream)
            key_sum[keys, :] += dot_tn(grad_scores, query)
            turned = dot(grad_scores, qkv[keys, lanes[1]]) * scale
            qkv[at, lanes[0]] = (turned * cos_ref[at, :] - pltpu.roll(turned, 64, 1) * sin_ref[at, :]).astype(bf)
            if i == 1:
                slot(14 + 2 * h)
        turned = key_sum[...] * scale
        qkv[:, lanes[1]] = (turned * cos_ref[...] - pltpu.roll(turned, 64, 1) * sin_ref[...]).astype(bf)
        qkv[:, lanes[2]] = value_sum[...].astype(bf)
        slot(15 + 2 * h)

    @pl.loop(0, 3)
    def _(part):
        for j in range(heads // 2):
            lane = pl.ds(pl.multiple_of(part * padded + j * 256, 256), 256)
            head_rows(qkv, lane, rows_one, base + (part + 1) * local + j * 2 * HEAD)
        slot(22 + part)

    result_o[...] = (resid[...] + settle(second)).astype(bf)
    for device in (ring.core, ring.chip):
        pl.semaphore_signal(free_sem, inc=1, device_id={"mp": device}, device_id_type=MESH)
    pl.semaphore_wait(free_sem, 2)

    @pl.loop(0, 4)
    def _(k):
        at = block_rows(order(k))

        @pl.loop(0, width // 256)
        def _(n):
            term_ref[:, tile(n)] = dot(qkv[at, :], w_qkv[:, tile(n)])

        hand_on(k, third, None)
        slot(25 + k)

    slot(29)
    grad_one = settle(third)
    normed, inverse = norm_rows(x[...].astype(f32))
    scaled = grad_one * gain_one[...]
    input_o[...] = input_o[...] + inverse * (scaled - normed * jnp.mean(scaled * normed, -1, keepdims=True))
    gain_acc[0, 0:1, :] = jnp.sum(grad_one * normed, axis=0, keepdims=True)

    def exchange(step):
        names = ({"mp": ring.core}, {"mp": ring.chip}, {"dp": red.twin}, {"dp": red.mate}, {"dp": red.across})
        return pltpu.make_async_remote_copy(
            src_ref=gain_acc.at[step], dst_ref=gain_recv.at[step], send_sem=gain_sem.at[0, step], recv_sem=gain_sem.at[1, step],
            device_id=names[step], device_id_type=MESH,
        )

    last = pairs + STAGES - 1

    @pl.loop(30, last)
    def _(index):
        for step in range(5):

            @pl.when(index == 30 + step)
            def _():
                if step:
                    exchange(step - 1).wait_recv()
                    gain_acc[step] = gain_acc[step - 1] + gain_recv[step - 1]
                exchange(step).start()

        slot(index)

    exchange(4).wait_recv()
    gains_o[...] = gain_acc[4] + gain_recv[4]
    for pair in range(pairs - 4, pairs):
        put(pair).wait()
    for step in range(5):
        exchange(step).wait_send()
    for part in range(2):
        one.near(part).wait_send()
        one.onward(part).wait_send()
    for gather in (all_g, two, all_branch):
        gather.sent()


def layer(x, g, seg, gain_one, gain_two, wq, wk, wv, wo, wup, wdown):
    bf, f32 = jnp.bfloat16, jnp.float32
    own, width = x.shape
    units = wup.shape[1]
    seq = seg.shape[1]
    local = wo.shape[0]
    padded = local // HEAD * HEAD_PAD
    total = 2 * units + 4 * local
    vm, hbm = pl.BlockSpec(memory_space=pltpu.VMEM), pl.BlockSpec(memory_space=pl.ANY)
    sem = pltpu.SemaphoreType.DMA
    shapes = [((own, width), bf), ((own, width), f32), ((8, width), f32), ((total, width), bf)]
    tall = pltpu.VMEM((seq, width), bf)
    return pl.pallas_call(
        layer_kernel,
        out_shape=[jax.ShapeDtypeStruct(s, d) for s, d in shapes],
        in_specs=[vm, hbm, vm, vm, vm] + [hbm] * 6,
        out_specs=[vm] * 3 + [hbm],
        scratch_shapes=[pltpu.VMEM((total, width), bf)]
        + reducer_scratch(width)
        + [
            sem((4,)),
            pltpu.VMEM((width, units), bf), pltpu.VMEM((units, width), bf), pltpu.VMEM((3 * padded, width), bf), pltpu.VMEM((padded, width), bf),
            tall, tall, tall, pltpu.VMEM((seq, units), bf), pltpu.VMEM((seq, units), bf), tall,
            pltpu.VMEM((seq, 3 * padded), bf), pltpu.VMEM((seq, padded), bf), pltpu.VMEM((seq, padded), bf),
            pltpu.VMEM((seq, 128), f32), pltpu.VMEM((seq, 128), f32), pltpu.VMEM((seq, SPAN + BLOCK_SEQ), bf),
            pltpu.VMEM((own, width), f32), pltpu.VMEM((own, width), f32), pltpu.VMEM((seq, HEAD_PAD), f32), pltpu.VMEM((seq, HEAD_PAD), f32),
            pltpu.VMEM((2, own, width), bf), pltpu.VMEM((2, own, width), bf), pltpu.VMEM((own, width), bf), pltpu.VMEM((own, width), bf),
            pltpu.VMEM((5, 8, width), f32), pltpu.VMEM((5, 8, width), f32),
            sem((7,)), sem((2, 6)), sem((2, 3)), sem((2, 6)), sem((2, 3)), sem((2, 6)), sem((2, 3)), sem((2, 3)), sem((2, 3)), sem((2, 5)),
            pltpu.SemaphoreType.REGULAR, pltpu.SemaphoreType.REGULAR,
        ],
        compiler_params=pltpu.CompilerParams(collective_id=0, has_side_effects=True, vmem_limit_bytes=67043328),
    )(x, g, seg, gain_one, gain_two, wq, wk, wv, wo, wup, wdown)


def finish_kernel(result, input_grad, gains, sums, result_o, input_o, one_o, two_o, down_o, up_o, out_o, q_o, k_o, v_o, inbox, outbox, side_one, side_two, in_sem, out_sem, side_sem):
    step = out_o.shape[0]
    targets = [(down_o, i * step) for i in range(down_o.shape[0] // step)] + [(up_o, i * step) for i in range(up_o.shape[0] // step)]
    targets += [(t, 0) for t in (out_o, q_o, k_o, v_o)]
    count, depth = len(targets), inbox.shape[0]
    bring = [pltpu.make_async_copy(result, side_one, side_sem.at[0]), pltpu.make_async_copy(input_grad, side_two, side_sem.at[1])]
    take = [pltpu.make_async_copy(side_one, result_o, side_sem.at[2]), pltpu.make_async_copy(side_two, input_o, side_sem.at[3])]

    def read(i):
        return pltpu.make_async_copy(sums.at[pl.ds(i * step, step), :], inbox.at[i % depth], in_sem.at[i % depth])

    def write(i):
        target, at = targets[i]
        return pltpu.make_async_copy(outbox.at[i % depth], target.at[pl.ds(at, step), :], out_sem.at[i % depth])

    for i in range(depth):
        read(i).start()
    for side in bring:
        side.start()
    one_o[...] = gains[0, :]
    two_o[...] = gains[1, :]
    for i in range(count):
        read(i).wait()
        if i >= depth:
            write(i - depth).wait()
        outbox[i % depth] = inbox[i % depth].astype(jnp.float32)
        write(i).start()
        if i + depth < count:
            read(i + depth).start()
        if i == depth:
            for come, go in zip(bring, take):
                come.wait()
                go.start()
    for i in range(count - depth, count):
        write(i).wait()
    for side in take:
        side.wait()


def finish(result, input_grad, gains, sums, units, local):
    bf, f32 = jnp.bfloat16, jnp.float32
    own, width = result.shape
    vm, hbm = pl.BlockSpec(memory_space=pltpu.VMEM), pl.BlockSpec(memory_space=pl.ANY)
    sem = pltpu.SemaphoreType.DMA
    shapes = [((own, width), bf), ((own, width), f32), ((width,), f32), ((width,), f32), ((units, width), f32), ((width, units), f32)] + [((local, width), f32)] * 4
    return pl.pallas_call(
        finish_kernel,
        out_shape=[jax.ShapeDtypeStruct(s, d) for s, d in shapes],
        in_specs=[hbm, hbm, vm, hbm],
        out_specs=[hbm, hbm, vm, vm] + [hbm] * 6,
        scratch_shapes=[pltpu.VMEM((3, local, width), bf), pltpu.VMEM((3, local, width), f32), pltpu.VMEM((own, width), bf), pltpu.VMEM((own, width), f32), sem((3,)), sem((3,)), sem((4,))],
        compiler_params=pltpu.CompilerParams(vmem_limit_bytes=67043328),
    )(result, input_grad, gains, sums)


def on_device(
    hidden_in,
    segment_ids,
    attn_gain,
    query_weight,
    key_weight,
    value_weight,
    out_weight,
    mlp_gain,
    up_weight,
    down_weight,
    out_cotangent,
):
    row_count = segment_ids.shape[0]
    seq_len = segment_ids.shape[1]
    local_width = query_weight.shape[1]
    head_count = local_width // HEAD
    scale = 1.0 / math.sqrt(HEAD)
    block = min(512, seq_len)
    head_shape = (row_count, seq_len, head_count, HEAD)
    x_float = hidden_in.astype(jnp.float32)
    scaled_one, normed_one, inverse_one = normalize(x_float, attn_gain)
    rows_one = lax.all_gather(scaled_one.astype(jnp.bfloat16), "mp", axis=1, tiled=True)
    cosine, sine = rotary_tables(segment_ids, HEAD)
    queries = rotate(project(rows_one, query_weight).reshape(head_shape), cosine, sine).astype(
        jnp.bfloat16
    )
    keys = rotate(project(rows_one, key_weight).reshape(head_shape), cosine, sine).astype(
        jnp.bfloat16
    )
    values = project(rows_one, value_weight).reshape(head_shape).astype(jnp.bfloat16)
    row_index = 0
    mixed_one, log_one = attend_forward(
        queries[row_index], keys[row_index], values[row_index], segment_ids[row_index], scale, block
    )
    mixed_rows = [mixed_one]
    log_rows = [log_one]
    mixed = jnp.stack(mixed_rows, 0).reshape(row_count, seq_len, local_width).astype(jnp.bfloat16)
    attn_share = lax.psum_scatter(project(mixed, out_weight), "mp", scatter_dimension=1, tiled=True)
    resid = x_float + attn_share
    scaled_two, normed_two, inverse_two = normalize(resid, mlp_gain)
    rows_two = lax.all_gather(scaled_two.astype(jnp.bfloat16), "mp", axis=1, tiled=True)
    up_pre = project(rows_two, up_weight)
    hidden = jax.nn.gelu(up_pre, approximate=True).astype(jnp.bfloat16)
    mlp_share = lax.psum_scatter(
        project(hidden, down_weight).astype(jnp.bfloat16), "mp", scatter_dimension=1, tiled=True
    ).astype(jnp.float32)
    result = (resid + mlp_share).astype(jnp.bfloat16)
    grad_top = out_cotangent.astype(jnp.float32)
    grad_rows = lax.all_gather(out_cotangent, "mp", axis=1, tiled=True)
    down_total = weight_grad(hidden, grad_rows)
    grad_hidden = project_back(grad_rows, down_weight)
    grad_up_pre = (grad_hidden * gelu_slope(up_pre)).astype(jnp.bfloat16)
    up_total = weight_grad(rows_two, grad_up_pre)
    grad_two = lax.psum_scatter(
        project_back(grad_up_pre, up_weight), "mp", scatter_dimension=1, tiled=True
    )
    resid_part, mlp_gain_part = norm_back(grad_two, normed_two, inverse_two, mlp_gain)
    grad_resid = grad_top + resid_part
    branch_rows = lax.all_gather(grad_resid.astype(jnp.bfloat16), "mp", axis=1, tiled=True)
    out_total = weight_grad(mixed, branch_rows)
    grad_mixed = project_back(branch_rows, out_weight).astype(jnp.bfloat16).reshape(head_shape)
    row_index = 0
    grad_q, grad_k, grad_v = attend_back(
        queries[row_index],
        keys[row_index],
        values[row_index],
        grad_mixed[row_index],
        log_rows[row_index],
        segment_ids[row_index],
        scale,
        block,
    )
    query_rows = [grad_q]
    key_rows = [grad_k]
    value_rows = [grad_v]
    grad_query = (
        rotate_back(jnp.stack(query_rows, 0), cosine, sine)
        .astype(jnp.bfloat16)
        .reshape(row_count, seq_len, local_width)
    )
    grad_key = (
        rotate_back(jnp.stack(key_rows, 0), cosine, sine)
        .astype(jnp.bfloat16)
        .reshape(row_count, seq_len, local_width)
    )
    grad_value = (
        jnp.stack(value_rows, 0).astype(jnp.bfloat16).reshape(row_count, seq_len, local_width)
    )
    query_total = weight_grad(rows_one, grad_query)
    key_total = weight_grad(rows_one, grad_key)
    value_total = weight_grad(rows_one, grad_value)
    grad_terms = (
        project_back(grad_query, query_weight)
        + project_back(grad_key, key_weight)
        + project_back(grad_value, value_weight)
    )
    grad_one = lax.psum_scatter(grad_terms, "mp", scatter_dimension=1, tiled=True)
    input_part, attn_gain_part = norm_back(grad_one, normed_one, inverse_one, attn_gain)
    input_grad = grad_resid + input_part
    attn_gain_part, mlp_gain_part = lax.psum((attn_gain_part, mlp_gain_part), "mp")
    (
        query_total,
        key_total,
        value_total,
        out_total,
        attn_gain_part,
        mlp_gain_part,
        up_total,
        down_total,
    ) = lax.psum(
        (
            query_total,
            key_total,
            value_total,
            out_total,
            attn_gain_part,
            mlp_gain_part,
            up_total,
            down_total,
        ),
        "dp",
    )
    return (
        result,
        input_grad,
        attn_gain_part,
        query_total,
        key_total,
        value_total,
        out_total,
        mlp_gain_part,
        up_total,
        down_total,
    )


def on_device_kernels(
    hidden_in, segment_ids, attn_gain, query_weight, key_weight, value_weight, out_weight, mlp_gain, up_weight, down_weight, out_cotangent
):
    sums = layer(
        hidden_in[0], out_cotangent[0], segment_ids, attn_gain, mlp_gain,
        query_weight.T, key_weight.T, value_weight.T, out_weight, up_weight, down_weight,
    )
    result, input_grad, one, two, down, up, out, query, key, value = finish(*sums, up_weight.shape[1], out_weight.shape[0])
    return (result[None], input_grad[None], one, query.T, key.T, value.T, out, two, up, down)


def solution(mesh):
    return jax.shard_map(
        on_device_kernels if mesh.shape["dp"] == 8 else on_device,
        mesh=mesh,
        in_specs=(
            P("dp", "mp", None),
            P("dp", None),
            P(),
            P(None, "mp"),
            P(None, "mp"),
            P(None, "mp"),
            P("mp", None),
            P(),
            P(None, "mp"),
            P("mp", None),
            P("dp", "mp", None),
        ),
        out_specs=(
            P("dp", "mp", None),
            P("dp", "mp", None),
            P(),
            P(None, "mp"),
            P(None, "mp"),
            P(None, "mp"),
            P("mp", None),
            P(),
            P(None, "mp"),
            P("mp", None),
        ),
        check_vma=False,
    )
```

```python
import math

import jax
import jax.numpy as jnp
from jax import lax
from jax.experimental import pallas as pl
from jax.experimental.pallas import tpu as pltpu
from jax.sharding import PartitionSpec as P

HEAD = 80


EPS = 1e-06
MASKED = -1e30
GELU_C = math.sqrt(2.0 / math.pi)
GELU_K = 0.044715


def normalize(values, gain):
    inverse = lax.rsqrt(jnp.mean(values * values, -1, keepdims=True) + EPS)
    normed = values * inverse
    return (normed * gain, normed, inverse)


def norm_back(upstream, normed, inverse, gain):
    scaled = upstream * gain
    inner = jnp.mean(scaled * normed, -1, keepdims=True)
    return (inverse * (scaled - normed * inner), jnp.sum(upstream * normed, axis=(0, 1)))


def gelu_slope(values):
    tangent = jnp.tanh(GELU_C * (values + GELU_K * values * values * values))
    return 0.5 * (1.0 + tangent) + 0.5 * values * (1.0 - tangent * tangent) * GELU_C * (
        1.0 + 3.0 * GELU_K * values * values
    )


def project(left, weight):
    return jnp.einsum("rsd,de->rse", left, weight, preferred_element_type=jnp.float32)


def project_back(left, weight):
    return jnp.einsum("rse,de->rsd", left, weight, preferred_element_type=jnp.float32)


def weight_grad(left, right):
    return jnp.einsum("rsd,rse->de", left, right, preferred_element_type=jnp.float32)


def rotary_tables(segments, head_size):
    seq_len = segments.shape[1]
    places = jnp.arange(seq_len, dtype=jnp.int32)
    starts_here = jnp.concatenate(
        [jnp.ones((segments.shape[0], 1), bool), segments[:, 1:] != segments[:, :-1]], axis=1
    )
    first = lax.cummax(jnp.where(starts_here, places[None, :], 0), axis=1)
    position = (places[None, :] - first).astype(jnp.float32)
    half = head_size // 2
    freqs = jnp.exp(jnp.arange(half, dtype=jnp.float32) * (-2.0 * math.log(10000.0) / head_size))
    angles = position[:, :, None] * freqs[None, None, :]
    return (jnp.cos(angles)[:, :, None, :], jnp.sin(angles)[:, :, None, :])


def rotate(values, cosine, sine):
    half = values.shape[-1] // 2
    first, second = (values[..., :half], values[..., half:])
    return jnp.concatenate([first * cosine - second * sine, second * cosine + first * sine], -1)


def rotate_back(grads, cosine, sine):
    half = grads.shape[-1] // 2
    first, second = (grads[..., :half], grads[..., half:])
    return jnp.concatenate([first * cosine + second * sine, second * cosine - first * sine], -1)


def allowed_block(segments_row, start, size):
    seq_len = segments_row.shape[0]
    query_pos = start + jnp.arange(size, dtype=jnp.int32)
    key_pos = jnp.arange(seq_len, dtype=jnp.int32)
    query_seg = segments_row[start : start + size]
    return (query_pos[:, None] >= key_pos[None, :]) & (query_seg[:, None] == segments_row[None, :])


def block_scores(query_block, keys, allowed, scale):
    scores = (
        jnp.einsum("qhd,khd->hqk", query_block, keys, preferred_element_type=jnp.float32) * scale
    )
    return jnp.where(allowed[None], scores, MASKED)


def attend_forward(queries, keys, values, segments_row, scale, block):
    outputs = []
    sums = []
    for start in range(0, queries.shape[0], block):
        allowed = allowed_block(segments_row, start, block)
        scores = block_scores(queries[start : start + block], keys, allowed, scale)
        top = jnp.max(scores, -1, keepdims=True)
        expo = jnp.exp(scores - top)
        total = jnp.sum(expo, -1, keepdims=True)
        probs = (expo / total).astype(jnp.bfloat16)
        outputs.append(
            jnp.einsum("hqk,khd->qhd", probs, values, preferred_element_type=jnp.float32)
        )
        sums.append(top + jnp.log(total))
    return (jnp.concatenate(outputs, 0), jnp.concatenate(sums, 1))


def attend_back(queries, keys, values, grad_mixed, log_sums, segments_row, scale, block):
    key_total = jnp.zeros(keys.shape, jnp.float32)
    value_total = jnp.zeros(values.shape, jnp.float32)
    query_parts = []
    for start in range(0, queries.shape[0], block):
        allowed = allowed_block(segments_row, start, block)
        query_block = queries[start : start + block]
        scores = block_scores(query_block, keys, allowed, scale)
        probs = jnp.exp(scores - log_sums[:, start : start + block])
        grad_block = grad_mixed[start : start + block]
        grad_probs = jnp.einsum(
            "qhd,khd->hqk", grad_block, values, preferred_element_type=jnp.float32
        )
        inner = jnp.sum(probs * grad_probs, -1, keepdims=True)
        grad_scores = (probs * (grad_probs - inner)).astype(jnp.bfloat16)
        query_parts.append(
            jnp.einsum("hqk,khd->qhd", grad_scores, keys, preferred_element_type=jnp.float32)
            * scale
        )
        key_total = (
            key_total
            + jnp.einsum(
                "hqk,qhd->khd", grad_scores, query_block, preferred_element_type=jnp.float32
            )
            * scale
        )
        value_total = value_total + jnp.einsum(
            "hqk,qhd->khd",
            probs.astype(jnp.bfloat16),
            grad_block,
            preferred_element_type=jnp.float32,
        )
    return (jnp.concatenate(query_parts, 0), key_total, value_total)


MESH = pl.DeviceIdType.MESH
CHUNK = 64
SLOTS = 6
STAGES = 6
(R1Z, R2Z, R3Z, FZM, FZA, FZB, R1Y, R2Y, R3Y, FYI, FYY) = range(11)
(S0Z, S0Y, S1Z, S1Y, S2Z, S2Y, S3ZM, S3ZE, S3YE, S3YY, S4Z, S4Y) = range(12)


def add_rows(total_ref, row, count, *others):
    value = total_ref[pl.ds(row, count), :].astype(jnp.float32)
    for other in others:
        value = value + other[...].astype(jnp.float32)
    total_ref[pl.ds(row, count), :] = value.astype(jnp.bfloat16)


class Reducer:
    def __init__(self, rows, bufs, send_sem, recv_sem, pairs):
        self.rows, self.bufs, self.send_sem, self.recv_sem, self.pairs = rows, bufs, send_sem, recv_sem, pairs
        dp = lax.axis_index("dp")
        self.place, self.side = lax.div(dp, 2), lax.rem(dp, 2)
        self.inner = (self.place == 1) | (self.place == 2)
        self.end = jnp.logical_not(self.inner)
        self.mate = 2 * (self.place + 1 - 2 * lax.rem(self.place, 2)) + self.side
        self.across = 2 * (3 - self.place) + self.side
        self.twin = 2 * self.place + 1 - self.side
        self.half_z = lax.div(self.place, 2)
        self.half_y = self.side

    def copy(self, source, target, send, recv, slot, device):
        return pltpu.make_async_remote_copy(
            src_ref=source,
            dst_ref=target,
            send_sem=self.send_sem.at[send, slot],
            recv_sem=self.recv_sem.at[recv, slot],
            device_id={"dp": device},
            device_id_type=MESH,
        )

    def whole_z(self, pair):
        return pl.multiple_of(pair * (2 * CHUNK), CHUNK)

    def at_z(self, pair, half):
        return pl.multiple_of(pair * (2 * CHUNK) + half * (CHUNK // 2), CHUNK // 2)

    def at_y(self, pair, half):
        return pl.multiple_of(pair * (2 * CHUNK) + CHUNK + half * (CHUNK // 2), CHUNK // 2)

    def moves(self, pair):
        slot = lax.rem(pair, SLOTS)
        rows, (one_z, two_z, three_z, one_y, two_y, three_y) = self.rows, self.bufs
        half = CHUNK // 2
        mine_z, mine_y = self.half_z, self.half_y
        own_z = rows.at[pl.ds(self.at_z(pair, mine_z), half), :]
        rest_z = rows.at[pl.ds(self.at_z(pair, 1 - mine_z), half), :]
        own_y = rows.at[pl.ds(self.at_y(pair, mine_y), half), :]
        rest_y = rows.at[pl.ds(self.at_y(pair, 1 - mine_y), half), :]
        all_z = rows.at[pl.ds(self.whole_z(pair), CHUNK), :]
        return dict(
            s0z=lambda: self.copy(all_z, one_z.at[slot], S0Z, R1Z, slot, self.mate),
            s0y=lambda: self.copy(rest_y, one_y.at[slot], S0Y, R1Y, slot, self.twin),
            s1z=lambda: self.copy(rest_z, two_z.at[slot], S1Z, R2Z, slot, self.across),
            s1y=lambda: self.copy(two_y.at[slot], two_y.at[slot], S1Y, R2Y, slot, self.mate),
            s2z=lambda: self.copy(own_z, three_z.at[slot], S2Z, R3Z, slot, self.twin),
            s2y=lambda: self.copy(own_y, three_y.at[slot], S2Y, R3Y, slot, self.across),
            s3zm=lambda: self.copy(own_z, own_z, S3ZM, FZM, slot, self.across),
            s3ze=lambda: self.copy(own_z, own_z, S3ZE, FZA, slot, self.mate),
            s3ye=lambda: self.copy(own_y, own_y, S3YE, FYI, slot, self.mate),
            s3yy=lambda: self.copy(own_y, own_y, S3YY, FYY, slot, self.twin),
            s4z=lambda: self.copy(rest_z, rest_z, S4Z, FZB, slot, self.mate),
            s4y=lambda: self.copy(own_y, own_y, S4Y, FYY, slot, self.twin),
        )

    def when(self, slot_index, stage, role, body):
        pair = slot_index - stage
        live = (pair >= 0) & (pair < self.pairs)
        if role is not None:
            live = live & role

        @pl.when(live)
        def _():
            body(pair)

    def slot(self, index):
        half = CHUNK // 2
        one_z, two_z, three_z, one_y, two_y, three_y = self.bufs

        def last(pair):
            m = self.moves(pair)
            @pl.when(self.end)
            def _():
                m["s3ze"]().wait_recv()
                m["s4z"]().wait_recv()
                m["s1y"]().wait_send()
                m["s4y"]().wait_send()
                m["s4y"]().wait_recv()

            @pl.when(self.inner)
            def _():
                m["s3zm"]().wait_send()
                m["s3ze"]().wait_send()
                m["s3ye"]().wait_send()
                m["s3yy"]().wait_send()
                m["s4z"]().wait_send()
                m["s3yy"]().wait_recv()

        def fourth_inner(pair):
            m = self.moves(pair)
            m["s3zm"]().wait_recv()
            m["s4z"]().start()

        def fourth_end(pair):
            m = self.moves(pair)
            m["s3ye"]().wait_recv()
            m["s4y"]().start()

        def third(pair):
            m = self.moves(pair)
            slot = lax.rem(pair, SLOTS)
            m["s2z"]().wait()
            m["s2y"]().wait()
            add_rows(self.rows, self.at_z(pair, self.half_z), half, three_z.at[slot])
            add_rows(self.rows, self.at_y(pair, self.half_y), half, three_y.at[slot])
            m["s3ze"]().start()
            m["s3zm"]().start()
            m["s3ye"]().start()
            m["s3yy"]().start()

        def second(pair):
            m = self.moves(pair)
            slot = lax.rem(pair, SLOTS)
            m["s1z"]().wait()
            m["s1y"]().wait_recv()
            m["s0y"]().wait_send()
            add_rows(
                self.rows, self.at_z(pair, self.half_z), half,
                one_z.at[slot, pl.ds(pl.multiple_of(self.half_z * half, half), half), :], two_z.at[slot],
            )
            add_rows(self.rows, self.at_y(pair, self.half_y), half, one_y.at[slot], two_y.at[slot])
            m["s2z"]().start()
            m["s2y"]().start()

        def first_inner(pair):
            m = self.moves(pair)
            slot = lax.rem(pair, SLOTS)
            m["s0z"]().wait_recv()
            m["s0y"]().wait_recv()
            other = 1 - self.half_z
            add_rows(
                self.rows, self.at_z(pair, other), half,
                one_z.at[slot, pl.ds(pl.multiple_of(other * half, half), half), :],
            )
            m["s1z"]().start()

        def first_end(pair):
            m = self.moves(pair)
            slot = lax.rem(pair, SLOTS)
            m["s0y"]().wait()
            m["s0z"]().wait_send()
            mine = self.rows[pl.ds(self.at_y(pair, self.half_y), half), :].astype(jnp.float32)
            two_y[slot] = (mine + one_y[slot].astype(jnp.float32)).astype(jnp.bfloat16)
            m["s1y"]().start()

        def start(pair):
            m = self.moves(pair)
            m["s0y"]().start()

            @pl.when(self.end)
            def _():
                m["s0z"]().start()

        self.when(index, 0, None, start)
        self.when(index, 1, self.end, first_end)
        self.when(index, 1, self.inner, first_inner)
        self.when(index, 2, self.inner, second)
        self.when(index, 3, self.inner, third)
        self.when(index, 4, self.inner, fourth_inner)
        self.when(index, 4, self.end, fourth_end)
        self.when(index, 5, None, last)

    def greet(self, barrier):
        for device in (self.mate, self.across, self.twin):
            pl.semaphore_signal(barrier, inc=1, device_id={"dp": device}, device_id_type=MESH)
        return 3


def reducer_scratch(width):
    half = CHUNK // 2
    return [
        pltpu.VMEM((SLOTS, CHUNK, width), jnp.bfloat16),
        pltpu.VMEM((SLOTS, half, width), jnp.bfloat16),
        pltpu.VMEM((SLOTS, half, width), jnp.bfloat16),
        pltpu.VMEM((SLOTS, half, width), jnp.bfloat16),
        pltpu.VMEM((SLOTS, half, width), jnp.bfloat16),
        pltpu.VMEM((SLOTS, half, width), jnp.bfloat16),
        pltpu.SemaphoreType.DMA((12, SLOTS)),
        pltpu.SemaphoreType.DMA((11, SLOTS)),
    ]


HEAD_PAD = 128
BLOCK_SEQ = 256
SPAN = 512


def pad_matrix(local, padded):
    shape = (padded, local)
    feature = lax.broadcasted_iota(jnp.int32, shape, 1)
    lane = lax.broadcasted_iota(jnp.int32, shape, 0)
    head = jnp.zeros(shape, jnp.int32)
    for h in range(1, local // HEAD):
        head = head + (feature >= h * HEAD).astype(jnp.int32)
    within = feature - head * HEAD
    target = head * HEAD_PAD + within + jnp.where(within >= HEAD // 2, HEAD_PAD // 2 - HEAD // 2, 0)
    return jnp.where(lane == target, 1.0, 0.0).astype(jnp.bfloat16)


def dot(a, b):
    return jnp.dot(a, b, preferred_element_type=jnp.float32)


def dot_nt(a, b):
    return lax.dot_general(a, b, (((1,), (1,)), ((), ())), preferred_element_type=jnp.float32)


def dot_tn(a, b):
    return lax.dot_general(a, b, (((0,), (0,)), ((), ())), preferred_element_type=jnp.float32)


def segment_columns(seg):
    lines = jnp.broadcast_to(seg.astype(jnp.float32), (16, seg.shape[1])).astype(jnp.bfloat16)
    pick = (lax.broadcasted_iota(jnp.int32, (16, 128), 0) == 0).astype(jnp.float32).astype(jnp.bfloat16)
    return dot_tn(lines, pick)


def rotary_into(seg, cos_ref, sin_ref):
    seq = seg.shape[1]
    ids = segment_columns(seg)
    first = jnp.zeros((seq, 128), jnp.float32)
    row = seg.astype(jnp.float32)
    for s in range(1, 16):
        before = jnp.sum(jnp.where(row < s, 1.0, 0.0), axis=1, keepdims=True)
        first = jnp.where(ids == s, before, first)
    position = lax.broadcasted_iota(jnp.int32, (seq, 128), 0).astype(jnp.float32) - first
    lane = lax.broadcasted_iota(jnp.int32, (1, 128), 1)
    upper = lane >= HEAD_PAD // 2
    index = jnp.where(upper, lane - HEAD_PAD // 2, lane)
    freqs = jnp.exp(index.astype(jnp.float32) * (-2.0 * math.log(10000.0) / HEAD))
    freqs = jnp.where(index < HEAD // 2, freqs, 0.0)
    angles = position * freqs
    cos_ref[...] = jnp.cos(angles)
    sin_ref[...] = jnp.where(upper, jnp.sin(angles), -jnp.sin(angles))


class Ring4:
    def __init__(self):
        mp = lax.axis_index("mp")
        chip, core = lax.div(mp, 2), lax.rem(mp, 2)
        self.me = mp
        self.core = 2 * chip + 1 - core
        self.chip = 2 * (1 - chip) + core
        self.far = 2 * (1 - chip) + 1 - core


def block_rows(index):
    return pl.ds(pl.multiple_of(index * BLOCK_SEQ, BLOCK_SEQ), BLOCK_SEQ)


class Gather:
    def __init__(self, ring, rows, sems, parts=1):
        self.parts = parts
        size = BLOCK_SEQ // parts

        def copy(block, device, which, part):
            at = pl.ds(pl.multiple_of(block * BLOCK_SEQ + part * size, size), size)
            return pltpu.make_async_remote_copy(
                src_ref=rows.at[at, :],
                dst_ref=rows.at[at, :],
                send_sem=sems.at[0, which * parts + part],
                recv_sem=sems.at[1, which * parts + part],
                device_id={"mp": device},
                device_id_type=MESH,
            )

        self.near = lambda part=0: copy(ring.me, ring.core, 0, part)
        self.across = lambda part=0: copy(ring.me, ring.chip, 1, part)
        self.onward = lambda part=0: copy(ring.chip, ring.core, 2, part)

    def start(self, part=0):
        self.across(part).start()
        self.near(part).start()

    def forward(self):
        for part in range(self.parts):
            self.across(part).wait_recv()
            self.onward(part).start()

    def near_in(self):
        for part in range(self.parts):
            self.near(part).wait_recv()

    def onward_in(self):
        for part in range(self.parts):
            self.onward(part).wait_recv()

    def sent(self):
        for part in range(self.parts):
            self.near(part).wait_send()
            self.across(part).wait_send()
            self.onward(part).wait_send()


class GatherColumns:
    def __init__(self, ring, rows, sems):
        parts = rows.shape[1] // 256

        def copy(block, device, which, part):
            view = rows.at[block_rows(block), pl.ds(pl.multiple_of(part * 256, 256), 256)]
            return pltpu.make_async_remote_copy(
                src_ref=view,
                dst_ref=view,
                send_sem=sems.at[0, which * parts + part],
                recv_sem=sems.at[1, which * parts + part],
                device_id={"mp": device},
                device_id_type=MESH,
            )

        self.parts = parts
        self.near = lambda part: copy(ring.me, ring.core, 0, part)
        self.across = lambda part: copy(ring.me, ring.chip, 1, part)
        self.onward = lambda part: copy(ring.chip, ring.core, 2, part)

    def forward(self, part):
        self.across(part).wait_recv()
        self.onward(part).start()

    def sent(self):
        for part in range(self.parts):
            self.near(part).wait_send()
            self.across(part).wait_send()
            self.onward(part).wait_send()


class Scatter:
    def __init__(self, ring, send_core, recv_core, send_chip, recv_chip, sems, parts=1):
        self.parts = parts
        size = BLOCK_SEQ // parts

        def copy(source, target, device, which, part):
            at = pl.ds(part * size, size)
            return pltpu.make_async_remote_copy(
                src_ref=source.at[at, :],
                dst_ref=target.at[at, :],
                send_sem=sems.at[0, which * parts + part],
                recv_sem=sems.at[1, which * parts + part],
                device_id={"mp": device},
                device_id_type=MESH,
            )

        self.far = lambda part=0: copy(send_core.at[0], recv_core.at[0], ring.core, 0, part)
        self.core = lambda part=0: copy(send_core.at[1], recv_core.at[1], ring.core, 1, part)
        self.chip = lambda part=0: copy(send_chip, recv_chip, ring.chip, 2, part)


def greet_mp(ring, barrier):
    for device in (ring.core, ring.chip):
        pl.semaphore_signal(barrier, inc=1, device_id={"mp": device}, device_id_type=MESH)
    return 2


def norm_rows(values):
    inverse = lax.rsqrt(jnp.mean(values * values, -1, keepdims=True) + EPS)
    return values * inverse, inverse


def qkv_block(rows, weights, cos_ref, sin_ref, out, at):
    turned = 2 * (weights.shape[0] // 3) // 256
    tiles = weights.shape[0] // 256

    def one(n, turn):
        cols = pl.ds(pl.multiple_of(n * 256, 256), 256)
        value = dot_nt(rows[at, :], weights[cols, :])
        if turn:
            cosine, sine = cos_ref[at, :], sin_ref[at, :]
            halves = [value[:, j * 128 : j * 128 + 128] for j in range(2)]
            value = jnp.concatenate([h * cosine + pltpu.roll(h, 64, 1) * sine for h in halves], axis=1)
        out[at, cols] = value.astype(jnp.bfloat16)

    @pl.loop(0, turned)
    def _(n):
        one(n, True)

    @pl.loop(turned, tiles)
    def _(n):
        one(n, False)


def masks_into(seg, ids_ref, bias_ref):
    seq = seg.shape[1]
    for i in range(seq // BLOCK_SEQ):
        low = max(0, i * BLOCK_SEQ - SPAN)
        high = (i + 1) * BLOCK_SEQ
        shape = (BLOCK_SEQ, high - low)
        query = i * BLOCK_SEQ + lax.broadcasted_iota(jnp.int32, shape, 0)
        key = low + lax.broadcasted_iota(jnp.int32, shape, 1)
        ids = ids_ref[pl.ds(i * BLOCK_SEQ, BLOCK_SEQ), :][:, :1]
        same = ids == seg[:, low:high].astype(jnp.float32)
        bias_ref[pl.ds(i * BLOCK_SEQ, BLOCK_SEQ), pl.ds(0, high - low)] = jnp.where((query >= key) & same, 0.0, MASKED).astype(bias_ref.dtype)


def attend(qkv, out, bias_ref, heads, scale, blocks):
    width = heads * HEAD_PAD

    @pl.loop(0, heads)
    def _(h):
        lanes = [pl.ds(pl.multiple_of(part * width + h * HEAD_PAD, HEAD_PAD), HEAD_PAD) for part in range(3)]
        for i in blocks:
            low, high = max(0, i * BLOCK_SEQ - SPAN), (i + 1) * BLOCK_SEQ
            rows, keys = pl.ds(i * BLOCK_SEQ, BLOCK_SEQ), pl.ds(low, high - low)
            scores = dot_nt(qkv[rows, lanes[0]], qkv[keys, lanes[1]]) + bias_ref[rows, pl.ds(0, high - low)]
            top = jnp.max(scores, -1, keepdims=True)
            expo = jnp.exp((scores - top) * scale)
            probs = expo * (1.0 / jnp.sum(expo, -1, keepdims=True))
            out[rows, lanes[0]] = dot(probs.astype(jnp.bfloat16), qkv[keys, lanes[2]]).astype(jnp.bfloat16)


def layer_kernel(
    x, g, seg, gain_one, gain_two, wq, wk, wv, wo, wup, wdown,
    result_o, input_o, gains_o, sums_o,
    rows, b0, b1, b2, b3, b4, b5, send_sem, recv_sem, save_sem,
    w_up, w_down, w_qkv, w_out, rows_one, rows_g, rows_two, hidden, grad_up, branch, qkv, mixed, grad_mixed,
    cos_ref, sin_ref, bias_ref, resid, term_ref, key_sum, value_sum,
    send_core, recv_core, send_chip, recv_chip, gain_acc, gain_recv,
    load_sem, one_sem, g_sem, two_sem, branch_sem, rs0_sem, rs_sem, rs2_sem, rs3_sem, gain_sem, free_sem, ready_sem, down_sem,
):
    bf, f32 = jnp.bfloat16, jnp.float32
    ring = Ring4()
    seq, width = rows_two.shape
    units = w_up.shape[1]
    padded = w_out.shape[0]
    heads = padded // HEAD_PAD
    local = heads * HEAD
    pairs = rows.shape[0] // (2 * CHUNK)
    scale = 1.0 / math.sqrt(HEAD)
    half = BLOCK_SEQ // 2
    chip = lax.div(ring.me, 2)
    red = Reducer(rows, (b0, b1, b2, b3, b4, b5), send_sem, recv_sem, pairs)
    barrier = pltpu.get_barrier_semaphore()
    count = greet_mp(ring, barrier) + red.greet(barrier)
    places = [(w, rows.at[pl.ds(i * local, local), :]) for i, w in enumerate((wq, wk, wv, wo))]
    places += [(g, rows_g.at[block_rows(ring.me), :]), (wup, w_up), (wdown, w_down)]
    loads = [pltpu.make_async_copy(source, target, load_sem.at[i]) for i, (source, target) in enumerate(places)]
    for load in loads[:5]:
        load.start()
    normed, _ = norm_rows(x[...].astype(f32))
    rows_one[block_rows(ring.me), :] = (normed * gain_one[...]).astype(bf)
    one, all_g = Gather(ring, rows_one, one_sem, 2), GatherColumns(ring, rows_g, g_sem)
    two, all_branch = Gather(ring, rows_two, two_sem, 2), Gather(ring, branch, branch_sem)
    ahead = Scatter(ring, send_core, recv_core, send_chip, recv_chip, rs0_sem, 2)
    first = Scatter(ring, send_core, recv_core, send_chip, recv_chip, rs_sem)
    second = Scatter(ring, send_core, recv_core, send_chip, recv_chip, rs2_sem)
    third = Scatter(ring, send_core, recv_core, send_chip, recv_chip, rs3_sem)
    pl.semaphore_wait(barrier, count)
    one.start(0)
    one.start(1)
    for load in loads[5:]:
        load.start()

    spread = pad_matrix(local, padded)
    for i in range(3):
        loads[i].wait()
        w_qkv[pl.ds(i * padded, padded), :] = dot(spread, rows[pl.ds(i * local, local), :]).astype(bf)
    loads[3].wait()
    w_out[...] = dot(spread, rows[pl.ds(3 * local, local), :]).astype(bf)
    rotary_into(seg[...], cos_ref, sin_ref)
    qkv_block(rows_one, w_qkv, cos_ref, sin_ref, qkv, block_rows(ring.me))
    one.near_in()
    qkv_block(rows_one, w_qkv, cos_ref, sin_ref, qkv, block_rows(ring.core))
    key_sum[...] = segment_columns(seg[...])
    masks_into(seg[...], key_sum, bias_ref)
    loads[4].wait()
    for part in range(all_g.parts):
        all_g.near(part).start()

    def half_rows(block, part):
        return pl.ds(pl.multiple_of(block * BLOCK_SEQ + part * half, half), half)

    @pl.loop(0, 2)
    def _(p):
        one.across(p).wait_recv()
        one.onward(p).start()

        @pl.when(p == 1)
        def _():
            one.across(0).wait_send()
            one.across(1).wait_send()
            all_g.across(0).start()
            all_g.across(1).start()

        qkv_block(rows_one, w_qkv, cos_ref, sin_ref, qkv, half_rows(ring.chip, p))
        one.onward(p).wait_recv()
        qkv_block(rows_one, w_qkv, cos_ref, sin_ref, qkv, half_rows(ring.far, p))

    early, late = (0, 1), (2, 3)

    @pl.when(chip == 0)
    def _():
        attend(qkv, mixed, bias_ref, heads, scale, late)

    @pl.when(chip == 1)
    def _():
        attend(qkv, mixed, bias_ref, heads, scale, early)

    def term(block, part):
        return dot(mixed[half_rows(block, part), :], w_out[...])

    parts = [pl.ds(p * half, half) for p in range(2)]
    for p in range(2):
        send_core[0, parts[p], :] = term(ring.far, p).astype(bf)
        ahead.far(p).start()
    for p in range(2):
        value = term(ring.chip, p)
        ahead.far(p).wait_recv()
        send_chip[parts[p], :] = (value + recv_core[0, parts[p], :].astype(f32)).astype(bf)
        ahead.chip(p).start()

    @pl.when(chip == 0)
    def _():
        attend(qkv, mixed, bias_ref, heads, scale, early)

    @pl.when(chip == 1)
    def _():
        attend(qkv, mixed, bias_ref, heads, scale, late)

    for p in range(2):
        send_core[1, parts[p], :] = term(ring.core, p).astype(bf)
        ahead.core(p).start()
    for part in range(2):
        all_g.forward(part)
    for p in range(2):
        resid[parts[p], :] = x[parts[p], :].astype(f32) + term(ring.me, p)
    for p in range(2):
        ahead.core(p).wait_recv()
        ahead.chip(p).wait_recv()
        value = resid[parts[p], :] + recv_core[1, parts[p], :].astype(f32) + recv_chip[parts[p], :].astype(f32)
        resid[parts[p], :] = value
        normed, _ = norm_rows(value)
        at = pl.ds(pl.multiple_of(ring.me * BLOCK_SEQ + p * half, half), half)
        rows_two[at, :] = (normed * gain_two[...]).astype(bf)
        two.start(p)
    for p in range(2):
        ahead.far(p).wait_send()
        ahead.core(p).wait_send()
        ahead.chip(p).wait_send()

    base = 2 * units
    turned_pairs = width // (2 * CHUNK)

    def put(pair):
        at = pl.ds(pl.multiple_of(pair * 2 * CHUNK, 2 * CHUNK), 2 * CHUNK)
        return pltpu.make_async_copy(rows.at[at, :], sums_o.at[at, :], save_sem.at[lax.rem(pair, 4)])

    def slot(index):
        red.slot(index)
        pair = index - (STAGES - 1)

        @pl.when(pair >= turned_pairs + 4)
        def _():
            put(pair - 4).wait()

        @pl.when(pair >= turned_pairs)
        def _():
            put(pair).start()

    def tile(n):
        return pl.ds(pl.multiple_of(n * 256, 256), 256)

    def up_rows_of(at):
        @pl.loop(0, units // 256)
        def _(n):
            u = dot(rows_two[at, :], w_up[:, tile(n)])
            tangent = jnp.tanh(GELU_C * (u + GELU_K * u * u * u))
            hidden[at, tile(n)] = (0.5 * u * (1.0 + tangent)).astype(bf)

    loads[5].wait()
    up_rows_of(block_rows(ring.me))
    two.near_in()
    up_rows_of(block_rows(ring.core))
    for part in range(all_g.parts):
        all_g.near(part).wait_recv()
    for part in range(2):
        all_g.onward(part).wait_recv()

    @pl.loop(0, 2)
    def _(p):
        two.across(p).wait_recv()
        two.onward(p).start()

        @pl.when(p == 1)
        def _():
            two.across(0).wait_send()
            two.across(1).wait_send()
            for part in range(2, all_g.parts):
                all_g.across(part).start()

        up_rows_of(half_rows(ring.chip, p))
        two.onward(p).wait_recv()
        up_rows_of(half_rows(ring.far, p))

    loads[6].wait()

    def order(k):
        there = k < 2
        core = lax.rem(ring.me, 2)
        flip = 1 - lax.rem(k, 2)
        to_chip = jnp.where(there, 1 - chip, chip)
        to_core = jnp.where(flip == 1, 1 - core, core)
        return 2 * to_chip + to_core

    def hand_on(k, scatter, start):
        @pl.when(k == 0)
        def _():
            send_core[0] = term_ref[...].astype(bf)
            scatter.far().start()

        @pl.when(k == 1)
        def _():
            scatter.far().wait_recv()
            send_chip[...] = (term_ref[...] + recv_core[0].astype(f32)).astype(bf)
            scatter.chip().start()

        @pl.when(k == 2)
        def _():
            send_core[1] = term_ref[...].astype(bf)
            scatter.core().start()

        @pl.when(k == 3)
        def _():
            scatter.core().wait_recv()
            term_ref[...] = term_ref[...] + recv_core[1].astype(f32)

    def settle(scatter):
        for copy in (scatter.far(), scatter.core()):
            copy.wait_send()
        scatter.chip().wait()
        return term_ref[...] + recv_chip[...].astype(f32)

    def grad_tile(at, n):
        u = dot(rows_two[at, :], w_up[:, tile(n)])
        upstream = dot_nt(rows_g[at, :], w_down[tile(n), :])
        tangent = jnp.tanh(GELU_C * (u + GELU_K * u * u * u))
        slope = 0.5 * (1.0 + tangent) + 0.5 * u * (1.0 - tangent * tangent) * GELU_C * (1.0 + 3.0 * GELU_K * u * u)
        grad_up[at, tile(n)] = (upstream * slope).astype(bf)

    @pl.loop(0, width // 256)
    def _(n):
        @pl.when(n == 2)
        def _():
            all_g.onward(2).wait_recv()

        @pl.when(n == 3)
        def _():
            all_g.onward(3).wait_recv()
            all_g.onward(4).wait_recv()

        rows[tile(n), :] = dot_tn(rows_g[:, tile(n)], hidden[...]).astype(bf)
        slot(n)

        @pl.when(n < 3)
        def _():
            all_g.forward(n + 2)

        @pl.loop(0, 2)
        def _(k):
            grad_tile(block_rows(order(2 + k)), n)

        @pl.when(n >= 3)
        def _():
            at = block_rows(order(n - 3))

            @pl.loop(0, units // 256)
            def _(m):
                grad_tile(at, m)

    @pl.loop(0, 4)
    def _(k):
        at = block_rows(order(k))

        @pl.loop(0, width // 256)
        def _(n):
            term_ref[:, tile(n)] = dot_nt(grad_up[at, :], w_up[tile(n), :])

        hand_on(k, first, None)
        slot(5 + k)

    def up_rows(i):
        rows[pl.ds(pl.multiple_of(units + i * 256, 256), 256), :] = dot_tn(rows_two[:, tile(i)], grad_up[...]).astype(bf)

    up_rows(0)
    slot(9)
    grad_two = settle(first)
    normed, inverse = norm_rows(resid[...])
    scaled = grad_two * gain_two[...]
    part = inverse * (scaled - normed * jnp.mean(scaled * normed, -1, keepdims=True))
    mlp_part = jnp.sum(grad_two * normed, axis=0, keepdims=True)
    gain_acc[0] = jnp.zeros(gain_acc.shape[1:], f32)
    gain_acc[0, 1:2, :] = mlp_part
    mine = rows_g[block_rows(ring.me), :].astype(f32) + part
    input_o[...] = mine
    branch[block_rows(ring.me), :] = mine.astype(bf)
    all_branch.across().start()
    all_branch.near().start()
    for device in (ring.core, ring.chip):
        pl.semaphore_signal(ready_sem, inc=1, device_id={"mp": device}, device_id_type=MESH)

    def head_rows(left, lane, right, row):
        value = dot_tn(left[:, lane], right[...])
        halves = [value[at : at + HEAD // 2, :] for at in (0, 64, 128, 192)]
        rows[pl.ds(pl.multiple_of(row, 16), 2 * HEAD), :] = jnp.concatenate(halves, axis=0).astype(bf)

    @pl.loop(1, units // 256)
    def _(i):
        up_rows(i)

        @pl.when(i == 1)
        def _():
            pl.semaphore_wait(ready_sem, 2)

        at = block_rows(order(i - 1))

        @pl.loop(0, width // 256)
        def _(n):
            term_ref[:, tile(n)] = dot(hidden[at, :], w_down[:, tile(n)])

        hand_on(i - 1, second, None)

        @pl.when(i == 4)
        def _():
            all_branch.near().wait_recv()
            all_branch.forward()
            all_branch.onward().wait_recv()

            @pl.loop(0, heads // 2)
            def _(j):
                head_rows(mixed, tile(j), branch, base + j * 2 * HEAD)

        slot(9 + i)

    @pl.loop(0, 4)
    def _(b):
        grad_mixed[block_rows(b), :] = dot_nt(branch[block_rows(b), :], w_out[...]).astype(bf)

    def turn_down(n, target, at):
        eye = jnp.where(
            lax.broadcasted_iota(jnp.int32, (256, 256), 0) == lax.broadcasted_iota(jnp.int32, (256, 256), 1), 1.0, 0.0
        ).astype(bf)
        for m in range(width // 256):
            target[at, pl.ds(m * 256, 256)] = dot_tn(rows[pl.ds(m * 256, 256), tile(n)], eye).astype(bf)

    @pl.loop(0, heads)
    def _(h):
        lanes = [pl.ds(pl.multiple_of(n * padded + h * HEAD_PAD, HEAD_PAD), HEAD_PAD) for n in range(3)]
        key_sum[...] = jnp.zeros_like(key_sum)
        value_sum[...] = jnp.zeros_like(value_sum)
        for i in range(seq // BLOCK_SEQ):
            low, high = max(0, i * BLOCK_SEQ - SPAN), (i + 1) * BLOCK_SEQ
            at, keys = pl.ds(i * BLOCK_SEQ, BLOCK_SEQ), pl.ds(low, high - low)
            query, upstream = qkv[at, lanes[0]], grad_mixed[at, lanes[0]]
            scores = dot_nt(query, qkv[keys, lanes[1]]) + bias_ref[at, pl.ds(0, high - low)]
            top = jnp.max(scores, -1, keepdims=True)
            expo = jnp.exp((scores - top) * scale)
            probs = expo * (1.0 / jnp.sum(expo, -1, keepdims=True))
            grad_probs = dot_nt(upstream, qkv[keys, lanes[2]])
            inner = jnp.sum(probs * grad_probs, -1, keepdims=True)
            grad_scores = (probs * (grad_probs - inner)).astype(bf)
            value_sum[keys, :] += dot_tn(probs.astype(bf), upstream)
            key_sum[keys, :] += dot_tn(grad_scores, query)
            turned = dot(grad_scores, qkv[keys, lanes[1]]) * scale
            qkv[at, lanes[0]] = (turned * cos_ref[at, :] - pltpu.roll(turned, 64, 1) * sin_ref[at, :]).astype(bf)
            if i == 1:
                slot(14 + 2 * h)
        turned = key_sum[...] * scale
        qkv[:, lanes[1]] = (turned * cos_ref[...] - pltpu.roll(turned, 64, 1) * sin_ref[...]).astype(bf)
        qkv[:, lanes[2]] = value_sum[...].astype(bf)
        slot(15 + 2 * h)
        turn_down(h, grad_up, tile(h))

    @pl.loop(0, 3)
    def _(part):
        for j in range(heads // 2):
            lane = pl.ds(pl.multiple_of(part * padded + j * 256, 256), 256)
            head_rows(qkv, lane, rows_one, base + (part + 1) * local + j * 2 * HEAD)
        slot(22 + part)

    turn_down(4, hidden, pl.ds(0, 256))
    result_o[...] = (resid[...] + settle(second)).astype(bf)
    for device in (ring.core, ring.chip):
        pl.semaphore_signal(free_sem, inc=1, device_id={"mp": device}, device_id_type=MESH)
    pl.semaphore_wait(free_sem, 2)

    @pl.loop(0, 4)
    def _(k):
        at = block_rows(order(k))

        @pl.loop(0, width // 256)
        def _(n):
            term_ref[:, tile(n)] = dot(qkv[at, :], w_qkv[:, tile(n)])

        hand_on(k, third, None)
        slot(25 + k)

    downs = [
        pltpu.make_async_copy(grad_up, sums_o.at[pl.ds(0, seq), :], down_sem.at[0]),
        pltpu.make_async_copy(hidden.at[pl.ds(0, units - seq), :], sums_o.at[pl.ds(seq, units - seq), :], down_sem.at[1]),
    ]
    for copy in downs:
        copy.start()
    slot(29)
    grad_one = settle(third)
    normed, inverse = norm_rows(x[...].astype(f32))
    scaled = grad_one * gain_one[...]
    input_o[...] = input_o[...] + inverse * (scaled - normed * jnp.mean(scaled * normed, -1, keepdims=True))
    gain_acc[0, 0:1, :] = jnp.sum(grad_one * normed, axis=0, keepdims=True)

    def exchange(step):
        names = ({"mp": ring.core}, {"mp": ring.chip}, {"dp": red.twin}, {"dp": red.mate}, {"dp": red.across})
        return pltpu.make_async_remote_copy(
            src_ref=gain_acc.at[step], dst_ref=gain_recv.at[step], send_sem=gain_sem.at[0, step], recv_sem=gain_sem.at[1, step],
            device_id=names[step], device_id_type=MESH,
        )

    last = pairs + STAGES - 1

    @pl.loop(30, last)
    def _(index):
        for step in range(5):

            @pl.when(index == 30 + step)
            def _():
                if step:
                    exchange(step - 1).wait_recv()
                    gain_acc[step] = gain_acc[step - 1] + gain_recv[step - 1]
                exchange(step).start()

        slot(index)

    exchange(4).wait_recv()
    gains_o[...] = gain_acc[4] + gain_recv[4]
    for pair in range(pairs - 4, pairs):
        put(pair).wait()
    for copy in downs:
        copy.wait()
    for step in range(5):
        exchange(step).wait_send()
    for gather in (one, two):
        for part in range(2):
            gather.near(part).wait_send()
            gather.onward(part).wait_send()
    all_g.sent()
    all_branch.sent()


def layer(x, g, seg, gain_one, gain_two, wq, wk, wv, wo, wup, wdown):
    bf, f32 = jnp.bfloat16, jnp.float32
    own, width = x.shape
    units = wup.shape[1]
    seq = seg.shape[1]
    local = wo.shape[0]
    padded = local // HEAD * HEAD_PAD
    total = 2 * units + 4 * local
    vm, hbm = pl.BlockSpec(memory_space=pltpu.VMEM), pl.BlockSpec(memory_space=pl.ANY)
    sem = pltpu.SemaphoreType.DMA
    shapes = [((own, width), bf), ((own, width), f32), ((8, width), f32), ((total, width), bf)]
    tall = pltpu.VMEM((seq, width), bf)
    return pl.pallas_call(
        layer_kernel,
        out_shape=[jax.ShapeDtypeStruct(s, d) for s, d in shapes],
        in_specs=[vm, hbm, vm, vm, vm] + [hbm] * 6,
        out_specs=[vm] * 3 + [hbm],
        scratch_shapes=[pltpu.VMEM((total, width), bf)]
        + reducer_scratch(width)
        + [
            sem((4,)),
            pltpu.VMEM((width, units), bf), pltpu.VMEM((units, width), bf), pltpu.VMEM((3 * padded, width), bf), pltpu.VMEM((padded, width), bf),
            tall, tall, tall, pltpu.VMEM((seq, units), bf), pltpu.VMEM((seq, units), bf), tall,
            pltpu.VMEM((seq, 3 * padded), bf), pltpu.VMEM((seq, padded), bf), pltpu.VMEM((seq, padded), bf),
            pltpu.VMEM((seq, 128), f32), pltpu.VMEM((seq, 128), f32), pltpu.VMEM((seq, SPAN + BLOCK_SEQ), bf),
            pltpu.VMEM((own, width), f32), pltpu.VMEM((own, width), f32), pltpu.VMEM((seq, HEAD_PAD), f32), pltpu.VMEM((seq, HEAD_PAD), f32),
            pltpu.VMEM((2, own, width), bf), pltpu.VMEM((2, own, width), bf), pltpu.VMEM((own, width), bf), pltpu.VMEM((own, width), bf),
            pltpu.VMEM((5, 8, width), f32), pltpu.VMEM((5, 8, width), f32),
            sem((7,)), sem((2, 6)), sem((2, 3 * (width // 256))), sem((2, 6)), sem((2, 3)), sem((2, 6)), sem((2, 3)), sem((2, 3)), sem((2, 3)), sem((2, 5)),
            pltpu.SemaphoreType.REGULAR, pltpu.SemaphoreType.REGULAR, sem((2,)),
        ],
        compiler_params=pltpu.CompilerParams(collective_id=0, has_side_effects=True, vmem_limit_bytes=67043328),
    )(x, g, seg, gain_one, gain_two, wq, wk, wv, wo, wup, wdown)


def finish_kernel(result, input_grad, gains, sums, result_o, input_o, one_o, two_o, down_o, up_o, out_o, q_o, k_o, v_o, inbox, outbox, side_one, side_two, in_sem, out_sem, side_sem):
    step = out_o.shape[0]
    targets = [(down_o, i * step) for i in range(down_o.shape[0] // step)] + [(up_o, i * step) for i in range(up_o.shape[0] // step)]
    targets += [(t, 0) for t in (out_o, q_o, k_o, v_o)]
    count, depth = len(targets), inbox.shape[0]
    bring = [pltpu.make_async_copy(result, side_one, side_sem.at[0]), pltpu.make_async_copy(input_grad, side_two, side_sem.at[1])]
    take = [pltpu.make_async_copy(side_one, result_o, side_sem.at[2]), pltpu.make_async_copy(side_two, input_o, side_sem.at[3])]

    def read(i):
        return pltpu.make_async_copy(sums.at[pl.ds(i * step, step), :], inbox.at[i % depth], in_sem.at[i % depth])

    def write(i):
        target, at = targets[i]
        return pltpu.make_async_copy(outbox.at[i % depth], target.at[pl.ds(at, step), :], out_sem.at[i % depth])

    for i in range(depth):
        read(i).start()
    for side in bring:
        side.start()
    one_o[...] = gains[0, :]
    two_o[...] = gains[1, :]
    for i in range(count):
        read(i).wait()
        if i >= depth:
            write(i - depth).wait()
        outbox[i % depth] = inbox[i % depth].astype(jnp.float32)
        write(i).start()
        if i + depth < count:
            read(i + depth).start()
        if i == depth:
            for come, go in zip(bring, take):
                come.wait()
                go.start()
    for i in range(count - depth, count):
        write(i).wait()
    for side in take:
        side.wait()


def finish(result, input_grad, gains, sums, units, local):
    bf, f32 = jnp.bfloat16, jnp.float32
    own, width = result.shape
    vm, hbm = pl.BlockSpec(memory_space=pltpu.VMEM), pl.BlockSpec(memory_space=pl.ANY)
    sem = pltpu.SemaphoreType.DMA
    shapes = [((own, width), bf), ((own, width), f32), ((width,), f32), ((width,), f32), ((units, width), f32), ((width, units), f32)] + [((local, width), f32)] * 4
    return pl.pallas_call(
        finish_kernel,
        out_shape=[jax.ShapeDtypeStruct(s, d) for s, d in shapes],
        in_specs=[hbm, hbm, vm, hbm],
        out_specs=[hbm, hbm, vm, vm] + [hbm] * 6,
        scratch_shapes=[pltpu.VMEM((3, local, width), bf), pltpu.VMEM((3, local, width), f32), pltpu.VMEM((own, width), bf), pltpu.VMEM((own, width), f32), sem((3,)), sem((3,)), sem((4,))],
        compiler_params=pltpu.CompilerParams(vmem_limit_bytes=67043328),
    )(result, input_grad, gains, sums)


def on_device(
    hidden_in,
    segment_ids,
    attn_gain,
    query_weight,
    key_weight,
    value_weight,
    out_weight,
    mlp_gain,
    up_weight,
    down_weight,
    out_cotangent,
):
    row_count = segment_ids.shape[0]
    seq_len = segment_ids.shape[1]
    local_width = query_weight.shape[1]
    head_count = local_width // HEAD
    scale = 1.0 / math.sqrt(HEAD)
    block = min(512, seq_len)
    head_shape = (row_count, seq_len, head_count, HEAD)
    x_float = hidden_in.astype(jnp.float32)
    scaled_one, normed_one, inverse_one = normalize(x_float, attn_gain)
    rows_one = lax.all_gather(scaled_one.astype(jnp.bfloat16), "mp", axis=1, tiled=True)
    cosine, sine = rotary_tables(segment_ids, HEAD)
    queries = rotate(project(rows_one, query_weight).reshape(head_shape), cosine, sine).astype(
        jnp.bfloat16
    )
    keys = rotate(project(rows_one, key_weight).reshape(head_shape), cosine, sine).astype(
        jnp.bfloat16
    )
    values = project(rows_one, value_weight).reshape(head_shape).astype(jnp.bfloat16)
    row_index = 0
    mixed_one, log_one = attend_forward(
        queries[row_index], keys[row_index], values[row_index], segment_ids[row_index], scale, block
    )
    mixed_rows = [mixed_one]
    log_rows = [log_one]
    mixed = jnp.stack(mixed_rows, 0).reshape(row_count, seq_len, local_width).astype(jnp.bfloat16)
    attn_share = lax.psum_scatter(project(mixed, out_weight), "mp", scatter_dimension=1, tiled=True)
    resid = x_float + attn_share
    scaled_two, normed_two, inverse_two = normalize(resid, mlp_gain)
    rows_two = lax.all_gather(scaled_two.astype(jnp.bfloat16), "mp", axis=1, tiled=True)
    up_pre = project(rows_two, up_weight)
    hidden = jax.nn.gelu(up_pre, approximate=True).astype(jnp.bfloat16)
    mlp_share = lax.psum_scatter(
        project(hidden, down_weight).astype(jnp.bfloat16), "mp", scatter_dimension=1, tiled=True
    ).astype(jnp.float32)
    result = (resid + mlp_share).astype(jnp.bfloat16)
    grad_top = out_cotangent.astype(jnp.float32)
    grad_rows = lax.all_gather(out_cotangent, "mp", axis=1, tiled=True)
    down_total = weight_grad(hidden, grad_rows)
    grad_hidden = project_back(grad_rows, down_weight)
    grad_up_pre = (grad_hidden * gelu_slope(up_pre)).astype(jnp.bfloat16)
    up_total = weight_grad(rows_two, grad_up_pre)
    grad_two = lax.psum_scatter(
        project_back(grad_up_pre, up_weight), "mp", scatter_dimension=1, tiled=True
    )
    resid_part, mlp_gain_part = norm_back(grad_two, normed_two, inverse_two, mlp_gain)
    grad_resid = grad_top + resid_part
    branch_rows = lax.all_gather(grad_resid.astype(jnp.bfloat16), "mp", axis=1, tiled=True)
    out_total = weight_grad(mixed, branch_rows)
    grad_mixed = project_back(branch_rows, out_weight).astype(jnp.bfloat16).reshape(head_shape)
    row_index = 0
    grad_q, grad_k, grad_v = attend_back(
        queries[row_index],
        keys[row_index],
        values[row_index],
        grad_mixed[row_index],
        log_rows[row_index],
        segment_ids[row_index],
        scale,
        block,
    )
    query_rows = [grad_q]
    key_rows = [grad_k]
    value_rows = [grad_v]
    grad_query = (
        rotate_back(jnp.stack(query_rows, 0), cosine, sine)
        .astype(jnp.bfloat16)
        .reshape(row_count, seq_len, local_width)
    )
    grad_key = (
        rotate_back(jnp.stack(key_rows, 0), cosine, sine)
        .astype(jnp.bfloat16)
        .reshape(row_count, seq_len, local_width)
    )
    grad_value = (
        jnp.stack(value_rows, 0).astype(jnp.bfloat16).reshape(row_count, seq_len, local_width)
    )
    query_total = weight_grad(rows_one, grad_query)
    key_total = weight_grad(rows_one, grad_key)
    value_total = weight_grad(rows_one, grad_value)
    grad_terms = (
        project_back(grad_query, query_weight)
        + project_back(grad_key, key_weight)
        + project_back(grad_value, value_weight)
    )
    grad_one = lax.psum_scatter(grad_terms, "mp", scatter_dimension=1, tiled=True)
    input_part, attn_gain_part = norm_back(grad_one, normed_one, inverse_one, attn_gain)
    input_grad = grad_resid + input_part
    attn_gain_part, mlp_gain_part = lax.psum((attn_gain_part, mlp_gain_part), "mp")
    (
        query_total,
        key_total,
        value_total,
        out_total,
        attn_gain_part,
        mlp_gain_part,
        up_total,
        down_total,
    ) = lax.psum(
        (
            query_total,
            key_total,
            value_total,
            out_total,
            attn_gain_part,
            mlp_gain_part,
            up_total,
            down_total,
        ),
        "dp",
    )
    return (
        result,
        input_grad,
        attn_gain_part,
        query_total,
        key_total,
        value_total,
        out_total,
        mlp_gain_part,
        up_total,
        down_total,
    )


def on_device_kernels(
    hidden_in, segment_ids, attn_gain, query_weight, key_weight, value_weight, out_weight, mlp_gain, up_weight, down_weight, out_cotangent
):
    sums = layer(
        hidden_in[0], out_cotangent[0], segment_ids, attn_gain, mlp_gain,
        query_weight.T, key_weight.T, value_weight.T, out_weight, up_weight, down_weight,
    )
    result, input_grad, one, two, down, up, out, query, key, value = finish(*sums, up_weight.shape[1], out_weight.shape[0])
    return (result[None], input_grad[None], one, query.T, key.T, value.T, out, two, up, down)


def solution(mesh):
    return jax.shard_map(
        on_device_kernels if mesh.shape["dp"] == 8 else on_device,
        mesh=mesh,
        in_specs=(
            P("dp", "mp", None),
            P("dp", None),
            P(),
            P(None, "mp"),
            P(None, "mp"),
            P(None, "mp"),
            P("mp", None),
            P(),
            P(None, "mp"),
            P("mp", None),
            P("dp", "mp", None),
        ),
        out_specs=(
            P("dp", "mp", None),
            P("dp", "mp", None),
            P(),
            P(None, "mp"),
            P(None, "mp"),
            P(None, "mp"),
            P("mp", None),
            P(),
            P(None, "mp"),
            P("mp", None),
        ),
        check_vma=False,
    )
```

```python
import math

import jax
import jax.numpy as jnp
from jax import lax
from jax.experimental import pallas as pl
from jax.experimental.pallas import tpu as pltpu
from jax.sharding import PartitionSpec as P

HEAD = 80


EPS = 1e-06
MASKED = -1e30
GELU_C = math.sqrt(2.0 / math.pi)
GELU_K = 0.044715


def normalize(values, gain):
    inverse = lax.rsqrt(jnp.mean(values * values, -1, keepdims=True) + EPS)
    normed = values * inverse
    return (normed * gain, normed, inverse)


def norm_back(upstream, normed, inverse, gain):
    scaled = upstream * gain
    inner = jnp.mean(scaled * normed, -1, keepdims=True)
    return (inverse * (scaled - normed * inner), jnp.sum(upstream * normed, axis=(0, 1)))


def gelu_slope(values):
    tangent = jnp.tanh(GELU_C * (values + GELU_K * values * values * values))
    return 0.5 * (1.0 + tangent) + 0.5 * values * (1.0 - tangent * tangent) * GELU_C * (
        1.0 + 3.0 * GELU_K * values * values
    )


def project(left, weight):
    return jnp.einsum("rsd,de->rse", left, weight, preferred_element_type=jnp.float32)


def project_back(left, weight):
    return jnp.einsum("rse,de->rsd", left, weight, preferred_element_type=jnp.float32)


def weight_grad(left, right):
    return jnp.einsum("rsd,rse->de", left, right, preferred_element_type=jnp.float32)


def rotary_tables(segments, head_size):
    seq_len = segments.shape[1]
    places = jnp.arange(seq_len, dtype=jnp.int32)
    starts_here = jnp.concatenate(
        [jnp.ones((segments.shape[0], 1), bool), segments[:, 1:] != segments[:, :-1]], axis=1
    )
    first = lax.cummax(jnp.where(starts_here, places[None, :], 0), axis=1)
    position = (places[None, :] - first).astype(jnp.float32)
    half = head_size // 2
    freqs = jnp.exp(jnp.arange(half, dtype=jnp.float32) * (-2.0 * math.log(10000.0) / head_size))
    angles = position[:, :, None] * freqs[None, None, :]
    return (jnp.cos(angles)[:, :, None, :], jnp.sin(angles)[:, :, None, :])


def rotate(values, cosine, sine):
    half = values.shape[-1] // 2
    first, second = (values[..., :half], values[..., half:])
    return jnp.concatenate([first * cosine - second * sine, second * cosine + first * sine], -1)


def rotate_back(grads, cosine, sine):
    half = grads.shape[-1] // 2
    first, second = (grads[..., :half], grads[..., half:])
    return jnp.concatenate([first * cosine + second * sine, second * cosine - first * sine], -1)


def allowed_block(segments_row, start, size):
    seq_len = segments_row.shape[0]
    query_pos = start + jnp.arange(size, dtype=jnp.int32)
    key_pos = jnp.arange(seq_len, dtype=jnp.int32)
    query_seg = segments_row[start : start + size]
    return (query_pos[:, None] >= key_pos[None, :]) & (query_seg[:, None] == segments_row[None, :])


def block_scores(query_block, keys, allowed, scale):
    scores = (
        jnp.einsum("qhd,khd->hqk", query_block, keys, preferred_element_type=jnp.float32) * scale
    )
    return jnp.where(allowed[None], scores, MASKED)


def attend_forward(queries, keys, values, segments_row, scale, block):
    outputs = []
    sums = []
    for start in range(0, queries.shape[0], block):
        allowed = allowed_block(segments_row, start, block)
        scores = block_scores(queries[start : start + block], keys, allowed, scale)
        top = jnp.max(scores, -1, keepdims=True)
        expo = jnp.exp(scores - top)
        total = jnp.sum(expo, -1, keepdims=True)
        probs = (expo / total).astype(jnp.bfloat16)
        outputs.append(
            jnp.einsum("hqk,khd->qhd", probs, values, preferred_element_type=jnp.float32)
        )
        sums.append(top + jnp.log(total))
    return (jnp.concatenate(outputs, 0), jnp.concatenate(sums, 1))


def attend_back(queries, keys, values, grad_mixed, log_sums, segments_row, scale, block):
    key_total = jnp.zeros(keys.shape, jnp.float32)
    value_total = jnp.zeros(values.shape, jnp.float32)
    query_parts = []
    for start in range(0, queries.shape[0], block):
        allowed = allowed_block(segments_row, start, block)
        query_block = queries[start : start + block]
        scores = block_scores(query_block, keys, allowed, scale)
        probs = jnp.exp(scores - log_sums[:, start : start + block])
        grad_block = grad_mixed[start : start + block]
        grad_probs = jnp.einsum(
            "qhd,khd->hqk", grad_block, values, preferred_element_type=jnp.float32
        )
        inner = jnp.sum(probs * grad_probs, -1, keepdims=True)
        grad_scores = (probs * (grad_probs - inner)).astype(jnp.bfloat16)
        query_parts.append(
            jnp.einsum("hqk,khd->qhd", grad_scores, keys, preferred_element_type=jnp.float32)
            * scale
        )
        key_total = (
            key_total
            + jnp.einsum(
                "hqk,qhd->khd", grad_scores, query_block, preferred_element_type=jnp.float32
            )
            * scale
        )
        value_total = value_total + jnp.einsum(
            "hqk,qhd->khd",
            probs.astype(jnp.bfloat16),
            grad_block,
            preferred_element_type=jnp.float32,
        )
    return (jnp.concatenate(query_parts, 0), key_total, value_total)


MESH = pl.DeviceIdType.MESH
CHUNK = 64
SLOTS = 6
STAGES = 6
(R1Z, R2Z, R3Z, FZM, FZA, FZB, R1Y, R2Y, R3Y, FYI, FYY) = range(11)
(S0Z, S0Y, S1Z, S1Y, S2Z, S2Y, S3ZM, S3ZE, S3YE, S3YY, S4Z, S4Y) = range(12)


def add_rows(total_ref, row, count, *others):
    value = total_ref[pl.ds(row, count), :].astype(jnp.float32)
    for other in others:
        value = value + other[...].astype(jnp.float32)
    total_ref[pl.ds(row, count), :] = value.astype(jnp.bfloat16)


class Reducer:
    def __init__(self, rows, bufs, send_sem, recv_sem, pairs):
        self.rows, self.bufs, self.send_sem, self.recv_sem, self.pairs = rows, bufs, send_sem, recv_sem, pairs
        dp = lax.axis_index("dp")
        self.place, self.side = lax.div(dp, 2), lax.rem(dp, 2)
        self.inner = (self.place == 1) | (self.place == 2)
        self.end = jnp.logical_not(self.inner)
        self.mate = 2 * (self.place + 1 - 2 * lax.rem(self.place, 2)) + self.side
        self.across = 2 * (3 - self.place) + self.side
        self.twin = 2 * self.place + 1 - self.side
        self.half_z = lax.div(self.place, 2)
        self.half_y = self.side

    def copy(self, source, target, send, recv, slot, device):
        return pltpu.make_async_remote_copy(
            src_ref=source,
            dst_ref=target,
            send_sem=self.send_sem.at[send, slot],
            recv_sem=self.recv_sem.at[recv, slot],
            device_id={"dp": device},
            device_id_type=MESH,
        )

    def whole_z(self, pair):
        return pl.multiple_of(pair * (2 * CHUNK), CHUNK)

    def at_z(self, pair, half):
        return pl.multiple_of(pair * (2 * CHUNK) + half * (CHUNK // 2), CHUNK // 2)

    def at_y(self, pair, half):
        return pl.multiple_of(pair * (2 * CHUNK) + CHUNK + half * (CHUNK // 2), CHUNK // 2)

    def moves(self, pair):
        slot = lax.rem(pair, SLOTS)
        rows, (one_z, two_z, three_z, one_y, two_y, three_y) = self.rows, self.bufs
        half = CHUNK // 2
        mine_z, mine_y = self.half_z, self.half_y
        own_z = rows.at[pl.ds(self.at_z(pair, mine_z), half), :]
        rest_z = rows.at[pl.ds(self.at_z(pair, 1 - mine_z), half), :]
        own_y = rows.at[pl.ds(self.at_y(pair, mine_y), half), :]
        rest_y = rows.at[pl.ds(self.at_y(pair, 1 - mine_y), half), :]
        all_z = rows.at[pl.ds(self.whole_z(pair), CHUNK), :]
        return dict(
            s0z=lambda: self.copy(all_z, one_z.at[slot], S0Z, R1Z, slot, self.mate),
            s0y=lambda: self.copy(rest_y, one_y.at[slot], S0Y, R1Y, slot, self.twin),
            s1z=lambda: self.copy(rest_z, two_z.at[slot], S1Z, R2Z, slot, self.across),
            s1y=lambda: self.copy(two_y.at[slot], two_y.at[slot], S1Y, R2Y, slot, self.mate),
            s2z=lambda: self.copy(own_z, three_z.at[slot], S2Z, R3Z, slot, self.twin),
            s2y=lambda: self.copy(own_y, three_y.at[slot], S2Y, R3Y, slot, self.across),
            s3zm=lambda: self.copy(own_z, own_z, S3ZM, FZM, slot, self.across),
            s3ze=lambda: self.copy(own_z, own_z, S3ZE, FZA, slot, self.mate),
            s3ye=lambda: self.copy(own_y, own_y, S3YE, FYI, slot, self.mate),
            s3yy=lambda: self.copy(own_y, own_y, S3YY, FYY, slot, self.twin),
            s4z=lambda: self.copy(rest_z, rest_z, S4Z, FZB, slot, self.mate),
            s4y=lambda: self.copy(own_y, own_y, S4Y, FYY, slot, self.twin),
        )

    def when(self, slot_index, stage, role, body):
        pair = slot_index - stage
        live = (pair >= 0) & (pair < self.pairs)
        if role is not None:
            live = live & role

        @pl.when(live)
        def _():
            body(pair)

    def slot(self, index):
        half = CHUNK // 2
        one_z, two_z, three_z, one_y, two_y, three_y = self.bufs

        def last(pair):
            m = self.moves(pair)
            @pl.when(self.end)
            def _():
                m["s3ze"]().wait_recv()
                m["s4z"]().wait_recv()
                m["s1y"]().wait_send()
                m["s4y"]().wait_send()
                m["s4y"]().wait_recv()

            @pl.when(self.inner)
            def _():
                m["s3zm"]().wait_send()
                m["s3ze"]().wait_send()
                m["s3ye"]().wait_send()
                m["s3yy"]().wait_send()
                m["s4z"]().wait_send()
                m["s3yy"]().wait_recv()

        def fourth_inner(pair):
            m = self.moves(pair)
            m["s3zm"]().wait_recv()
            m["s4z"]().start()

        def fourth_end(pair):
            m = self.moves(pair)
            m["s3ye"]().wait_recv()
            m["s4y"]().start()

        def third(pair):
            m = self.moves(pair)
            slot = lax.rem(pair, SLOTS)
            m["s2z"]().wait()
            m["s2y"]().wait()
            add_rows(self.rows, self.at_z(pair, self.half_z), half, three_z.at[slot])
            add_rows(self.rows, self.at_y(pair, self.half_y), half, three_y.at[slot])
            m["s3ze"]().start()
            m["s3zm"]().start()
            m["s3ye"]().start()
            m["s3yy"]().start()

        def second(pair):
            m = self.moves(pair)
            slot = lax.rem(pair, SLOTS)
            m["s1z"]().wait()
            m["s1y"]().wait_recv()
            m["s0y"]().wait_send()
            add_rows(
                self.rows, self.at_z(pair, self.half_z), half,
                one_z.at[slot, pl.ds(pl.multiple_of(self.half_z * half, half), half), :], two_z.at[slot],
            )
            add_rows(self.rows, self.at_y(pair, self.half_y), half, one_y.at[slot], two_y.at[slot])
            m["s2z"]().start()
            m["s2y"]().start()

        def first_inner(pair):
            m = self.moves(pair)
            slot = lax.rem(pair, SLOTS)
            m["s0z"]().wait_recv()
            m["s0y"]().wait_recv()
            other = 1 - self.half_z
            add_rows(
                self.rows, self.at_z(pair, other), half,
                one_z.at[slot, pl.ds(pl.multiple_of(other * half, half), half), :],
            )
            m["s1z"]().start()

        def first_end(pair):
            m = self.moves(pair)
            slot = lax.rem(pair, SLOTS)
            m["s0y"]().wait()
            m["s0z"]().wait_send()
            mine = self.rows[pl.ds(self.at_y(pair, self.half_y), half), :].astype(jnp.float32)
            two_y[slot] = (mine + one_y[slot].astype(jnp.float32)).astype(jnp.bfloat16)
            m["s1y"]().start()

        def start(pair):
            m = self.moves(pair)
            m["s0y"]().start()

            @pl.when(self.end)
            def _():
                m["s0z"]().start()

        self.when(index, 0, None, start)
        self.when(index, 1, self.end, first_end)
        self.when(index, 1, self.inner, first_inner)
        self.when(index, 2, self.inner, second)
        self.when(index, 3, self.inner, third)
        self.when(index, 4, self.inner, fourth_inner)
        self.when(index, 4, self.end, fourth_end)
        self.when(index, 5, None, last)

    def greet(self, barrier):
        for device in (self.mate, self.across, self.twin):
            pl.semaphore_signal(barrier, inc=1, device_id={"dp": device}, device_id_type=MESH)
        return 3


def reducer_scratch(width):
    half = CHUNK // 2
    return [
        pltpu.VMEM((SLOTS, CHUNK, width), jnp.bfloat16),
        pltpu.VMEM((SLOTS, half, width), jnp.bfloat16),
        pltpu.VMEM((SLOTS, half, width), jnp.bfloat16),
        pltpu.VMEM((SLOTS, half, width), jnp.bfloat16),
        pltpu.VMEM((SLOTS, half, width), jnp.bfloat16),
        pltpu.VMEM((SLOTS, half, width), jnp.bfloat16),
        pltpu.SemaphoreType.DMA((12, SLOTS)),
        pltpu.SemaphoreType.DMA((11, SLOTS)),
    ]


HEAD_PAD = 128
BLOCK_SEQ = 256
SPAN = 512


def pad_matrix(local, padded):
    shape = (padded, local)
    feature = lax.broadcasted_iota(jnp.int32, shape, 1)
    lane = lax.broadcasted_iota(jnp.int32, shape, 0)
    head = jnp.zeros(shape, jnp.int32)
    for h in range(1, local // HEAD):
        head = head + (feature >= h * HEAD).astype(jnp.int32)
    within = feature - head * HEAD
    target = head * HEAD_PAD + within + jnp.where(within >= HEAD // 2, HEAD_PAD // 2 - HEAD // 2, 0)
    return jnp.where(lane == target, 1.0, 0.0).astype(jnp.bfloat16)


def dot(a, b):
    return jnp.dot(a, b, preferred_element_type=jnp.float32)


def dot_nt(a, b):
    return lax.dot_general(a, b, (((1,), (1,)), ((), ())), preferred_element_type=jnp.float32)


def dot_tn(a, b):
    return lax.dot_general(a, b, (((0,), (0,)), ((), ())), preferred_element_type=jnp.float32)


def segment_columns(seg):
    lines = jnp.broadcast_to(seg.astype(jnp.float32), (16, seg.shape[1])).astype(jnp.bfloat16)
    pick = (lax.broadcasted_iota(jnp.int32, (16, 128), 0) == 0).astype(jnp.float32).astype(jnp.bfloat16)
    return dot_tn(lines, pick)


def rotary_into(seg, cos_ref, sin_ref):
    seq = seg.shape[1]
    ids = segment_columns(seg)
    first = jnp.zeros((seq, 128), jnp.float32)
    row = seg.astype(jnp.float32)
    for s in range(1, 16):
        before = jnp.sum(jnp.where(row < s, 1.0, 0.0), axis=1, keepdims=True)
        first = jnp.where(ids == s, before, first)
    position = lax.broadcasted_iota(jnp.int32, (seq, 128), 0).astype(jnp.float32) - first
    lane = lax.broadcasted_iota(jnp.int32, (1, 128), 1)
    upper = lane >= HEAD_PAD // 2
    index = jnp.where(upper, lane - HEAD_PAD // 2, lane)
    freqs = jnp.exp(index.astype(jnp.float32) * (-2.0 * math.log(10000.0) / HEAD))
    freqs = jnp.where(index < HEAD // 2, freqs, 0.0)
    angles = position * freqs
    cos_ref[...] = jnp.cos(angles)
    sin_ref[...] = jnp.where(upper, jnp.sin(angles), -jnp.sin(angles))


class Ring4:
    def __init__(self):
        mp = lax.axis_index("mp")
        chip, core = lax.div(mp, 2), lax.rem(mp, 2)
        self.me = mp
        self.core = 2 * chip + 1 - core
        self.chip = 2 * (1 - chip) + core
        self.far = 2 * (1 - chip) + 1 - core


def block_rows(index):
    return pl.ds(pl.multiple_of(index * BLOCK_SEQ, BLOCK_SEQ), BLOCK_SEQ)


class Gather:
    def __init__(self, ring, rows, sems, parts=1):
        self.parts = parts
        size = BLOCK_SEQ // parts

        def copy(block, device, which, part):
            at = pl.ds(pl.multiple_of(block * BLOCK_SEQ + part * size, size), size)
            return pltpu.make_async_remote_copy(
                src_ref=rows.at[at, :],
                dst_ref=rows.at[at, :],
                send_sem=sems.at[0, which * parts + part],
                recv_sem=sems.at[1, which * parts + part],
                device_id={"mp": device},
                device_id_type=MESH,
            )

        self.near = lambda part=0: copy(ring.me, ring.core, 0, part)
        self.across = lambda part=0: copy(ring.me, ring.chip, 1, part)
        self.onward = lambda part=0: copy(ring.chip, ring.core, 2, part)

    def start(self, part=0):
        self.across(part).start()
        self.near(part).start()

    def forward(self):
        for part in range(self.parts):
            self.across(part).wait_recv()
            self.onward(part).start()

    def near_in(self):
        for part in range(self.parts):
            self.near(part).wait_recv()

    def onward_in(self):
        for part in range(self.parts):
            self.onward(part).wait_recv()

    def sent(self):
        for part in range(self.parts):
            self.near(part).wait_send()
            self.across(part).wait_send()
            self.onward(part).wait_send()


class Scatter:
    def __init__(self, ring, send_core, recv_core, send_chip, recv_chip, sems, parts=1):
        self.parts = parts
        size = BLOCK_SEQ // parts

        def copy(source, target, device, which, part):
            at = pl.ds(part * size, size)
            return pltpu.make_async_remote_copy(
                src_ref=source.at[at, :],
                dst_ref=target.at[at, :],
                send_sem=sems.at[0, which * parts + part],
                recv_sem=sems.at[1, which * parts + part],
                device_id={"mp": device},
                device_id_type=MESH,
            )

        self.far = lambda part=0: copy(send_core.at[0], recv_core.at[0], ring.core, 0, part)
        self.core = lambda part=0: copy(send_core.at[1], recv_core.at[1], ring.core, 1, part)
        self.chip = lambda part=0: copy(send_chip, recv_chip, ring.chip, 2, part)


def greet_mp(ring, barrier):
    for device in (ring.core, ring.chip):
        pl.semaphore_signal(barrier, inc=1, device_id={"mp": device}, device_id_type=MESH)
    return 2


def norm_rows(values):
    inverse = lax.rsqrt(jnp.mean(values * values, -1, keepdims=True) + EPS)
    return values * inverse, inverse


def qkv_block(rows, weights, cos_ref, sin_ref, out, block):
    at = block_rows(block)
    turned = 2 * (weights.shape[0] // 3) // 256
    tiles = weights.shape[0] // 256

    def one(n, turn):
        cols = pl.ds(pl.multiple_of(n * 256, 256), 256)
        value = dot_nt(rows[at, :], weights[cols, :])
        if turn:
            cosine, sine = cos_ref[at, :], sin_ref[at, :]
            halves = [value[:, j * 128 : j * 128 + 128] for j in range(2)]
            value = jnp.concatenate([h * cosine + pltpu.roll(h, 64, 1) * sine for h in halves], axis=1)
        out[at, cols] = value.astype(jnp.bfloat16)

    @pl.loop(0, turned)
    def _(n):
        one(n, True)

    @pl.loop(turned, tiles)
    def _(n):
        one(n, False)


def masks_into(seg, ids_ref, bias_ref):
    seq = seg.shape[1]
    for i in range(seq // BLOCK_SEQ):
        low = max(0, i * BLOCK_SEQ - SPAN)
        high = (i + 1) * BLOCK_SEQ
        shape = (BLOCK_SEQ, high - low)
        query = i * BLOCK_SEQ + lax.broadcasted_iota(jnp.int32, shape, 0)
        key = low + lax.broadcasted_iota(jnp.int32, shape, 1)
        ids = ids_ref[pl.ds(i * BLOCK_SEQ, BLOCK_SEQ), :][:, :1]
        same = ids == seg[:, low:high].astype(jnp.float32)
        bias_ref[pl.ds(i * BLOCK_SEQ, BLOCK_SEQ), pl.ds(0, high - low)] = jnp.where((query >= key) & same, 0.0, MASKED).astype(bias_ref.dtype)


def attend(qkv, out, bias_ref, heads, scale, blocks):
    width = heads * HEAD_PAD

    @pl.loop(0, heads)
    def _(h):
        lanes = [pl.ds(pl.multiple_of(part * width + h * HEAD_PAD, HEAD_PAD), HEAD_PAD) for part in range(3)]
        for i in blocks:
            low, high = max(0, i * BLOCK_SEQ - SPAN), (i + 1) * BLOCK_SEQ
            rows, keys = pl.ds(i * BLOCK_SEQ, BLOCK_SEQ), pl.ds(low, high - low)
            scores = dot_nt(qkv[rows, lanes[0]], qkv[keys, lanes[1]]) + bias_ref[rows, pl.ds(0, high - low)]
            top = jnp.max(scores, -1, keepdims=True)
            expo = jnp.exp((scores - top) * scale)
            probs = expo * (1.0 / jnp.sum(expo, -1, keepdims=True))
            out[rows, lanes[0]] = dot(probs.astype(jnp.bfloat16), qkv[keys, lanes[2]]).astype(jnp.bfloat16)


def layer_kernel(
    x, g, seg, gain_one, gain_two, wq, wk, wv, wo, wup, wdown,
    result_o, input_o, gains_o, sums_o,
    result, input_grad, out_sem, rows, b0, b1, b2, b3, b4, b5, send_sem, recv_sem, save_sem,
    w_up, w_down, w_qkv, w_out, rows_one, rows_g, rows_two, hidden, grad_up, branch, qkv, mixed, grad_mixed,
    cos_ref, sin_ref, bias_ref, resid, term_ref, key_sum, value_sum,
    send_core, recv_core, send_chip, recv_chip, gain_acc, gain_recv,
    load_sem, one_sem, g_sem, two_sem, branch_sem, rs0_sem, rs_sem, rs2_sem, rs3_sem, gain_sem, free_sem, ready_sem,
):
    bf, f32 = jnp.bfloat16, jnp.float32
    ring = Ring4()
    seq, width = rows_two.shape
    units = w_up.shape[1]
    padded = w_out.shape[0]
    heads = padded // HEAD_PAD
    local = heads * HEAD
    pairs = rows.shape[0] // (2 * CHUNK)
    scale = 1.0 / math.sqrt(HEAD)
    half = BLOCK_SEQ // 2
    chip = lax.div(ring.me, 2)
    red = Reducer(rows, (b0, b1, b2, b3, b4, b5), send_sem, recv_sem, pairs)
    barrier = pltpu.get_barrier_semaphore()
    count = greet_mp(ring, barrier) + red.greet(barrier)
    places = [(w, rows.at[pl.ds(i * local, local), :]) for i, w in enumerate((wq, wk, wv, wo))]
    places += [(g, rows_g.at[block_rows(ring.me), :]), (wup, w_up), (wdown, w_down)]
    loads = [pltpu.make_async_copy(source, target, load_sem.at[i]) for i, (source, target) in enumerate(places)]
    for load in loads[:5]:
        load.start()
    normed, _ = norm_rows(x[...].astype(f32))
    rows_one[block_rows(ring.me), :] = (normed * gain_one[...]).astype(bf)
    one, all_g = Gather(ring, rows_one, one_sem, 2), Gather(ring, rows_g, g_sem)
    two, all_branch = Gather(ring, rows_two, two_sem, 2), Gather(ring, branch, branch_sem)
    ahead = Scatter(ring, send_core, recv_core, send_chip, recv_chip, rs0_sem, 2)
    first = Scatter(ring, send_core, recv_core, send_chip, recv_chip, rs_sem)
    second = Scatter(ring, send_core, recv_core, send_chip, recv_chip, rs2_sem)
    third = Scatter(ring, send_core, recv_core, send_chip, recv_chip, rs3_sem)
    pl.semaphore_wait(barrier, count)
    one.start(0)
    one.start(1)
    for load in loads[5:]:
        load.start()

    spread = pad_matrix(local, padded)
    for i in range(3):
        loads[i].wait()
        w_qkv[pl.ds(i * padded, padded), :] = dot(spread, rows[pl.ds(i * local, local), :]).astype(bf)
    loads[3].wait()
    w_out[...] = dot(spread, rows[pl.ds(3 * local, local), :]).astype(bf)
    rotary_into(seg[...], cos_ref, sin_ref)
    qkv_block(rows_one, w_qkv, cos_ref, sin_ref, qkv, ring.me)
    one.near_in()
    qkv_block(rows_one, w_qkv, cos_ref, sin_ref, qkv, ring.core)
    key_sum[...] = segment_columns(seg[...])
    masks_into(seg[...], key_sum, bias_ref)
    loads[4].wait()
    one.forward()
    one.across(0).wait_send()
    one.across(1).wait_send()
    all_g.start()
    qkv_block(rows_one, w_qkv, cos_ref, sin_ref, qkv, ring.chip)
    one.onward_in()
    qkv_block(rows_one, w_qkv, cos_ref, sin_ref, qkv, ring.far)

    early, late = (0, 1), (2, 3)

    @pl.when(chip == 0)
    def _():
        attend(qkv, mixed, bias_ref, heads, scale, late)

    @pl.when(chip == 1)
    def _():
        attend(qkv, mixed, bias_ref, heads, scale, early)

    def term(block, part):
        at = pl.ds(pl.multiple_of(block * BLOCK_SEQ + part * half, half), half)
        return dot(mixed[at, :], w_out[...])

    parts = [pl.ds(p * half, half) for p in range(2)]
    for p in range(2):
        send_core[0, parts[p], :] = term(ring.far, p).astype(bf)
        ahead.far(p).start()
    for p in range(2):
        value = term(ring.chip, p)
        ahead.far(p).wait_recv()
        send_chip[parts[p], :] = (value + recv_core[0, parts[p], :].astype(f32)).astype(bf)
        ahead.chip(p).start()

    @pl.when(chip == 0)
    def _():
        attend(qkv, mixed, bias_ref, heads, scale, early)

    @pl.when(chip == 1)
    def _():
        attend(qkv, mixed, bias_ref, heads, scale, late)

    for p in range(2):
        send_core[1, parts[p], :] = term(ring.core, p).astype(bf)
        ahead.core(p).start()
    all_g.forward()
    for p in range(2):
        resid[parts[p], :] = x[parts[p], :].astype(f32) + term(ring.me, p)
    for p in range(2):
        ahead.core(p).wait_recv()
        ahead.chip(p).wait_recv()
        value = resid[parts[p], :] + recv_core[1, parts[p], :].astype(f32) + recv_chip[parts[p], :].astype(f32)
        resid[parts[p], :] = value
        normed, _ = norm_rows(value)
        at = pl.ds(pl.multiple_of(ring.me * BLOCK_SEQ + p * half, half), half)
        rows_two[at, :] = (normed * gain_two[...]).astype(bf)
        two.start(p)
    for p in range(2):
        ahead.far(p).wait_send()
        ahead.core(p).wait_send()
        ahead.chip(p).wait_send()

    base = 2 * units

    def put(pair):
        at = pl.ds(pl.multiple_of(pair * 2 * CHUNK, 2 * CHUNK), 2 * CHUNK)
        return pltpu.make_async_copy(rows.at[at, :], sums_o.at[at, :], save_sem.at[lax.rem(pair, 4)])

    def slot(index):
        red.slot(index)
        pair = index - (STAGES - 1)

        @pl.when(pair >= 4)
        def _():
            put(pair - 4).wait()

        @pl.when(pair >= 0)
        def _():
            put(pair).start()

    def tile(n):
        return pl.ds(pl.multiple_of(n * 256, 256), 256)

    def up_tile(block, n):
        u = dot(rows_two[block_rows(block), :], w_up[:, tile(n)])
        tangent = jnp.tanh(GELU_C * (u + GELU_K * u * u * u))
        hidden[block_rows(block), tile(n)] = (0.5 * u * (1.0 + tangent)).astype(bf)

    def up_block(block):
        @pl.loop(0, units // 256)
        def _(n):
            up_tile(block, n)

    loads[5].wait()
    up_block(ring.me)
    two.near_in()
    up_block(ring.core)
    all_g.near_in()
    all_g.onward_in()
    two.forward()
    two.onward_in()

    loads[6].wait()

    def order(k):
        there = k < 2
        core = lax.rem(ring.me, 2)
        flip = 1 - lax.rem(k, 2)
        to_chip = jnp.where(there, 1 - chip, chip)
        to_core = jnp.where(flip == 1, 1 - core, core)
        return 2 * to_chip + to_core

    def hand_on(k, scatter, start):
        @pl.when(k == 0)
        def _():
            send_core[0] = term_ref[...].astype(bf)
            scatter.far().start()

        @pl.when(k == 1)
        def _():
            scatter.far().wait_recv()
            send_chip[...] = (term_ref[...] + recv_core[0].astype(f32)).astype(bf)
            scatter.chip().start()

        @pl.when(k == 2)
        def _():
            send_core[1] = term_ref[...].astype(bf)
            scatter.core().start()

        @pl.when(k == 3)
        def _():
            scatter.core().wait_recv()
            term_ref[...] = term_ref[...] + recv_core[1].astype(f32)

    def settle(scatter):
        for copy in (scatter.far(), scatter.core()):
            copy.wait_send()
        scatter.chip().wait()
        return term_ref[...] + recv_chip[...].astype(f32)

    def grad_tile(at, n):
        u = dot(rows_two[at, :], w_up[:, tile(n)])
        upstream = dot_nt(rows_g[at, :], w_down[tile(n), :])
        tangent = jnp.tanh(GELU_C * (u + GELU_K * u * u * u))
        slope = 0.5 * (1.0 + tangent) + 0.5 * u * (1.0 - tangent * tangent) * GELU_C * (1.0 + 3.0 * GELU_K * u * u)
        grad_up[at, tile(n)] = (upstream * slope).astype(bf)

    @pl.loop(0, units // 256)
    def _(n):
        for block in (ring.chip, ring.far):
            up_tile(block, n)
        rows[tile(n), :] = dot_tn(hidden[:, tile(n)], rows_g[...]).astype(bf)
        slot(n)

        @pl.loop(0, 2)
        def _(k):
            grad_tile(block_rows(order(k)), n)

    @pl.loop(0, 4)
    def _(k):
        late = lax.rem(k, 2)

        @pl.loop(0, 3)
        def _(j):
            @pl.when(3 * late + j < units // 256)
            def _():
                grad_tile(block_rows(order(2 + lax.div(k, 2))), 3 * late + j)

        at = block_rows(order(k))

        @pl.loop(0, width // 256)
        def _(n):
            term_ref[:, tile(n)] = dot_nt(grad_up[at, :], w_up[tile(n), :])

        hand_on(k, first, None)
        slot(5 + k)

    def up_rows(i):
        rows[pl.ds(pl.multiple_of(units + i * 256, 256), 256), :] = dot_tn(rows_two[:, tile(i)], grad_up[...]).astype(bf)

    up_rows(0)
    slot(9)
    grad_two = settle(first)
    normed, inverse = norm_rows(resid[...])
    scaled = grad_two * gain_two[...]
    part = inverse * (scaled - normed * jnp.mean(scaled * normed, -1, keepdims=True))
    mlp_part = jnp.sum(grad_two * normed, axis=0, keepdims=True)
    gain_acc[0] = jnp.zeros(gain_acc.shape[1:], f32)
    gain_acc[0, 1:2, :] = mlp_part
    mine = rows_g[block_rows(ring.me), :].astype(f32) + part
    input_grad[...] = mine
    branch[block_rows(ring.me), :] = mine.astype(bf)
    all_branch.across().start()
    all_branch.near().start()
    for device in (ring.core, ring.chip):
        pl.semaphore_signal(ready_sem, inc=1, device_id={"mp": device}, device_id_type=MESH)

    def head_rows(left, lane, right, row):
        value = dot_tn(left[:, lane], right[...])
        halves = [value[at : at + HEAD // 2, :] for at in (0, 64, 128, 192)]
        rows[pl.ds(pl.multiple_of(row, 16), 2 * HEAD), :] = jnp.concatenate(halves, axis=0).astype(bf)

    @pl.loop(1, units // 256)
    def _(i):
        up_rows(i)

        @pl.when(i == 1)
        def _():
            pl.semaphore_wait(ready_sem, 2)

        at = block_rows(order(i - 1))

        @pl.loop(0, width // 256)
        def _(n):
            term_ref[:, tile(n)] = dot(hidden[at, :], w_down[:, tile(n)])

        hand_on(i - 1, second, None)

        @pl.when(i == 4)
        def _():
            all_branch.near().wait_recv()
            all_branch.forward()
            all_branch.onward().wait_recv()

            @pl.loop(0, heads // 2)
            def _(j):
                head_rows(mixed, tile(j), branch, base + j * 2 * HEAD)

        slot(9 + i)

    @pl.loop(0, 4)
    def _(b):
        grad_mixed[block_rows(b), :] = dot_nt(branch[block_rows(b), :], w_out[...]).astype(bf)

    @pl.loop(0, heads)
    def _(h):
        lanes = [pl.ds(pl.multiple_of(n * padded + h * HEAD_PAD, HEAD_PAD), HEAD_PAD) for n in range(3)]
        key_sum[...] = jnp.zeros_like(key_sum)
        value_sum[...] = jnp.zeros_like(value_sum)
        for i in range(seq // BLOCK_SEQ):
            low, high = max(0, i * BLOCK_SEQ - SPAN), (i + 1) * BLOCK_SEQ
            at, keys = pl.ds(i * BLOCK_SEQ, BLOCK_SEQ), pl.ds(low, high - low)
            query, upstream = qkv[at, lanes[0]], grad_mixed[at, lanes[0]]
            scores = dot_nt(query, qkv[keys, lanes[1]]) + bias_ref[at, pl.ds(0, high - low)]
            top = jnp.max(scores, -1, keepdims=True)
            expo = jnp.exp((scores - top) * scale)
            probs = expo * (1.0 / jnp.sum(expo, -1, keepdims=True))
            grad_probs = dot_nt(upstream, qkv[keys, lanes[2]])
            inner = jnp.sum(probs * grad_probs, -1, keepdims=True)
            grad_scores = (probs * (grad_probs - inner)).astype(bf)
            value_sum[keys, :] += dot_tn(probs.astype(bf), upstream)
            key_sum[keys, :] += dot_tn(grad_scores, query)
            turned = dot(grad_scores, qkv[keys, lanes[1]]) * scale
            qkv[at, lanes[0]] = (turned * cos_ref[at, :] - pltpu.roll(turned, 64, 1) * sin_ref[at, :]).astype(bf)
            if i == 1:
                slot(14 + 2 * h)
        turned = key_sum[...] * scale
        qkv[:, lanes[1]] = (turned * cos_ref[...] - pltpu.roll(turned, 64, 1) * sin_ref[...]).astype(bf)
        qkv[:, lanes[2]] = value_sum[...].astype(bf)
        slot(15 + 2 * h)

    @pl.loop(0, 3)
    def _(part):
        for j in range(heads // 2):
            lane = pl.ds(pl.multiple_of(part * padded + j * 256, 256), 256)
            head_rows(qkv, lane, rows_one, base + (part + 1) * local + j * 2 * HEAD)
        slot(22 + part)

    result[...] = (resid[...] + settle(second)).astype(bf)
    for device in (ring.core, ring.chip):
        pl.semaphore_signal(free_sem, inc=1, device_id={"mp": device}, device_id_type=MESH)
    pl.semaphore_wait(free_sem, 2)

    @pl.loop(0, 4)
    def _(k):
        at = block_rows(order(k))

        @pl.loop(0, width // 256)
        def _(n):
            term_ref[:, tile(n)] = dot(qkv[at, :], w_qkv[:, tile(n)])

        hand_on(k, third, None)
        slot(25 + k)

    slot(29)
    grad_one = settle(third)
    normed, inverse = norm_rows(x[...].astype(f32))
    scaled = grad_one * gain_one[...]
    input_grad[...] = input_grad[...] + inverse * (scaled - normed * jnp.mean(scaled * normed, -1, keepdims=True))
    gain_acc[0, 0:1, :] = jnp.sum(grad_one * normed, axis=0, keepdims=True)

    def exchange(step):
        names = ({"mp": ring.core}, {"mp": ring.chip}, {"dp": red.twin}, {"dp": red.mate}, {"dp": red.across})
        return pltpu.make_async_remote_copy(
            src_ref=gain_acc.at[step], dst_ref=gain_recv.at[step], send_sem=gain_sem.at[0, step], recv_sem=gain_sem.at[1, step],
            device_id=names[step], device_id_type=MESH,
        )

    leave = [pltpu.make_async_copy(result, result_o, out_sem.at[0]), pltpu.make_async_copy(input_grad, input_o, out_sem.at[1])]
    last = pairs + STAGES - 1

    @pl.loop(30, last)
    def _(index):
        @pl.when(index == 31)
        def _():
            for copy in leave:
                copy.start()

        for step in range(5):

            @pl.when(index == 30 + step)
            def _():
                if step:
                    exchange(step - 1).wait_recv()
                    gain_acc[step] = gain_acc[step - 1] + gain_recv[step - 1]
                exchange(step).start()

        slot(index)

    exchange(4).wait_recv()
    gains_o[...] = gain_acc[4] + gain_recv[4]
    for pair in range(pairs - 4, pairs):
        put(pair).wait()
    for copy in leave:
        copy.wait()
    for step in range(5):
        exchange(step).wait_send()
    for part in range(2):
        one.near(part).wait_send()
        one.onward(part).wait_send()
    for gather in (all_g, two, all_branch):
        gather.sent()


def layer(x, g, seg, gain_one, gain_two, wq, wk, wv, wo, wup, wdown):
    bf, f32 = jnp.bfloat16, jnp.float32
    own, width = x.shape
    units = wup.shape[1]
    seq = seg.shape[1]
    local = wo.shape[0]
    padded = local // HEAD * HEAD_PAD
    total = 2 * units + 4 * local
    vm, hbm = pl.BlockSpec(memory_space=pltpu.VMEM), pl.BlockSpec(memory_space=pl.ANY)
    sem = pltpu.SemaphoreType.DMA
    shapes = [((own, width), bf), ((own, width), f32), ((8, width), f32), ((total, width), bf)]
    tall = pltpu.VMEM((seq, width), bf)
    return pl.pallas_call(
        layer_kernel,
        out_shape=[jax.ShapeDtypeStruct(s, d) for s, d in shapes],
        in_specs=[vm, hbm, vm, vm, vm] + [hbm] * 6,
        out_specs=[hbm, hbm, vm, hbm],
        scratch_shapes=[pltpu.VMEM((own, width), bf), pltpu.VMEM((own, width), f32), sem((2,)), pltpu.VMEM((total, width), bf)]
        + reducer_scratch(width)
        + [
            sem((4,)),
            pltpu.VMEM((width, units), bf), pltpu.VMEM((units, width), bf), pltpu.VMEM((3 * padded, width), bf), pltpu.VMEM((padded, width), bf),
            tall, tall, tall, pltpu.VMEM((seq, units), bf), pltpu.VMEM((seq, units), bf), tall,
            pltpu.VMEM((seq, 3 * padded), bf), pltpu.VMEM((seq, padded), bf), pltpu.VMEM((seq, padded), bf),
            pltpu.VMEM((seq, 128), f32), pltpu.VMEM((seq, 128), f32), pltpu.VMEM((seq, SPAN + BLOCK_SEQ), bf),
            pltpu.VMEM((own, width), f32), pltpu.VMEM((own, width), f32), pltpu.VMEM((seq, HEAD_PAD), f32), pltpu.VMEM((seq, HEAD_PAD), f32),
            pltpu.VMEM((2, own, width), bf), pltpu.VMEM((2, own, width), bf), pltpu.VMEM((own, width), bf), pltpu.VMEM((own, width), bf),
            pltpu.VMEM((5, 8, width), f32), pltpu.VMEM((5, 8, width), f32),
            sem((7,)), sem((2, 6)), sem((2, 3)), sem((2, 6)), sem((2, 3)), sem((2, 6)), sem((2, 3)), sem((2, 3)), sem((2, 3)), sem((2, 5)),
            pltpu.SemaphoreType.REGULAR, pltpu.SemaphoreType.REGULAR,
        ],
        compiler_params=pltpu.CompilerParams(collective_id=0, has_side_effects=True, vmem_limit_bytes=67043328),
    )(x, g, seg, gain_one, gain_two, wq, wk, wv, wo, wup, wdown)


def finish_kernel(result, input_grad, gains, sums, result_o, input_o, one_o, two_o, down_o, up_o, out_o, q_o, k_o, v_o, inbox, outbox, side_one, side_two, in_sem, out_sem, side_sem):
    step = inbox.shape[1]
    targets = [(t, i * step) for t in (down_o, up_o, out_o, q_o, k_o, v_o) for i in range(t.shape[0] // step)]
    count, depth = len(targets), inbox.shape[0]
    bring = [pltpu.make_async_copy(result, side_one, side_sem.at[0]), pltpu.make_async_copy(input_grad, side_two, side_sem.at[1])]
    take = [pltpu.make_async_copy(side_one, result_o, side_sem.at[2]), pltpu.make_async_copy(side_two, input_o, side_sem.at[3])]

    def read(i):
        return pltpu.make_async_copy(sums.at[pl.ds(i * step, step), :], inbox.at[i % depth], in_sem.at[i % depth])

    def write(i):
        target, at = targets[i]
        return pltpu.make_async_copy(outbox.at[i % depth], target.at[pl.ds(at, step), :], out_sem.at[i % depth])

    for i in range(depth):
        read(i).start()
    for side in bring:
        side.start()
    one_o[...] = gains[0, :]
    two_o[...] = gains[1, :]
    for i in range(count):
        read(i).wait()
        if i >= depth:
            write(i - depth).wait()
        outbox[i % depth] = inbox[i % depth].astype(jnp.float32)
        write(i).start()
        if i + depth < count:
            read(i + depth).start()
        if i == depth:
            for come, go in zip(bring, take):
                come.wait()
                go.start()
    for i in range(count - depth, count):
        write(i).wait()
    for side in take:
        side.wait()


def finish(result, input_grad, gains, sums, units, local):
    bf, f32 = jnp.bfloat16, jnp.float32
    own, width = result.shape
    vm, hbm = pl.BlockSpec(memory_space=pltpu.VMEM), pl.BlockSpec(memory_space=pl.ANY)
    sem = pltpu.SemaphoreType.DMA
    shapes = [((own, width), bf), ((own, width), f32), ((width,), f32), ((width,), f32), ((units, width), f32), ((width, units), f32)] + [((local, width), f32)] * 4
    return pl.pallas_call(
        finish_kernel,
        out_shape=[jax.ShapeDtypeStruct(s, d) for s, d in shapes],
        in_specs=[hbm, hbm, vm, hbm],
        out_specs=[hbm, hbm, vm, vm] + [hbm] * 6,
        scratch_shapes=[pltpu.VMEM((6, local // 2, width), bf), pltpu.VMEM((6, local // 2, width), f32), pltpu.VMEM((own, width), bf), pltpu.VMEM((own, width), f32), sem((6,)), sem((6,)), sem((4,))],
        compiler_params=pltpu.CompilerParams(vmem_limit_bytes=67043328),
    )(result, input_grad, gains, sums)


def on_device(
    hidden_in,
    segment_ids,
    attn_gain,
    query_weight,
    key_weight,
    value_weight,
    out_weight,
    mlp_gain,
    up_weight,
    down_weight,
    out_cotangent,
):
    row_count = segment_ids.shape[0]
    seq_len = segment_ids.shape[1]
    local_width = query_weight.shape[1]
    head_count = local_width // HEAD
    scale = 1.0 / math.sqrt(HEAD)
    block = min(512, seq_len)
    head_shape = (row_count, seq_len, head_count, HEAD)
    x_float = hidden_in.astype(jnp.float32)
    scaled_one, normed_one, inverse_one = normalize(x_float, attn_gain)
    rows_one = lax.all_gather(scaled_one.astype(jnp.bfloat16), "mp", axis=1, tiled=True)
    cosine, sine = rotary_tables(segment_ids, HEAD)
    queries = rotate(project(rows_one, query_weight).reshape(head_shape), cosine, sine).astype(
        jnp.bfloat16
    )
    keys = rotate(project(rows_one, key_weight).reshape(head_shape), cosine, sine).astype(
        jnp.bfloat16
    )
    values = project(rows_one, value_weight).reshape(head_shape).astype(jnp.bfloat16)
    row_index = 0
    mixed_one, log_one = attend_forward(
        queries[row_index], keys[row_index], values[row_index], segment_ids[row_index], scale, block
    )
    mixed_rows = [mixed_one]
    log_rows = [log_one]
    mixed = jnp.stack(mixed_rows, 0).reshape(row_count, seq_len, local_width).astype(jnp.bfloat16)
    attn_share = lax.psum_scatter(project(mixed, out_weight), "mp", scatter_dimension=1, tiled=True)
    resid = x_float + attn_share
    scaled_two, normed_two, inverse_two = normalize(resid, mlp_gain)
    rows_two = lax.all_gather(scaled_two.astype(jnp.bfloat16), "mp", axis=1, tiled=True)
    up_pre = project(rows_two, up_weight)
    hidden = jax.nn.gelu(up_pre, approximate=True).astype(jnp.bfloat16)
    mlp_share = lax.psum_scatter(
        project(hidden, down_weight).astype(jnp.bfloat16), "mp", scatter_dimension=1, tiled=True
    ).astype(jnp.float32)
    result = (resid + mlp_share).astype(jnp.bfloat16)
    grad_top = out_cotangent.astype(jnp.float32)
    grad_rows = lax.all_gather(out_cotangent, "mp", axis=1, tiled=True)
    down_total = weight_grad(hidden, grad_rows)
    grad_hidden = project_back(grad_rows, down_weight)
    grad_up_pre = (grad_hidden * gelu_slope(up_pre)).astype(jnp.bfloat16)
    up_total = weight_grad(rows_two, grad_up_pre)
    grad_two = lax.psum_scatter(
        project_back(grad_up_pre, up_weight), "mp", scatter_dimension=1, tiled=True
    )
    resid_part, mlp_gain_part = norm_back(grad_two, normed_two, inverse_two, mlp_gain)
    grad_resid = grad_top + resid_part
    branch_rows = lax.all_gather(grad_resid.astype(jnp.bfloat16), "mp", axis=1, tiled=True)
    out_total = weight_grad(mixed, branch_rows)
    grad_mixed = project_back(branch_rows, out_weight).astype(jnp.bfloat16).reshape(head_shape)
    row_index = 0
    grad_q, grad_k, grad_v = attend_back(
        queries[row_index],
        keys[row_index],
        values[row_index],
        grad_mixed[row_index],
        log_rows[row_index],
        segment_ids[row_index],
        scale,
        block,
    )
    query_rows = [grad_q]
    key_rows = [grad_k]
    value_rows = [grad_v]
    grad_query = (
        rotate_back(jnp.stack(query_rows, 0), cosine, sine)
        .astype(jnp.bfloat16)
        .reshape(row_count, seq_len, local_width)
    )
    grad_key = (
        rotate_back(jnp.stack(key_rows, 0), cosine, sine)
        .astype(jnp.bfloat16)
        .reshape(row_count, seq_len, local_width)
    )
    grad_value = (
        jnp.stack(value_rows, 0).astype(jnp.bfloat16).reshape(row_count, seq_len, local_width)
    )
    query_total = weight_grad(rows_one, grad_query)
    key_total = weight_grad(rows_one, grad_key)
    value_total = weight_grad(rows_one, grad_value)
    grad_terms = (
        project_back(grad_query, query_weight)
        + project_back(grad_key, key_weight)
        + project_back(grad_value, value_weight)
    )
    grad_one = lax.psum_scatter(grad_terms, "mp", scatter_dimension=1, tiled=True)
    input_part, attn_gain_part = norm_back(grad_one, normed_one, inverse_one, attn_gain)
    input_grad = grad_resid + input_part
    attn_gain_part, mlp_gain_part = lax.psum((attn_gain_part, mlp_gain_part), "mp")
    (
        query_total,
        key_total,
        value_total,
        out_total,
        attn_gain_part,
        mlp_gain_part,
        up_total,
        down_total,
    ) = lax.psum(
        (
            query_total,
            key_total,
            value_total,
            out_total,
            attn_gain_part,
            mlp_gain_part,
            up_total,
            down_total,
        ),
        "dp",
    )
    return (
        result,
        input_grad,
        attn_gain_part,
        query_total,
        key_total,
        value_total,
        out_total,
        mlp_gain_part,
        up_total,
        down_total,
    )


def on_device_kernels(
    hidden_in, segment_ids, attn_gain, query_weight, key_weight, value_weight, out_weight, mlp_gain, up_weight, down_weight, out_cotangent
):
    sums = layer(
        hidden_in[0], out_cotangent[0], segment_ids, attn_gain, mlp_gain,
        query_weight.T, key_weight.T, value_weight.T, out_weight, up_weight, down_weight,
    )
    result, input_grad, one, two, down, up, out, query, key, value = finish(*sums, up_weight.shape[1], out_weight.shape[0])
    return (result[None], input_grad[None], one, query.T, key.T, value.T, out, two, up, down)


def solution(mesh):
    return jax.shard_map(
        on_device_kernels if mesh.shape["dp"] == 8 else on_device,
        mesh=mesh,
        in_specs=(
            P("dp", "mp", None),
            P("dp", None),
            P(),
            P(None, "mp"),
            P(None, "mp"),
            P(None, "mp"),
            P("mp", None),
            P(),
            P(None, "mp"),
            P("mp", None),
            P("dp", "mp", None),
        ),
        out_specs=(
            P("dp", "mp", None),
            P("dp", "mp", None),
            P(),
            P(None, "mp"),
            P(None, "mp"),
            P(None, "mp"),
            P("mp", None),
            P(),
            P(None, "mp"),
            P("mp", None),
        ),
        check_vma=False,
    )
```

```python
import math

import jax
import jax.numpy as jnp
from jax import lax
from jax.experimental import pallas as pl
from jax.experimental.pallas import tpu as pltpu
from jax.sharding import PartitionSpec as P

HEAD = 80


EPS = 1e-06
MASKED = -1e30
GELU_C = math.sqrt(2.0 / math.pi)
GELU_K = 0.044715


def normalize(values, gain):
    inverse = lax.rsqrt(jnp.mean(values * values, -1, keepdims=True) + EPS)
    normed = values * inverse
    return (normed * gain, normed, inverse)


def norm_back(upstream, normed, inverse, gain):
    scaled = upstream * gain
    inner = jnp.mean(scaled * normed, -1, keepdims=True)
    return (inverse * (scaled - normed * inner), jnp.sum(upstream * normed, axis=(0, 1)))


def gelu_slope(values):
    tangent = jnp.tanh(GELU_C * (values + GELU_K * values * values * values))
    return 0.5 * (1.0 + tangent) + 0.5 * values * (1.0 - tangent * tangent) * GELU_C * (
        1.0 + 3.0 * GELU_K * values * values
    )


def project(left, weight):
    return jnp.einsum("rsd,de->rse", left, weight, preferred_element_type=jnp.float32)


def project_back(left, weight):
    return jnp.einsum("rse,de->rsd", left, weight, preferred_element_type=jnp.float32)


def weight_grad(left, right):
    return jnp.einsum("rsd,rse->de", left, right, preferred_element_type=jnp.float32)


def rotary_tables(segments, head_size):
    seq_len = segments.shape[1]
    places = jnp.arange(seq_len, dtype=jnp.int32)
    starts_here = jnp.concatenate(
        [jnp.ones((segments.shape[0], 1), bool), segments[:, 1:] != segments[:, :-1]], axis=1
    )
    first = lax.cummax(jnp.where(starts_here, places[None, :], 0), axis=1)
    position = (places[None, :] - first).astype(jnp.float32)
    half = head_size // 2
    freqs = jnp.exp(jnp.arange(half, dtype=jnp.float32) * (-2.0 * math.log(10000.0) / head_size))
    angles = position[:, :, None] * freqs[None, None, :]
    return (jnp.cos(angles)[:, :, None, :], jnp.sin(angles)[:, :, None, :])


def rotate(values, cosine, sine):
    half = values.shape[-1] // 2
    first, second = (values[..., :half], values[..., half:])
    return jnp.concatenate([first * cosine - second * sine, second * cosine + first * sine], -1)


def rotate_back(grads, cosine, sine):
    half = grads.shape[-1] // 2
    first, second = (grads[..., :half], grads[..., half:])
    return jnp.concatenate([first * cosine + second * sine, second * cosine - first * sine], -1)


def allowed_block(segments_row, start, size):
    seq_len = segments_row.shape[0]
    query_pos = start + jnp.arange(size, dtype=jnp.int32)
    key_pos = jnp.arange(seq_len, dtype=jnp.int32)
    query_seg = segments_row[start : start + size]
    return (query_pos[:, None] >= key_pos[None, :]) & (query_seg[:, None] == segments_row[None, :])


def block_scores(query_block, keys, allowed, scale):
    scores = (
        jnp.einsum("qhd,khd->hqk", query_block, keys, preferred_element_type=jnp.float32) * scale
    )
    return jnp.where(allowed[None], scores, MASKED)


def attend_forward(queries, keys, values, segments_row, scale, block):
    outputs = []
    sums = []
    for start in range(0, queries.shape[0], block):
        allowed = allowed_block(segments_row, start, block)
        scores = block_scores(queries[start : start + block], keys, allowed, scale)
        top = jnp.max(scores, -1, keepdims=True)
        expo = jnp.exp(scores - top)
        total = jnp.sum(expo, -1, keepdims=True)
        probs = (expo / total).astype(jnp.bfloat16)
        outputs.append(
            jnp.einsum("hqk,khd->qhd", probs, values, preferred_element_type=jnp.float32)
        )
        sums.append(top + jnp.log(total))
    return (jnp.concatenate(outputs, 0), jnp.concatenate(sums, 1))


def attend_back(queries, keys, values, grad_mixed, log_sums, segments_row, scale, block):
    key_total = jnp.zeros(keys.shape, jnp.float32)
    value_total = jnp.zeros(values.shape, jnp.float32)
    query_parts = []
    for start in range(0, queries.shape[0], block):
        allowed = allowed_block(segments_row, start, block)
        query_block = queries[start : start + block]
        scores = block_scores(query_block, keys, allowed, scale)
        probs = jnp.exp(scores - log_sums[:, start : start + block])
        grad_block = grad_mixed[start : start + block]
        grad_probs = jnp.einsum(
            "qhd,khd->hqk", grad_block, values, preferred_element_type=jnp.float32
        )
        inner = jnp.sum(probs * grad_probs, -1, keepdims=True)
        grad_scores = (probs * (grad_probs - inner)).astype(jnp.bfloat16)
        query_parts.append(
            jnp.einsum("hqk,khd->qhd", grad_scores, keys, preferred_element_type=jnp.float32)
            * scale
        )
        key_total = (
            key_total
            + jnp.einsum(
                "hqk,qhd->khd", grad_scores, query_block, preferred_element_type=jnp.float32
            )
            * scale
        )
        value_total = value_total + jnp.einsum(
            "hqk,qhd->khd",
            probs.astype(jnp.bfloat16),
            grad_block,
            preferred_element_type=jnp.float32,
        )
    return (jnp.concatenate(query_parts, 0), key_total, value_total)


MESH = pl.DeviceIdType.MESH
CHUNK = 64
SLOTS = 6
STAGES = 6
(R1Z, R2Z, R3Z, FZM, FZA, FZB, R1Y, R2Y, R3Y, FYI, FYY) = range(11)
(S0Z, S0Y, S1Z, S1Y, S2Z, S2Y, S3ZM, S3ZE, S3YE, S3YY, S4Z, S4Y) = range(12)


def add_rows(total_ref, row, count, *others):
    value = total_ref[pl.ds(row, count), :].astype(jnp.float32)
    for other in others:
        value = value + other[...].astype(jnp.float32)
    total_ref[pl.ds(row, count), :] = value.astype(jnp.bfloat16)


class Reducer:
    def __init__(self, rows, bufs, send_sem, recv_sem, pairs):
        self.rows, self.bufs, self.send_sem, self.recv_sem, self.pairs = rows, bufs, send_sem, recv_sem, pairs
        dp = lax.axis_index("dp")
        self.place, self.side = lax.div(dp, 2), lax.rem(dp, 2)
        self.inner = (self.place == 1) | (self.place == 2)
        self.end = jnp.logical_not(self.inner)
        self.mate = 2 * (self.place + 1 - 2 * lax.rem(self.place, 2)) + self.side
        self.across = 2 * (3 - self.place) + self.side
        self.twin = 2 * self.place + 1 - self.side
        self.half_z = lax.div(self.place, 2)
        self.half_y = self.side

    def copy(self, source, target, send, recv, slot, device):
        return pltpu.make_async_remote_copy(
            src_ref=source,
            dst_ref=target,
            send_sem=self.send_sem.at[send, slot],
            recv_sem=self.recv_sem.at[recv, slot],
            device_id={"dp": device},
            device_id_type=MESH,
        )

    def whole_z(self, pair):
        return pl.multiple_of(pair * (2 * CHUNK), CHUNK)

    def at_z(self, pair, half):
        return pl.multiple_of(pair * (2 * CHUNK) + half * (CHUNK // 2), CHUNK // 2)

    def at_y(self, pair, half):
        return pl.multiple_of(pair * (2 * CHUNK) + CHUNK + half * (CHUNK // 2), CHUNK // 2)

    def moves(self, pair):
        slot = lax.rem(pair, SLOTS)
        rows, (one_z, two_z, three_z, one_y, two_y, three_y) = self.rows, self.bufs
        half = CHUNK // 2
        mine_z, mine_y = self.half_z, self.half_y
        own_z = rows.at[pl.ds(self.at_z(pair, mine_z), half), :]
        rest_z = rows.at[pl.ds(self.at_z(pair, 1 - mine_z), half), :]
        own_y = rows.at[pl.ds(self.at_y(pair, mine_y), half), :]
        rest_y = rows.at[pl.ds(self.at_y(pair, 1 - mine_y), half), :]
        all_z = rows.at[pl.ds(self.whole_z(pair), CHUNK), :]
        return dict(
            s0z=lambda: self.copy(all_z, one_z.at[slot], S0Z, R1Z, slot, self.mate),
            s0y=lambda: self.copy(rest_y, one_y.at[slot], S0Y, R1Y, slot, self.twin),
            s1z=lambda: self.copy(rest_z, two_z.at[slot], S1Z, R2Z, slot, self.across),
            s1y=lambda: self.copy(two_y.at[slot], two_y.at[slot], S1Y, R2Y, slot, self.mate),
            s2z=lambda: self.copy(own_z, three_z.at[slot], S2Z, R3Z, slot, self.twin),
            s2y=lambda: self.copy(own_y, three_y.at[slot], S2Y, R3Y, slot, self.across),
            s3zm=lambda: self.copy(own_z, own_z, S3ZM, FZM, slot, self.across),
            s3ze=lambda: self.copy(own_z, own_z, S3ZE, FZA, slot, self.mate),
            s3ye=lambda: self.copy(own_y, own_y, S3YE, FYI, slot, self.mate),
            s3yy=lambda: self.copy(own_y, own_y, S3YY, FYY, slot, self.twin),
            s4z=lambda: self.copy(rest_z, rest_z, S4Z, FZB, slot, self.mate),
            s4y=lambda: self.copy(own_y, own_y, S4Y, FYY, slot, self.twin),
        )

    def when(self, slot_index, stage, role, body):
        pair = slot_index - stage
        live = (pair >= 0) & (pair < self.pairs)
        if role is not None:
            live = live & role

        @pl.when(live)
        def _():
            body(pair)

    def slot(self, index):
        half = CHUNK // 2
        one_z, two_z, three_z, one_y, two_y, three_y = self.bufs

        def last(pair):
            m = self.moves(pair)
            @pl.when(self.end)
            def _():
                m["s3ze"]().wait_recv()
                m["s4z"]().wait_recv()
                m["s1y"]().wait_send()
                m["s4y"]().wait_send()
                m["s4y"]().wait_recv()

            @pl.when(self.inner)
            def _():
                m["s3zm"]().wait_send()
                m["s3ze"]().wait_send()
                m["s3ye"]().wait_send()
                m["s3yy"]().wait_send()
                m["s4z"]().wait_send()
                m["s3yy"]().wait_recv()

        def fourth_inner(pair):
            m = self.moves(pair)
            m["s3zm"]().wait_recv()
            m["s4z"]().start()

        def fourth_end(pair):
            m = self.moves(pair)
            m["s3ye"]().wait_recv()
            m["s4y"]().start()

        def third(pair):
            m = self.moves(pair)
            slot = lax.rem(pair, SLOTS)
            m["s2z"]().wait()
            m["s2y"]().wait()
            add_rows(self.rows, self.at_z(pair, self.half_z), half, three_z.at[slot])
            add_rows(self.rows, self.at_y(pair, self.half_y), half, three_y.at[slot])
            m["s3ze"]().start()
            m["s3zm"]().start()
            m["s3ye"]().start()
            m["s3yy"]().start()

        def second(pair):
            m = self.moves(pair)
            slot = lax.rem(pair, SLOTS)
            m["s1z"]().wait()
            m["s1y"]().wait_recv()
            m["s0y"]().wait_send()
            add_rows(
                self.rows, self.at_z(pair, self.half_z), half,
                one_z.at[slot, pl.ds(pl.multiple_of(self.half_z * half, half), half), :], two_z.at[slot],
            )
            add_rows(self.rows, self.at_y(pair, self.half_y), half, one_y.at[slot], two_y.at[slot])
            m["s2z"]().start()
            m["s2y"]().start()

        def first_inner(pair):
            m = self.moves(pair)
            slot = lax.rem(pair, SLOTS)
            m["s0z"]().wait_recv()
            m["s0y"]().wait_recv()
            other = 1 - self.half_z
            add_rows(
                self.rows, self.at_z(pair, other), half,
                one_z.at[slot, pl.ds(pl.multiple_of(other * half, half), half), :],
            )
            m["s1z"]().start()

        def first_end(pair):
            m = self.moves(pair)
            slot = lax.rem(pair, SLOTS)
            m["s0y"]().wait()
            m["s0z"]().wait_send()
            mine = self.rows[pl.ds(self.at_y(pair, self.half_y), half), :].astype(jnp.float32)
            two_y[slot] = (mine + one_y[slot].astype(jnp.float32)).astype(jnp.bfloat16)
            m["s1y"]().start()

        def start(pair):
            m = self.moves(pair)
            m["s0y"]().start()

            @pl.when(self.end)
            def _():
                m["s0z"]().start()

        self.when(index, 0, None, start)
        self.when(index, 1, self.end, first_end)
        self.when(index, 1, self.inner, first_inner)
        self.when(index, 2, self.inner, second)
        self.when(index, 3, self.inner, third)
        self.when(index, 4, self.inner, fourth_inner)
        self.when(index, 4, self.end, fourth_end)
        self.when(index, 5, None, last)

    def greet(self, barrier):
        for device in (self.mate, self.across, self.twin):
            pl.semaphore_signal(barrier, inc=1, device_id={"dp": device}, device_id_type=MESH)
        return 3


def reducer_scratch(width):
    half = CHUNK // 2
    return [
        pltpu.VMEM((SLOTS, CHUNK, width), jnp.bfloat16),
        pltpu.VMEM((SLOTS, half, width), jnp.bfloat16),
        pltpu.VMEM((SLOTS, half, width), jnp.bfloat16),
        pltpu.VMEM((SLOTS, half, width), jnp.bfloat16),
        pltpu.VMEM((SLOTS, half, width), jnp.bfloat16),
        pltpu.VMEM((SLOTS, half, width), jnp.bfloat16),
        pltpu.SemaphoreType.DMA((12, SLOTS)),
        pltpu.SemaphoreType.DMA((11, SLOTS)),
    ]


HEAD_PAD = 128
BLOCK_SEQ = 256
SPAN = 512


def pad_matrix(local, padded):
    shape = (padded, local)
    feature = lax.broadcasted_iota(jnp.int32, shape, 1)
    lane = lax.broadcasted_iota(jnp.int32, shape, 0)
    head = jnp.zeros(shape, jnp.int32)
    for h in range(1, local // HEAD):
        head = head + (feature >= h * HEAD).astype(jnp.int32)
    within = feature - head * HEAD
    target = head * HEAD_PAD + within + jnp.where(within >= HEAD // 2, HEAD_PAD // 2 - HEAD // 2, 0)
    return jnp.where(lane == target, 1.0, 0.0).astype(jnp.bfloat16)


def dot(a, b):
    return jnp.dot(a, b, preferred_element_type=jnp.float32)


def dot_nt(a, b):
    return lax.dot_general(a, b, (((1,), (1,)), ((), ())), preferred_element_type=jnp.float32)


def dot_tn(a, b):
    return lax.dot_general(a, b, (((0,), (0,)), ((), ())), preferred_element_type=jnp.float32)


def segment_columns(seg):
    lines = jnp.broadcast_to(seg.astype(jnp.float32), (16, seg.shape[1])).astype(jnp.bfloat16)
    pick = (lax.broadcasted_iota(jnp.int32, (16, 128), 0) == 0).astype(jnp.float32).astype(jnp.bfloat16)
    return dot_tn(lines, pick)


def rotary_into(seg, cos_ref, sin_ref):
    seq = seg.shape[1]
    ids = segment_columns(seg)
    first = jnp.zeros((seq, 128), jnp.float32)
    row = seg.astype(jnp.float32)
    for s in range(1, 16):
        before = jnp.sum(jnp.where(row < s, 1.0, 0.0), axis=1, keepdims=True)
        first = jnp.where(ids == s, before, first)
    position = lax.broadcasted_iota(jnp.int32, (seq, 128), 0).astype(jnp.float32) - first
    lane = lax.broadcasted_iota(jnp.int32, (1, 128), 1)
    upper = lane >= HEAD_PAD // 2
    index = jnp.where(upper, lane - HEAD_PAD // 2, lane)
    freqs = jnp.exp(index.astype(jnp.float32) * (-2.0 * math.log(10000.0) / HEAD))
    freqs = jnp.where(index < HEAD // 2, freqs, 0.0)
    angles = position * freqs
    cos_ref[...] = jnp.cos(angles)
    sin_ref[...] = jnp.where(upper, jnp.sin(angles), -jnp.sin(angles))


class Ring4:
    def __init__(self):
        mp = lax.axis_index("mp")
        chip, core = lax.div(mp, 2), lax.rem(mp, 2)
        self.me = mp
        self.core = 2 * chip + 1 - core
        self.chip = 2 * (1 - chip) + core
        self.far = 2 * (1 - chip) + 1 - core


def block_rows(index):
    return pl.ds(pl.multiple_of(index * BLOCK_SEQ, BLOCK_SEQ), BLOCK_SEQ)


class Gather:
    def __init__(self, ring, rows, sems, parts=1):
        self.parts = parts
        size = BLOCK_SEQ // parts

        def copy(block, device, which, part):
            at = pl.ds(pl.multiple_of(block * BLOCK_SEQ + part * size, size), size)
            return pltpu.make_async_remote_copy(
                src_ref=rows.at[at, :],
                dst_ref=rows.at[at, :],
                send_sem=sems.at[0, which * parts + part],
                recv_sem=sems.at[1, which * parts + part],
                device_id={"mp": device},
                device_id_type=MESH,
            )

        self.near = lambda part=0: copy(ring.me, ring.core, 0, part)
        self.across = lambda part=0: copy(ring.me, ring.chip, 1, part)
        self.onward = lambda part=0: copy(ring.chip, ring.core, 2, part)

    def start(self, part=0):
        self.across(part).start()
        self.near(part).start()

    def forward(self):
        for part in range(self.parts):
            self.across(part).wait_recv()
            self.onward(part).start()

    def near_in(self):
        for part in range(self.parts):
            self.near(part).wait_recv()

    def onward_in(self):
        for part in range(self.parts):
            self.onward(part).wait_recv()

    def sent(self):
        for part in range(self.parts):
            self.near(part).wait_send()
            self.across(part).wait_send()
            self.onward(part).wait_send()


class Scatter:
    def __init__(self, ring, send_core, recv_core, send_chip, recv_chip, sems, parts=1):
        self.parts = parts
        size = BLOCK_SEQ // parts

        def copy(source, target, device, which, part):
            at = pl.ds(part * size, size)
            return pltpu.make_async_remote_copy(
                src_ref=source.at[at, :],
                dst_ref=target.at[at, :],
                send_sem=sems.at[0, which * parts + part],
                recv_sem=sems.at[1, which * parts + part],
                device_id={"mp": device},
                device_id_type=MESH,
            )

        self.far = lambda part=0: copy(send_core.at[0], recv_core.at[0], ring.core, 0, part)
        self.core = lambda part=0: copy(send_core.at[1], recv_core.at[1], ring.core, 1, part)
        self.chip = lambda part=0: copy(send_chip, recv_chip, ring.chip, 2, part)


def greet_mp(ring, barrier):
    for device in (ring.core, ring.chip):
        pl.semaphore_signal(barrier, inc=1, device_id={"mp": device}, device_id_type=MESH)
    return 2


def norm_rows(values):
    inverse = lax.rsqrt(jnp.mean(values * values, -1, keepdims=True) + EPS)
    return values * inverse, inverse


def qkv_block(rows, weights, cos_ref, sin_ref, out, block):
    at = block_rows(block)
    turned = 2 * (weights.shape[0] // 3) // 256
    tiles = weights.shape[0] // 256

    def one(n, turn):
        cols = pl.ds(pl.multiple_of(n * 256, 256), 256)
        value = dot_nt(rows[at, :], weights[cols, :])
        if turn:
            cosine, sine = cos_ref[at, :], sin_ref[at, :]
            halves = [value[:, j * 128 : j * 128 + 128] for j in range(2)]
            value = jnp.concatenate([h * cosine + pltpu.roll(h, 64, 1) * sine for h in halves], axis=1)
        out[at, cols] = value.astype(jnp.bfloat16)

    @pl.loop(0, turned)
    def _(n):
        one(n, True)

    @pl.loop(turned, tiles)
    def _(n):
        one(n, False)


def masks_into(seg, ids_ref, bias_ref):
    seq = seg.shape[1]
    for i in range(seq // BLOCK_SEQ):
        low = max(0, i * BLOCK_SEQ - SPAN)
        high = (i + 1) * BLOCK_SEQ
        shape = (BLOCK_SEQ, high - low)
        query = i * BLOCK_SEQ + lax.broadcasted_iota(jnp.int32, shape, 0)
        key = low + lax.broadcasted_iota(jnp.int32, shape, 1)
        ids = ids_ref[pl.ds(i * BLOCK_SEQ, BLOCK_SEQ), :][:, :1]
        same = ids == seg[:, low:high].astype(jnp.float32)
        bias_ref[pl.ds(i * BLOCK_SEQ, BLOCK_SEQ), pl.ds(0, high - low)] = jnp.where((query >= key) & same, 0.0, MASKED).astype(bias_ref.dtype)


def attend(qkv, out, bias_ref, heads, scale, blocks):
    width = heads * HEAD_PAD

    @pl.loop(0, heads)
    def _(h):
        lanes = [pl.ds(pl.multiple_of(part * width + h * HEAD_PAD, HEAD_PAD), HEAD_PAD) for part in range(3)]
        for i in blocks:
            low, high = max(0, i * BLOCK_SEQ - SPAN), (i + 1) * BLOCK_SEQ
            rows, keys = pl.ds(i * BLOCK_SEQ, BLOCK_SEQ), pl.ds(low, high - low)
            scores = dot_nt(qkv[rows, lanes[0]], qkv[keys, lanes[1]]) + bias_ref[rows, pl.ds(0, high - low)]
            top = jnp.max(scores, -1, keepdims=True)
            expo = jnp.exp((scores - top) * scale)
            probs = expo * (1.0 / jnp.sum(expo, -1, keepdims=True))
            out[rows, lanes[0]] = dot(probs.astype(jnp.bfloat16), qkv[keys, lanes[2]]).astype(jnp.bfloat16)


def layer_kernel(
    x, g, seg, gain_one, gain_two, wq, wk, wv, wo, wup, wdown,
    result_o, input_o, gains_o, sums_o,
    rows, b0, b1, b2, b3, b4, b5, send_sem, recv_sem, save_sem,
    w_up, w_down, w_qkv, w_out, rows_one, rows_g, rows_two, hidden, grad_up, branch, qkv, mixed, grad_mixed,
    cos_ref, sin_ref, bias_ref, resid, term_ref, key_sum, value_sum,
    send_core, recv_core, send_chip, recv_chip, gain_acc, gain_recv,
    load_sem, one_sem, g_sem, two_sem, branch_sem, rs0_sem, rs_sem, rs2_sem, rs3_sem, gain_sem, free_sem, ready_sem,
):
    bf, f32 = jnp.bfloat16, jnp.float32
    ring = Ring4()
    seq, width = rows_two.shape
    units = w_up.shape[1]
    padded = w_out.shape[0]
    heads = padded // HEAD_PAD
    local = heads * HEAD
    pairs = rows.shape[0] // (2 * CHUNK)
    scale = 1.0 / math.sqrt(HEAD)
    half = BLOCK_SEQ // 2
    chip = lax.div(ring.me, 2)
    red = Reducer(rows, (b0, b1, b2, b3, b4, b5), send_sem, recv_sem, pairs)
    barrier = pltpu.get_barrier_semaphore()
    count = greet_mp(ring, barrier) + red.greet(barrier)
    places = [(w, rows.at[pl.ds(i * local, local), :]) for i, w in enumerate((wq, wk, wv, wo))]
    places += [(g, rows_g.at[block_rows(ring.me), :]), (wup, w_up), (wdown, w_down)]
    loads = [pltpu.make_async_copy(source, target, load_sem.at[i]) for i, (source, target) in enumerate(places)]
    for load in loads[:5]:
        load.start()
    normed, _ = norm_rows(x[...].astype(f32))
    rows_one[block_rows(ring.me), :] = (normed * gain_one[...]).astype(bf)
    one, all_g = Gather(ring, rows_one, one_sem, 2), Gather(ring, rows_g, g_sem)
    two, all_branch = Gather(ring, rows_two, two_sem, 2), Gather(ring, branch, branch_sem)
    ahead = Scatter(ring, send_core, recv_core, send_chip, recv_chip, rs0_sem, 2)
    first = Scatter(ring, send_core, recv_core, send_chip, recv_chip, rs_sem)
    second = Scatter(ring, send_core, recv_core, send_chip, recv_chip, rs2_sem)
    third = Scatter(ring, send_core, recv_core, send_chip, recv_chip, rs3_sem)
    pl.semaphore_wait(barrier, count)
    one.start(0)
    one.start(1)
    for load in loads[5:]:
        load.start()

    spread = pad_matrix(local, padded)
    for i in range(3):
        loads[i].wait()
        w_qkv[pl.ds(i * padded, padded), :] = dot(spread, rows[pl.ds(i * local, local), :]).astype(bf)
    loads[3].wait()
    w_out[...] = dot(spread, rows[pl.ds(3 * local, local), :]).astype(bf)
    rotary_into(seg[...], cos_ref, sin_ref)
    qkv_block(rows_one, w_qkv, cos_ref, sin_ref, qkv, ring.me)
    one.near_in()
    qkv_block(rows_one, w_qkv, cos_ref, sin_ref, qkv, ring.core)
    key_sum[...] = segment_columns(seg[...])
    masks_into(seg[...], key_sum, bias_ref)
    loads[4].wait()
    one.forward()
    one.across(0).wait_send()
    one.across(1).wait_send()
    all_g.start()
    qkv_block(rows_one, w_qkv, cos_ref, sin_ref, qkv, ring.chip)
    one.onward_in()
    qkv_block(rows_one, w_qkv, cos_ref, sin_ref, qkv, ring.far)

    early, late = (0, 1), (2, 3)

    @pl.when(chip == 0)
    def _():
        attend(qkv, mixed, bias_ref, heads, scale, late)

    @pl.when(chip == 1)
    def _():
        attend(qkv, mixed, bias_ref, heads, scale, early)

    def term(block, part):
        at = pl.ds(pl.multiple_of(block * BLOCK_SEQ + part * half, half), half)
        return dot(mixed[at, :], w_out[...])

    parts = [pl.ds(p * half, half) for p in range(2)]
    for p in range(2):
        send_core[0, parts[p], :] = term(ring.far, p).astype(bf)
        ahead.far(p).start()
    for p in range(2):
        value = term(ring.chip, p)
        ahead.far(p).wait_recv()
        send_chip[parts[p], :] = (value + recv_core[0, parts[p], :].astype(f32)).astype(bf)
        ahead.chip(p).start()

    @pl.when(chip == 0)
    def _():
        attend(qkv, mixed, bias_ref, heads, scale, early)

    @pl.when(chip == 1)
    def _():
        attend(qkv, mixed, bias_ref, heads, scale, late)

    for p in range(2):
        send_core[1, parts[p], :] = term(ring.core, p).astype(bf)
        ahead.core(p).start()
    all_g.forward()
    for p in range(2):
        resid[parts[p], :] = x[parts[p], :].astype(f32) + term(ring.me, p)
    for p in range(2):
        ahead.core(p).wait_recv()
        ahead.chip(p).wait_recv()
        value = resid[parts[p], :] + recv_core[1, parts[p], :].astype(f32) + recv_chip[parts[p], :].astype(f32)
        resid[parts[p], :] = value
        normed, _ = norm_rows(value)
        at = pl.ds(pl.multiple_of(ring.me * BLOCK_SEQ + p * half, half), half)
        rows_two[at, :] = (normed * gain_two[...]).astype(bf)
        two.start(p)
    for p in range(2):
        ahead.far(p).wait_send()
        ahead.core(p).wait_send()
        ahead.chip(p).wait_send()

    base = 2 * units

    def put(pair):
        at = pl.ds(pl.multiple_of(pair * 2 * CHUNK, 2 * CHUNK), 2 * CHUNK)
        return pltpu.make_async_copy(rows.at[at, :], sums_o.at[at, :], save_sem.at[lax.rem(pair, 4)])

    def slot(index):
        red.slot(index)
        pair = index - (STAGES - 1)

        @pl.when(pair >= 4)
        def _():
            put(pair - 4).wait()

        @pl.when(pair >= 0)
        def _():
            put(pair).start()

    def tile(n):
        return pl.ds(pl.multiple_of(n * 256, 256), 256)

    def up_tile(block, n):
        u = dot(rows_two[block_rows(block), :], w_up[:, tile(n)])
        tangent = jnp.tanh(GELU_C * (u + GELU_K * u * u * u))
        hidden[block_rows(block), tile(n)] = (0.5 * u * (1.0 + tangent)).astype(bf)

    def up_block(block):
        @pl.loop(0, units // 256)
        def _(n):
            up_tile(block, n)

    loads[5].wait()
    up_block(ring.me)
    two.near_in()
    up_block(ring.core)
    all_g.near_in()
    all_g.onward_in()
    two.forward()
    two.onward_in()

    loads[6].wait()

    def order(k):
        there = k < 2
        core = lax.rem(ring.me, 2)
        flip = 1 - lax.rem(k, 2)
        to_chip = jnp.where(there, 1 - chip, chip)
        to_core = jnp.where(flip == 1, 1 - core, core)
        return 2 * to_chip + to_core

    def hand_on(k, scatter, start):
        @pl.when(k == 0)
        def _():
            send_core[0] = term_ref[...].astype(bf)
            scatter.far().start()

        @pl.when(k == 1)
        def _():
            scatter.far().wait_recv()
            send_chip[...] = (term_ref[...] + recv_core[0].astype(f32)).astype(bf)
            scatter.chip().start()

        @pl.when(k == 2)
        def _():
            send_core[1] = term_ref[...].astype(bf)
            scatter.core().start()

        @pl.when(k == 3)
        def _():
            scatter.core().wait_recv()
            term_ref[...] = term_ref[...] + recv_core[1].astype(f32)

    def settle(scatter):
        for copy in (scatter.far(), scatter.core()):
            copy.wait_send()
        scatter.chip().wait()
        return term_ref[...] + recv_chip[...].astype(f32)

    def grad_tile(at, n):
        u = dot(rows_two[at, :], w_up[:, tile(n)])
        upstream = dot_nt(rows_g[at, :], w_down[tile(n), :])
        tangent = jnp.tanh(GELU_C * (u + GELU_K * u * u * u))
        slope = 0.5 * (1.0 + tangent) + 0.5 * u * (1.0 - tangent * tangent) * GELU_C * (1.0 + 3.0 * GELU_K * u * u)
        grad_up[at, tile(n)] = (upstream * slope).astype(bf)

    @pl.loop(0, units // 256)
    def _(n):
        for block in (ring.chip, ring.far):
            up_tile(block, n)
        rows[tile(n), :] = dot_tn(hidden[:, tile(n)], rows_g[...]).astype(bf)
        slot(n)

        @pl.loop(0, 3)
        def _(k):
            grad_tile(block_rows(order(k)), n)

    def up_rows(i):
        rows[pl.ds(pl.multiple_of(units + i * 256, 256), 256), :] = dot_tn(rows_two[:, tile(i)], grad_up[...]).astype(bf)

    @pl.loop(0, 4)
    def _(k):
        @pl.loop(0, 2)
        def _(j):
            @pl.when(2 * k + j < units // 256)
            def _():
                grad_tile(block_rows(order(3)), 2 * k + j)

        at = block_rows(order(k))

        @pl.loop(0, width // 256)
        def _(n):
            term_ref[:, tile(n)] = dot_nt(grad_up[at, :], w_up[tile(n), :])

        hand_on(k, first, None)

        @pl.when(k == 3)
        def _():
            up_rows(0)

        slot(5 + k)

    @pl.loop(1, 3)
    def _(i):
        up_rows(i)

    slot(9)
    grad_two = settle(first)
    normed, inverse = norm_rows(resid[...])
    scaled = grad_two * gain_two[...]
    part = inverse * (scaled - normed * jnp.mean(scaled * normed, -1, keepdims=True))
    mlp_part = jnp.sum(grad_two * normed, axis=0, keepdims=True)
    gain_acc[0] = jnp.zeros(gain_acc.shape[1:], f32)
    gain_acc[0, 1:2, :] = mlp_part
    mine = rows_g[block_rows(ring.me), :].astype(f32) + part
    input_o[...] = mine
    branch[block_rows(ring.me), :] = mine.astype(bf)
    all_branch.across().start()
    all_branch.near().start()
    for device in (ring.core, ring.chip):
        pl.semaphore_signal(ready_sem, inc=1, device_id={"mp": device}, device_id_type=MESH)

    def head_rows(left, lane, right, row):
        value = dot_tn(left[:, lane], right[...])
        halves = [value[at : at + HEAD // 2, :] for at in (0, 64, 128, 192)]
        rows[pl.ds(pl.multiple_of(row, 16), 2 * HEAD), :] = jnp.concatenate(halves, axis=0).astype(bf)

    @pl.loop(1, 5)
    def _(i):
        @pl.when(i <= 2)
        def _():
            up_rows(2 + i)

        @pl.when(i == 1)
        def _():
            pl.semaphore_wait(ready_sem, 2)

        @pl.loop(0, 2)
        def _(j):
            @pl.when(((j == 0) & (i <= 3)) | (i == 3))
            def _():
                at = block_rows(order(i - 1 + j))

                @pl.loop(0, width // 256)
                def _(n):
                    term_ref[:, tile(n)] = dot(hidden[at, :], w_down[:, tile(n)])

                hand_on(i - 1 + j, second, None)

        @pl.when(i == 4)
        def _():
            all_branch.near().wait_recv()
            all_branch.forward()
            all_branch.onward().wait_recv()

            @pl.loop(0, heads // 2)
            def _(j):
                head_rows(mixed, tile(j), branch, base + j * 2 * HEAD)

            @pl.loop(0, 4)
            def _(b):
                grad_mixed[block_rows(b), :] = dot_nt(branch[block_rows(b), :], w_out[...]).astype(bf)

        slot(9 + i)

    @pl.loop(0, heads)
    def _(h):
        lanes = [pl.ds(pl.multiple_of(n * padded + h * HEAD_PAD, HEAD_PAD), HEAD_PAD) for n in range(3)]
        key_sum[...] = jnp.zeros_like(key_sum)
        value_sum[...] = jnp.zeros_like(value_sum)
        for step, i in enumerate((1, 2, 0, 3)):
            low, high = max(0, i * BLOCK_SEQ - SPAN), (i + 1) * BLOCK_SEQ
            at, keys = pl.ds(i * BLOCK_SEQ, BLOCK_SEQ), pl.ds(low, high - low)
            query, upstream = qkv[at, lanes[0]], grad_mixed[at, lanes[0]]
            scores = dot_nt(query, qkv[keys, lanes[1]]) + bias_ref[at, pl.ds(0, high - low)]
            top = jnp.max(scores, -1, keepdims=True)
            expo = jnp.exp((scores - top) * scale)
            probs = expo * (1.0 / jnp.sum(expo, -1, keepdims=True))
            grad_probs = dot_nt(upstream, qkv[keys, lanes[2]])
            inner = jnp.sum(probs * grad_probs, -1, keepdims=True)
            grad_scores = (probs * (grad_probs - inner)).astype(bf)
            value_sum[keys, :] += dot_tn(probs.astype(bf), upstream)
            key_sum[keys, :] += dot_tn(grad_scores, query)
            turned = dot(grad_scores, qkv[keys, lanes[1]]) * scale
            qkv[at, lanes[0]] = (turned * cos_ref[at, :] - pltpu.roll(turned, 64, 1) * sin_ref[at, :]).astype(bf)
            if step == 1:
                slot(14 + 2 * h)
        turned = key_sum[...] * scale
        qkv[:, lanes[1]] = (turned * cos_ref[...] - pltpu.roll(turned, 64, 1) * sin_ref[...]).astype(bf)
        qkv[:, lanes[2]] = value_sum[...].astype(bf)
        slot(15 + 2 * h)

    @pl.loop(0, 3)
    def _(part):
        for j in range(heads // 2):
            lane = pl.ds(pl.multiple_of(part * padded + j * 256, 256), 256)
            head_rows(qkv, lane, rows_one, base + (part + 1) * local + j * 2 * HEAD)
        slot(22 + part)

    result_o[...] = (resid[...] + settle(second)).astype(bf)
    for device in (ring.core, ring.chip):
        pl.semaphore_signal(free_sem, inc=1, device_id={"mp": device}, device_id_type=MESH)
    pl.semaphore_wait(free_sem, 2)

    @pl.loop(0, 4)
    def _(k):
        at = block_rows(order(k))

        @pl.loop(0, width // 256)
        def _(n):
            term_ref[:, tile(n)] = dot(qkv[at, :], w_qkv[:, tile(n)])

        hand_on(k, third, None)
        slot(25 + k)

    slot(29)
    grad_one = settle(third)
    normed, inverse = norm_rows(x[...].astype(f32))
    scaled = grad_one * gain_one[...]
    input_o[...] = input_o[...] + inverse * (scaled - normed * jnp.mean(scaled * normed, -1, keepdims=True))
    gain_acc[0, 0:1, :] = jnp.sum(grad_one * normed, axis=0, keepdims=True)

    def exchange(step):
        names = ({"mp": ring.core}, {"mp": ring.chip}, {"dp": red.twin}, {"dp": red.mate}, {"dp": red.across})
        return pltpu.make_async_remote_copy(
            src_ref=gain_acc.at[step], dst_ref=gain_recv.at[step], send_sem=gain_sem.at[0, step], recv_sem=gain_sem.at[1, step],
            device_id=names[step], device_id_type=MESH,
        )

    last = pairs + STAGES - 1

    @pl.loop(30, last)
    def _(index):
        for step in range(5):

            @pl.when(index == 30 + step)
            def _():
                if step:
                    exchange(step - 1).wait_recv()
                    gain_acc[step] = gain_acc[step - 1] + gain_recv[step - 1]
                exchange(step).start()

        slot(index)

    exchange(4).wait_recv()
    gains_o[...] = gain_acc[4] + gain_recv[4]
    for pair in range(pairs - 4, pairs):
        put(pair).wait()
    for step in range(5):
        exchange(step).wait_send()
    for part in range(2):
        one.near(part).wait_send()
        one.onward(part).wait_send()
    for gather in (all_g, two, all_branch):
        gather.sent()


def layer(x, g, seg, gain_one, gain_two, wq, wk, wv, wo, wup, wdown):
    bf, f32 = jnp.bfloat16, jnp.float32
    own, width = x.shape
    units = wup.shape[1]
    seq = seg.shape[1]
    local = wo.shape[0]
    padded = local // HEAD * HEAD_PAD
    total = 2 * units + 4 * local
    vm, hbm = pl.BlockSpec(memory_space=pltpu.VMEM), pl.BlockSpec(memory_space=pl.ANY)
    sem = pltpu.SemaphoreType.DMA
    shapes = [((own, width), bf), ((own, width), f32), ((8, width), f32), ((total, width), bf)]
    tall = pltpu.VMEM((seq, width), bf)
    return pl.pallas_call(
        layer_kernel,
        out_shape=[jax.ShapeDtypeStruct(s, d) for s, d in shapes],
        in_specs=[vm, hbm, vm, vm, vm] + [hbm] * 6,
        out_specs=[vm] * 3 + [hbm],
        scratch_shapes=[pltpu.VMEM((total, width), bf)]
        + reducer_scratch(width)
        + [
            sem((4,)),
            pltpu.VMEM((width, units), bf), pltpu.VMEM((units, width), bf), pltpu.VMEM((3 * padded, width), bf), pltpu.VMEM((padded, width), bf),
            tall, tall, tall, pltpu.VMEM((seq, units), bf), pltpu.VMEM((seq, units), bf), tall,
            pltpu.VMEM((seq, 3 * padded), bf), pltpu.VMEM((seq, padded), bf), pltpu.VMEM((seq, padded), bf),
            pltpu.VMEM((seq, 128), f32), pltpu.VMEM((seq, 128), f32), pltpu.VMEM((seq, SPAN + BLOCK_SEQ), bf),
            pltpu.VMEM((own, width), f32), pltpu.VMEM((own, width), f32), pltpu.VMEM((seq, HEAD_PAD), f32), pltpu.VMEM((seq, HEAD_PAD), f32),
            pltpu.VMEM((2, own, width), bf), pltpu.VMEM((2, own, width), bf), pltpu.VMEM((own, width), bf), pltpu.VMEM((own, width), bf),
            pltpu.VMEM((5, 8, width), f32), pltpu.VMEM((5, 8, width), f32),
            sem((7,)), sem((2, 6)), sem((2, 3)), sem((2, 6)), sem((2, 3)), sem((2, 6)), sem((2, 3)), sem((2, 3)), sem((2, 3)), sem((2, 5)),
            pltpu.SemaphoreType.REGULAR, pltpu.SemaphoreType.REGULAR,
        ],
        compiler_params=pltpu.CompilerParams(collective_id=0, has_side_effects=True, vmem_limit_bytes=67043328),
    )(x, g, seg, gain_one, gain_two, wq, wk, wv, wo, wup, wdown)


def finish_kernel(result, input_grad, gains, sums, result_o, input_o, one_o, two_o, down_o, up_o, out_o, q_o, k_o, v_o, inbox, outbox, side_one, side_two, in_sem, out_sem, side_sem):
    step = out_o.shape[0]
    targets = [(down_o, i * step) for i in range(down_o.shape[0] // step)] + [(up_o, i * step) for i in range(up_o.shape[0] // step)]
    targets += [(t, 0) for t in (out_o, q_o, k_o, v_o)]
    count, depth = len(targets), inbox.shape[0]
    bring = [pltpu.make_async_copy(result, side_one, side_sem.at[0]), pltpu.make_async_copy(input_grad, side_two, side_sem.at[1])]
    take = [pltpu.make_async_copy(side_one, result_o, side_sem.at[2]), pltpu.make_async_copy(side_two, input_o, side_sem.at[3])]

    def read(i):
        return pltpu.make_async_copy(sums.at[pl.ds(i * step, step), :], inbox.at[i % depth], in_sem.at[i % depth])

    def write(i):
        target, at = targets[i]
        return pltpu.make_async_copy(outbox.at[i % depth], target.at[pl.ds(at, step), :], out_sem.at[i % depth])

    for i in range(depth):
        read(i).start()
    for side in bring:
        side.start()
    one_o[...] = gains[0, :]
    two_o[...] = gains[1, :]
    for i in range(count):
        read(i).wait()
        if i >= depth:
            write(i - depth).wait()
        outbox[i % depth] = inbox[i % depth].astype(jnp.float32)
        write(i).start()
        if i + depth < count:
            read(i + depth).start()
        if i == depth:
            for come, go in zip(bring, take):
                come.wait()
                go.start()
    for i in range(count - depth, count):
        write(i).wait()
    for side in take:
        side.wait()


def finish(result, input_grad, gains, sums, units, local):
    bf, f32 = jnp.bfloat16, jnp.float32
    own, width = result.shape
    vm, hbm = pl.BlockSpec(memory_space=pltpu.VMEM), pl.BlockSpec(memory_space=pl.ANY)
    sem = pltpu.SemaphoreType.DMA
    shapes = [((own, width), bf), ((own, width), f32), ((width,), f32), ((width,), f32), ((units, width), f32), ((width, units), f32)] + [((local, width), f32)] * 4
    return pl.pallas_call(
        finish_kernel,
        out_shape=[jax.ShapeDtypeStruct(s, d) for s, d in shapes],
        in_specs=[hbm, hbm, vm, hbm],
        out_specs=[hbm, hbm, vm, vm] + [hbm] * 6,
        scratch_shapes=[pltpu.VMEM((3, local, width), bf), pltpu.VMEM((3, local, width), f32), pltpu.VMEM((own, width), bf), pltpu.VMEM((own, width), f32), sem((3,)), sem((3,)), sem((4,))],
        compiler_params=pltpu.CompilerParams(vmem_limit_bytes=67043328),
    )(result, input_grad, gains, sums)


def on_device(
    hidden_in,
    segment_ids,
    attn_gain,
    query_weight,
    key_weight,
    value_weight,
    out_weight,
    mlp_gain,
    up_weight,
    down_weight,
    out_cotangent,
):
    row_count = segment_ids.shape[0]
    seq_len = segment_ids.shape[1]
    local_width = query_weight.shape[1]
    head_count = local_width // HEAD
    scale = 1.0 / math.sqrt(HEAD)
    block = min(512, seq_len)
    head_shape = (row_count, seq_len, head_count, HEAD)
    x_float = hidden_in.astype(jnp.float32)
    scaled_one, normed_one, inverse_one = normalize(x_float, attn_gain)
    rows_one = lax.all_gather(scaled_one.astype(jnp.bfloat16), "mp", axis=1, tiled=True)
    cosine, sine = rotary_tables(segment_ids, HEAD)
    queries = rotate(project(rows_one, query_weight).reshape(head_shape), cosine, sine).astype(
        jnp.bfloat16
    )
    keys = rotate(project(rows_one, key_weight).reshape(head_shape), cosine, sine).astype(
        jnp.bfloat16
    )
    values = project(rows_one, value_weight).reshape(head_shape).astype(jnp.bfloat16)
    row_index = 0
    mixed_one, log_one = attend_forward(
        queries[row_index], keys[row_index], values[row_index], segment_ids[row_index], scale, block
    )
    mixed_rows = [mixed_one]
    log_rows = [log_one]
    mixed = jnp.stack(mixed_rows, 0).reshape(row_count, seq_len, local_width).astype(jnp.bfloat16)
    attn_share = lax.psum_scatter(project(mixed, out_weight), "mp", scatter_dimension=1, tiled=True)
    resid = x_float + attn_share
    scaled_two, normed_two, inverse_two = normalize(resid, mlp_gain)
    rows_two = lax.all_gather(scaled_two.astype(jnp.bfloat16), "mp", axis=1, tiled=True)
    up_pre = project(rows_two, up_weight)
    hidden = jax.nn.gelu(up_pre, approximate=True).astype(jnp.bfloat16)
    mlp_share = lax.psum_scatter(
        project(hidden, down_weight).astype(jnp.bfloat16), "mp", scatter_dimension=1, tiled=True
    ).astype(jnp.float32)
    result = (resid + mlp_share).astype(jnp.bfloat16)
    grad_top = out_cotangent.astype(jnp.float32)
    grad_rows = lax.all_gather(out_cotangent, "mp", axis=1, tiled=True)
    down_total = weight_grad(hidden, grad_rows)
    grad_hidden = project_back(grad_rows, down_weight)
    grad_up_pre = (grad_hidden * gelu_slope(up_pre)).astype(jnp.bfloat16)
    up_total = weight_grad(rows_two, grad_up_pre)
    grad_two = lax.psum_scatter(
        project_back(grad_up_pre, up_weight), "mp", scatter_dimension=1, tiled=True
    )
    resid_part, mlp_gain_part = norm_back(grad_two, normed_two, inverse_two, mlp_gain)
    grad_resid = grad_top + resid_part
    branch_rows = lax.all_gather(grad_resid.astype(jnp.bfloat16), "mp", axis=1, tiled=True)
    out_total = weight_grad(mixed, branch_rows)
    grad_mixed = project_back(branch_rows, out_weight).astype(jnp.bfloat16).reshape(head_shape)
    row_index = 0
    grad_q, grad_k, grad_v = attend_back(
        queries[row_index],
        keys[row_index],
        values[row_index],
        grad_mixed[row_index],
        log_rows[row_index],
        segment_ids[row_index],
        scale,
        block,
    )
    query_rows = [grad_q]
    key_rows = [grad_k]
    value_rows = [grad_v]
    grad_query = (
        rotate_back(jnp.stack(query_rows, 0), cosine, sine)
        .astype(jnp.bfloat16)
        .reshape(row_count, seq_len, local_width)
    )
    grad_key = (
        rotate_back(jnp.stack(key_rows, 0), cosine, sine)
        .astype(jnp.bfloat16)
        .reshape(row_count, seq_len, local_width)
    )
    grad_value = (
        jnp.stack(value_rows, 0).astype(jnp.bfloat16).reshape(row_count, seq_len, local_width)
    )
    query_total = weight_grad(rows_one, grad_query)
    key_total = weight_grad(rows_one, grad_key)
    value_total = weight_grad(rows_one, grad_value)
    grad_terms = (
        project_back(grad_query, query_weight)
        + project_back(grad_key, key_weight)
        + project_back(grad_value, value_weight)
    )
    grad_one = lax.psum_scatter(grad_terms, "mp", scatter_dimension=1, tiled=True)
    input_part, attn_gain_part = norm_back(grad_one, normed_one, inverse_one, attn_gain)
    input_grad = grad_resid + input_part
    attn_gain_part, mlp_gain_part = lax.psum((attn_gain_part, mlp_gain_part), "mp")
    (
        query_total,
        key_total,
        value_total,
        out_total,
        attn_gain_part,
        mlp_gain_part,
        up_total,
        down_total,
    ) = lax.psum(
        (
            query_total,
            key_total,
            value_total,
            out_total,
            attn_gain_part,
            mlp_gain_part,
            up_total,
            down_total,
        ),
        "dp",
    )
    return (
        result,
        input_grad,
        attn_gain_part,
        query_total,
        key_total,
        value_total,
        out_total,
        mlp_gain_part,
        up_total,
        down_total,
    )


def on_device_kernels(
    hidden_in, segment_ids, attn_gain, query_weight, key_weight, value_weight, out_weight, mlp_gain, up_weight, down_weight, out_cotangent
):
    sums = layer(
        hidden_in[0], out_cotangent[0], segment_ids, attn_gain, mlp_gain,
        query_weight.T, key_weight.T, value_weight.T, out_weight, up_weight, down_weight,
    )
    result, input_grad, one, two, down, up, out, query, key, value = finish(*sums, up_weight.shape[1], out_weight.shape[0])
    return (result[None], input_grad[None], one, query.T, key.T, value.T, out, two, up, down)


def solution(mesh):
    return jax.shard_map(
        on_device_kernels if mesh.shape["dp"] == 8 else on_device,
        mesh=mesh,
        in_specs=(
            P("dp", "mp", None),
            P("dp", None),
            P(),
            P(None, "mp"),
            P(None, "mp"),
            P(None, "mp"),
            P("mp", None),
            P(),
            P(None, "mp"),
            P("mp", None),
            P("dp", "mp", None),
        ),
        out_specs=(
            P("dp", "mp", None),
            P("dp", "mp", None),
            P(),
            P(None, "mp"),
            P(None, "mp"),
            P(None, "mp"),
            P("mp", None),
            P(),
            P(None, "mp"),
            P("mp", None),
        ),
        check_vma=False,
    )
```

```python
import math

import jax
import jax.numpy as jnp
from jax import lax
from jax.experimental import pallas as pl
from jax.experimental.pallas import tpu as pltpu
from jax.sharding import PartitionSpec as P

HEAD = 80


EPS = 1e-06
MASKED = -1e30
GELU_C = math.sqrt(2.0 / math.pi)
GELU_K = 0.044715


def normalize(values, gain):
    inverse = lax.rsqrt(jnp.mean(values * values, -1, keepdims=True) + EPS)
    normed = values * inverse
    return (normed * gain, normed, inverse)


def norm_back(upstream, normed, inverse, gain):
    scaled = upstream * gain
    inner = jnp.mean(scaled * normed, -1, keepdims=True)
    return (inverse * (scaled - normed * inner), jnp.sum(upstream * normed, axis=(0, 1)))


def gelu_slope(values):
    tangent = jnp.tanh(GELU_C * (values + GELU_K * values * values * values))
    return 0.5 * (1.0 + tangent) + 0.5 * values * (1.0 - tangent * tangent) * GELU_C * (
        1.0 + 3.0 * GELU_K * values * values
    )


def project(left, weight):
    return jnp.einsum("rsd,de->rse", left, weight, preferred_element_type=jnp.float32)


def project_back(left, weight):
    return jnp.einsum("rse,de->rsd", left, weight, preferred_element_type=jnp.float32)


def weight_grad(left, right):
    return jnp.einsum("rsd,rse->de", left, right, preferred_element_type=jnp.float32)


def rotary_tables(segments, head_size):
    seq_len = segments.shape[1]
    places = jnp.arange(seq_len, dtype=jnp.int32)
    starts_here = jnp.concatenate(
        [jnp.ones((segments.shape[0], 1), bool), segments[:, 1:] != segments[:, :-1]], axis=1
    )
    first = lax.cummax(jnp.where(starts_here, places[None, :], 0), axis=1)
    position = (places[None, :] - first).astype(jnp.float32)
    half = head_size // 2
    freqs = jnp.exp(jnp.arange(half, dtype=jnp.float32) * (-2.0 * math.log(10000.0) / head_size))
    angles = position[:, :, None] * freqs[None, None, :]
    return (jnp.cos(angles)[:, :, None, :], jnp.sin(angles)[:, :, None, :])


def rotate(values, cosine, sine):
    half = values.shape[-1] // 2
    first, second = (values[..., :half], values[..., half:])
    return jnp.concatenate([first * cosine - second * sine, second * cosine + first * sine], -1)


def rotate_back(grads, cosine, sine):
    half = grads.shape[-1] // 2
    first, second = (grads[..., :half], grads[..., half:])
    return jnp.concatenate([first * cosine + second * sine, second * cosine - first * sine], -1)


def allowed_block(segments_row, start, size):
    seq_len = segments_row.shape[0]
    query_pos = start + jnp.arange(size, dtype=jnp.int32)
    key_pos = jnp.arange(seq_len, dtype=jnp.int32)
    query_seg = segments_row[start : start + size]
    return (query_pos[:, None] >= key_pos[None, :]) & (query_seg[:, None] == segments_row[None, :])


def block_scores(query_block, keys, allowed, scale):
    scores = (
        jnp.einsum("qhd,khd->hqk", query_block, keys, preferred_element_type=jnp.float32) * scale
    )
    return jnp.where(allowed[None], scores, MASKED)


def attend_forward(queries, keys, values, segments_row, scale, block):
    outputs = []
    sums = []
    for start in range(0, queries.shape[0], block):
        allowed = allowed_block(segments_row, start, block)
        scores = block_scores(queries[start : start + block], keys, allowed, scale)
        top = jnp.max(scores, -1, keepdims=True)
        expo = jnp.exp(scores - top)
        total = jnp.sum(expo, -1, keepdims=True)
        probs = (expo / total).astype(jnp.bfloat16)
        outputs.append(
            jnp.einsum("hqk,khd->qhd", probs, values, preferred_element_type=jnp.float32)
        )
        sums.append(top + jnp.log(total))
    return (jnp.concatenate(outputs, 0), jnp.concatenate(sums, 1))


def attend_back(queries, keys, values, grad_mixed, log_sums, segments_row, scale, block):
    key_total = jnp.zeros(keys.shape, jnp.float32)
    value_total = jnp.zeros(values.shape, jnp.float32)
    query_parts = []
    for start in range(0, queries.shape[0], block):
        allowed = allowed_block(segments_row, start, block)
        query_block = queries[start : start + block]
        scores = block_scores(query_block, keys, allowed, scale)
        probs = jnp.exp(scores - log_sums[:, start : start + block])
        grad_block = grad_mixed[start : start + block]
        grad_probs = jnp.einsum(
            "qhd,khd->hqk", grad_block, values, preferred_element_type=jnp.float32
        )
        inner = jnp.sum(probs * grad_probs, -1, keepdims=True)
        grad_scores = (probs * (grad_probs - inner)).astype(jnp.bfloat16)
        query_parts.append(
            jnp.einsum("hqk,khd->qhd", grad_scores, keys, preferred_element_type=jnp.float32)
            * scale
        )
        key_total = (
            key_total
            + jnp.einsum(
                "hqk,qhd->khd", grad_scores, query_block, preferred_element_type=jnp.float32
            )
            * scale
        )
        value_total = value_total + jnp.einsum(
            "hqk,qhd->khd",
            probs.astype(jnp.bfloat16),
            grad_block,
            preferred_element_type=jnp.float32,
        )
    return (jnp.concatenate(query_parts, 0), key_total, value_total)


MESH = pl.DeviceIdType.MESH
CHUNK = 64
SLOTS = 6
STAGES = 6
(R1Z, R2Z, R3Z, FZM, FZA, FZB, R1Y, R2Y, R3Y, FYI, FYY) = range(11)
(S0Z, S0Y, S1Z, S1Y, S2Z, S2Y, S3ZM, S3ZE, S3YE, S3YY, S4Z, S4Y) = range(12)


def add_rows(total_ref, row, count, *others):
    value = total_ref[pl.ds(row, count), :].astype(jnp.float32)
    for other in others:
        value = value + other[...].astype(jnp.float32)
    total_ref[pl.ds(row, count), :] = value.astype(jnp.bfloat16)


class Reducer:
    def __init__(self, rows, bufs, send_sem, recv_sem, pairs):
        self.rows, self.bufs, self.send_sem, self.recv_sem, self.pairs = rows, bufs, send_sem, recv_sem, pairs
        dp = lax.axis_index("dp")
        self.place, self.side = lax.div(dp, 2), lax.rem(dp, 2)
        self.inner = (self.place == 1) | (self.place == 2)
        self.end = jnp.logical_not(self.inner)
        self.mate = 2 * (self.place + 1 - 2 * lax.rem(self.place, 2)) + self.side
        self.across = 2 * (3 - self.place) + self.side
        self.twin = 2 * self.place + 1 - self.side
        self.half_z = lax.div(self.place, 2)
        self.half_y = self.side

    def copy(self, source, target, send, recv, slot, device):
        return pltpu.make_async_remote_copy(
            src_ref=source,
            dst_ref=target,
            send_sem=self.send_sem.at[send, slot],
            recv_sem=self.recv_sem.at[recv, slot],
            device_id={"dp": device},
            device_id_type=MESH,
        )

    def whole_z(self, pair):
        return pl.multiple_of(pair * (2 * CHUNK), CHUNK)

    def at_z(self, pair, half):
        return pl.multiple_of(pair * (2 * CHUNK) + half * (CHUNK // 2), CHUNK // 2)

    def at_y(self, pair, half):
        return pl.multiple_of(pair * (2 * CHUNK) + CHUNK + half * (CHUNK // 2), CHUNK // 2)

    def moves(self, pair):
        slot = lax.rem(pair, SLOTS)
        rows, (one_z, two_z, three_z, one_y, two_y, three_y) = self.rows, self.bufs
        half = CHUNK // 2
        mine_z, mine_y = self.half_z, self.half_y
        own_z = rows.at[pl.ds(self.at_z(pair, mine_z), half), :]
        rest_z = rows.at[pl.ds(self.at_z(pair, 1 - mine_z), half), :]
        own_y = rows.at[pl.ds(self.at_y(pair, mine_y), half), :]
        rest_y = rows.at[pl.ds(self.at_y(pair, 1 - mine_y), half), :]
        all_z = rows.at[pl.ds(self.whole_z(pair), CHUNK), :]
        return dict(
            s0z=lambda: self.copy(all_z, one_z.at[slot], S0Z, R1Z, slot, self.mate),
            s0y=lambda: self.copy(rest_y, one_y.at[slot], S0Y, R1Y, slot, self.twin),
            s1z=lambda: self.copy(rest_z, two_z.at[slot], S1Z, R2Z, slot, self.across),
            s1y=lambda: self.copy(two_y.at[slot], two_y.at[slot], S1Y, R2Y, slot, self.mate),
            s2z=lambda: self.copy(own_z, three_z.at[slot], S2Z, R3Z, slot, self.twin),
            s2y=lambda: self.copy(own_y, three_y.at[slot], S2Y, R3Y, slot, self.across),
            s3zm=lambda: self.copy(own_z, own_z, S3ZM, FZM, slot, self.across),
            s3ze=lambda: self.copy(own_z, own_z, S3ZE, FZA, slot, self.mate),
            s3ye=lambda: self.copy(own_y, own_y, S3YE, FYI, slot, self.mate),
            s3yy=lambda: self.copy(own_y, own_y, S3YY, FYY, slot, self.twin),
            s4z=lambda: self.copy(rest_z, rest_z, S4Z, FZB, slot, self.mate),
            s4y=lambda: self.copy(own_y, own_y, S4Y, FYY, slot, self.twin),
        )

    def when(self, slot_index, stage, role, body):
        pair = slot_index - stage
        live = (pair >= 0) & (pair < self.pairs)
        if role is not None:
            live = live & role

        @pl.when(live)
        def _():
            body(pair)

    def slot(self, index):
        half = CHUNK // 2
        one_z, two_z, three_z, one_y, two_y, three_y = self.bufs

        def last(pair):
            m = self.moves(pair)
            @pl.when(self.end)
            def _():
                m["s3ze"]().wait_recv()
                m["s4z"]().wait_recv()
                m["s1y"]().wait_send()
                m["s4y"]().wait_send()
                m["s4y"]().wait_recv()

            @pl.when(self.inner)
            def _():
                m["s3zm"]().wait_send()
                m["s3ze"]().wait_send()
                m["s3ye"]().wait_send()
                m["s3yy"]().wait_send()
                m["s4z"]().wait_send()
                m["s3yy"]().wait_recv()

        def fourth_inner(pair):
            m = self.moves(pair)
            m["s3zm"]().wait_recv()
            m["s4z"]().start()

        def fourth_end(pair):
            m = self.moves(pair)
            m["s3ye"]().wait_recv()
            m["s4y"]().start()

        def third(pair):
            m = self.moves(pair)
            slot = lax.rem(pair, SLOTS)
            m["s2z"]().wait()
            m["s2y"]().wait()
            add_rows(self.rows, self.at_z(pair, self.half_z), half, three_z.at[slot])
            add_rows(self.rows, self.at_y(pair, self.half_y), half, three_y.at[slot])
            m["s3ze"]().start()
            m["s3zm"]().start()
            m["s3ye"]().start()
            m["s3yy"]().start()

        def second(pair):
            m = self.moves(pair)
            slot = lax.rem(pair, SLOTS)
            m["s1z"]().wait()
            m["s1y"]().wait_recv()
            m["s0y"]().wait_send()
            add_rows(
                self.rows, self.at_z(pair, self.half_z), half,
                one_z.at[slot, pl.ds(pl.multiple_of(self.half_z * half, half), half), :], two_z.at[slot],
            )
            add_rows(self.rows, self.at_y(pair, self.half_y), half, one_y.at[slot], two_y.at[slot])
            m["s2z"]().start()
            m["s2y"]().start()

        def first_inner(pair):
            m = self.moves(pair)
            slot = lax.rem(pair, SLOTS)
            m["s0z"]().wait_recv()
            m["s0y"]().wait_recv()
            other = 1 - self.half_z
            add_rows(
                self.rows, self.at_z(pair, other), half,
                one_z.at[slot, pl.ds(pl.multiple_of(other * half, half), half), :],
            )
            m["s1z"]().start()

        def first_end(pair):
            m = self.moves(pair)
            slot = lax.rem(pair, SLOTS)
            m["s0y"]().wait()
            m["s0z"]().wait_send()
            mine = self.rows[pl.ds(self.at_y(pair, self.half_y), half), :].astype(jnp.float32)
            two_y[slot] = (mine + one_y[slot].astype(jnp.float32)).astype(jnp.bfloat16)
            m["s1y"]().start()

        def start(pair):
            m = self.moves(pair)
            m["s0y"]().start()

            @pl.when(self.end)
            def _():
                m["s0z"]().start()

        self.when(index, 0, None, start)
        self.when(index, 1, self.end, first_end)
        self.when(index, 1, self.inner, first_inner)
        self.when(index, 2, self.inner, second)
        self.when(index, 3, self.inner, third)
        self.when(index, 4, self.inner, fourth_inner)
        self.when(index, 4, self.end, fourth_end)
        self.when(index, 5, None, last)

    def greet(self, barrier):
        for device in (self.mate, self.across, self.twin):
            pl.semaphore_signal(barrier, inc=1, device_id={"dp": device}, device_id_type=MESH)
        return 3


def reducer_scratch(width):
    half = CHUNK // 2
    return [
        pltpu.VMEM((SLOTS, CHUNK, width), jnp.bfloat16),
        pltpu.VMEM((SLOTS, half, width), jnp.bfloat16),
        pltpu.VMEM((SLOTS, half, width), jnp.bfloat16),
        pltpu.VMEM((SLOTS, half, width), jnp.bfloat16),
        pltpu.VMEM((SLOTS, half, width), jnp.bfloat16),
        pltpu.VMEM((SLOTS, half, width), jnp.bfloat16),
        pltpu.SemaphoreType.DMA((12, SLOTS)),
        pltpu.SemaphoreType.DMA((11, SLOTS)),
    ]


HEAD_PAD = 128
BLOCK_SEQ = 256
SPAN = 512


def pad_matrix(local, padded):
    shape = (padded, local)
    feature = lax.broadcasted_iota(jnp.int32, shape, 1)
    lane = lax.broadcasted_iota(jnp.int32, shape, 0)
    head = jnp.zeros(shape, jnp.int32)
    for h in range(1, local // HEAD):
        head = head + (feature >= h * HEAD).astype(jnp.int32)
    within = feature - head * HEAD
    target = head * HEAD_PAD + within + jnp.where(within >= HEAD // 2, HEAD_PAD // 2 - HEAD // 2, 0)
    return jnp.where(lane == target, 1.0, 0.0).astype(jnp.bfloat16)


def dot(a, b):
    return jnp.dot(a, b, preferred_element_type=jnp.float32)


def dot_nt(a, b):
    return lax.dot_general(a, b, (((1,), (1,)), ((), ())), preferred_element_type=jnp.float32)


def dot_tn(a, b):
    return lax.dot_general(a, b, (((0,), (0,)), ((), ())), preferred_element_type=jnp.float32)


def segment_columns(seg):
    lines = jnp.broadcast_to(seg.astype(jnp.float32), (16, seg.shape[1])).astype(jnp.bfloat16)
    pick = (lax.broadcasted_iota(jnp.int32, (16, 128), 0) == 0).astype(jnp.float32).astype(jnp.bfloat16)
    return dot_tn(lines, pick)


def rotary_into(seg, cos_ref, sin_ref):
    seq = seg.shape[1]
    ids = segment_columns(seg)
    first = jnp.zeros((seq, 128), jnp.float32)
    row = seg.astype(jnp.float32)
    for s in range(1, 16):
        before = jnp.sum(jnp.where(row < s, 1.0, 0.0), axis=1, keepdims=True)
        first = jnp.where(ids == s, before, first)
    position = lax.broadcasted_iota(jnp.int32, (seq, 128), 0).astype(jnp.float32) - first
    lane = lax.broadcasted_iota(jnp.int32, (1, 128), 1)
    upper = lane >= HEAD_PAD // 2
    index = jnp.where(upper, lane - HEAD_PAD // 2, lane)
    freqs = jnp.exp(index.astype(jnp.float32) * (-2.0 * math.log(10000.0) / HEAD))
    freqs = jnp.where(index < HEAD // 2, freqs, 0.0)
    angles = position * freqs
    cos_ref[...] = jnp.cos(angles)
    sin_ref[...] = jnp.where(upper, jnp.sin(angles), -jnp.sin(angles))


class Ring4:
    def __init__(self):
        mp = lax.axis_index("mp")
        chip, core = lax.div(mp, 2), lax.rem(mp, 2)
        self.me = mp
        self.core = 2 * chip + 1 - core
        self.chip = 2 * (1 - chip) + core
        self.far = 2 * (1 - chip) + 1 - core


def block_rows(index):
    return pl.ds(pl.multiple_of(index * BLOCK_SEQ, BLOCK_SEQ), BLOCK_SEQ)


class Gather:
    def __init__(self, ring, rows, sems, parts=1):
        self.parts = parts
        size = BLOCK_SEQ // parts

        def copy(block, device, which, part):
            at = pl.ds(pl.multiple_of(block * BLOCK_SEQ + part * size, size), size)
            return pltpu.make_async_remote_copy(
                src_ref=rows.at[at, :],
                dst_ref=rows.at[at, :],
                send_sem=sems.at[0, which * parts + part],
                recv_sem=sems.at[1, which * parts + part],
                device_id={"mp": device},
                device_id_type=MESH,
            )

        self.near = lambda part=0: copy(ring.me, ring.core, 0, part)
        self.across = lambda part=0: copy(ring.me, ring.chip, 1, part)
        self.onward = lambda part=0: copy(ring.chip, ring.core, 2, part)

    def start(self, part=0):
        self.across(part).start()
        self.near(part).start()

    def forward(self):
        for part in range(self.parts):
            self.across(part).wait_recv()
            self.onward(part).start()

    def near_in(self):
        for part in range(self.parts):
            self.near(part).wait_recv()

    def onward_in(self):
        for part in range(self.parts):
            self.onward(part).wait_recv()

    def sent(self):
        for part in range(self.parts):
            self.near(part).wait_send()
            self.across(part).wait_send()
            self.onward(part).wait_send()


class Scatter:
    def __init__(self, ring, send_core, recv_core, send_chip, recv_chip, sems, parts=1):
        self.parts = parts
        size = BLOCK_SEQ // parts

        def copy(source, target, device, which, part):
            at = pl.ds(part * size, size)
            return pltpu.make_async_remote_copy(
                src_ref=source.at[at, :],
                dst_ref=target.at[at, :],
                send_sem=sems.at[0, which * parts + part],
                recv_sem=sems.at[1, which * parts + part],
                device_id={"mp": device},
                device_id_type=MESH,
            )

        self.far = lambda part=0: copy(send_core.at[0], recv_core.at[0], ring.core, 0, part)
        self.core = lambda part=0: copy(send_core.at[1], recv_core.at[1], ring.core, 1, part)
        self.chip = lambda part=0: copy(send_chip, recv_chip, ring.chip, 2, part)


def greet_mp(ring, barrier):
    for device in (ring.core, ring.chip):
        pl.semaphore_signal(barrier, inc=1, device_id={"mp": device}, device_id_type=MESH)
    return 2


def norm_rows(values):
    inverse = lax.rsqrt(jnp.mean(values * values, -1, keepdims=True) + EPS)
    return values * inverse, inverse


def qkv_block(rows, weights, cos_ref, sin_ref, out, block):
    at = block_rows(block)
    turned = 2 * (weights.shape[0] // 3) // 256
    tiles = weights.shape[0] // 256

    def one(n, turn):
        cols = pl.ds(pl.multiple_of(n * 256, 256), 256)
        value = dot_nt(rows[at, :], weights[cols, :])
        if turn:
            cosine, sine = cos_ref[at, :], sin_ref[at, :]
            halves = [value[:, j * 128 : j * 128 + 128] for j in range(2)]
            value = jnp.concatenate([h * cosine + pltpu.roll(h, 64, 1) * sine for h in halves], axis=1)
        out[at, cols] = value.astype(jnp.bfloat16)

    @pl.loop(0, turned)
    def _(n):
        one(n, True)

    @pl.loop(turned, tiles)
    def _(n):
        one(n, False)


def masks_into(seg, ids_ref, bias_ref):
    seq = seg.shape[1]
    for i in range(seq // BLOCK_SEQ):
        low = max(0, i * BLOCK_SEQ - SPAN)
        high = (i + 1) * BLOCK_SEQ
        shape = (BLOCK_SEQ, high - low)
        query = i * BLOCK_SEQ + lax.broadcasted_iota(jnp.int32, shape, 0)
        key = low + lax.broadcasted_iota(jnp.int32, shape, 1)
        ids = ids_ref[pl.ds(i * BLOCK_SEQ, BLOCK_SEQ), :][:, :1]
        same = ids == seg[:, low:high].astype(jnp.float32)
        bias_ref[pl.ds(i * BLOCK_SEQ, BLOCK_SEQ), pl.ds(0, high - low)] = jnp.where((query >= key) & same, 0.0, MASKED).astype(bias_ref.dtype)


def attend(qkv, out, bias_ref, stats, heads, scale, blocks):
    width = heads * HEAD_PAD
    lane = lax.broadcasted_iota(jnp.int32, (BLOCK_SEQ, 128), 1)

    @pl.loop(0, heads)
    def _(h):
        lanes = [pl.ds(pl.multiple_of(part * width + h * HEAD_PAD, HEAD_PAD), HEAD_PAD) for part in range(3)]
        for i in blocks:
            low, high = max(0, i * BLOCK_SEQ - SPAN), (i + 1) * BLOCK_SEQ
            rows, keys = pl.ds(i * BLOCK_SEQ, BLOCK_SEQ), pl.ds(low, high - low)
            scores = dot_nt(qkv[rows, lanes[0]], qkv[keys, lanes[1]]) + bias_ref[rows, pl.ds(0, high - low)]
            top = jnp.max(scores, -1, keepdims=True)
            expo = jnp.exp((scores - top) * scale)
            total = jnp.sum(expo, -1, keepdims=True)
            probs = expo * (1.0 / total)
            stats[rows, :] = jnp.where(lane == h, top * scale + jnp.log(total), stats[rows, :])
            out[rows, lanes[0]] = dot(probs.astype(jnp.bfloat16), qkv[keys, lanes[2]]).astype(jnp.bfloat16)


def layer_kernel(
    x, g, seg, gain_one, gain_two, wq, wk, wv, wo, wup, wdown,
    result_o, input_o, gains_o, sums_o,
    rows, b0, b1, b2, b3, b4, b5, send_sem, recv_sem, save_sem,
    w_up, w_down, w_qkv, w_out, rows_one, rows_g, rows_two, hidden, grad_up, branch, qkv, mixed, grad_mixed,
    cos_ref, sin_ref, bias_ref, resid, term_ref, key_sum, value_sum,
    send_core, recv_core, send_chip, recv_chip, gain_acc, gain_recv,
    load_sem, one_sem, g_sem, two_sem, branch_sem, rs0_sem, rs_sem, rs2_sem, rs3_sem, gain_sem, free_sem, ready_sem, stats,
):
    bf, f32 = jnp.bfloat16, jnp.float32
    ring = Ring4()
    seq, width = rows_two.shape
    units = w_up.shape[1]
    padded = w_out.shape[0]
    heads = padded // HEAD_PAD
    local = heads * HEAD
    pairs = rows.shape[0] // (2 * CHUNK)
    scale = 1.0 / math.sqrt(HEAD)
    half = BLOCK_SEQ // 2
    chip = lax.div(ring.me, 2)
    red = Reducer(rows, (b0, b1, b2, b3, b4, b5), send_sem, recv_sem, pairs)
    barrier = pltpu.get_barrier_semaphore()
    count = greet_mp(ring, barrier) + red.greet(barrier)
    places = [(w, rows.at[pl.ds(i * local, local), :]) for i, w in enumerate((wq, wk, wv, wo))]
    places += [(g, rows_g.at[block_rows(ring.me), :]), (wup, w_up), (wdown, w_down)]
    loads = [pltpu.make_async_copy(source, target, load_sem.at[i]) for i, (source, target) in enumerate(places)]
    for load in loads[:5]:
        load.start()
    normed, _ = norm_rows(x[...].astype(f32))
    rows_one[block_rows(ring.me), :] = (normed * gain_one[...]).astype(bf)
    one, all_g = Gather(ring, rows_one, one_sem, 2), Gather(ring, rows_g, g_sem)
    two, all_branch = Gather(ring, rows_two, two_sem, 2), Gather(ring, branch, branch_sem)
    ahead = Scatter(ring, send_core, recv_core, send_chip, recv_chip, rs0_sem, 2)
    first = Scatter(ring, send_core, recv_core, send_chip, recv_chip, rs_sem)
    second = Scatter(ring, send_core, recv_core, send_chip, recv_chip, rs2_sem)
    third = Scatter(ring, send_core, recv_core, send_chip, recv_chip, rs3_sem)
    pl.semaphore_wait(barrier, count)
    one.start(0)
    one.start(1)
    for load in loads[5:]:
        load.start()

    spread = pad_matrix(local, padded)
    for i in range(3):
        loads[i].wait()
        w_qkv[pl.ds(i * padded, padded), :] = dot(spread, rows[pl.ds(i * local, local), :]).astype(bf)
    loads[3].wait()
    w_out[...] = dot(spread, rows[pl.ds(3 * local, local), :]).astype(bf)
    rotary_into(seg[...], cos_ref, sin_ref)
    qkv_block(rows_one, w_qkv, cos_ref, sin_ref, qkv, ring.me)
    one.near_in()
    qkv_block(rows_one, w_qkv, cos_ref, sin_ref, qkv, ring.core)
    key_sum[...] = segment_columns(seg[...])
    masks_into(seg[...], key_sum, bias_ref)
    loads[4].wait()
    one.forward()
    one.across(0).wait_send()
    one.across(1).wait_send()
    all_g.start()
    qkv_block(rows_one, w_qkv, cos_ref, sin_ref, qkv, ring.chip)
    one.onward_in()
    qkv_block(rows_one, w_qkv, cos_ref, sin_ref, qkv, ring.far)

    stats[...] = jnp.zeros_like(stats)
    early, late = (0, 1), (2, 3)

    @pl.when(chip == 0)
    def _():
        attend(qkv, mixed, bias_ref, stats, heads, scale, late)

    @pl.when(chip == 1)
    def _():
        attend(qkv, mixed, bias_ref, stats, heads, scale, early)

    def term(block, part):
        at = pl.ds(pl.multiple_of(block * BLOCK_SEQ + part * half, half), half)
        return dot(mixed[at, :], w_out[...])

    parts = [pl.ds(p * half, half) for p in range(2)]
    for p in range(2):
        send_core[0, parts[p], :] = term(ring.far, p).astype(bf)
        ahead.far(p).start()
    for p in range(2):
        value = term(ring.chip, p)
        ahead.far(p).wait_recv()
        send_chip[parts[p], :] = (value + recv_core[0, parts[p], :].astype(f32)).astype(bf)
        ahead.chip(p).start()

    @pl.when(chip == 0)
    def _():
        attend(qkv, mixed, bias_ref, stats, heads, scale, early)

    @pl.when(chip == 1)
    def _():
        attend(qkv, mixed, bias_ref, stats, heads, scale, late)

    for p in range(2):
        send_core[1, parts[p], :] = term(ring.core, p).astype(bf)
        ahead.core(p).start()
    all_g.forward()
    for p in range(2):
        resid[parts[p], :] = x[parts[p], :].astype(f32) + term(ring.me, p)
    for p in range(2):
        ahead.core(p).wait_recv()
        ahead.chip(p).wait_recv()
        value = resid[parts[p], :] + recv_core[1, parts[p], :].astype(f32) + recv_chip[parts[p], :].astype(f32)
        resid[parts[p], :] = value
        normed, _ = norm_rows(value)
        at = pl.ds(pl.multiple_of(ring.me * BLOCK_SEQ + p * half, half), half)
        rows_two[at, :] = (normed * gain_two[...]).astype(bf)
        two.start(p)
    for p in range(2):
        ahead.far(p).wait_send()
        ahead.core(p).wait_send()
        ahead.chip(p).wait_send()

    base = 2 * units

    def put(pair):
        at = pl.ds(pl.multiple_of(pair * 2 * CHUNK, 2 * CHUNK), 2 * CHUNK)
        return pltpu.make_async_copy(rows.at[at, :], sums_o.at[at, :], save_sem.at[lax.rem(pair, 4)])

    def slot(index):
        red.slot(index)
        pair = index - (STAGES - 1)

        @pl.when(pair >= 4)
        def _():
            put(pair - 4).wait()

        @pl.when(pair >= 0)
        def _():
            put(pair).start()

    def tile(n):
        return pl.ds(pl.multiple_of(n * 256, 256), 256)

    def half_rows(block, part):
        return pl.ds(pl.multiple_of(block * BLOCK_SEQ + part * half, half), half)

    def up_tile(at, n):
        u = dot(rows_two[at, :], w_up[:, tile(n)])
        tangent = jnp.tanh(GELU_C * (u + GELU_K * u * u * u))
        hidden[at, tile(n)] = (0.5 * u * (1.0 + tangent)).astype(bf)

    def up_rows_of(at):
        @pl.loop(0, units // 256)
        def _(n):
            up_tile(at, n)

    loads[5].wait()
    up_rows_of(block_rows(ring.me))
    two.near_in()
    up_rows_of(block_rows(ring.core))
    all_g.near_in()
    all_g.onward_in()
    two.across(0).wait_recv()
    two.onward(0).start()
    up_rows_of(half_rows(ring.chip, 0))
    two.onward(0).wait_recv()
    up_rows_of(half_rows(ring.far, 0))
    two.across(1).wait_recv()
    two.onward(1).start()

    loads[6].wait()

    def order(k):
        there = k < 2
        core = lax.rem(ring.me, 2)
        flip = 1 - lax.rem(k, 2)
        to_chip = jnp.where(there, 1 - chip, chip)
        to_core = jnp.where(flip == 1, 1 - core, core)
        return 2 * to_chip + to_core

    def hand_on(k, scatter, start):
        @pl.when(k == 0)
        def _():
            send_core[0] = term_ref[...].astype(bf)
            scatter.far().start()

        @pl.when(k == 1)
        def _():
            scatter.far().wait_recv()
            send_chip[...] = (term_ref[...] + recv_core[0].astype(f32)).astype(bf)
            scatter.chip().start()

        @pl.when(k == 2)
        def _():
            send_core[1] = term_ref[...].astype(bf)
            scatter.core().start()

        @pl.when(k == 3)
        def _():
            scatter.core().wait_recv()
            term_ref[...] = term_ref[...] + recv_core[1].astype(f32)

    def settle(scatter):
        for copy in (scatter.far(), scatter.core()):
            copy.wait_send()
        scatter.chip().wait()
        return term_ref[...] + recv_chip[...].astype(f32)

    def grad_tile(at, n):
        u = dot(rows_two[at, :], w_up[:, tile(n)])
        upstream = dot_nt(rows_g[at, :], w_down[tile(n), :])
        tangent = jnp.tanh(GELU_C * (u + GELU_K * u * u * u))
        slope = 0.5 * (1.0 + tangent) + 0.5 * u * (1.0 - tangent * tangent) * GELU_C * (1.0 + 3.0 * GELU_K * u * u)
        grad_up[at, tile(n)] = (upstream * slope).astype(bf)

    @pl.loop(0, units // 256)
    def _(n):
        up_tile(half_rows(ring.chip, 1), n)

        @pl.when(n == 0)
        def _():
            two.onward(1).wait_recv()

        up_tile(half_rows(ring.far, 1), n)
        rows[tile(n), :] = dot_tn(hidden[:, tile(n)], rows_g[...]).astype(bf)
        slot(n)

        @pl.loop(0, 3)
        def _(k):
            grad_tile(block_rows(order(k)), n)

    @pl.loop(0, 4)
    def _(k):
        @pl.loop(0, 2)
        def _(j):
            @pl.when(2 * k + j < units // 256)
            def _():
                grad_tile(block_rows(order(3)), 2 * k + j)

        at = block_rows(order(k))

        @pl.loop(0, width // 256)
        def _(n):
            term_ref[:, tile(n)] = dot_nt(grad_up[at, :], w_up[tile(n), :])

        hand_on(k, first, None)
        slot(5 + k)

    def up_rows(i):
        rows[pl.ds(pl.multiple_of(units + i * 256, 256), 256), :] = dot_tn(rows_two[:, tile(i)], grad_up[...]).astype(bf)

    up_rows(0)
    slot(9)
    grad_two = settle(first)
    normed, inverse = norm_rows(resid[...])
    scaled = grad_two * gain_two[...]
    part = inverse * (scaled - normed * jnp.mean(scaled * normed, -1, keepdims=True))
    mlp_part = jnp.sum(grad_two * normed, axis=0, keepdims=True)
    gain_acc[0] = jnp.zeros(gain_acc.shape[1:], f32)
    gain_acc[0, 1:2, :] = mlp_part
    mine = rows_g[block_rows(ring.me), :].astype(f32) + part
    input_o[...] = mine
    branch[block_rows(ring.me), :] = mine.astype(bf)
    all_branch.across().start()
    all_branch.near().start()
    for device in (ring.core, ring.chip):
        pl.semaphore_signal(ready_sem, inc=1, device_id={"mp": device}, device_id_type=MESH)

    def head_rows(left, lane, right, row):
        value = dot_tn(left[:, lane], right[...])
        halves = [value[at : at + HEAD // 2, :] for at in (0, 64, 128, 192)]
        rows[pl.ds(pl.multiple_of(row, 16), 2 * HEAD), :] = jnp.concatenate(halves, axis=0).astype(bf)

    @pl.loop(1, units // 256)
    def _(i):
        up_rows(i)

        @pl.when(i == 1)
        def _():
            pl.semaphore_wait(ready_sem, 2)

        at = block_rows(order(i - 1))

        @pl.loop(0, width // 256)
        def _(n):
            term_ref[:, tile(n)] = dot(hidden[at, :], w_down[:, tile(n)])

        hand_on(i - 1, second, None)

        @pl.when(i == 4)
        def _():
            all_branch.near().wait_recv()
            all_branch.forward()
            all_branch.onward().wait_recv()

            @pl.loop(0, heads // 2)
            def _(j):
                head_rows(mixed, tile(j), branch, base + j * 2 * HEAD)

        slot(9 + i)

    @pl.loop(0, 4)
    def _(b):
        grad_mixed[block_rows(b), :] = dot_nt(branch[block_rows(b), :], w_out[...]).astype(bf)

    lane = lax.broadcasted_iota(jnp.int32, (BLOCK_SEQ, 128), 1)

    @pl.loop(0, heads)
    def _(h):
        lanes = [pl.ds(pl.multiple_of(n * padded + h * HEAD_PAD, HEAD_PAD), HEAD_PAD) for n in range(3)]
        key_sum[...] = jnp.zeros_like(key_sum)
        value_sum[...] = jnp.zeros_like(value_sum)
        for i in range(seq // BLOCK_SEQ):
            low, high = max(0, i * BLOCK_SEQ - SPAN), (i + 1) * BLOCK_SEQ
            at, keys = pl.ds(i * BLOCK_SEQ, BLOCK_SEQ), pl.ds(low, high - low)
            query, upstream = qkv[at, lanes[0]], grad_mixed[at, lanes[0]]
            scores = dot_nt(query, qkv[keys, lanes[1]]) + bias_ref[at, pl.ds(0, high - low)]
            level = jnp.sum(jnp.where(lane == h, stats[at, :], 0.0), -1, keepdims=True)
            probs = jnp.exp(scores * scale - level)
            grad_probs = dot_nt(upstream, qkv[keys, lanes[2]])
            inner = jnp.sum(probs * grad_probs, -1, keepdims=True)
            grad_scores = (probs * (grad_probs - inner)).astype(bf)
            value_sum[keys, :] += dot_tn(probs.astype(bf), upstream)
            key_sum[keys, :] += dot_tn(grad_scores, query)
            turned = dot(grad_scores, qkv[keys, lanes[1]]) * scale
            qkv[at, lanes[0]] = (turned * cos_ref[at, :] - pltpu.roll(turned, 64, 1) * sin_ref[at, :]).astype(bf)
            if i == 1:
                slot(14 + 2 * h)
        turned = key_sum[...] * scale
        qkv[:, lanes[1]] = (turned * cos_ref[...] - pltpu.roll(turned, 64, 1) * sin_ref[...]).astype(bf)
        qkv[:, lanes[2]] = value_sum[...].astype(bf)
        slot(15 + 2 * h)

    @pl.loop(0, 3)
    def _(part):
        for j in range(heads // 2):
            lane = pl.ds(pl.multiple_of(part * padded + j * 256, 256), 256)
            head_rows(qkv, lane, rows_one, base + (part + 1) * local + j * 2 * HEAD)
        slot(22 + part)

    result_o[...] = (resid[...] + settle(second)).astype(bf)
    for device in (ring.core, ring.chip):
        pl.semaphore_signal(free_sem, inc=1, device_id={"mp": device}, device_id_type=MESH)
    pl.semaphore_wait(free_sem, 2)

    @pl.loop(0, 4)
    def _(k):
        at = block_rows(order(k))

        @pl.loop(0, width // 256)
        def _(n):
            term_ref[:, tile(n)] = dot(qkv[at, :], w_qkv[:, tile(n)])

        hand_on(k, third, None)
        slot(25 + k)

    slot(29)
    grad_one = settle(third)
    normed, inverse = norm_rows(x[...].astype(f32))
    scaled = grad_one * gain_one[...]
    input_o[...] = input_o[...] + inverse * (scaled - normed * jnp.mean(scaled * normed, -1, keepdims=True))
    gain_acc[0, 0:1, :] = jnp.sum(grad_one * normed, axis=0, keepdims=True)

    def exchange(step):
        names = ({"mp": ring.core}, {"mp": ring.chip}, {"dp": red.twin}, {"dp": red.mate}, {"dp": red.across})
        return pltpu.make_async_remote_copy(
            src_ref=gain_acc.at[step], dst_ref=gain_recv.at[step], send_sem=gain_sem.at[0, step], recv_sem=gain_sem.at[1, step],
            device_id=names[step], device_id_type=MESH,
        )

    last = pairs + STAGES - 1

    @pl.loop(30, last)
    def _(index):
        for step in range(5):

            @pl.when(index == 30 + step)
            def _():
                if step:
                    exchange(step - 1).wait_recv()
                    gain_acc[step] = gain_acc[step - 1] + gain_recv[step - 1]
                exchange(step).start()

        slot(index)

    exchange(4).wait_recv()
    gains_o[...] = gain_acc[4] + gain_recv[4]
    for pair in range(pairs - 4, pairs):
        put(pair).wait()
    for step in range(5):
        exchange(step).wait_send()
    for part in range(2):
        one.near(part).wait_send()
        one.onward(part).wait_send()
    for gather in (all_g, two, all_branch):
        gather.sent()


def layer(x, g, seg, gain_one, gain_two, wq, wk, wv, wo, wup, wdown):
    bf, f32 = jnp.bfloat16, jnp.float32
    own, width = x.shape
    units = wup.shape[1]
    seq = seg.shape[1]
    local = wo.shape[0]
    padded = local // HEAD * HEAD_PAD
    total = 2 * units + 4 * local
    vm, hbm = pl.BlockSpec(memory_space=pltpu.VMEM), pl.BlockSpec(memory_space=pl.ANY)
    sem = pltpu.SemaphoreType.DMA
    shapes = [((own, width), bf), ((own, width), f32), ((8, width), f32), ((total, width), bf)]
    tall = pltpu.VMEM((seq, width), bf)
    return pl.pallas_call(
        layer_kernel,
        out_shape=[jax.ShapeDtypeStruct(s, d) for s, d in shapes],
        in_specs=[vm, hbm, vm, vm, vm] + [hbm] * 6,
        out_specs=[vm] * 3 + [hbm],
        scratch_shapes=[pltpu.VMEM((total, width), bf)]
        + reducer_scratch(width)
        + [
            sem((4,)),
            pltpu.VMEM((width, units), bf), pltpu.VMEM((units, width), bf), pltpu.VMEM((3 * padded, width), bf), pltpu.VMEM((padded, width), bf),
            tall, tall, tall, pltpu.VMEM((seq, units), bf), pltpu.VMEM((seq, units), bf), tall,
            pltpu.VMEM((seq, 3 * padded), bf), pltpu.VMEM((seq, padded), bf), pltpu.VMEM((seq, padded), bf),
            pltpu.VMEM((seq, 128), f32), pltpu.VMEM((seq, 128), f32), pltpu.VMEM((seq, SPAN + BLOCK_SEQ), bf),
            pltpu.VMEM((own, width), f32), pltpu.VMEM((own, width), f32), pltpu.VMEM((seq, HEAD_PAD), f32), pltpu.VMEM((seq, HEAD_PAD), f32),
            pltpu.VMEM((2, own, width), bf), pltpu.VMEM((2, own, width), bf), pltpu.VMEM((own, width), bf), pltpu.VMEM((own, width), bf),
            pltpu.VMEM((5, 8, width), f32), pltpu.VMEM((5, 8, width), f32),
            sem((7,)), sem((2, 6)), sem((2, 3)), sem((2, 6)), sem((2, 3)), sem((2, 6)), sem((2, 3)), sem((2, 3)), sem((2, 3)), sem((2, 5)),
            pltpu.SemaphoreType.REGULAR, pltpu.SemaphoreType.REGULAR, pltpu.VMEM((seq, 128), f32),
        ],
        compiler_params=pltpu.CompilerParams(collective_id=0, has_side_effects=True, vmem_limit_bytes=67043328),
    )(x, g, seg, gain_one, gain_two, wq, wk, wv, wo, wup, wdown)


def finish_kernel(result, input_grad, gains, sums, result_o, input_o, one_o, two_o, down_o, up_o, out_o, q_o, k_o, v_o, inbox, outbox, side_one, side_two, in_sem, out_sem, side_sem):
    step = out_o.shape[0]
    targets = [(down_o, i * step) for i in range(down_o.shape[0] // step)] + [(up_o, i * step) for i in range(up_o.shape[0] // step)]
    targets += [(t, 0) for t in (out_o, q_o, k_o, v_o)]
    count, depth = len(targets), inbox.shape[0]
    bring = [pltpu.make_async_copy(result, side_one, side_sem.at[0]), pltpu.make_async_copy(input_grad, side_two, side_sem.at[1])]
    take = [pltpu.make_async_copy(side_one, result_o, side_sem.at[2]), pltpu.make_async_copy(side_two, input_o, side_sem.at[3])]

    def read(i):
        return pltpu.make_async_copy(sums.at[pl.ds(i * step, step), :], inbox.at[i % depth], in_sem.at[i % depth])

    def write(i):
        target, at = targets[i]
        return pltpu.make_async_copy(outbox.at[i % depth], target.at[pl.ds(at, step), :], out_sem.at[i % depth])

    for i in range(depth):
        read(i).start()
    for side in bring:
        side.start()
    one_o[...] = gains[0, :]
    two_o[...] = gains[1, :]
    for i in range(count):
        read(i).wait()
        if i >= depth:
            write(i - depth).wait()
        outbox[i % depth] = inbox[i % depth].astype(jnp.float32)
        write(i).start()
        if i + depth < count:
            read(i + depth).start()
        if i == depth:
            for come, go in zip(bring, take):
                come.wait()
                go.start()
    for i in range(count - depth, count):
        write(i).wait()
    for side in take:
        side.wait()


def finish(result, input_grad, gains, sums, units, local):
    bf, f32 = jnp.bfloat16, jnp.float32
    own, width = result.shape
    vm, hbm = pl.BlockSpec(memory_space=pltpu.VMEM), pl.BlockSpec(memory_space=pl.ANY)
    sem = pltpu.SemaphoreType.DMA
    shapes = [((own, width), bf), ((own, width), f32), ((width,), f32), ((width,), f32), ((units, width), f32), ((width, units), f32)] + [((local, width), f32)] * 4
    return pl.pallas_call(
        finish_kernel,
        out_shape=[jax.ShapeDtypeStruct(s, d) for s, d in shapes],
        in_specs=[hbm, hbm, vm, hbm],
        out_specs=[hbm, hbm, vm, vm] + [hbm] * 6,
        scratch_shapes=[pltpu.VMEM((3, local, width), bf), pltpu.VMEM((3, local, width), f32), pltpu.VMEM((own, width), bf), pltpu.VMEM((own, width), f32), sem((3,)), sem((3,)), sem((4,))],
        compiler_params=pltpu.CompilerParams(vmem_limit_bytes=67043328),
    )(result, input_grad, gains, sums)


def on_device(
    hidden_in,
    segment_ids,
    attn_gain,
    query_weight,
    key_weight,
    value_weight,
    out_weight,
    mlp_gain,
    up_weight,
    down_weight,
    out_cotangent,
):
    row_count = segment_ids.shape[0]
    seq_len = segment_ids.shape[1]
    local_width = query_weight.shape[1]
    head_count = local_width // HEAD
    scale = 1.0 / math.sqrt(HEAD)
    block = min(512, seq_len)
    head_shape = (row_count, seq_len, head_count, HEAD)
    x_float = hidden_in.astype(jnp.float32)
    scaled_one, normed_one, inverse_one = normalize(x_float, attn_gain)
    rows_one = lax.all_gather(scaled_one.astype(jnp.bfloat16), "mp", axis=1, tiled=True)
    cosine, sine = rotary_tables(segment_ids, HEAD)
    queries = rotate(project(rows_one, query_weight).reshape(head_shape), cosine, sine).astype(
        jnp.bfloat16
    )
    keys = rotate(project(rows_one, key_weight).reshape(head_shape), cosine, sine).astype(
        jnp.bfloat16
    )
    values = project(rows_one, value_weight).reshape(head_shape).astype(jnp.bfloat16)
    row_index = 0
    mixed_one, log_one = attend_forward(
        queries[row_index], keys[row_index], values[row_index], segment_ids[row_index], scale, block
    )
    mixed_rows = [mixed_one]
    log_rows = [log_one]
    mixed = jnp.stack(mixed_rows, 0).reshape(row_count, seq_len, local_width).astype(jnp.bfloat16)
    attn_share = lax.psum_scatter(project(mixed, out_weight), "mp", scatter_dimension=1, tiled=True)
    resid = x_float + attn_share
    scaled_two, normed_two, inverse_two = normalize(resid, mlp_gain)
    rows_two = lax.all_gather(scaled_two.astype(jnp.bfloat16), "mp", axis=1, tiled=True)
    up_pre = project(rows_two, up_weight)
    hidden = jax.nn.gelu(up_pre, approximate=True).astype(jnp.bfloat16)
    mlp_share = lax.psum_scatter(
        project(hidden, down_weight).astype(jnp.bfloat16), "mp", scatter_dimension=1, tiled=True
    ).astype(jnp.float32)
    result = (resid + mlp_share).astype(jnp.bfloat16)
    grad_top = out_cotangent.astype(jnp.float32)
    grad_rows = lax.all_gather(out_cotangent, "mp", axis=1, tiled=True)
    down_total = weight_grad(hidden, grad_rows)
    grad_hidden = project_back(grad_rows, down_weight)
    grad_up_pre = (grad_hidden * gelu_slope(up_pre)).astype(jnp.bfloat16)
    up_total = weight_grad(rows_two, grad_up_pre)
    grad_two = lax.psum_scatter(
        project_back(grad_up_pre, up_weight), "mp", scatter_dimension=1, tiled=True
    )
    resid_part, mlp_gain_part = norm_back(grad_two, normed_two, inverse_two, mlp_gain)
    grad_resid = grad_top + resid_part
    branch_rows = lax.all_gather(grad_resid.astype(jnp.bfloat16), "mp", axis=1, tiled=True)
    out_total = weight_grad(mixed, branch_rows)
    grad_mixed = project_back(branch_rows, out_weight).astype(jnp.bfloat16).reshape(head_shape)
    row_index = 0
    grad_q, grad_k, grad_v = attend_back(
        queries[row_index],
        keys[row_index],
        values[row_index],
        grad_mixed[row_index],
        log_rows[row_index],
        segment_ids[row_index],
        scale,
        block,
    )
    query_rows = [grad_q]
    key_rows = [grad_k]
    value_rows = [grad_v]
    grad_query = (
        rotate_back(jnp.stack(query_rows, 0), cosine, sine)
        .astype(jnp.bfloat16)
        .reshape(row_count, seq_len, local_width)
    )
    grad_key = (
        rotate_back(jnp.stack(key_rows, 0), cosine, sine)
        .astype(jnp.bfloat16)
        .reshape(row_count, seq_len, local_width)
    )
    grad_value = (
        jnp.stack(value_rows, 0).astype(jnp.bfloat16).reshape(row_count, seq_len, local_width)
    )
    query_total = weight_grad(rows_one, grad_query)
    key_total = weight_grad(rows_one, grad_key)
    value_total = weight_grad(rows_one, grad_value)
    grad_terms = (
        project_back(grad_query, query_weight)
        + project_back(grad_key, key_weight)
        + project_back(grad_value, value_weight)
    )
    grad_one = lax.psum_scatter(grad_terms, "mp", scatter_dimension=1, tiled=True)
    input_part, attn_gain_part = norm_back(grad_one, normed_one, inverse_one, attn_gain)
    input_grad = grad_resid + input_part
    attn_gain_part, mlp_gain_part = lax.psum((attn_gain_part, mlp_gain_part), "mp")
    (
        query_total,
        key_total,
        value_total,
        out_total,
        attn_gain_part,
        mlp_gain_part,
        up_total,
        down_total,
    ) = lax.psum(
        (
            query_total,
            key_total,
            value_total,
            out_total,
            attn_gain_part,
            mlp_gain_part,
            up_total,
            down_total,
        ),
        "dp",
    )
    return (
        result,
        input_grad,
        attn_gain_part,
        query_total,
        key_total,
        value_total,
        out_total,
        mlp_gain_part,
        up_total,
        down_total,
    )


def on_device_kernels(
    hidden_in, segment_ids, attn_gain, query_weight, key_weight, value_weight, out_weight, mlp_gain, up_weight, down_weight, out_cotangent
):
    sums = layer(
        hidden_in[0], out_cotangent[0], segment_ids, attn_gain, mlp_gain,
        query_weight.T, key_weight.T, value_weight.T, out_weight, up_weight, down_weight,
    )
    result, input_grad, one, two, down, up, out, query, key, value = finish(*sums, up_weight.shape[1], out_weight.shape[0])
    return (result[None], input_grad[None], one, query.T, key.T, value.T, out, two, up, down)


def solution(mesh):
    return jax.shard_map(
        on_device_kernels if mesh.shape["dp"] == 8 else on_device,
        mesh=mesh,
        in_specs=(
            P("dp", "mp", None),
            P("dp", None),
            P(),
            P(None, "mp"),
            P(None, "mp"),
            P(None, "mp"),
            P("mp", None),
            P(),
            P(None, "mp"),
            P("mp", None),
            P("dp", "mp", None),
        ),
        out_specs=(
            P("dp", "mp", None),
            P("dp", "mp", None),
            P(),
            P(None, "mp"),
            P(None, "mp"),
            P(None, "mp"),
            P("mp", None),
            P(),
            P(None, "mp"),
            P("mp", None),
        ),
        check_vma=False,
    )
```

```python
import math

import jax
import jax.numpy as jnp
from jax import lax
from jax.experimental import pallas as pl
from jax.experimental.pallas import tpu as pltpu
from jax.sharding import PartitionSpec as P

HEAD = 80


EPS = 1e-06
MASKED = -1e30
GELU_C = math.sqrt(2.0 / math.pi)
GELU_K = 0.044715


def normalize(values, gain):
    inverse = lax.rsqrt(jnp.mean(values * values, -1, keepdims=True) + EPS)
    normed = values * inverse
    return (normed * gain, normed, inverse)


def norm_back(upstream, normed, inverse, gain):
    scaled = upstream * gain
    inner = jnp.mean(scaled * normed, -1, keepdims=True)
    return (inverse * (scaled - normed * inner), jnp.sum(upstream * normed, axis=(0, 1)))


def gelu_slope(values):
    tangent = jnp.tanh(GELU_C * (values + GELU_K * values * values * values))
    return 0.5 * (1.0 + tangent) + 0.5 * values * (1.0 - tangent * tangent) * GELU_C * (
        1.0 + 3.0 * GELU_K * values * values
    )


def project(left, weight):
    return jnp.einsum("rsd,de->rse", left, weight, preferred_element_type=jnp.float32)


def project_back(left, weight):
    return jnp.einsum("rse,de->rsd", left, weight, preferred_element_type=jnp.float32)


def weight_grad(left, right):
    return jnp.einsum("rsd,rse->de", left, right, preferred_element_type=jnp.float32)


def rotary_tables(segments, head_size):
    seq_len = segments.shape[1]
    places = jnp.arange(seq_len, dtype=jnp.int32)
    starts_here = jnp.concatenate(
        [jnp.ones((segments.shape[0], 1), bool), segments[:, 1:] != segments[:, :-1]], axis=1
    )
    first = lax.cummax(jnp.where(starts_here, places[None, :], 0), axis=1)
    position = (places[None, :] - first).astype(jnp.float32)
    half = head_size // 2
    freqs = jnp.exp(jnp.arange(half, dtype=jnp.float32) * (-2.0 * math.log(10000.0) / head_size))
    angles = position[:, :, None] * freqs[None, None, :]
    return (jnp.cos(angles)[:, :, None, :], jnp.sin(angles)[:, :, None, :])


def rotate(values, cosine, sine):
    half = values.shape[-1] // 2
    first, second = (values[..., :half], values[..., half:])
    return jnp.concatenate([first * cosine - second * sine, second * cosine + first * sine], -1)


def rotate_back(grads, cosine, sine):
    half = grads.shape[-1] // 2
    first, second = (grads[..., :half], grads[..., half:])
    return jnp.concatenate([first * cosine + second * sine, second * cosine - first * sine], -1)


def allowed_block(segments_row, start, size):
    seq_len = segments_row.shape[0]
    query_pos = start + jnp.arange(size, dtype=jnp.int32)
    key_pos = jnp.arange(seq_len, dtype=jnp.int32)
    query_seg = segments_row[start : start + size]
    return (query_pos[:, None] >= key_pos[None, :]) & (query_seg[:, None] == segments_row[None, :])


def block_scores(query_block, keys, allowed, scale):
    scores = (
        jnp.einsum("qhd,khd->hqk", query_block, keys, preferred_element_type=jnp.float32) * scale
    )
    return jnp.where(allowed[None], scores, MASKED)


def attend_forward(queries, keys, values, segments_row, scale, block):
    outputs = []
    sums = []
    for start in range(0, queries.shape[0], block):
        allowed = allowed_block(segments_row, start, block)
        scores = block_scores(queries[start : start + block], keys, allowed, scale)
        top = jnp.max(scores, -1, keepdims=True)
        expo = jnp.exp(scores - top)
        total = jnp.sum(expo, -1, keepdims=True)
        probs = (expo / total).astype(jnp.bfloat16)
        outputs.append(
            jnp.einsum("hqk,khd->qhd", probs, values, preferred_element_type=jnp.float32)
        )
        sums.append(top + jnp.log(total))
    return (jnp.concatenate(outputs, 0), jnp.concatenate(sums, 1))


def attend_back(queries, keys, values, grad_mixed, log_sums, segments_row, scale, block):
    key_total = jnp.zeros(keys.shape, jnp.float32)
    value_total = jnp.zeros(values.shape, jnp.float32)
    query_parts = []
    for start in range(0, queries.shape[0], block):
        allowed = allowed_block(segments_row, start, block)
        query_block = queries[start : start + block]
        scores = block_scores(query_block, keys, allowed, scale)
        probs = jnp.exp(scores - log_sums[:, start : start + block])
        grad_block = grad_mixed[start : start + block]
        grad_probs = jnp.einsum(
            "qhd,khd->hqk", grad_block, values, preferred_element_type=jnp.float32
        )
        inner = jnp.sum(probs * grad_probs, -1, keepdims=True)
        grad_scores = (probs * (grad_probs - inner)).astype(jnp.bfloat16)
        query_parts.append(
            jnp.einsum("hqk,khd->qhd", grad_scores, keys, preferred_element_type=jnp.float32)
            * scale
        )
        key_total = (
            key_total
            + jnp.einsum(
                "hqk,qhd->khd", grad_scores, query_block, preferred_element_type=jnp.float32
            )
            * scale
        )
        value_total = value_total + jnp.einsum(
            "hqk,qhd->khd",
            probs.astype(jnp.bfloat16),
            grad_block,
            preferred_element_type=jnp.float32,
        )
    return (jnp.concatenate(query_parts, 0), key_total, value_total)


MESH = pl.DeviceIdType.MESH
CHUNK = 64
SLOTS = 6
STAGES = 6
(R1Z, R2Z, R3Z, FZM, FZA, FZB, R1Y, R2Y, R3Y, FYI, FYY) = range(11)
(S0Z, S0Y, S1Z, S1Y, S2Z, S2Y, S3ZM, S3ZE, S3YE, S3YY, S4Z, S4Y) = range(12)


def add_rows(total_ref, row, count, *others):
    value = total_ref[pl.ds(row, count), :].astype(jnp.float32)
    for other in others:
        value = value + other[...].astype(jnp.float32)
    total_ref[pl.ds(row, count), :] = value.astype(jnp.bfloat16)


class Reducer:
    def __init__(self, rows, bufs, send_sem, recv_sem, pairs):
        self.rows, self.bufs, self.send_sem, self.recv_sem, self.pairs = rows, bufs, send_sem, recv_sem, pairs
        dp = lax.axis_index("dp")
        self.place, self.side = lax.div(dp, 2), lax.rem(dp, 2)
        self.inner = (self.place == 1) | (self.place == 2)
        self.end = jnp.logical_not(self.inner)
        self.mate = 2 * (self.place + 1 - 2 * lax.rem(self.place, 2)) + self.side
        self.across = 2 * (3 - self.place) + self.side
        self.twin = 2 * self.place + 1 - self.side
        self.half_z = lax.div(self.place, 2)
        self.half_y = self.side

    def copy(self, source, target, send, recv, slot, device):
        return pltpu.make_async_remote_copy(
            src_ref=source,
            dst_ref=target,
            send_sem=self.send_sem.at[send, slot],
            recv_sem=self.recv_sem.at[recv, slot],
            device_id={"dp": device},
            device_id_type=MESH,
        )

    def whole_z(self, pair):
        return pl.multiple_of(pair * (2 * CHUNK), CHUNK)

    def at_z(self, pair, half):
        return pl.multiple_of(pair * (2 * CHUNK) + half * (CHUNK // 2), CHUNK // 2)

    def at_y(self, pair, half):
        return pl.multiple_of(pair * (2 * CHUNK) + CHUNK + half * (CHUNK // 2), CHUNK // 2)

    def moves(self, pair):
        slot = lax.rem(pair, SLOTS)
        rows, (one_z, two_z, three_z, one_y, two_y, three_y) = self.rows, self.bufs
        half = CHUNK // 2
        mine_z, mine_y = self.half_z, self.half_y
        own_z = rows.at[pl.ds(self.at_z(pair, mine_z), half), :]
        rest_z = rows.at[pl.ds(self.at_z(pair, 1 - mine_z), half), :]
        own_y = rows.at[pl.ds(self.at_y(pair, mine_y), half), :]
        rest_y = rows.at[pl.ds(self.at_y(pair, 1 - mine_y), half), :]
        all_z = rows.at[pl.ds(self.whole_z(pair), CHUNK), :]
        return dict(
            s0z=lambda: self.copy(all_z, one_z.at[slot], S0Z, R1Z, slot, self.mate),
            s0y=lambda: self.copy(rest_y, one_y.at[slot], S0Y, R1Y, slot, self.twin),
            s1z=lambda: self.copy(rest_z, two_z.at[slot], S1Z, R2Z, slot, self.across),
            s1y=lambda: self.copy(two_y.at[slot], two_y.at[slot], S1Y, R2Y, slot, self.mate),
            s2z=lambda: self.copy(own_z, three_z.at[slot], S2Z, R3Z, slot, self.twin),
            s2y=lambda: self.copy(own_y, three_y.at[slot], S2Y, R3Y, slot, self.across),
            s3zm=lambda: self.copy(own_z, own_z, S3ZM, FZM, slot, self.across),
            s3ze=lambda: self.copy(own_z, own_z, S3ZE, FZA, slot, self.mate),
            s3ye=lambda: self.copy(own_y, own_y, S3YE, FYI, slot, self.mate),
            s3yy=lambda: self.copy(own_y, own_y, S3YY, FYY, slot, self.twin),
            s4z=lambda: self.copy(rest_z, rest_z, S4Z, FZB, slot, self.mate),
            s4y=lambda: self.copy(own_y, own_y, S4Y, FYY, slot, self.twin),
        )

    def when(self, slot_index, stage, role, body):
        pair = slot_index - stage
        live = (pair >= 0) & (pair < self.pairs)
        if role is not None:
            live = live & role

        @pl.when(live)
        def _():
            body(pair)

    def slot(self, index):
        half = CHUNK // 2
        one_z, two_z, three_z, one_y, two_y, three_y = self.bufs

        def last(pair):
            m = self.moves(pair)
            @pl.when(self.end)
            def _():
                m["s3ze"]().wait_recv()
                m["s4z"]().wait_recv()
                m["s1y"]().wait_send()
                m["s4y"]().wait_send()
                m["s4y"]().wait_recv()

            @pl.when(self.inner)
            def _():
                m["s3zm"]().wait_send()
                m["s3ze"]().wait_send()
                m["s3ye"]().wait_send()
                m["s3yy"]().wait_send()
                m["s4z"]().wait_send()
                m["s3yy"]().wait_recv()

        def fourth_inner(pair):
            m = self.moves(pair)
            m["s3zm"]().wait_recv()
            m["s4z"]().start()

        def fourth_end(pair):
            m = self.moves(pair)
            m["s3ye"]().wait_recv()
            m["s4y"]().start()

        def third(pair):
            m = self.moves(pair)
            slot = lax.rem(pair, SLOTS)
            m["s2z"]().wait()
            m["s2y"]().wait()
            add_rows(self.rows, self.at_z(pair, self.half_z), half, three_z.at[slot])
            add_rows(self.rows, self.at_y(pair, self.half_y), half, three_y.at[slot])
            m["s3ze"]().start()
            m["s3zm"]().start()
            m["s3ye"]().start()
            m["s3yy"]().start()

        def second(pair):
            m = self.moves(pair)
            slot = lax.rem(pair, SLOTS)
            m["s1z"]().wait()
            m["s1y"]().wait_recv()
            m["s0y"]().wait_send()
            add_rows(
                self.rows, self.at_z(pair, self.half_z), half,
                one_z.at[slot, pl.ds(pl.multiple_of(self.half_z * half, half), half), :], two_z.at[slot],
            )
            add_rows(self.rows, self.at_y(pair, self.half_y), half, one_y.at[slot], two_y.at[slot])
            m["s2z"]().start()
            m["s2y"]().start()

        def first_inner(pair):
            m = self.moves(pair)
            slot = lax.rem(pair, SLOTS)
            m["s0z"]().wait_recv()
            m["s0y"]().wait_recv()
            other = 1 - self.half_z
            add_rows(
                self.rows, self.at_z(pair, other), half,
                one_z.at[slot, pl.ds(pl.multiple_of(other * half, half), half), :],
            )
            m["s1z"]().start()

        def first_end(pair):
            m = self.moves(pair)
            slot = lax.rem(pair, SLOTS)
            m["s0y"]().wait()
            m["s0z"]().wait_send()
            mine = self.rows[pl.ds(self.at_y(pair, self.half_y), half), :].astype(jnp.float32)
            two_y[slot] = (mine + one_y[slot].astype(jnp.float32)).astype(jnp.bfloat16)
            m["s1y"]().start()

        def start(pair):
            m = self.moves(pair)
            m["s0y"]().start()

            @pl.when(self.end)
            def _():
                m["s0z"]().start()

        self.when(index, 0, None, start)
        self.when(index, 1, self.end, first_end)
        self.when(index, 1, self.inner, first_inner)
        self.when(index, 2, self.inner, second)
        self.when(index, 3, self.inner, third)
        self.when(index, 4, self.inner, fourth_inner)
        self.when(index, 4, self.end, fourth_end)
        self.when(index, 5, None, last)

    def greet(self, barrier):
        for device in (self.mate, self.across, self.twin):
            pl.semaphore_signal(barrier, inc=1, device_id={"dp": device}, device_id_type=MESH)
        return 3


def reducer_scratch(width):
    half = CHUNK // 2
    return [
        pltpu.VMEM((SLOTS, CHUNK, width), jnp.bfloat16),
        pltpu.VMEM((SLOTS, half, width), jnp.bfloat16),
        pltpu.VMEM((SLOTS, half, width), jnp.bfloat16),
        pltpu.VMEM((SLOTS, half, width), jnp.bfloat16),
        pltpu.VMEM((SLOTS, half, width), jnp.bfloat16),
        pltpu.VMEM((SLOTS, half, width), jnp.bfloat16),
        pltpu.SemaphoreType.DMA((12, SLOTS)),
        pltpu.SemaphoreType.DMA((11, SLOTS)),
    ]


HEAD_PAD = 128
BLOCK_SEQ = 256
SPAN = 512


def pad_matrix(local, padded):
    shape = (padded, local)
    feature = lax.broadcasted_iota(jnp.int32, shape, 1)
    lane = lax.broadcasted_iota(jnp.int32, shape, 0)
    head = jnp.zeros(shape, jnp.int32)
    for h in range(1, local // HEAD):
        head = head + (feature >= h * HEAD).astype(jnp.int32)
    within = feature - head * HEAD
    target = head * HEAD_PAD + within + jnp.where(within >= HEAD // 2, HEAD_PAD // 2 - HEAD // 2, 0)
    return jnp.where(lane == target, 1.0, 0.0).astype(jnp.bfloat16)


def dot(a, b):
    return jnp.dot(a, b, preferred_element_type=jnp.float32)


def dot_nt(a, b):
    return lax.dot_general(a, b, (((1,), (1,)), ((), ())), preferred_element_type=jnp.float32)


def dot_tn(a, b):
    return lax.dot_general(a, b, (((0,), (0,)), ((), ())), preferred_element_type=jnp.float32)


def segment_columns(seg):
    lines = jnp.broadcast_to(seg.astype(jnp.float32), (16, seg.shape[1])).astype(jnp.bfloat16)
    pick = (lax.broadcasted_iota(jnp.int32, (16, 128), 0) == 0).astype(jnp.float32).astype(jnp.bfloat16)
    return dot_tn(lines, pick)


def rotary_into(seg, cos_ref, sin_ref):
    seq = seg.shape[1]
    ids = segment_columns(seg)
    first = jnp.zeros((seq, 128), jnp.float32)
    row = seg.astype(jnp.float32)
    for s in range(1, 16):
        before = jnp.sum(jnp.where(row < s, 1.0, 0.0), axis=1, keepdims=True)
        first = jnp.where(ids == s, before, first)
    position = lax.broadcasted_iota(jnp.int32, (seq, 128), 0).astype(jnp.float32) - first
    lane = lax.broadcasted_iota(jnp.int32, (1, 128), 1)
    upper = lane >= HEAD_PAD // 2
    index = jnp.where(upper, lane - HEAD_PAD // 2, lane)
    freqs = jnp.exp(index.astype(jnp.float32) * (-2.0 * math.log(10000.0) / HEAD))
    freqs = jnp.where(index < HEAD // 2, freqs, 0.0)
    angles = position * freqs
    cos_ref[...] = jnp.cos(angles)
    sin_ref[...] = jnp.where(upper, jnp.sin(angles), -jnp.sin(angles))


class Ring4:
    def __init__(self):
        mp = lax.axis_index("mp")
        chip, core = lax.div(mp, 2), lax.rem(mp, 2)
        self.me = mp
        self.core = 2 * chip + 1 - core
        self.chip = 2 * (1 - chip) + core
        self.far = 2 * (1 - chip) + 1 - core


def block_rows(index):
    return pl.ds(pl.multiple_of(index * BLOCK_SEQ, BLOCK_SEQ), BLOCK_SEQ)


class Gather:
    def __init__(self, ring, rows, sems, parts=1):
        self.parts = parts
        size = BLOCK_SEQ // parts

        def copy(block, device, which, part):
            at = pl.ds(pl.multiple_of(block * BLOCK_SEQ + part * size, size), size)
            return pltpu.make_async_remote_copy(
                src_ref=rows.at[at, :],
                dst_ref=rows.at[at, :],
                send_sem=sems.at[0, which * parts + part],
                recv_sem=sems.at[1, which * parts + part],
                device_id={"mp": device},
                device_id_type=MESH,
            )

        self.near = lambda part=0: copy(ring.me, ring.core, 0, part)
        self.across = lambda part=0: copy(ring.me, ring.chip, 1, part)
        self.onward = lambda part=0: copy(ring.chip, ring.core, 2, part)

    def start(self, part=0):
        self.across(part).start()
        self.near(part).start()

    def forward(self):
        for part in range(self.parts):
            self.across(part).wait_recv()
            self.onward(part).start()

    def near_in(self):
        for part in range(self.parts):
            self.near(part).wait_recv()

    def onward_in(self):
        for part in range(self.parts):
            self.onward(part).wait_recv()

    def sent(self):
        for part in range(self.parts):
            self.near(part).wait_send()
            self.across(part).wait_send()
            self.onward(part).wait_send()


class Scatter:
    def __init__(self, ring, send_core, recv_core, send_chip, recv_chip, sems, parts=1):
        self.parts = parts
        size = BLOCK_SEQ // parts

        def copy(source, target, device, which, part):
            at = pl.ds(part * size, size)
            return pltpu.make_async_remote_copy(
                src_ref=source.at[at, :],
                dst_ref=target.at[at, :],
                send_sem=sems.at[0, which * parts + part],
                recv_sem=sems.at[1, which * parts + part],
                device_id={"mp": device},
                device_id_type=MESH,
            )

        self.far = lambda part=0: copy(send_core.at[0], recv_core.at[0], ring.core, 0, part)
        self.core = lambda part=0: copy(send_core.at[1], recv_core.at[1], ring.core, 1, part)
        self.chip = lambda part=0: copy(send_chip, recv_chip, ring.chip, 2, part)


def greet_mp(ring, barrier):
    for device in (ring.core, ring.chip):
        pl.semaphore_signal(barrier, inc=1, device_id={"mp": device}, device_id_type=MESH)
    return 2


def norm_rows(values):
    inverse = lax.rsqrt(jnp.mean(values * values, -1, keepdims=True) + EPS)
    return values * inverse, inverse


def qkv_block(rows, weights, cos_ref, sin_ref, out, block):
    at = block_rows(block)
    turned = 2 * (weights.shape[0] // 3) // 256
    tiles = weights.shape[0] // 256

    def one(n, turn):
        cols = pl.ds(pl.multiple_of(n * 256, 256), 256)
        value = dot_nt(rows[at, :], weights[cols, :])
        if turn:
            cosine, sine = cos_ref[at, :], sin_ref[at, :]
            halves = [value[:, j * 128 : j * 128 + 128] for j in range(2)]
            value = jnp.concatenate([h * cosine + pltpu.roll(h, 64, 1) * sine for h in halves], axis=1)
        out[at, cols] = value.astype(jnp.bfloat16)

    @pl.loop(0, turned)
    def _(n):
        one(n, True)

    @pl.loop(turned, tiles)
    def _(n):
        one(n, False)


def masks_into(seg, ids_ref, bias_ref):
    seq = seg.shape[1]
    for i in range(seq // BLOCK_SEQ):
        low = max(0, i * BLOCK_SEQ - SPAN)
        high = (i + 1) * BLOCK_SEQ
        shape = (BLOCK_SEQ, high - low)
        query = i * BLOCK_SEQ + lax.broadcasted_iota(jnp.int32, shape, 0)
        key = low + lax.broadcasted_iota(jnp.int32, shape, 1)
        ids = ids_ref[pl.ds(i * BLOCK_SEQ, BLOCK_SEQ), :][:, :1]
        same = ids == seg[:, low:high].astype(jnp.float32)
        bias_ref[pl.ds(i * BLOCK_SEQ, BLOCK_SEQ), pl.ds(0, high - low)] = jnp.where((query >= key) & same, 0.0, MASKED).astype(bias_ref.dtype)


def attend(qkv, out, bias_ref, stats, heads, scale, blocks):
    width = heads * HEAD_PAD
    lane = lax.broadcasted_iota(jnp.int32, (BLOCK_SEQ, 128), 1)

    @pl.loop(0, heads)
    def _(h):
        lanes = [pl.ds(pl.multiple_of(part * width + h * HEAD_PAD, HEAD_PAD), HEAD_PAD) for part in range(3)]
        for i in blocks:
            low, high = max(0, i * BLOCK_SEQ - SPAN), (i + 1) * BLOCK_SEQ
            rows, keys = pl.ds(i * BLOCK_SEQ, BLOCK_SEQ), pl.ds(low, high - low)
            scores = dot_nt(qkv[rows, lanes[0]], qkv[keys, lanes[1]]) + bias_ref[rows, pl.ds(0, high - low)]
            top = jnp.max(scores, -1, keepdims=True)
            expo = jnp.exp((scores - top) * scale)
            total = jnp.sum(expo, -1, keepdims=True)
            stats[rows, :] = jnp.where(lane == h, top * scale + jnp.log(total), stats[rows, :])
            out[rows, lanes[0]] = (dot(expo.astype(jnp.bfloat16), qkv[keys, lanes[2]]) * (1.0 / total)).astype(jnp.bfloat16)


def layer_kernel(
    x, g, seg, gain_one, gain_two, wq, wk, wv, wo, wup, wdown,
    result_o, input_o, gains_o, sums_o,
    rows, b0, b1, b2, b3, b4, b5, send_sem, recv_sem, save_sem,
    w_up, w_down, w_qkv, w_out, rows_one, rows_g, rows_two, hidden, grad_up, branch, qkv, mixed, grad_mixed,
    cos_ref, sin_ref, bias_ref, resid, term_ref, key_sum, value_sum,
    send_core, recv_core, send_chip, recv_chip, gain_acc, gain_recv,
    load_sem, one_sem, g_sem, two_sem, branch_sem, rs0_sem, rs_sem, rs2_sem, rs3_sem, gain_sem, free_sem, ready_sem, stats,
):
    bf, f32 = jnp.bfloat16, jnp.float32
    ring = Ring4()
    seq, width = rows_two.shape
    units = w_up.shape[1]
    padded = w_out.shape[0]
    heads = padded // HEAD_PAD
    local = heads * HEAD
    pairs = rows.shape[0] // (2 * CHUNK)
    scale = 1.0 / math.sqrt(HEAD)
    half = BLOCK_SEQ // 2
    chip = lax.div(ring.me, 2)
    red = Reducer(rows, (b0, b1, b2, b3, b4, b5), send_sem, recv_sem, pairs)
    barrier = pltpu.get_barrier_semaphore()
    count = greet_mp(ring, barrier) + red.greet(barrier)
    places = [(w, rows.at[pl.ds(i * local, local), :]) for i, w in enumerate((wq, wk, wv, wo))]
    places += [(g, rows_g.at[block_rows(ring.me), :]), (wup, w_up), (wdown, w_down)]
    loads = [pltpu.make_async_copy(source, target, load_sem.at[i]) for i, (source, target) in enumerate(places)]
    for load in loads[:5]:
        load.start()
    normed, _ = norm_rows(x[...].astype(f32))
    rows_one[block_rows(ring.me), :] = (normed * gain_one[...]).astype(bf)
    one, all_g = Gather(ring, rows_one, one_sem, 2), Gather(ring, rows_g, g_sem)
    two, all_branch = Gather(ring, rows_two, two_sem, 2), Gather(ring, branch, branch_sem)
    ahead = Scatter(ring, send_core, recv_core, send_chip, recv_chip, rs0_sem, 2)
    first = Scatter(ring, send_core, recv_core, send_chip, recv_chip, rs_sem)
    second = Scatter(ring, send_core, recv_core, send_chip, recv_chip, rs2_sem)
    third = Scatter(ring, send_core, recv_core, send_chip, recv_chip, rs3_sem)
    pl.semaphore_wait(barrier, count)
    one.start(0)
    one.start(1)
    for load in loads[5:]:
        load.start()

    spread = pad_matrix(local, padded)
    for i in range(3):
        loads[i].wait()
        w_qkv[pl.ds(i * padded, padded), :] = dot(spread, rows[pl.ds(i * local, local), :]).astype(bf)
    loads[3].wait()
    w_out[...] = dot(spread, rows[pl.ds(3 * local, local), :]).astype(bf)
    loads[4].wait()
    all_g.start()
    rotary_into(seg[...], cos_ref, sin_ref)
    qkv_block(rows_one, w_qkv, cos_ref, sin_ref, qkv, ring.me)
    one.near_in()
    qkv_block(rows_one, w_qkv, cos_ref, sin_ref, qkv, ring.core)
    key_sum[...] = segment_columns(seg[...])
    masks_into(seg[...], key_sum, bias_ref)
    one.forward()
    one.across(0).wait_send()
    one.across(1).wait_send()
    qkv_block(rows_one, w_qkv, cos_ref, sin_ref, qkv, ring.chip)
    one.onward_in()
    qkv_block(rows_one, w_qkv, cos_ref, sin_ref, qkv, ring.far)

    stats[...] = jnp.zeros_like(stats)
    early, late = (0, 1), (2, 3)

    @pl.when(chip == 0)
    def _():
        attend(qkv, mixed, bias_ref, stats, heads, scale, late)

    @pl.when(chip == 1)
    def _():
        attend(qkv, mixed, bias_ref, stats, heads, scale, early)

    def term(block, part):
        at = pl.ds(pl.multiple_of(block * BLOCK_SEQ + part * half, half), half)
        return dot(mixed[at, :], w_out[...])

    parts = [pl.ds(p * half, half) for p in range(2)]
    for p in range(2):
        send_core[0, parts[p], :] = term(ring.far, p).astype(bf)
        ahead.far(p).start()
    for p in range(2):
        value = term(ring.chip, p)
        ahead.far(p).wait_recv()
        send_chip[parts[p], :] = (value + recv_core[0, parts[p], :].astype(f32)).astype(bf)
        ahead.chip(p).start()

    @pl.when(chip == 0)
    def _():
        attend(qkv, mixed, bias_ref, stats, heads, scale, early)

    @pl.when(chip == 1)
    def _():
        attend(qkv, mixed, bias_ref, stats, heads, scale, late)

    for p in range(2):
        send_core[1, parts[p], :] = term(ring.core, p).astype(bf)
        ahead.core(p).start()
    all_g.forward()
    for p in range(2):
        resid[parts[p], :] = x[parts[p], :].astype(f32) + term(ring.me, p)
    for p in range(2):
        ahead.core(p).wait_recv()
        ahead.chip(p).wait_recv()
        value = resid[parts[p], :] + recv_core[1, parts[p], :].astype(f32) + recv_chip[parts[p], :].astype(f32)
        resid[parts[p], :] = value
        normed, _ = norm_rows(value)
        at = pl.ds(pl.multiple_of(ring.me * BLOCK_SEQ + p * half, half), half)
        rows_two[at, :] = (normed * gain_two[...]).astype(bf)
        two.start(p)
    for p in range(2):
        ahead.far(p).wait_send()
        ahead.core(p).wait_send()
        ahead.chip(p).wait_send()

    base = 2 * units

    def put(pair):
        at = pl.ds(pl.multiple_of(pair * 2 * CHUNK, 2 * CHUNK), 2 * CHUNK)
        return pltpu.make_async_copy(rows.at[at, :], sums_o.at[at, :], save_sem.at[lax.rem(pair, 4)])

    def slot(index):
        red.slot(index)
        pair = index - (STAGES - 1)

        @pl.when(pair >= 4)
        def _():
            put(pair - 4).wait()

        @pl.when(pair >= 0)
        def _():
            put(pair).start()

    def tile(n):
        return pl.ds(pl.multiple_of(n * 256, 256), 256)

    def half_rows(block, part):
        return pl.ds(pl.multiple_of(block * BLOCK_SEQ + part * half, half), half)

    def up_tile(at, n):
        u = dot(rows_two[at, :], w_up[:, tile(n)])
        tangent = jnp.tanh(GELU_C * (u + GELU_K * u * u * u))
        hidden[at, tile(n)] = (0.5 * u * (1.0 + tangent)).astype(bf)

    def up_rows_of(at):
        @pl.loop(0, units // 256)
        def _(n):
            up_tile(at, n)

    loads[5].wait()
    up_rows_of(block_rows(ring.me))
    two.near_in()
    up_rows_of(block_rows(ring.core))
    all_g.near_in()
    all_g.onward_in()
    two.across(0).wait_recv()
    two.onward(0).start()
    up_rows_of(half_rows(ring.chip, 0))
    two.onward(0).wait_recv()
    up_rows_of(half_rows(ring.far, 0))
    two.across(1).wait_recv()
    two.onward(1).start()

    loads[6].wait()

    def order(k):
        there = k < 2
        core = lax.rem(ring.me, 2)
        flip = 1 - lax.rem(k, 2)
        to_chip = jnp.where(there, 1 - chip, chip)
        to_core = jnp.where(flip == 1, 1 - core, core)
        return 2 * to_chip + to_core

    def hand_on(k, scatter, start):
        @pl.when(k == 0)
        def _():
            send_core[0] = term_ref[...].astype(bf)
            scatter.far().start()

        @pl.when(k == 1)
        def _():
            scatter.far().wait_recv()
            send_chip[...] = (term_ref[...] + recv_core[0].astype(f32)).astype(bf)
            scatter.chip().start()

        @pl.when(k == 2)
        def _():
            send_core[1] = term_ref[...].astype(bf)
            scatter.core().start()

        @pl.when(k == 3)
        def _():
            scatter.core().wait_recv()
            term_ref[...] = term_ref[...] + recv_core[1].astype(f32)

    def settle(scatter):
        for copy in (scatter.far(), scatter.core()):
            copy.wait_send()
        scatter.chip().wait()
        return term_ref[...] + recv_chip[...].astype(f32)

    def grad_tile(at, n):
        u = dot(rows_two[at, :], w_up[:, tile(n)])
        upstream = dot_nt(rows_g[at, :], w_down[tile(n), :])
        tangent = jnp.tanh(GELU_C * (u + GELU_K * u * u * u))
        slope = 0.5 * (1.0 + tangent) + 0.5 * u * (1.0 - tangent * tangent) * GELU_C * (1.0 + 3.0 * GELU_K * u * u)
        grad_up[at, tile(n)] = (upstream * slope).astype(bf)

    @pl.loop(0, units // 256)
    def _(n):
        up_tile(half_rows(ring.chip, 1), n)

        @pl.when(n == 0)
        def _():
            two.onward(1).wait_recv()

        up_tile(half_rows(ring.far, 1), n)
        rows[tile(n), :] = dot_tn(hidden[:, tile(n)], rows_g[...]).astype(bf)
        slot(n)

        @pl.loop(0, 3)
        def _(k):
            grad_tile(block_rows(order(k)), n)

    @pl.loop(0, 4)
    def _(k):
        @pl.loop(0, 2)
        def _(j):
            @pl.when(2 * k + j < units // 256)
            def _():
                grad_tile(block_rows(order(3)), 2 * k + j)

        at = block_rows(order(k))

        @pl.loop(0, width // 256)
        def _(n):
            term_ref[:, tile(n)] = dot_nt(grad_up[at, :], w_up[tile(n), :])

        hand_on(k, first, None)
        slot(5 + k)

    def up_rows(i):
        rows[pl.ds(pl.multiple_of(units + i * 256, 256), 256), :] = dot_tn(rows_two[:, tile(i)], grad_up[...]).astype(bf)

    up_rows(0)
    slot(9)
    grad_two = settle(first)
    normed, inverse = norm_rows(resid[...])
    scaled = grad_two * gain_two[...]
    part = inverse * (scaled - normed * jnp.mean(scaled * normed, -1, keepdims=True))
    mlp_part = jnp.sum(grad_two * normed, axis=0, keepdims=True)
    gain_acc[0] = jnp.zeros(gain_acc.shape[1:], f32)
    gain_acc[0, 1:2, :] = mlp_part
    mine = rows_g[block_rows(ring.me), :].astype(f32) + part
    input_o[...] = mine
    branch[block_rows(ring.me), :] = mine.astype(bf)
    all_branch.across().start()
    all_branch.near().start()
    for device in (ring.core, ring.chip):
        pl.semaphore_signal(ready_sem, inc=1, device_id={"mp": device}, device_id_type=MESH)

    def head_rows(left, lane, right, row):
        value = dot_tn(left[:, lane], right[...])
        halves = [value[at : at + HEAD // 2, :] for at in (0, 64, 128, 192)]
        rows[pl.ds(pl.multiple_of(row, 16), 2 * HEAD), :] = jnp.concatenate(halves, axis=0).astype(bf)

    @pl.loop(1, units // 256)
    def _(i):
        up_rows(i)

        @pl.when(i == 1)
        def _():
            pl.semaphore_wait(ready_sem, 2)

        at = block_rows(order(i - 1))

        @pl.loop(0, width // 256)
        def _(n):
            term_ref[:, tile(n)] = dot(hidden[at, :], w_down[:, tile(n)])

        hand_on(i - 1, second, None)

        @pl.when(i == 4)
        def _():
            all_branch.near().wait_recv()
            all_branch.forward()
            all_branch.onward().wait_recv()

            @pl.loop(0, heads // 2)
            def _(j):
                head_rows(mixed, tile(j), branch, base + j * 2 * HEAD)

        slot(9 + i)

    @pl.loop(0, 4)
    def _(b):
        grad_mixed[block_rows(b), :] = dot_nt(branch[block_rows(b), :], w_out[...]).astype(bf)

    lane = lax.broadcasted_iota(jnp.int32, (BLOCK_SEQ, 128), 1)

    @pl.loop(0, heads)
    def _(h):
        lanes = [pl.ds(pl.multiple_of(n * padded + h * HEAD_PAD, HEAD_PAD), HEAD_PAD) for n in range(3)]
        key_sum[...] = jnp.zeros_like(key_sum)
        value_sum[...] = jnp.zeros_like(value_sum)
        for i in range(seq // BLOCK_SEQ):
            low, high = max(0, i * BLOCK_SEQ - SPAN), (i + 1) * BLOCK_SEQ
            at, keys = pl.ds(i * BLOCK_SEQ, BLOCK_SEQ), pl.ds(low, high - low)
            query, upstream = qkv[at, lanes[0]], grad_mixed[at, lanes[0]]
            scores = dot_nt(query, qkv[keys, lanes[1]]) + bias_ref[at, pl.ds(0, high - low)]
            level = jnp.sum(jnp.where(lane == h, stats[at, :], 0.0), -1, keepdims=True)
            probs = jnp.exp(scores * scale - level)
            grad_probs = dot_nt(upstream, qkv[keys, lanes[2]])
            inner = jnp.sum(probs * grad_probs, -1, keepdims=True)
            grad_scores = (probs * (grad_probs - inner)).astype(bf)
            value_sum[keys, :] += dot_tn(probs.astype(bf), upstream)
            key_sum[keys, :] += dot_tn(grad_scores, query)
            turned = dot(grad_scores, qkv[keys, lanes[1]]) * scale
            qkv[at, lanes[0]] = (turned * cos_ref[at, :] - pltpu.roll(turned, 64, 1) * sin_ref[at, :]).astype(bf)
            if i == 1:
                slot(14 + 2 * h)
        turned = key_sum[...] * scale
        qkv[:, lanes[1]] = (turned * cos_ref[...] - pltpu.roll(turned, 64, 1) * sin_ref[...]).astype(bf)
        qkv[:, lanes[2]] = value_sum[...].astype(bf)
        slot(15 + 2 * h)

    @pl.loop(0, 3)
    def _(part):
        for j in range(heads // 2):
            lane = pl.ds(pl.multiple_of(part * padded + j * 256, 256), 256)
            head_rows(qkv, lane, rows_one, base + (part + 1) * local + j * 2 * HEAD)
        slot(22 + part)

    result_o[...] = (resid[...] + settle(second)).astype(bf)
    for device in (ring.core, ring.chip):
        pl.semaphore_signal(free_sem, inc=1, device_id={"mp": device}, device_id_type=MESH)
    pl.semaphore_wait(free_sem, 2)

    @pl.loop(0, 4)
    def _(k):
        at = block_rows(order(k))

        @pl.loop(0, width // 256)
        def _(n):
            term_ref[:, tile(n)] = dot(qkv[at, :], w_qkv[:, tile(n)])

        hand_on(k, third, None)
        slot(25 + k)

    slot(29)
    grad_one = settle(third)
    normed, inverse = norm_rows(x[...].astype(f32))
    scaled = grad_one * gain_one[...]
    input_o[...] = input_o[...] + inverse * (scaled - normed * jnp.mean(scaled * normed, -1, keepdims=True))
    gain_acc[0, 0:1, :] = jnp.sum(grad_one * normed, axis=0, keepdims=True)

    def exchange(step):
        names = ({"mp": ring.core}, {"mp": ring.chip}, {"dp": red.twin}, {"dp": red.mate}, {"dp": red.across})
        return pltpu.make_async_remote_copy(
            src_ref=gain_acc.at[step], dst_ref=gain_recv.at[step], send_sem=gain_sem.at[0, step], recv_sem=gain_sem.at[1, step],
            device_id=names[step], device_id_type=MESH,
        )

    exchange(0).start()
    last = pairs + STAGES - 1

    @pl.loop(30, last)
    def _(index):
        for step in range(1, 5):

            @pl.when(index == 29 + step)
            def _():
                exchange(step - 1).wait_recv()
                gain_acc[step] = gain_acc[step - 1] + gain_recv[step - 1]
                exchange(step).start()

        slot(index)

    exchange(4).wait_recv()
    gains_o[...] = gain_acc[4] + gain_recv[4]
    for pair in range(pairs - 4, pairs):
        put(pair).wait()
    for step in range(5):
        exchange(step).wait_send()
    for part in range(2):
        one.near(part).wait_send()
        one.onward(part).wait_send()
    for gather in (all_g, two, all_branch):
        gather.sent()


def layer(x, g, seg, gain_one, gain_two, wq, wk, wv, wo, wup, wdown):
    bf, f32 = jnp.bfloat16, jnp.float32
    own, width = x.shape
    units = wup.shape[1]
    seq = seg.shape[1]
    local = wo.shape[0]
    padded = local // HEAD * HEAD_PAD
    total = 2 * units + 4 * local
    vm, hbm = pl.BlockSpec(memory_space=pltpu.VMEM), pl.BlockSpec(memory_space=pl.ANY)
    sem = pltpu.SemaphoreType.DMA
    shapes = [((own, width), bf), ((own, width), f32), ((8, width), f32), ((total, width), bf)]
    tall = pltpu.VMEM((seq, width), bf)
    return pl.pallas_call(
        layer_kernel,
        out_shape=[jax.ShapeDtypeStruct(s, d) for s, d in shapes],
        in_specs=[vm, hbm, vm, vm, vm] + [hbm] * 6,
        out_specs=[vm] * 3 + [hbm],
        scratch_shapes=[pltpu.VMEM((total, width), bf)]
        + reducer_scratch(width)
        + [
            sem((4,)),
            pltpu.VMEM((width, units), bf), pltpu.VMEM((units, width), bf), pltpu.VMEM((3 * padded, width), bf), pltpu.VMEM((padded, width), bf),
            tall, tall, tall, pltpu.VMEM((seq, units), bf), pltpu.VMEM((seq, units), bf), tall,
            pltpu.VMEM((seq, 3 * padded), bf), pltpu.VMEM((seq, padded), bf), pltpu.VMEM((seq, padded), bf),
            pltpu.VMEM((seq, 128), f32), pltpu.VMEM((seq, 128), f32), pltpu.VMEM((seq, SPAN + BLOCK_SEQ), bf),
            pltpu.VMEM((own, width), f32), pltpu.VMEM((own, width), f32), pltpu.VMEM((seq, HEAD_PAD), f32), pltpu.VMEM((seq, HEAD_PAD), f32),
            pltpu.VMEM((2, own, width), bf), pltpu.VMEM((2, own, width), bf), pltpu.VMEM((own, width), bf), pltpu.VMEM((own, width), bf),
            pltpu.VMEM((5, 8, width), f32), pltpu.VMEM((5, 8, width), f32),
            sem((7,)), sem((2, 6)), sem((2, 3)), sem((2, 6)), sem((2, 3)), sem((2, 6)), sem((2, 3)), sem((2, 3)), sem((2, 3)), sem((2, 5)),
            pltpu.SemaphoreType.REGULAR, pltpu.SemaphoreType.REGULAR, pltpu.VMEM((seq, 128), f32),
        ],
        compiler_params=pltpu.CompilerParams(collective_id=0, has_side_effects=True, vmem_limit_bytes=67043328),
    )(x, g, seg, gain_one, gain_two, wq, wk, wv, wo, wup, wdown)


def finish_kernel(result, input_grad, gains, sums, result_o, input_o, one_o, two_o, down_o, up_o, out_o, q_o, k_o, v_o, inbox, outbox, side_one, side_two, in_sem, out_sem, side_sem):
    step = out_o.shape[0]
    targets = [(down_o, i * step) for i in range(down_o.shape[0] // step)] + [(up_o, i * step) for i in range(up_o.shape[0] // step)]
    targets += [(t, 0) for t in (out_o, q_o, k_o, v_o)]
    count, depth = len(targets), inbox.shape[0]
    bring = [pltpu.make_async_copy(result, side_one, side_sem.at[0]), pltpu.make_async_copy(input_grad, side_two, side_sem.at[1])]
    take = [pltpu.make_async_copy(side_one, result_o, side_sem.at[2]), pltpu.make_async_copy(side_two, input_o, side_sem.at[3])]

    def read(i):
        return pltpu.make_async_copy(sums.at[pl.ds(i * step, step), :], inbox.at[i % depth], in_sem.at[i % depth])

    def write(i):
        target, at = targets[i]
        return pltpu.make_async_copy(outbox.at[i % depth], target.at[pl.ds(at, step), :], out_sem.at[i % depth])

    for i in range(depth):
        read(i).start()
    for side in bring:
        side.start()
    one_o[...] = gains[0, :]
    two_o[...] = gains[1, :]
    for i in range(count):
        read(i).wait()
        if i >= depth:
            write(i - depth).wait()
        outbox[i % depth] = inbox[i % depth].astype(jnp.float32)
        write(i).start()
        if i + depth < count:
            read(i + depth).start()
        if i == depth:
            for come, go in zip(bring, take):
                come.wait()
                go.start()
    for i in range(count - depth, count):
        write(i).wait()
    for side in take:
        side.wait()


def finish(result, input_grad, gains, sums, units, local):
    bf, f32 = jnp.bfloat16, jnp.float32
    own, width = result.shape
    vm, hbm = pl.BlockSpec(memory_space=pltpu.VMEM), pl.BlockSpec(memory_space=pl.ANY)
    sem = pltpu.SemaphoreType.DMA
    shapes = [((own, width), bf), ((own, width), f32), ((width,), f32), ((width,), f32), ((units, width), f32), ((width, units), f32)] + [((local, width), f32)] * 4
    return pl.pallas_call(
        finish_kernel,
        out_shape=[jax.ShapeDtypeStruct(s, d) for s, d in shapes],
        in_specs=[hbm, hbm, vm, hbm],
        out_specs=[hbm, hbm, vm, vm] + [hbm] * 6,
        scratch_shapes=[pltpu.VMEM((3, local, width), bf), pltpu.VMEM((3, local, width), f32), pltpu.VMEM((own, width), bf), pltpu.VMEM((own, width), f32), sem((3,)), sem((3,)), sem((4,))],
        compiler_params=pltpu.CompilerParams(vmem_limit_bytes=67043328),
    )(result, input_grad, gains, sums)


def on_device(
    hidden_in,
    segment_ids,
    attn_gain,
    query_weight,
    key_weight,
    value_weight,
    out_weight,
    mlp_gain,
    up_weight,
    down_weight,
    out_cotangent,
):
    row_count = segment_ids.shape[0]
    seq_len = segment_ids.shape[1]
    local_width = query_weight.shape[1]
    head_count = local_width // HEAD
    scale = 1.0 / math.sqrt(HEAD)
    block = min(512, seq_len)
    head_shape = (row_count, seq_len, head_count, HEAD)
    x_float = hidden_in.astype(jnp.float32)
    scaled_one, normed_one, inverse_one = normalize(x_float, attn_gain)
    rows_one = lax.all_gather(scaled_one.astype(jnp.bfloat16), "mp", axis=1, tiled=True)
    cosine, sine = rotary_tables(segment_ids, HEAD)
    queries = rotate(project(rows_one, query_weight).reshape(head_shape), cosine, sine).astype(
        jnp.bfloat16
    )
    keys = rotate(project(rows_one, key_weight).reshape(head_shape), cosine, sine).astype(
        jnp.bfloat16
    )
    values = project(rows_one, value_weight).reshape(head_shape).astype(jnp.bfloat16)
    row_index = 0
    mixed_one, log_one = attend_forward(
        queries[row_index], keys[row_index], values[row_index], segment_ids[row_index], scale, block
    )
    mixed_rows = [mixed_one]
    log_rows = [log_one]
    mixed = jnp.stack(mixed_rows, 0).reshape(row_count, seq_len, local_width).astype(jnp.bfloat16)
    attn_share = lax.psum_scatter(project(mixed, out_weight), "mp", scatter_dimension=1, tiled=True)
    resid = x_float + attn_share
    scaled_two, normed_two, inverse_two = normalize(resid, mlp_gain)
    rows_two = lax.all_gather(scaled_two.astype(jnp.bfloat16), "mp", axis=1, tiled=True)
    up_pre = project(rows_two, up_weight)
    hidden = jax.nn.gelu(up_pre, approximate=True).astype(jnp.bfloat16)
    mlp_share = lax.psum_scatter(
        project(hidden, down_weight).astype(jnp.bfloat16), "mp", scatter_dimension=1, tiled=True
    ).astype(jnp.float32)
    result = (resid + mlp_share).astype(jnp.bfloat16)
    grad_top = out_cotangent.astype(jnp.float32)
    grad_rows = lax.all_gather(out_cotangent, "mp", axis=1, tiled=True)
    down_total = weight_grad(hidden, grad_rows)
    grad_hidden = project_back(grad_rows, down_weight)
    grad_up_pre = (grad_hidden * gelu_slope(up_pre)).astype(jnp.bfloat16)
    up_total = weight_grad(rows_two, grad_up_pre)
    grad_two = lax.psum_scatter(
        project_back(grad_up_pre, up_weight), "mp", scatter_dimension=1, tiled=True
    )
    resid_part, mlp_gain_part = norm_back(grad_two, normed_two, inverse_two, mlp_gain)
    grad_resid = grad_top + resid_part
    branch_rows = lax.all_gather(grad_resid.astype(jnp.bfloat16), "mp", axis=1, tiled=True)
    out_total = weight_grad(mixed, branch_rows)
    grad_mixed = project_back(branch_rows, out_weight).astype(jnp.bfloat16).reshape(head_shape)
    row_index = 0
    grad_q, grad_k, grad_v = attend_back(
        queries[row_index],
        keys[row_index],
        values[row_index],
        grad_mixed[row_index],
        log_rows[row_index],
        segment_ids[row_index],
        scale,
        block,
    )
    query_rows = [grad_q]
    key_rows = [grad_k]
    value_rows = [grad_v]
    grad_query = (
        rotate_back(jnp.stack(query_rows, 0), cosine, sine)
        .astype(jnp.bfloat16)
        .reshape(row_count, seq_len, local_width)
    )
    grad_key = (
        rotate_back(jnp.stack(key_rows, 0), cosine, sine)
        .astype(jnp.bfloat16)
        .reshape(row_count, seq_len, local_width)
    )
    grad_value = (
        jnp.stack(value_rows, 0).astype(jnp.bfloat16).reshape(row_count, seq_len, local_width)
    )
    query_total = weight_grad(rows_one, grad_query)
    key_total = weight_grad(rows_one, grad_key)
    value_total = weight_grad(rows_one, grad_value)
    grad_terms = (
        project_back(grad_query, query_weight)
        + project_back(grad_key, key_weight)
        + project_back(grad_value, value_weight)
    )
    grad_one = lax.psum_scatter(grad_terms, "mp", scatter_dimension=1, tiled=True)
    input_part, attn_gain_part = norm_back(grad_one, normed_one, inverse_one, attn_gain)
    input_grad = grad_resid + input_part
    attn_gain_part, mlp_gain_part = lax.psum((attn_gain_part, mlp_gain_part), "mp")
    (
        query_total,
        key_total,
        value_total,
        out_total,
        attn_gain_part,
        mlp_gain_part,
        up_total,
        down_total,
    ) = lax.psum(
        (
            query_total,
            key_total,
            value_total,
            out_total,
            attn_gain_part,
            mlp_gain_part,
            up_total,
            down_total,
        ),
        "dp",
    )
    return (
        result,
        input_grad,
        attn_gain_part,
        query_total,
        key_total,
        value_total,
        out_total,
        mlp_gain_part,
        up_total,
        down_total,
    )


def on_device_kernels(
    hidden_in, segment_ids, attn_gain, query_weight, key_weight, value_weight, out_weight, mlp_gain, up_weight, down_weight, out_cotangent
):
    sums = layer(
        hidden_in[0], out_cotangent[0], segment_ids, attn_gain, mlp_gain,
        query_weight.T, key_weight.T, value_weight.T, out_weight, up_weight, down_weight,
    )
    result, input_grad, one, two, down, up, out, query, key, value = finish(*sums, up_weight.shape[1], out_weight.shape[0])
    return (result[None], input_grad[None], one, query.T, key.T, value.T, out, two, up, down)


def solution(mesh):
    return jax.shard_map(
        on_device_kernels if mesh.shape["dp"] == 8 else on_device,
        mesh=mesh,
        in_specs=(
            P("dp", "mp", None),
            P("dp", None),
            P(),
            P(None, "mp"),
            P(None, "mp"),
            P(None, "mp"),
            P("mp", None),
            P(),
            P(None, "mp"),
            P("mp", None),
            P("dp", "mp", None),
        ),
        out_specs=(
            P("dp", "mp", None),
            P("dp", "mp", None),
            P(),
            P(None, "mp"),
            P(None, "mp"),
            P(None, "mp"),
            P("mp", None),
            P(),
            P(None, "mp"),
            P("mp", None),
        ),
        check_vma=False,
    )
```

```python
import math

import jax
import jax.numpy as jnp
from jax import lax
from jax.experimental import pallas as pl
from jax.experimental.pallas import tpu as pltpu
from jax.sharding import PartitionSpec as P

HEAD = 80


EPS = 1e-06
MASKED = -1e30
GELU_C = math.sqrt(2.0 / math.pi)
GELU_K = 0.044715


def normalize(values, gain):
    inverse = lax.rsqrt(jnp.mean(values * values, -1, keepdims=True) + EPS)
    normed = values * inverse
    return (normed * gain, normed, inverse)


def norm_back(upstream, normed, inverse, gain):
    scaled = upstream * gain
    inner = jnp.mean(scaled * normed, -1, keepdims=True)
    return (inverse * (scaled - normed * inner), jnp.sum(upstream * normed, axis=(0, 1)))


def gelu_slope(values):
    tangent = jnp.tanh(GELU_C * (values + GELU_K * values * values * values))
    return 0.5 * (1.0 + tangent) + 0.5 * values * (1.0 - tangent * tangent) * GELU_C * (
        1.0 + 3.0 * GELU_K * values * values
    )


def project(left, weight):
    return jnp.einsum("rsd,de->rse", left, weight, preferred_element_type=jnp.float32)


def project_back(left, weight):
    return jnp.einsum("rse,de->rsd", left, weight, preferred_element_type=jnp.float32)


def weight_grad(left, right):
    return jnp.einsum("rsd,rse->de", left, right, preferred_element_type=jnp.float32)


def rotary_tables(segments, head_size):
    seq_len = segments.shape[1]
    places = jnp.arange(seq_len, dtype=jnp.int32)
    starts_here = jnp.concatenate(
        [jnp.ones((segments.shape[0], 1), bool), segments[:, 1:] != segments[:, :-1]], axis=1
    )
    first = lax.cummax(jnp.where(starts_here, places[None, :], 0), axis=1)
    position = (places[None, :] - first).astype(jnp.float32)
    half = head_size // 2
    freqs = jnp.exp(jnp.arange(half, dtype=jnp.float32) * (-2.0 * math.log(10000.0) / head_size))
    angles = position[:, :, None] * freqs[None, None, :]
    return (jnp.cos(angles)[:, :, None, :], jnp.sin(angles)[:, :, None, :])


def rotate(values, cosine, sine):
    half = values.shape[-1] // 2
    first, second = (values[..., :half], values[..., half:])
    return jnp.concatenate([first * cosine - second * sine, second * cosine + first * sine], -1)


def rotate_back(grads, cosine, sine):
    half = grads.shape[-1] // 2
    first, second = (grads[..., :half], grads[..., half:])
    return jnp.concatenate([first * cosine + second * sine, second * cosine - first * sine], -1)


def allowed_block(segments_row, start, size):
    seq_len = segments_row.shape[0]
    query_pos = start + jnp.arange(size, dtype=jnp.int32)
    key_pos = jnp.arange(seq_len, dtype=jnp.int32)
    query_seg = segments_row[start : start + size]
    return (query_pos[:, None] >= key_pos[None, :]) & (query_seg[:, None] == segments_row[None, :])


def block_scores(query_block, keys, allowed, scale):
    scores = (
        jnp.einsum("qhd,khd->hqk", query_block, keys, preferred_element_type=jnp.float32) * scale
    )
    return jnp.where(allowed[None], scores, MASKED)


def attend_forward(queries, keys, values, segments_row, scale, block):
    outputs = []
    sums = []
    for start in range(0, queries.shape[0], block):
        allowed = allowed_block(segments_row, start, block)
        scores = block_scores(queries[start : start + block], keys, allowed, scale)
        top = jnp.max(scores, -1, keepdims=True)
        expo = jnp.exp(scores - top)
        total = jnp.sum(expo, -1, keepdims=True)
        probs = (expo / total).astype(jnp.bfloat16)
        outputs.append(
            jnp.einsum("hqk,khd->qhd", probs, values, preferred_element_type=jnp.float32)
        )
        sums.append(top + jnp.log(total))
    return (jnp.concatenate(outputs, 0), jnp.concatenate(sums, 1))


def attend_back(queries, keys, values, grad_mixed, log_sums, segments_row, scale, block):
    key_total = jnp.zeros(keys.shape, jnp.float32)
    value_total = jnp.zeros(values.shape, jnp.float32)
    query_parts = []
    for start in range(0, queries.shape[0], block):
        allowed = allowed_block(segments_row, start, block)
        query_block = queries[start : start + block]
        scores = block_scores(query_block, keys, allowed, scale)
        probs = jnp.exp(scores - log_sums[:, start : start + block])
        grad_block = grad_mixed[start : start + block]
        grad_probs = jnp.einsum(
            "qhd,khd->hqk", grad_block, values, preferred_element_type=jnp.float32
        )
        inner = jnp.sum(probs * grad_probs, -1, keepdims=True)
        grad_scores = (probs * (grad_probs - inner)).astype(jnp.bfloat16)
        query_parts.append(
            jnp.einsum("hqk,khd->qhd", grad_scores, keys, preferred_element_type=jnp.float32)
            * scale
        )
        key_total = (
            key_total
            + jnp.einsum(
                "hqk,qhd->khd", grad_scores, query_block, preferred_element_type=jnp.float32
            )
            * scale
        )
        value_total = value_total + jnp.einsum(
            "hqk,qhd->khd",
            probs.astype(jnp.bfloat16),
            grad_block,
            preferred_element_type=jnp.float32,
        )
    return (jnp.concatenate(query_parts, 0), key_total, value_total)


MESH = pl.DeviceIdType.MESH
CHUNK = 64
SLOTS = 6
STAGES = 6
(R1Z, R2Z, R3Z, FZM, FZA, FZB, R1Y, R2Y, R3Y, FYI, FYY) = range(11)
(S0Z, S0Y, S1Z, S1Y, S2Z, S2Y, S3ZM, S3ZE, S3YE, S3YY, S4Z, S4Y) = range(12)


def add_rows(total_ref, row, count, *others):
    value = total_ref[pl.ds(row, count), :].astype(jnp.float32)
    for other in others:
        value = value + other[...].astype(jnp.float32)
    total_ref[pl.ds(row, count), :] = value.astype(jnp.bfloat16)


class Reducer:
    def __init__(self, rows, bufs, send_sem, recv_sem, pairs):
        self.rows, self.bufs, self.send_sem, self.recv_sem, self.pairs = rows, bufs, send_sem, recv_sem, pairs
        dp = lax.axis_index("dp")
        self.place, self.side = lax.div(dp, 2), lax.rem(dp, 2)
        self.inner = (self.place == 1) | (self.place == 2)
        self.end = jnp.logical_not(self.inner)
        self.mate = 2 * (self.place + 1 - 2 * lax.rem(self.place, 2)) + self.side
        self.across = 2 * (3 - self.place) + self.side
        self.twin = 2 * self.place + 1 - self.side
        self.half_z = lax.div(self.place, 2)
        self.half_y = self.side

    def copy(self, source, target, send, recv, slot, device):
        return pltpu.make_async_remote_copy(
            src_ref=source,
            dst_ref=target,
            send_sem=self.send_sem.at[send, slot],
            recv_sem=self.recv_sem.at[recv, slot],
            device_id={"dp": device},
            device_id_type=MESH,
        )

    def whole_z(self, pair):
        return pl.multiple_of(pair * (2 * CHUNK), CHUNK)

    def at_z(self, pair, half):
        return pl.multiple_of(pair * (2 * CHUNK) + half * (CHUNK // 2), CHUNK // 2)

    def at_y(self, pair, half):
        return pl.multiple_of(pair * (2 * CHUNK) + CHUNK + half * (CHUNK // 2), CHUNK // 2)

    def moves(self, pair):
        slot = lax.rem(pair, SLOTS)
        rows, (one_z, two_z, three_z, one_y, two_y, three_y) = self.rows, self.bufs
        half = CHUNK // 2
        mine_z, mine_y = self.half_z, self.half_y
        own_z = rows.at[pl.ds(self.at_z(pair, mine_z), half), :]
        rest_z = rows.at[pl.ds(self.at_z(pair, 1 - mine_z), half), :]
        own_y = rows.at[pl.ds(self.at_y(pair, mine_y), half), :]
        rest_y = rows.at[pl.ds(self.at_y(pair, 1 - mine_y), half), :]
        all_z = rows.at[pl.ds(self.whole_z(pair), CHUNK), :]
        return dict(
            s0z=lambda: self.copy(all_z, one_z.at[slot], S0Z, R1Z, slot, self.mate),
            s0y=lambda: self.copy(rest_y, one_y.at[slot], S0Y, R1Y, slot, self.twin),
            s1z=lambda: self.copy(rest_z, two_z.at[slot], S1Z, R2Z, slot, self.across),
            s1y=lambda: self.copy(two_y.at[slot], two_y.at[slot], S1Y, R2Y, slot, self.mate),
            s2z=lambda: self.copy(own_z, three_z.at[slot], S2Z, R3Z, slot, self.twin),
            s2y=lambda: self.copy(own_y, three_y.at[slot], S2Y, R3Y, slot, self.across),
            s3zm=lambda: self.copy(own_z, own_z, S3ZM, FZM, slot, self.across),
            s3ze=lambda: self.copy(own_z, own_z, S3ZE, FZA, slot, self.mate),
            s3ye=lambda: self.copy(own_y, own_y, S3YE, FYI, slot, self.mate),
            s3yy=lambda: self.copy(own_y, own_y, S3YY, FYY, slot, self.twin),
            s4z=lambda: self.copy(rest_z, rest_z, S4Z, FZB, slot, self.mate),
            s4y=lambda: self.copy(own_y, own_y, S4Y, FYY, slot, self.twin),
        )

    def when(self, slot_index, stage, role, body):
        pair = slot_index - stage
        live = (pair >= 0) & (pair < self.pairs)
        if role is not None:
            live = live & role

        @pl.when(live)
        def _():
            body(pair)

    def slot(self, index):
        half = CHUNK // 2
        one_z, two_z, three_z, one_y, two_y, three_y = self.bufs

        def last(pair):
            m = self.moves(pair)
            @pl.when(self.end)
            def _():
                m["s3ze"]().wait_recv()
                m["s4z"]().wait_recv()
                m["s1y"]().wait_send()
                m["s4y"]().wait_send()
                m["s4y"]().wait_recv()

            @pl.when(self.inner)
            def _():
                m["s3zm"]().wait_send()
                m["s3ze"]().wait_send()
                m["s3ye"]().wait_send()
                m["s3yy"]().wait_send()
                m["s4z"]().wait_send()
                m["s3yy"]().wait_recv()

        def fourth_inner(pair):
            m = self.moves(pair)
            m["s3zm"]().wait_recv()
            m["s4z"]().start()

        def fourth_end(pair):
            m = self.moves(pair)
            m["s3ye"]().wait_recv()
            m["s4y"]().start()

        def third(pair):
            m = self.moves(pair)
            slot = lax.rem(pair, SLOTS)
            m["s2z"]().wait()
            m["s2y"]().wait()
            add_rows(self.rows, self.at_z(pair, self.half_z), half, three_z.at[slot])
            add_rows(self.rows, self.at_y(pair, self.half_y), half, three_y.at[slot])
            m["s3ze"]().start()
            m["s3zm"]().start()
            m["s3ye"]().start()
            m["s3yy"]().start()

        def second(pair):
            m = self.moves(pair)
            slot = lax.rem(pair, SLOTS)
            m["s1z"]().wait()
            m["s1y"]().wait_recv()
            m["s0y"]().wait_send()
            add_rows(
                self.rows, self.at_z(pair, self.half_z), half,
                one_z.at[slot, pl.ds(pl.multiple_of(self.half_z * half, half), half), :], two_z.at[slot],
            )
            add_rows(self.rows, self.at_y(pair, self.half_y), half, one_y.at[slot], two_y.at[slot])
            m["s2z"]().start()
            m["s2y"]().start()

        def first_inner(pair):
            m = self.moves(pair)
            slot = lax.rem(pair, SLOTS)
            m["s0z"]().wait_recv()
            m["s0y"]().wait_recv()
            other = 1 - self.half_z
            add_rows(
                self.rows, self.at_z(pair, other), half,
                one_z.at[slot, pl.ds(pl.multiple_of(other * half, half), half), :],
            )
            m["s1z"]().start()

        def first_end(pair):
            m = self.moves(pair)
            slot = lax.rem(pair, SLOTS)
            m["s0y"]().wait()
            m["s0z"]().wait_send()
            mine = self.rows[pl.ds(self.at_y(pair, self.half_y), half), :].astype(jnp.float32)
            two_y[slot] = (mine + one_y[slot].astype(jnp.float32)).astype(jnp.bfloat16)
            m["s1y"]().start()

        def start(pair):
            m = self.moves(pair)
            m["s0y"]().start()

            @pl.when(self.end)
            def _():
                m["s0z"]().start()

        self.when(index, 0, None, start)
        self.when(index, 1, self.end, first_end)
        self.when(index, 1, self.inner, first_inner)
        self.when(index, 2, self.inner, second)
        self.when(index, 3, self.inner, third)
        self.when(index, 4, self.inner, fourth_inner)
        self.when(index, 4, self.end, fourth_end)
        self.when(index, 5, None, last)

    def greet(self, barrier):
        for device in (self.mate, self.across, self.twin):
            pl.semaphore_signal(barrier, inc=1, device_id={"dp": device}, device_id_type=MESH)
        return 3


def reducer_scratch(width):
    half = CHUNK // 2
    return [
        pltpu.VMEM((SLOTS, CHUNK, width), jnp.bfloat16),
        pltpu.VMEM((SLOTS, half, width), jnp.bfloat16),
        pltpu.VMEM((SLOTS, half, width), jnp.bfloat16),
        pltpu.VMEM((SLOTS, half, width), jnp.bfloat16),
        pltpu.VMEM((SLOTS, half, width), jnp.bfloat16),
        pltpu.VMEM((SLOTS, half, width), jnp.bfloat16),
        pltpu.SemaphoreType.DMA((12, SLOTS)),
        pltpu.SemaphoreType.DMA((11, SLOTS)),
    ]


HEAD_PAD = 128
BLOCK_SEQ = 256
SPAN = 512


def pad_matrix(local, padded):
    shape = (padded, local)
    feature = lax.broadcasted_iota(jnp.int32, shape, 1)
    lane = lax.broadcasted_iota(jnp.int32, shape, 0)
    head = jnp.zeros(shape, jnp.int32)
    for h in range(1, local // HEAD):
        head = head + (feature >= h * HEAD).astype(jnp.int32)
    within = feature - head * HEAD
    target = head * HEAD_PAD + within + jnp.where(within >= HEAD // 2, HEAD_PAD // 2 - HEAD // 2, 0)
    return jnp.where(lane == target, 1.0, 0.0).astype(jnp.bfloat16)


def dot(a, b):
    return jnp.dot(a, b, preferred_element_type=jnp.float32)


def dot_nt(a, b):
    return lax.dot_general(a, b, (((1,), (1,)), ((), ())), preferred_element_type=jnp.float32)


def dot_tn(a, b):
    return lax.dot_general(a, b, (((0,), (0,)), ((), ())), preferred_element_type=jnp.float32)


def segment_columns(seg):
    lines = jnp.broadcast_to(seg.astype(jnp.float32), (16, seg.shape[1])).astype(jnp.bfloat16)
    pick = (lax.broadcasted_iota(jnp.int32, (16, 128), 0) == 0).astype(jnp.float32).astype(jnp.bfloat16)
    return dot_tn(lines, pick)


def rotary_into(seg, cos_ref, sin_ref):
    seq = seg.shape[1]
    ids = segment_columns(seg)
    first = jnp.zeros((seq, 128), jnp.float32)
    row = seg.astype(jnp.float32)
    for s in range(1, 16):
        before = jnp.sum(jnp.where(row < s, 1.0, 0.0), axis=1, keepdims=True)
        first = jnp.where(ids == s, before, first)
    position = lax.broadcasted_iota(jnp.int32, (seq, 128), 0).astype(jnp.float32) - first
    lane = lax.broadcasted_iota(jnp.int32, (1, 128), 1)
    upper = lane >= HEAD_PAD // 2
    index = jnp.where(upper, lane - HEAD_PAD // 2, lane)
    freqs = jnp.exp(index.astype(jnp.float32) * (-2.0 * math.log(10000.0) / HEAD))
    freqs = jnp.where(index < HEAD // 2, freqs, 0.0)
    angles = position * freqs
    cos_ref[...] = jnp.cos(angles)
    sin_ref[...] = jnp.where(upper, jnp.sin(angles), -jnp.sin(angles))


class Ring4:
    def __init__(self):
        mp = lax.axis_index("mp")
        chip, core = lax.div(mp, 2), lax.rem(mp, 2)
        self.me = mp
        self.core = 2 * chip + 1 - core
        self.chip = 2 * (1 - chip) + core
        self.far = 2 * (1 - chip) + 1 - core


def block_rows(index):
    return pl.ds(pl.multiple_of(index * BLOCK_SEQ, BLOCK_SEQ), BLOCK_SEQ)


class Gather:
    def __init__(self, ring, rows, sems, parts=1):
        self.parts = parts
        size = BLOCK_SEQ // parts

        def copy(block, device, which, part):
            at = pl.ds(pl.multiple_of(block * BLOCK_SEQ + part * size, size), size)
            return pltpu.make_async_remote_copy(
                src_ref=rows.at[at, :],
                dst_ref=rows.at[at, :],
                send_sem=sems.at[0, which * parts + part],
                recv_sem=sems.at[1, which * parts + part],
                device_id={"mp": device},
                device_id_type=MESH,
            )

        self.near = lambda part=0: copy(ring.me, ring.core, 0, part)
        self.across = lambda part=0: copy(ring.me, ring.chip, 1, part)
        self.onward = lambda part=0: copy(ring.chip, ring.core, 2, part)

    def start(self, part=0):
        self.across(part).start()
        self.near(part).start()

    def forward(self):
        for part in range(self.parts):
            self.across(part).wait_recv()
            self.onward(part).start()

    def near_in(self):
        for part in range(self.parts):
            self.near(part).wait_recv()

    def onward_in(self):
        for part in range(self.parts):
            self.onward(part).wait_recv()

    def sent(self):
        for part in range(self.parts):
            self.near(part).wait_send()
            self.across(part).wait_send()
            self.onward(part).wait_send()


class Scatter:
    def __init__(self, ring, send_core, recv_core, send_chip, recv_chip, sems, parts=1):
        self.parts = parts
        size = BLOCK_SEQ // parts

        def copy(source, target, device, which, part):
            at = pl.ds(part * size, size)
            return pltpu.make_async_remote_copy(
                src_ref=source.at[at, :],
                dst_ref=target.at[at, :],
                send_sem=sems.at[0, which * parts + part],
                recv_sem=sems.at[1, which * parts + part],
                device_id={"mp": device},
                device_id_type=MESH,
            )

        self.far = lambda part=0: copy(send_core.at[0], recv_core.at[0], ring.core, 0, part)
        self.core = lambda part=0: copy(send_core.at[1], recv_core.at[1], ring.core, 1, part)
        self.chip = lambda part=0: copy(send_chip, recv_chip, ring.chip, 2, part)


def greet_mp(ring, barrier):
    for device in (ring.core, ring.chip):
        pl.semaphore_signal(barrier, inc=1, device_id={"mp": device}, device_id_type=MESH)
    return 2


def norm_rows(values):
    inverse = lax.rsqrt(jnp.mean(values * values, -1, keepdims=True) + EPS)
    return values * inverse, inverse


def qkv_block(rows, weights, cos_ref, sin_ref, out, at):
    turned = 2 * (weights.shape[0] // 3) // 256
    tiles = weights.shape[0] // 256

    def one(n, turn):
        cols = pl.ds(pl.multiple_of(n * 256, 256), 256)
        value = dot_nt(rows[at, :], weights[cols, :])
        if turn:
            cosine, sine = cos_ref[at, :], sin_ref[at, :]
            halves = [value[:, j * 128 : j * 128 + 128] for j in range(2)]
            value = jnp.concatenate([h * cosine + pltpu.roll(h, 64, 1) * sine for h in halves], axis=1)
        out[at, cols] = value.astype(jnp.bfloat16)

    @pl.loop(0, turned)
    def _(n):
        one(n, True)

    @pl.loop(turned, tiles)
    def _(n):
        one(n, False)


def masks_into(seg, ids_ref, bias_ref):
    seq = seg.shape[1]
    for i in range(seq // BLOCK_SEQ):
        low = max(0, i * BLOCK_SEQ - SPAN)
        high = (i + 1) * BLOCK_SEQ
        shape = (BLOCK_SEQ, high - low)
        query = i * BLOCK_SEQ + lax.broadcasted_iota(jnp.int32, shape, 0)
        key = low + lax.broadcasted_iota(jnp.int32, shape, 1)
        ids = ids_ref[pl.ds(i * BLOCK_SEQ, BLOCK_SEQ), :][:, :1]
        same = ids == seg[:, low:high].astype(jnp.float32)
        bias_ref[pl.ds(i * BLOCK_SEQ, BLOCK_SEQ), pl.ds(0, high - low)] = jnp.where((query >= key) & same, 0.0, MASKED).astype(bias_ref.dtype)


def attend(qkv, out, bias_ref, stats, heads, scale, blocks):
    width = heads * HEAD_PAD
    lane = lax.broadcasted_iota(jnp.int32, (BLOCK_SEQ, 128), 1)

    @pl.loop(0, heads)
    def _(h):
        lanes = [pl.ds(pl.multiple_of(part * width + h * HEAD_PAD, HEAD_PAD), HEAD_PAD) for part in range(3)]
        for i in blocks:
            low, high = max(0, i * BLOCK_SEQ - SPAN), (i + 1) * BLOCK_SEQ
            rows, keys = pl.ds(i * BLOCK_SEQ, BLOCK_SEQ), pl.ds(low, high - low)
            scores = dot_nt(qkv[rows, lanes[0]], qkv[keys, lanes[1]]) + bias_ref[rows, pl.ds(0, high - low)]
            top = jnp.max(scores, -1, keepdims=True)
            expo = jnp.exp((scores - top) * scale)
            total = jnp.sum(expo, -1, keepdims=True)
            stats[rows, :] = jnp.where(lane == h, top * scale + jnp.log(total), stats[rows, :])
            out[rows, lanes[0]] = (dot(expo.astype(jnp.bfloat16), qkv[keys, lanes[2]]) * (1.0 / total)).astype(jnp.bfloat16)


def layer_kernel(
    x, g, seg, gain_one, gain_two, wq, wk, wv, wo, wup, wdown,
    result_o, input_o, gains_o, sums_o,
    rows, b0, b1, b2, b3, b4, b5, send_sem, recv_sem, save_sem,
    w_up, w_down, w_qkv, w_out, rows_one, rows_g, rows_two, hidden, grad_up, branch, qkv, mixed, grad_mixed,
    cos_ref, sin_ref, bias_ref, resid, term_ref, key_sum, value_sum,
    send_core, recv_core, send_chip, recv_chip, gain_acc, gain_recv,
    load_sem, one_sem, g_sem, two_sem, branch_sem, rs0_sem, rs_sem, rs2_sem, rs3_sem, gain_sem, free_sem, ready_sem, stats,
):
    bf, f32 = jnp.bfloat16, jnp.float32
    ring = Ring4()
    seq, width = rows_two.shape
    units = w_up.shape[1]
    padded = w_out.shape[0]
    heads = padded // HEAD_PAD
    local = heads * HEAD
    pairs = rows.shape[0] // (2 * CHUNK)
    scale = 1.0 / math.sqrt(HEAD)
    half = BLOCK_SEQ // 2
    chip = lax.div(ring.me, 2)
    red = Reducer(rows, (b0, b1, b2, b3, b4, b5), send_sem, recv_sem, pairs)
    barrier = pltpu.get_barrier_semaphore()
    count = greet_mp(ring, barrier) + red.greet(barrier)
    places = [(w, rows.at[pl.ds(i * local, local), :]) for i, w in enumerate((wq, wk, wv, wo))]
    places += [(g, rows_g.at[block_rows(ring.me), :]), (wup, w_up), (wdown, w_down)]
    loads = [pltpu.make_async_copy(source, target, load_sem.at[i]) for i, (source, target) in enumerate(places)]
    for load in loads[:5]:
        load.start()
    normed, _ = norm_rows(x[...].astype(f32))
    rows_one[block_rows(ring.me), :] = (normed * gain_one[...]).astype(bf)
    one, all_g = Gather(ring, rows_one, one_sem, 2), Gather(ring, rows_g, g_sem)
    two, all_branch = Gather(ring, rows_two, two_sem, 2), Gather(ring, branch, branch_sem)
    ahead = Scatter(ring, send_core, recv_core, send_chip, recv_chip, rs0_sem, 2)
    first = Scatter(ring, send_core, recv_core, send_chip, recv_chip, rs_sem)
    second = Scatter(ring, send_core, recv_core, send_chip, recv_chip, rs2_sem)
    third = Scatter(ring, send_core, recv_core, send_chip, recv_chip, rs3_sem)
    pl.semaphore_wait(barrier, count)
    one.start(0)
    one.start(1)
    for load in loads[5:]:
        load.start()

    spread = pad_matrix(local, padded)
    for i in range(3):
        loads[i].wait()
        w_qkv[pl.ds(i * padded, padded), :] = dot(spread, rows[pl.ds(i * local, local), :]).astype(bf)
    loads[3].wait()
    w_out[...] = dot(spread, rows[pl.ds(3 * local, local), :]).astype(bf)
    loads[4].wait()
    all_g.start()
    rotary_into(seg[...], cos_ref, sin_ref)
    qkv_block(rows_one, w_qkv, cos_ref, sin_ref, qkv, block_rows(ring.me))
    one.near_in()
    qkv_block(rows_one, w_qkv, cos_ref, sin_ref, qkv, block_rows(ring.core))
    key_sum[...] = segment_columns(seg[...])
    masks_into(seg[...], key_sum, bias_ref)
    def half_rows(block, part):
        return pl.ds(pl.multiple_of(block * BLOCK_SEQ + part * half, half), half)

    @pl.loop(0, 2)
    def _(p):
        one.across(p).wait_recv()
        one.onward(p).start()
        qkv_block(rows_one, w_qkv, cos_ref, sin_ref, qkv, half_rows(ring.chip, p))
        one.onward(p).wait_recv()
        qkv_block(rows_one, w_qkv, cos_ref, sin_ref, qkv, half_rows(ring.far, p))

    one.across(0).wait_send()
    one.across(1).wait_send()

    stats[...] = jnp.zeros_like(stats)
    early, late = (0, 1), (2, 3)

    @pl.when(chip == 0)
    def _():
        attend(qkv, mixed, bias_ref, stats, heads, scale, late)

    @pl.when(chip == 1)
    def _():
        attend(qkv, mixed, bias_ref, stats, heads, scale, early)

    def term(block, part):
        at = pl.ds(pl.multiple_of(block * BLOCK_SEQ + part * half, half), half)
        return dot(mixed[at, :], w_out[...])

    parts = [pl.ds(p * half, half) for p in range(2)]
    for p in range(2):
        send_core[0, parts[p], :] = term(ring.far, p).astype(bf)
        ahead.far(p).start()
    for p in range(2):
        value = term(ring.chip, p)
        ahead.far(p).wait_recv()
        send_chip[parts[p], :] = (value + recv_core[0, parts[p], :].astype(f32)).astype(bf)
        ahead.chip(p).start()

    @pl.when(chip == 0)
    def _():
        attend(qkv, mixed, bias_ref, stats, heads, scale, early)

    @pl.when(chip == 1)
    def _():
        attend(qkv, mixed, bias_ref, stats, heads, scale, late)

    for p in range(2):
        send_core[1, parts[p], :] = term(ring.core, p).astype(bf)
        ahead.core(p).start()
    all_g.forward()
    for p in range(2):
        resid[parts[p], :] = x[parts[p], :].astype(f32) + term(ring.me, p)
    for p in range(2):
        ahead.core(p).wait_recv()
        ahead.chip(p).wait_recv()
        value = resid[parts[p], :] + recv_core[1, parts[p], :].astype(f32) + recv_chip[parts[p], :].astype(f32)
        resid[parts[p], :] = value
        normed, _ = norm_rows(value)
        at = pl.ds(pl.multiple_of(ring.me * BLOCK_SEQ + p * half, half), half)
        rows_two[at, :] = (normed * gain_two[...]).astype(bf)
        two.start(p)
    for p in range(2):
        ahead.far(p).wait_send()
        ahead.core(p).wait_send()
        ahead.chip(p).wait_send()

    base = 2 * units

    def put(pair):
        at = pl.ds(pl.multiple_of(pair * 2 * CHUNK, 2 * CHUNK), 2 * CHUNK)
        return pltpu.make_async_copy(rows.at[at, :], sums_o.at[at, :], save_sem.at[lax.rem(pair, 4)])

    def slot(index):
        red.slot(index)
        pair = index - (STAGES - 1)

        @pl.when(pair >= 4)
        def _():
            put(pair - 4).wait()

        @pl.when(pair >= 0)
        def _():
            put(pair).start()

    def tile(n):
        return pl.ds(pl.multiple_of(n * 256, 256), 256)

    def up_tile(at, n):
        u = dot(rows_two[at, :], w_up[:, tile(n)])
        tangent = jnp.tanh(GELU_C * (u + GELU_K * u * u * u))
        hidden[at, tile(n)] = (0.5 * u * (1.0 + tangent)).astype(bf)

    def up_rows_of(at):
        @pl.loop(0, units // 256)
        def _(n):
            up_tile(at, n)

    loads[5].wait()
    up_rows_of(block_rows(ring.me))
    two.near_in()
    up_rows_of(block_rows(ring.core))
    all_g.near_in()
    all_g.onward_in()
    two.across(0).wait_recv()
    two.onward(0).start()
    up_rows_of(half_rows(ring.chip, 0))
    two.onward(0).wait_recv()
    up_rows_of(half_rows(ring.far, 0))
    two.across(1).wait_recv()
    two.onward(1).start()

    loads[6].wait()

    def order(k):
        there = k < 2
        core = lax.rem(ring.me, 2)
        flip = 1 - lax.rem(k, 2)
        to_chip = jnp.where(there, 1 - chip, chip)
        to_core = jnp.where(flip == 1, 1 - core, core)
        return 2 * to_chip + to_core

    def hand_on(k, scatter, start):
        @pl.when(k == 0)
        def _():
            send_core[0] = term_ref[...].astype(bf)
            scatter.far().start()

        @pl.when(k == 1)
        def _():
            scatter.far().wait_recv()
            send_chip[...] = (term_ref[...] + recv_core[0].astype(f32)).astype(bf)
            scatter.chip().start()

        @pl.when(k == 2)
        def _():
            send_core[1] = term_ref[...].astype(bf)
            scatter.core().start()

        @pl.when(k == 3)
        def _():
            scatter.core().wait_recv()
            term_ref[...] = term_ref[...] + recv_core[1].astype(f32)

    def settle(scatter):
        for copy in (scatter.far(), scatter.core()):
            copy.wait_send()
        scatter.chip().wait()
        return term_ref[...] + recv_chip[...].astype(f32)

    def grad_tile(at, n):
        u = dot(rows_two[at, :], w_up[:, tile(n)])
        upstream = dot_nt(rows_g[at, :], w_down[tile(n), :])
        tangent = jnp.tanh(GELU_C * (u + GELU_K * u * u * u))
        slope = 0.5 * (1.0 + tangent) + 0.5 * u * (1.0 - tangent * tangent) * GELU_C * (1.0 + 3.0 * GELU_K * u * u)
        grad_up[at, tile(n)] = (upstream * slope).astype(bf)

    @pl.loop(0, units // 256)
    def _(n):
        up_tile(half_rows(ring.chip, 1), n)

        @pl.when(n == 0)
        def _():
            two.onward(1).wait_recv()

        up_tile(half_rows(ring.far, 1), n)
        rows[tile(n), :] = dot_tn(hidden[:, tile(n)], rows_g[...]).astype(bf)
        slot(n)

        @pl.loop(0, 3)
        def _(k):
            grad_tile(block_rows(order(k)), n)

    @pl.loop(0, 4)
    def _(k):
        @pl.loop(0, 2)
        def _(j):
            @pl.when(2 * k + j < units // 256)
            def _():
                grad_tile(block_rows(order(3)), 2 * k + j)

        at = block_rows(order(k))

        @pl.loop(0, width // 256)
        def _(n):
            term_ref[:, tile(n)] = dot_nt(grad_up[at, :], w_up[tile(n), :])

        hand_on(k, first, None)
        slot(5 + k)

    def up_rows(i):
        rows[pl.ds(pl.multiple_of(units + i * 256, 256), 256), :] = dot_tn(rows_two[:, tile(i)], grad_up[...]).astype(bf)

    up_rows(0)
    slot(9)
    grad_two = settle(first)
    normed, inverse = norm_rows(resid[...])
    scaled = grad_two * gain_two[...]
    part = inverse * (scaled - normed * jnp.mean(scaled * normed, -1, keepdims=True))
    mlp_part = jnp.sum(grad_two * normed, axis=0, keepdims=True)
    gain_acc[0] = jnp.zeros(gain_acc.shape[1:], f32)
    gain_acc[0, 1:2, :] = mlp_part
    mine = rows_g[block_rows(ring.me), :].astype(f32) + part
    input_o[...] = mine
    branch[block_rows(ring.me), :] = mine.astype(bf)
    all_branch.across().start()
    all_branch.near().start()
    for device in (ring.core, ring.chip):
        pl.semaphore_signal(ready_sem, inc=1, device_id={"mp": device}, device_id_type=MESH)

    def head_rows(left, lane, right, row):
        value = dot_tn(left[:, lane], right[...])
        halves = [value[at : at + HEAD // 2, :] for at in (0, 64, 128, 192)]
        rows[pl.ds(pl.multiple_of(row, 16), 2 * HEAD), :] = jnp.concatenate(halves, axis=0).astype(bf)

    @pl.loop(1, units // 256)
    def _(i):
        up_rows(i)

        @pl.when(i == 1)
        def _():
            pl.semaphore_wait(ready_sem, 2)

        at = block_rows(order(i - 1))

        @pl.loop(0, width // 256)
        def _(n):
            term_ref[:, tile(n)] = dot(hidden[at, :], w_down[:, tile(n)])

        hand_on(i - 1, second, None)

        @pl.when(i == 4)
        def _():
            all_branch.near().wait_recv()
            all_branch.forward()
            all_branch.onward().wait_recv()

            @pl.loop(0, heads // 2)
            def _(j):
                head_rows(mixed, tile(j), branch, base + j * 2 * HEAD)

        slot(9 + i)

    @pl.loop(0, 4)
    def _(b):
        grad_mixed[block_rows(b), :] = dot_nt(branch[block_rows(b), :], w_out[...]).astype(bf)

    lane = lax.broadcasted_iota(jnp.int32, (BLOCK_SEQ, 128), 1)

    @pl.loop(0, heads)
    def _(h):
        lanes = [pl.ds(pl.multiple_of(n * padded + h * HEAD_PAD, HEAD_PAD), HEAD_PAD) for n in range(3)]
        key_sum[...] = jnp.zeros_like(key_sum)
        value_sum[...] = jnp.zeros_like(value_sum)
        for i in range(seq // BLOCK_SEQ):
            low, high = max(0, i * BLOCK_SEQ - SPAN), (i + 1) * BLOCK_SEQ
            at, keys = pl.ds(i * BLOCK_SEQ, BLOCK_SEQ), pl.ds(low, high - low)
            query, upstream = qkv[at, lanes[0]], grad_mixed[at, lanes[0]]
            scores = dot_nt(query, qkv[keys, lanes[1]]) + bias_ref[at, pl.ds(0, high - low)]
            level = jnp.sum(jnp.where(lane == h, stats[at, :], 0.0), -1, keepdims=True)
            probs = jnp.exp(scores * scale - level)
            grad_probs = dot_nt(upstream, qkv[keys, lanes[2]])
            inner = jnp.sum(probs * grad_probs, -1, keepdims=True)
            grad_scores = (probs * (grad_probs - inner)).astype(bf)
            value_sum[keys, :] += dot_tn(probs.astype(bf), upstream)
            key_sum[keys, :] += dot_tn(grad_scores, query)
            turned = dot(grad_scores, qkv[keys, lanes[1]]) * scale
            qkv[at, lanes[0]] = (turned * cos_ref[at, :] - pltpu.roll(turned, 64, 1) * sin_ref[at, :]).astype(bf)
            if i == 1:
                slot(14 + 2 * h)
        turned = key_sum[...] * scale
        qkv[:, lanes[1]] = (turned * cos_ref[...] - pltpu.roll(turned, 64, 1) * sin_ref[...]).astype(bf)
        qkv[:, lanes[2]] = value_sum[...].astype(bf)
        slot(15 + 2 * h)

    @pl.loop(0, 3)
    def _(part):
        for j in range(heads // 2):
            lane = pl.ds(pl.multiple_of(part * padded + j * 256, 256), 256)
            head_rows(qkv, lane, rows_one, base + (part + 1) * local + j * 2 * HEAD)
        slot(22 + part)

    result_o[...] = (resid[...] + settle(second)).astype(bf)
    for device in (ring.core, ring.chip):
        pl.semaphore_signal(free_sem, inc=1, device_id={"mp": device}, device_id_type=MESH)
    pl.semaphore_wait(free_sem, 2)

    @pl.loop(0, 4)
    def _(k):
        at = block_rows(order(k))

        @pl.loop(0, width // 256)
        def _(n):
            term_ref[:, tile(n)] = dot(qkv[at, :], w_qkv[:, tile(n)])

        hand_on(k, third, None)
        slot(25 + k)

    slot(29)
    grad_one = settle(third)
    normed, inverse = norm_rows(x[...].astype(f32))
    scaled = grad_one * gain_one[...]
    input_o[...] = input_o[...] + inverse * (scaled - normed * jnp.mean(scaled * normed, -1, keepdims=True))
    gain_acc[0, 0:1, :] = jnp.sum(grad_one * normed, axis=0, keepdims=True)

    def exchange(step):
        names = ({"mp": ring.core}, {"mp": ring.chip}, {"dp": red.twin}, {"dp": red.mate}, {"dp": red.across})
        return pltpu.make_async_remote_copy(
            src_ref=gain_acc.at[step], dst_ref=gain_recv.at[step], send_sem=gain_sem.at[0, step], recv_sem=gain_sem.at[1, step],
            device_id=names[step], device_id_type=MESH,
        )

    exchange(0).start()
    last = pairs + STAGES - 1

    @pl.loop(30, last)
    def _(index):
        for step in range(1, 5):

            @pl.when(index == 29 + step)
            def _():
                exchange(step - 1).wait_recv()
                gain_acc[step] = gain_acc[step - 1] + gain_recv[step - 1]
                exchange(step).start()

        slot(index)

    exchange(4).wait_recv()
    gains_o[...] = gain_acc[4] + gain_recv[4]
    for pair in range(pairs - 4, pairs):
        put(pair).wait()
    for step in range(5):
        exchange(step).wait_send()
    for part in range(2):
        one.near(part).wait_send()
        one.onward(part).wait_send()
    for gather in (all_g, two, all_branch):
        gather.sent()


def layer(x, g, seg, gain_one, gain_two, wq, wk, wv, wo, wup, wdown):
    bf, f32 = jnp.bfloat16, jnp.float32
    own, width = x.shape
    units = wup.shape[1]
    seq = seg.shape[1]
    local = wo.shape[0]
    padded = local // HEAD * HEAD_PAD
    total = 2 * units + 4 * local
    vm, hbm = pl.BlockSpec(memory_space=pltpu.VMEM), pl.BlockSpec(memory_space=pl.ANY)
    sem = pltpu.SemaphoreType.DMA
    shapes = [((own, width), bf), ((own, width), f32), ((8, width), f32), ((total, width), bf)]
    tall = pltpu.VMEM((seq, width), bf)
    return pl.pallas_call(
        layer_kernel,
        out_shape=[jax.ShapeDtypeStruct(s, d) for s, d in shapes],
        in_specs=[vm, hbm, vm, vm, vm] + [hbm] * 6,
        out_specs=[vm] * 3 + [hbm],
        scratch_shapes=[pltpu.VMEM((total, width), bf)]
        + reducer_scratch(width)
        + [
            sem((4,)),
            pltpu.VMEM((width, units), bf), pltpu.VMEM((units, width), bf), pltpu.VMEM((3 * padded, width), bf), pltpu.VMEM((padded, width), bf),
            tall, tall, tall, pltpu.VMEM((seq, units), bf), pltpu.VMEM((seq, units), bf), tall,
            pltpu.VMEM((seq, 3 * padded), bf), pltpu.VMEM((seq, padded), bf), pltpu.VMEM((seq, padded), bf),
            pltpu.VMEM((seq, 128), f32), pltpu.VMEM((seq, 128), f32), pltpu.VMEM((seq, SPAN + BLOCK_SEQ), bf),
            pltpu.VMEM((own, width), f32), pltpu.VMEM((own, width), f32), pltpu.VMEM((seq, HEAD_PAD), f32), pltpu.VMEM((seq, HEAD_PAD), f32),
            pltpu.VMEM((2, own, width), bf), pltpu.VMEM((2, own, width), bf), pltpu.VMEM((own, width), bf), pltpu.VMEM((own, width), bf),
            pltpu.VMEM((5, 8, width), f32), pltpu.VMEM((5, 8, width), f32),
            sem((7,)), sem((2, 6)), sem((2, 3)), sem((2, 6)), sem((2, 3)), sem((2, 6)), sem((2, 3)), sem((2, 3)), sem((2, 3)), sem((2, 5)),
            pltpu.SemaphoreType.REGULAR, pltpu.SemaphoreType.REGULAR, pltpu.VMEM((seq, 128), f32),
        ],
        compiler_params=pltpu.CompilerParams(collective_id=0, has_side_effects=True, vmem_limit_bytes=67043328),
    )(x, g, seg, gain_one, gain_two, wq, wk, wv, wo, wup, wdown)


def finish_kernel(result, input_grad, gains, sums, result_o, input_o, one_o, two_o, down_o, up_o, out_o, q_o, k_o, v_o, inbox, outbox, side_one, side_two, in_sem, out_sem, side_sem):
    step = out_o.shape[0]
    targets = [(down_o, i * step) for i in range(down_o.shape[0] // step)] + [(up_o, i * step) for i in range(up_o.shape[0] // step)]
    targets += [(t, 0) for t in (out_o, q_o, k_o, v_o)]
    count, depth = len(targets), inbox.shape[0]
    bring = [pltpu.make_async_copy(result, side_one, side_sem.at[0]), pltpu.make_async_copy(input_grad, side_two, side_sem.at[1])]
    take = [pltpu.make_async_copy(side_one, result_o, side_sem.at[2]), pltpu.make_async_copy(side_two, input_o, side_sem.at[3])]

    def read(i):
        return pltpu.make_async_copy(sums.at[pl.ds(i * step, step), :], inbox.at[i % depth], in_sem.at[i % depth])

    def write(i):
        target, at = targets[i]
        return pltpu.make_async_copy(outbox.at[i % depth], target.at[pl.ds(at, step), :], out_sem.at[i % depth])

    for i in range(depth):
        read(i).start()
    for side in bring:
        side.start()
    one_o[...] = gains[0, :]
    two_o[...] = gains[1, :]
    for i in range(count):
        read(i).wait()
        if i >= depth:
            write(i - depth).wait()
        outbox[i % depth] = inbox[i % depth].astype(jnp.float32)
        write(i).start()
        if i + depth < count:
            read(i + depth).start()
        if i == depth:
            for come, go in zip(bring, take):
                come.wait()
                go.start()
    for i in range(count - depth, count):
        write(i).wait()
    for side in take:
        side.wait()


def finish(result, input_grad, gains, sums, units, local):
    bf, f32 = jnp.bfloat16, jnp.float32
    own, width = result.shape
    vm, hbm = pl.BlockSpec(memory_space=pltpu.VMEM), pl.BlockSpec(memory_space=pl.ANY)
    sem = pltpu.SemaphoreType.DMA
    shapes = [((own, width), bf), ((own, width), f32), ((width,), f32), ((width,), f32), ((units, width), f32), ((width, units), f32)] + [((local, width), f32)] * 4
    return pl.pallas_call(
        finish_kernel,
        out_shape=[jax.ShapeDtypeStruct(s, d) for s, d in shapes],
        in_specs=[hbm, hbm, vm, hbm],
        out_specs=[hbm, hbm, vm, vm] + [hbm] * 6,
        scratch_shapes=[pltpu.VMEM((3, local, width), bf), pltpu.VMEM((3, local, width), f32), pltpu.VMEM((own, width), bf), pltpu.VMEM((own, width), f32), sem((3,)), sem((3,)), sem((4,))],
        compiler_params=pltpu.CompilerParams(vmem_limit_bytes=67043328),
    )(result, input_grad, gains, sums)


def on_device(
    hidden_in,
    segment_ids,
    attn_gain,
    query_weight,
    key_weight,
    value_weight,
    out_weight,
    mlp_gain,
    up_weight,
    down_weight,
    out_cotangent,
):
    row_count = segment_ids.shape[0]
    seq_len = segment_ids.shape[1]
    local_width = query_weight.shape[1]
    head_count = local_width // HEAD
    scale = 1.0 / math.sqrt(HEAD)
    block = min(512, seq_len)
    head_shape = (row_count, seq_len, head_count, HEAD)
    x_float = hidden_in.astype(jnp.float32)
    scaled_one, normed_one, inverse_one = normalize(x_float, attn_gain)
    rows_one = lax.all_gather(scaled_one.astype(jnp.bfloat16), "mp", axis=1, tiled=True)
    cosine, sine = rotary_tables(segment_ids, HEAD)
    queries = rotate(project(rows_one, query_weight).reshape(head_shape), cosine, sine).astype(
        jnp.bfloat16
    )
    keys = rotate(project(rows_one, key_weight).reshape(head_shape), cosine, sine).astype(
        jnp.bfloat16
    )
    values = project(rows_one, value_weight).reshape(head_shape).astype(jnp.bfloat16)
    row_index = 0
    mixed_one, log_one = attend_forward(
        queries[row_index], keys[row_index], values[row_index], segment_ids[row_index], scale, block
    )
    mixed_rows = [mixed_one]
    log_rows = [log_one]
    mixed = jnp.stack(mixed_rows, 0).reshape(row_count, seq_len, local_width).astype(jnp.bfloat16)
    attn_share = lax.psum_scatter(project(mixed, out_weight), "mp", scatter_dimension=1, tiled=True)
    resid = x_float + attn_share
    scaled_two, normed_two, inverse_two = normalize(resid, mlp_gain)
    rows_two = lax.all_gather(scaled_two.astype(jnp.bfloat16), "mp", axis=1, tiled=True)
    up_pre = project(rows_two, up_weight)
    hidden = jax.nn.gelu(up_pre, approximate=True).astype(jnp.bfloat16)
    mlp_share = lax.psum_scatter(
        project(hidden, down_weight).astype(jnp.bfloat16), "mp", scatter_dimension=1, tiled=True
    ).astype(jnp.float32)
    result = (resid + mlp_share).astype(jnp.bfloat16)
    grad_top = out_cotangent.astype(jnp.float32)
    grad_rows = lax.all_gather(out_cotangent, "mp", axis=1, tiled=True)
    down_total = weight_grad(hidden, grad_rows)
    grad_hidden = project_back(grad_rows, down_weight)
    grad_up_pre = (grad_hidden * gelu_slope(up_pre)).astype(jnp.bfloat16)
    up_total = weight_grad(rows_two, grad_up_pre)
    grad_two = lax.psum_scatter(
        project_back(grad_up_pre, up_weight), "mp", scatter_dimension=1, tiled=True
    )
    resid_part, mlp_gain_part = norm_back(grad_two, normed_two, inverse_two, mlp_gain)
    grad_resid = grad_top + resid_part
    branch_rows = lax.all_gather(grad_resid.astype(jnp.bfloat16), "mp", axis=1, tiled=True)
    out_total = weight_grad(mixed, branch_rows)
    grad_mixed = project_back(branch_rows, out_weight).astype(jnp.bfloat16).reshape(head_shape)
    row_index = 0
    grad_q, grad_k, grad_v = attend_back(
        queries[row_index],
        keys[row_index],
        values[row_index],
        grad_mixed[row_index],
        log_rows[row_index],
        segment_ids[row_index],
        scale,
        block,
    )
    query_rows = [grad_q]
    key_rows = [grad_k]
    value_rows = [grad_v]
    grad_query = (
        rotate_back(jnp.stack(query_rows, 0), cosine, sine)
        .astype(jnp.bfloat16)
        .reshape(row_count, seq_len, local_width)
    )
    grad_key = (
        rotate_back(jnp.stack(key_rows, 0), cosine, sine)
        .astype(jnp.bfloat16)
        .reshape(row_count, seq_len, local_width)
    )
    grad_value = (
        jnp.stack(value_rows, 0).astype(jnp.bfloat16).reshape(row_count, seq_len, local_width)
    )
    query_total = weight_grad(rows_one, grad_query)
    key_total = weight_grad(rows_one, grad_key)
    value_total = weight_grad(rows_one, grad_value)
    grad_terms = (
        project_back(grad_query, query_weight)
        + project_back(grad_key, key_weight)
        + project_back(grad_value, value_weight)
    )
    grad_one = lax.psum_scatter(grad_terms, "mp", scatter_dimension=1, tiled=True)
    input_part, attn_gain_part = norm_back(grad_one, normed_one, inverse_one, attn_gain)
    input_grad = grad_resid + input_part
    attn_gain_part, mlp_gain_part = lax.psum((attn_gain_part, mlp_gain_part), "mp")
    (
        query_total,
        key_total,
        value_total,
        out_total,
        attn_gain_part,
        mlp_gain_part,
        up_total,
        down_total,
    ) = lax.psum(
        (
            query_total,
            key_total,
            value_total,
            out_total,
            attn_gain_part,
            mlp_gain_part,
            up_total,
            down_total,
        ),
        "dp",
    )
    return (
        result,
        input_grad,
        attn_gain_part,
        query_total,
        key_total,
        value_total,
        out_total,
        mlp_gain_part,
        up_total,
        down_total,
    )


def on_device_kernels(
    hidden_in, segment_ids, attn_gain, query_weight, key_weight, value_weight, out_weight, mlp_gain, up_weight, down_weight, out_cotangent
):
    sums = layer(
        hidden_in[0], out_cotangent[0], segment_ids, attn_gain, mlp_gain,
        query_weight.T, key_weight.T, value_weight.T, out_weight, up_weight, down_weight,
    )
    result, input_grad, one, two, down, up, out, query, key, value = finish(*sums, up_weight.shape[1], out_weight.shape[0])
    return (result[None], input_grad[None], one, query.T, key.T, value.T, out, two, up, down)


def solution(mesh):
    return jax.shard_map(
        on_device_kernels if mesh.shape["dp"] == 8 else on_device,
        mesh=mesh,
        in_specs=(
            P("dp", "mp", None),
            P("dp", None),
            P(),
            P(None, "mp"),
            P(None, "mp"),
            P(None, "mp"),
            P("mp", None),
            P(),
            P(None, "mp"),
            P("mp", None),
            P("dp", "mp", None),
        ),
        out_specs=(
            P("dp", "mp", None),
            P("dp", "mp", None),
            P(),
            P(None, "mp"),
            P(None, "mp"),
            P(None, "mp"),
            P("mp", None),
            P(),
            P(None, "mp"),
            P("mp", None),
        ),
        check_vma=False,
    )
```
